8 devices in a mesh: dp: 1 (over z), tp: 2 (over y), sp: 4 (over x, core).
Axes of the slice: x: 2, y: 2, z: 1, core: 2. Of those that a mesh axis runs over, the one named last changes fastest.
Arguments:
- tokens: bfloat16 [64, 2560], P('dp')
- positions: int32 [64], P('dp')
- cache_k: bfloat16 [64, 1024, 4, 256], P('dp', 'sp', 'tp')
- cache_v: bfloat16 [64, 1024, 4, 256], P('dp', 'sp', 'tp')
- attn_gain: bfloat16 [2560], replicated
- w_q: bfloat16 [2560, 2048], P(None, 'tp')
- w_k: bfloat16 [2560, 1024], P(None, 'tp')
- w_v: bfloat16 [2560, 1024], P(None, 'tp')
- w_o: bfloat16 [2048, 2560], P('tp')
- mlp_gain: bfloat16 [2560], replicated
- w_gate: bfloat16 [2560, 10240], P(None, 'tp')
- w_up: bfloat16 [2560, 10240], P(None, 'tp')
- w_down: bfloat16 [10240, 2560], P('tp')
Outputs:
- output 1: bfloat16 [64, 2560], P('dp')
- output 2: bfloat16 [64, 1024, 4, 256], P('dp', 'sp', 'tp')
- output 3: bfloat16 [64, 1024, 4, 256], P('dp', 'sp', 'tp')
All inputs are finite; a program needn't handle non-finite values.
Results may differ from the reference program's by a relative error of at most 0.00835539.
Values sent between devices are 32-bit elements.
A program may use at most 1 GiB of HBM per device.

```python
import math
import jax
import jax.numpy as jnp
from jax import lax

BATCH = 64
MODEL_DIM = 2560
HEADS = 8
KV_HEADS = 4
HEAD_DIM = 256
MLP_DIM = 10240
SLOTS = 1024
GROUP = HEADS // KV_HEADS
POS_LIMIT = 8 * SLOTS
LOG_SLOTS = int(math.log2(SLOTS))
NORM_EPS = 1e-5
ROPE_THETA = 10000.0
KEY_STD = math.sqrt(math.log(SLOTS / 8.0))
VALUE_STD = 1.5


def draw_positions(key):
    rank_key, scale_key, young_key, old_key = jax.random.split(key, 4)
    order = jax.random.permutation(rank_key, BATCH)
    is_young = order < BATCH // 2
    exponent = jax.random.randint(scale_key, (BATCH,), 0, LOG_SLOTS + 1)
    limit = jnp.minimum(jnp.left_shift(jnp.ones_like(exponent), exponent), SLOTS)
    young_pos = jax.random.randint(young_key, (BATCH,), 0, limit)
    old_pos = jax.random.randint(old_key, (BATCH,), SLOTS, POS_LIMIT)
    return jnp.where(is_young, young_pos, old_pos).astype(jnp.int32)


def normal_matrix(key, rows, columns, scale):
    return (jax.random.normal(key, (rows, columns), jnp.float32) * scale).astype(jnp.bfloat16)


def normal_gain(key):
    return (1.0 + 0.3 * jax.random.normal(key, (MODEL_DIM,), jnp.float32)).astype(jnp.bfloat16)


def setup_inputs(seed: int = 0, part: int = 0) -> dict:
    base_key = jax.random.key(seed)
    part_keys = jax.random.split(jax.random.fold_in(base_key, part), 4)
    weight_keys = jax.random.split(base_key, 9)
    cache_shape = (BATCH, SLOTS, KV_HEADS, HEAD_DIM)
    query_width = HEADS * HEAD_DIM
    kv_width = KV_HEADS * HEAD_DIM
    tokens = jax.random.normal(part_keys[0], (BATCH, MODEL_DIM), jnp.float32).astype(jnp.bfloat16)
    positions = draw_positions(part_keys[1])
    cache_k = (KEY_STD * jax.random.normal(part_keys[2], cache_shape, jnp.float32)).astype(jnp.bfloat16)
    cache_v = (VALUE_STD * jax.random.normal(part_keys[3], cache_shape, jnp.float32)).astype(jnp.bfloat16)
    return {
        "tokens": tokens,
        "positions": positions,
        "cache_k": cache_k,
        "cache_v": cache_v,
        "attn_gain": normal_gain(weight_keys[0]),
        "w_q": normal_matrix(weight_keys[1], MODEL_DIM, query_width, MODEL_DIM ** -0.5),
        "w_k": normal_matrix(weight_keys[2], MODEL_DIM, kv_width, KEY_STD * MODEL_DIM ** -0.5),
        "w_v": normal_matrix(weight_keys[3], MODEL_DIM, kv_width, VALUE_STD * MODEL_DIM ** -0.5),
        "w_o": normal_matrix(weight_keys[4], query_width, MODEL_DIM, query_width ** -0.5),
        "mlp_gain": normal_gain(weight_keys[5]),
        "w_gate": normal_matrix(weight_keys[6], MODEL_DIM, MLP_DIM, MODEL_DIM ** -0.5),
        "w_up": normal_matrix(weight_keys[7], MODEL_DIM, MLP_DIM, MODEL_DIM ** -0.5),
        "w_down": normal_matrix(weight_keys[8], MLP_DIM, MODEL_DIM, MLP_DIM ** -0.5),
    }


def rms_norm(values, gain):
    wide = values.astype(jnp.float32)
    inv_rms = lax.rsqrt(jnp.mean(wide * wide, axis=-1, keepdims=True) + NORM_EPS)
    return (wide * inv_rms * gain.astype(jnp.float32)).astype(jnp.bfloat16)


def rope_tables(positions):
    frequencies = ROPE_THETA ** (-2.0 * jnp.arange(HEAD_DIM // 2, dtype=jnp.float32) / HEAD_DIM)
    angles = positions.astype(jnp.float32)[:, None] * frequencies[None, :]
    return jnp.cos(angles)[:, None, :], jnp.sin(angles)[:, None, :]


def apply_rope(vectors, cos_table, sin_table):
    half = vectors.shape[-1] // 2
    first = vectors[..., :half]
    second = vectors[..., half:]
    return jnp.concatenate([first * cos_table - second * sin_table, second * cos_table + first * sin_table], axis=-1)


def reference(tokens, positions, cache_k, cache_v, attn_gain, w_q, w_k, w_v, w_o, mlp_gain, w_gate, w_up, w_down):
    normed = rms_norm(tokens, attn_gain)
    cos_table, sin_table = rope_tables(positions)
    q_lin = jnp.dot(normed, w_q, preferred_element_type=jnp.float32).reshape(BATCH, HEADS, HEAD_DIM)
    k_lin = jnp.dot(normed, w_k, preferred_element_type=jnp.float32).reshape(BATCH, KV_HEADS, HEAD_DIM)
    v_new = jnp.dot(normed, w_v, preferred_element_type=jnp.float32).astype(jnp.bfloat16).reshape(BATCH, KV_HEADS, HEAD_DIM)
    q_rot = apply_rope(q_lin, cos_table, sin_table).astype(jnp.bfloat16)
    k_rot = apply_rope(k_lin, cos_table, sin_table).astype(jnp.bfloat16)
    slot_ids = jnp.arange(SLOTS)
    hit_mask = (slot_ids[None, :] == (positions % SLOTS)[:, None])[:, :, None, None]
    new_k = jnp.where(hit_mask, k_rot[:, None], cache_k)
    new_v = jnp.where(hit_mask, v_new[:, None], cache_v)

    def attend_one(item):
        q_seq, k_seq, v_seq, pos_one = item
        query = q_seq.astype(jnp.float32).reshape(KV_HEADS, GROUP, HEAD_DIM)
        scores = jnp.einsum("kgd,skd->kgs", query, k_seq.astype(jnp.float32)) / math.sqrt(HEAD_DIM)
        valid = (pos_one >= SLOTS - 1) | (slot_ids <= pos_one)
        scores = jnp.where(valid[None, None, :], scores, -jnp.inf)
        weights = jax.nn.softmax(scores, axis=-1)
        return jnp.einsum("kgs,skd->kgd", weights, v_seq.astype(jnp.float32)).reshape(HEADS, HEAD_DIM)

    attended = lax.map(attend_one, (q_rot, new_k, new_v, positions))
    attended = attended.reshape(BATCH, HEADS * HEAD_DIM).astype(jnp.bfloat16)
    attn_proj = jnp.dot(attended, w_o, preferred_element_type=jnp.float32)
    hidden = (tokens.astype(jnp.float32) + attn_proj).astype(jnp.bfloat16)
    normed_mlp = rms_norm(hidden, mlp_gain)
    gate_proj = jnp.dot(normed_mlp, w_gate, preferred_element_type=jnp.float32)
    up_proj = jnp.dot(normed_mlp, w_up, preferred_element_type=jnp.float32)
    activated = (jax.nn.silu(gate_proj) * up_proj).astype(jnp.bfloat16)
    mlp_down = jnp.dot(activated, w_down, preferred_element_type=jnp.float32)
    layer_out = (hidden.astype(jnp.float32) + mlp_down).astype(jnp.bfloat16)
    return (layer_out, new_k, new_v)
```

```python
import functools
import math

import jax
import jax.numpy as jnp
from jax import lax
from jax.experimental import pallas as pl
from jax.experimental.pallas import tpu as pltpu
from jax.sharding import PartitionSpec as P

NORM_EPS = 1e-5
ROPE_THETA = 10000.0
LANES = 128
F32 = jnp.float32
BF16 = jnp.bfloat16
FAR = 1 << 28
BLOCK = 4
AHEAD = 5


def rms_norm(values, gain):
    wide = values.astype(F32)
    inv_rms = lax.rsqrt(jnp.mean(wide * wide, axis=-1, keepdims=True) + NORM_EPS)
    return (wide * inv_rms * gain.astype(F32)).astype(BF16)


def attention_kernel(
    pos, x_ref, gain_ref, wq_hbm, wk_hbm, wv_hbm, ck_hbm, cv_hbm,
    part_ref, nk_hbm, nv_hbm,
    wbuf, kbuf, vbuf, q_s, kn_s, vn_s, ang_s, o_s, m_s, l_s,
    w_sem, k_sem, v_sem, out_sem,
):
    rows = x_ref.shape[0]
    head_dim = 2 * LANES
    heads = wq_hbm.shape[1] // head_dim
    kvs = wk_hbm.shape[1] // head_dim
    group = heads // kvs
    per_slot = 2 * kvs
    qrows = 2 * heads
    key_rows = ck_hbm.shape[1]
    local_slots = key_rows // per_slot
    slots = local_slots * lax.axis_size("sp")
    slices = key_rows // LANES
    n_blocks = rows // BLOCK
    base = lax.axis_index("sp") * local_slots

    def w_copy(n):
        src, col = (
            (wk_hbm, n) if n < kvs else (wv_hbm, n - kvs) if n < 2 * kvs else (wq_hbm, n - 2 * kvs)
        )
        return pltpu.make_async_copy(src.at[:, pl.ds(col * head_dim, head_dim)], wbuf.at[n], w_sem.at[n])

    def in_copies(j):
        span = pl.ds(j * BLOCK, BLOCK)
        return (
            pltpu.make_async_copy(ck_hbm.at[span], kbuf.at[span], k_sem.at[j]),
            pltpu.make_async_copy(cv_hbm.at[span], vbuf.at[span], v_sem.at[j]),
        )

    def out_copies(j):
        span = pl.ds(j * BLOCK, BLOCK)
        return (
            pltpu.make_async_copy(kbuf.at[span], nk_hbm.at[span], out_sem.at[0]),
            pltpu.make_async_copy(vbuf.at[span], nv_hbm.at[span], out_sem.at[1]),
        )

    n_w = heads + 2 * kvs
    for n in range(n_w):
        w_copy(n).start()
    for j in range(AHEAD):
        for copy in in_copies(j):
            copy.start()

    lane = lax.broadcasted_iota(jnp.int32, (1, LANES), 1).astype(F32)
    freq = jnp.exp2(lane * (-math.log2(ROPE_THETA) / LANES))

    def angle_row(b, carry):
        ang_s[pl.ds(b, 1), :] = freq * pos[b].astype(F32)
        return carry

    lax.fori_loop(0, rows, angle_row, 0, unroll=8)
    angles = ang_s[...]
    cos_t, sin_t = jnp.cos(angles), jnp.sin(angles)
    normed = rms_norm(x_ref[...], gain_ref[...])

    for n in range(n_w):
        w_copy(n).wait()
        lin = jnp.dot(normed, wbuf[n], preferred_element_type=F32)
        first, second = lin[:, :LANES], lin[:, LANES:]
        if not kvs <= n < 2 * kvs:
            first, second = first * cos_t - second * sin_t, second * cos_t + first * sin_t
        if n >= 2 * kvs:
            h = n - 2 * kvs
            q_s[pl.ds(h, rows, stride=qrows), :] = first
            q_s[pl.ds(heads + h, rows, stride=qrows), :] = second
        else:
            dst, kv = (kn_s, n) if n < kvs else (vn_s, n - kvs)
            for rep in range(16 // per_slot):
                dst[pl.ds(rep * per_slot + kv, rows, stride=16), :] = first
                dst[pl.ds(rep * per_slot + kvs + kv, rows, stride=16), :] = second

    row = lax.broadcasted_iota(jnp.int32, (qrows, LANES), 0)
    col = lax.broadcasted_iota(jnp.int32, (qrows, LANES), 1)
    half_of_col = (col // kvs) % 2
    fits = (half_of_col == row // heads) & (col % kvs == (row % heads) // group)
    slot_of_col = jnp.where(fits, col // per_slot, FAR)
    low_half = half_of_col == 0
    patch_row = lax.broadcasted_iota(jnp.int32, (16, LANES), 0) // per_slot
    scale = 1.0 / math.sqrt(head_dim)

    def block_step(j, carry):
        @pl.when(j + AHEAD < n_blocks)
        def _():
            for copy in in_copies(j + AHEAD):
                copy.start()

        for copy in in_copies(j):
            copy.wait()
        for i in range(BLOCK):
            b = j * BLOCK + i
            local = lax.rem(pos[b], slots) - base
            owned = (local >= 0) & (local < local_slots)
            safe = jnp.where(owned, local, 0)
            hit = jnp.where(owned, lax.rem(safe, 16 // per_slot), -1)
            span = pl.ds(pl.multiple_of((safe // (16 // per_slot)) * 16, 16), 16)
            for buf, new in ((kbuf, kn_s), (vbuf, vn_s)):
                old = buf[b, span, :].astype(F32)
                fresh = new[pl.ds(pl.multiple_of(b * 16, 16), 16), :]
                buf[b, span, :] = jnp.where(patch_row == hit, fresh, old).astype(BF16)
        scores = []
        for i in range(BLOCK):
            b = j * BLOCK + i
            q = q_s[pl.ds(pl.multiple_of(b * qrows, qrows), qrows), :].astype(BF16)
            scores.append(
                lax.dot_general(q, kbuf[b], (((1,), (1,)), ((), ())), preferred_element_type=F32)
            )
        probs = []
        for i in range(BLOCK):
            b = j * BLOCK + i
            limit = jnp.where(pos[b] >= slots - 1, FAR // 2, pos[b]) - base
            parts = []
            for t in range(slices):
                own = scores[i][:, t * LANES : (t + 1) * LANES]
                other = pltpu.roll(own, heads, 0)
                other = jnp.where(
                    low_half, pltpu.roll(other, LANES - kvs, 1), pltpu.roll(other, kvs, 1)
                )
                ok = slot_of_col <= limit - t * (LANES // per_slot)
                parts.append(jnp.where(ok, (own + other) * scale, -jnp.inf))
            top = functools.reduce(jnp.maximum, parts)
            top = jnp.max(top, axis=1, keepdims=True)
            floor = jnp.where(top == -jnp.inf, 0.0, top)
            parts = [jnp.exp(part - floor) for part in parts]
            total = jnp.sum(functools.reduce(jnp.add, parts), axis=1, keepdims=True)
            span = pl.ds(pl.multiple_of(b * qrows, qrows), qrows)
            m_s[span, :] = jnp.broadcast_to(top, (qrows, LANES))
            l_s[span, :] = jnp.broadcast_to(total, (qrows, LANES))
            probs.append(jnp.concatenate([part.astype(BF16) for part in parts], axis=1))
        for i in range(BLOCK):
            b = j * BLOCK + i
            span = pl.ds(pl.multiple_of(b * qrows, qrows), qrows)
            o_s[span, :] = jnp.dot(probs[i], vbuf[b], preferred_element_type=F32)
        for copy in out_copies(j):
            copy.start()
        return carry

    lax.fori_loop(0, n_blocks, block_step, 0)

    left = lax.broadcasted_iota(jnp.int32, (rows, LANES), 1) < LANES // 2
    for h in range(heads):
        part_ref[h, 0] = o_s[pl.ds(h, rows, stride=qrows), :]
        part_ref[h, 1] = o_s[pl.ds(heads + h, rows, stride=qrows), :]
        part_ref[h, 2] = jnp.where(
            left, m_s[pl.ds(h, rows, stride=qrows), :], l_s[pl.ds(h, rows, stride=qrows), :]
        )
    for j in range(n_blocks):
        for copy in out_copies(j):
            copy.wait()


def attention(positions, tokens, gain, w_q, w_k, w_v, rows_k, rows_v):
    rows, width = tokens.shape
    head_dim = 2 * LANES
    heads = w_q.shape[1] // head_dim
    kvs = w_k.shape[1] // head_dim
    qrows = 2 * heads
    vmem = pl.BlockSpec(memory_space=pltpu.VMEM)
    hbm = pl.BlockSpec(memory_space=pl.ANY)
    n_blocks = rows // BLOCK
    return pl.pallas_call(
        attention_kernel,
        out_shape=(
            jax.ShapeDtypeStruct((heads, 3, rows, LANES), F32),
            jax.ShapeDtypeStruct(rows_k.shape, BF16),
            jax.ShapeDtypeStruct(rows_v.shape, BF16),
        ),
        in_specs=[pl.BlockSpec(memory_space=pltpu.SMEM), vmem, vmem] + [hbm] * 5,
        out_specs=(vmem, hbm, hbm),
        scratch_shapes=[
            pltpu.VMEM((heads + 2 * kvs, width, head_dim), BF16),
            pltpu.VMEM(rows_k.shape, BF16),
            pltpu.VMEM(rows_v.shape, BF16),
            pltpu.VMEM((rows * qrows, LANES), F32),
            pltpu.VMEM((rows * 16, LANES), F32),
            pltpu.VMEM((rows * 16, LANES), F32),
            pltpu.VMEM((rows, LANES), F32),
            pltpu.VMEM((rows * qrows, LANES), F32),
            pltpu.VMEM((rows * qrows, LANES), F32),
            pltpu.VMEM((rows * qrows, LANES), F32),
            pltpu.SemaphoreType.DMA((heads + 2 * kvs,)),
            pltpu.SemaphoreType.DMA((n_blocks,)),
            pltpu.SemaphoreType.DMA((n_blocks,)),
            pltpu.SemaphoreType.DMA((2,)),
        ],
        compiler_params=pltpu.CompilerParams(vmem_limit_bytes=60 << 20),
        name="attention_part",
    )(positions, tokens, gain, w_q, w_k, w_v, rows_k, rows_v)


def to_rows(cache):
    b, s, kv, d = cache.shape
    return cache.reshape(b, s, kv, d // LANES, LANES).transpose(0, 1, 3, 2, 4).reshape(b, -1, LANES)


def from_rows(rows, shape):
    b, s, kv, d = shape
    return rows.reshape(b, s, d // LANES, kv, LANES).transpose(0, 1, 3, 2, 4).reshape(shape)


def solution(mesh):
    cache_spec = P("dp", "sp", "tp", None)
    row_spec = P("dp", None)
    col_spec = P(None, "tp")
    in_specs = (row_spec, P("dp"), cache_spec, cache_spec, P(None), col_spec, col_spec, col_spec, P("tp", None), P(None), col_spec, col_spec, P("tp", None))
    out_specs = (row_spec, cache_spec, cache_spec)

    def local_step(tokens, positions, cache_k, cache_v, attn_gain, w_q, w_k, w_v, w_o, mlp_gain, w_gate, w_up, w_down):
        rows = tokens.shape[0]
        part, rows_k, rows_v = attention(
            positions, tokens, attn_gain, w_q, w_k, w_v, to_rows(cache_k), to_rows(cache_v)
        )
        new_k = from_rows(rows_k, cache_k.shape)
        new_v = from_rows(rows_v, cache_v.shape)
        heads = part.shape[0]
        local_max, local_sum = part[:, 2, :, 0], part[:, 2, :, LANES // 2]
        global_max = lax.pmax(local_max, "sp")
        factor = jnp.exp(local_max - global_max)[..., None]
        packed = jnp.concatenate([part[:, 0] * factor, part[:, 1] * factor, local_sum[..., None] * factor], axis=-1)
        total = lax.psum(packed, "sp")
        attended = (total[..., : 2 * LANES] / total[..., 2 * LANES :]).astype(BF16)
        attended = attended.transpose(1, 0, 2).reshape(rows, heads * 2 * LANES)

        attn_proj = lax.psum(jnp.dot(attended, w_o, preferred_element_type=F32), "tp")
        hidden = (tokens.astype(F32) + attn_proj).astype(BF16)
        normed_mlp = rms_norm(hidden, mlp_gain)
        gate_proj = jnp.dot(normed_mlp, w_gate, preferred_element_type=F32)
        up_proj = jnp.dot(normed_mlp, w_up, preferred_element_type=F32)
        activated = (jax.nn.silu(gate_proj) * up_proj).astype(BF16)
        mlp_down = lax.psum(jnp.dot(activated, w_down, preferred_element_type=F32), "tp")
        layer_out = (hidden.astype(F32) + mlp_down).astype(BF16)
        return layer_out, new_k, new_v

    return jax.shard_map(local_step, mesh=mesh, in_specs=in_specs, out_specs=out_specs, check_vma=False)
```

```python
import functools
import math

import jax
import jax.numpy as jnp
from jax import lax
from jax.experimental import pallas as pl
from jax.experimental.pallas import tpu as pltpu
from jax.sharding import PartitionSpec as P

NORM_EPS = 1e-5
ROPE_THETA = 10000.0
LANES = 128
F32 = jnp.float32
BF16 = jnp.bfloat16
FAR = 1 << 28
BLOCK = 4
AHEAD = 5


def rms_norm(values, gain):
    wide = values.astype(F32)
    inv_rms = lax.rsqrt(jnp.mean(wide * wide, axis=-1, keepdims=True) + NORM_EPS)
    return (wide * inv_rms * gain.astype(F32)).astype(BF16)


def attention_kernel(
    pos, x_ref, gain_ref, wq_hbm, wk_hbm, wv_hbm, ck_hbm, cv_hbm,
    part_ref, nk_hbm, nv_hbm,
    wbuf, kbuf, vbuf, q_s, kn_s, vn_s, ang_s, o_s, m_s, l_s,
    w_sem, k_sem, v_sem, out_sem,
):
    rows = x_ref.shape[0]
    head_dim = 2 * LANES
    heads = wq_hbm.shape[1] // head_dim
    kvs = wk_hbm.shape[1] // head_dim
    group = heads // kvs
    per_slot = 2 * kvs
    qrows = 2 * heads
    key_rows = ck_hbm.shape[1]
    local_slots = key_rows // per_slot
    slots = local_slots * lax.axis_size("sp")
    slices = key_rows // LANES
    n_blocks = rows // BLOCK
    base = lax.axis_index("sp") * local_slots

    def w_copy(n):
        src, col = (
            (wk_hbm, n) if n < kvs else (wv_hbm, n - kvs) if n < 2 * kvs else (wq_hbm, n - 2 * kvs)
        )
        return pltpu.make_async_copy(src.at[:, pl.ds(col * head_dim, head_dim)], wbuf.at[n], w_sem.at[n])

    def in_copies(j):
        span = pl.ds(j * BLOCK, BLOCK)
        return (
            pltpu.make_async_copy(ck_hbm.at[span], kbuf.at[span], k_sem.at[j]),
            pltpu.make_async_copy(cv_hbm.at[span], vbuf.at[span], v_sem.at[j]),
        )

    def out_copies(j):
        span = pl.ds(j * BLOCK, BLOCK)
        return (
            pltpu.make_async_copy(kbuf.at[span], nk_hbm.at[span], out_sem.at[0]),
            pltpu.make_async_copy(vbuf.at[span], nv_hbm.at[span], out_sem.at[1]),
        )

    n_w = heads + 2 * kvs
    for n in range(n_w):
        w_copy(n).start()
    for j in range(AHEAD):
        for copy in in_copies(j):
            copy.start()

    lane = lax.broadcasted_iota(jnp.int32, (1, LANES), 1).astype(F32)
    freq = jnp.exp2(lane * (-math.log2(ROPE_THETA) / LANES))

    def angle_row(b, carry):
        ang_s[pl.ds(b, 1), :] = freq * pos[b].astype(F32)
        return carry

    lax.fori_loop(0, rows, angle_row, 0, unroll=8)
    angles = ang_s[...]
    cos_t, sin_t = jnp.cos(angles), jnp.sin(angles)
    normed = rms_norm(x_ref[...], gain_ref[...])

    for n in range(n_w):
        w_copy(n).wait()
        lin = jnp.dot(normed, wbuf[n], preferred_element_type=F32)
        first, second = lin[:, :LANES], lin[:, LANES:]
        if not kvs <= n < 2 * kvs:
            first, second = first * cos_t - second * sin_t, second * cos_t + first * sin_t
        if n >= 2 * kvs:
            h = n - 2 * kvs
            q_s[pl.ds(h, rows, stride=qrows), :] = first
            q_s[pl.ds(heads + h, rows, stride=qrows), :] = second
        else:
            dst, kv = (kn_s, n) if n < kvs else (vn_s, n - kvs)
            for rep in range(16 // per_slot):
                dst[pl.ds(rep * per_slot + kv, rows, stride=16), :] = first
                dst[pl.ds(rep * per_slot + kvs + kv, rows, stride=16), :] = second

    row = lax.broadcasted_iota(jnp.int32, (qrows, LANES), 0)
    col = lax.broadcasted_iota(jnp.int32, (qrows, LANES), 1)
    half_of_col = (col // kvs) % 2
    fits = (half_of_col == row // heads) & (col % kvs == (row % heads) // group)
    slot_of_col = jnp.where(fits, col // per_slot, FAR)
    low_half = half_of_col == 0
    patch_row = lax.broadcasted_iota(jnp.int32, (16, LANES), 0) // per_slot
    scale = 1.0 / math.sqrt(head_dim)

    def block_step(j, carry):
        @pl.when(j + AHEAD < n_blocks)
        def _():
            for copy in in_copies(j + AHEAD):
                copy.start()

        for copy in in_copies(j):
            copy.wait()
        for i in range(BLOCK):
            b = j * BLOCK + i
            local = lax.rem(pos[b], slots) - base
            owned = (local >= 0) & (local < local_slots)
            safe = jnp.where(owned, local, 0)
            hit = jnp.where(owned, lax.rem(safe, 16 // per_slot), -1)
            span = pl.ds(pl.multiple_of((safe // (16 // per_slot)) * 16, 16), 16)
            for buf, new in ((kbuf, kn_s), (vbuf, vn_s)):
                old = buf[b, span, :].astype(F32)
                fresh = new[pl.ds(pl.multiple_of(b * 16, 16), 16), :]
                buf[b, span, :] = jnp.where(patch_row == hit, fresh, old).astype(BF16)
        scores = []
        for i in range(BLOCK):
            b = j * BLOCK + i
            q = q_s[pl.ds(pl.multiple_of(b * qrows, qrows), qrows), :].astype(BF16)
            scores.append(
                lax.dot_general(q, kbuf[b], (((1,), (1,)), ((), ())), preferred_element_type=F32)
            )
        probs = []
        for i in range(BLOCK):
            b = j * BLOCK + i
            limit = jnp.where(pos[b] >= slots - 1, FAR // 2, pos[b]) - base
            parts = []
            for t in range(slices):
                own = scores[i][:, t * LANES : (t + 1) * LANES]
                other = pltpu.roll(own, heads, 0)
                other = jnp.where(
                    low_half, pltpu.roll(other, LANES - kvs, 1), pltpu.roll(other, kvs, 1)
                )
                ok = slot_of_col <= limit - t * (LANES // per_slot)
                parts.append(jnp.where(ok, (own + other) * scale, -jnp.inf))
            top = functools.reduce(jnp.maximum, parts)
            top = jnp.max(top, axis=1, keepdims=True)
            floor = jnp.where(top == -jnp.inf, 0.0, top)
            parts = [jnp.exp(part - floor) for part in parts]
            total = jnp.sum(functools.reduce(jnp.add, parts), axis=1, keepdims=True)
            span = pl.ds(pl.multiple_of(b * qrows, qrows), qrows)
            m_s[span, :] = jnp.broadcast_to(top, (qrows, LANES))
            l_s[span, :] = jnp.broadcast_to(total, (qrows, LANES))
            probs.append(jnp.concatenate([part.astype(BF16) for part in parts], axis=1))
        for i in range(BLOCK):
            b = j * BLOCK + i
            span = pl.ds(pl.multiple_of(b * qrows, qrows), qrows)
            o_s[span, :] = jnp.dot(probs[i], vbuf[b], preferred_element_type=F32)
        for copy in out_copies(j):
            copy.start()
        return carry

    lax.fori_loop(0, n_blocks, block_step, 0)

    left = lax.broadcasted_iota(jnp.int32, (rows, LANES), 1) < LANES // 2
    for h in range(heads):
        part_ref[h, 0] = o_s[pl.ds(h, rows, stride=qrows), :]
        part_ref[h, 1] = o_s[pl.ds(heads + h, rows, stride=qrows), :]
        part_ref[h, 2] = jnp.where(
            left, m_s[pl.ds(h, rows, stride=qrows), :], l_s[pl.ds(h, rows, stride=qrows), :]
        )
    for j in range(n_blocks):
        for copy in out_copies(j):
            copy.wait()


def attention(positions, tokens, gain, w_q, w_k, w_v, rows_k, rows_v):
    rows, width = tokens.shape
    head_dim = 2 * LANES
    heads = w_q.shape[1] // head_dim
    kvs = w_k.shape[1] // head_dim
    qrows = 2 * heads
    vmem = pl.BlockSpec(memory_space=pltpu.VMEM)
    hbm = pl.BlockSpec(memory_space=pl.ANY)
    n_blocks = rows // BLOCK
    return pl.pallas_call(
        attention_kernel,
        out_shape=(
            jax.ShapeDtypeStruct((heads, 3, rows, LANES), F32),
            jax.ShapeDtypeStruct(rows_k.shape, BF16),
            jax.ShapeDtypeStruct(rows_v.shape, BF16),
        ),
        in_specs=[pl.BlockSpec(memory_space=pltpu.SMEM), vmem, vmem] + [hbm] * 5,
        out_specs=(vmem, hbm, hbm),
        scratch_shapes=[
            pltpu.VMEM((heads + 2 * kvs, width, head_dim), BF16),
            pltpu.VMEM(rows_k.shape, BF16),
            pltpu.VMEM(rows_v.shape, BF16),
            pltpu.VMEM((rows * qrows, LANES), F32),
            pltpu.VMEM((rows * 16, LANES), F32),
            pltpu.VMEM((rows * 16, LANES), F32),
            pltpu.VMEM((rows, LANES), F32),
            pltpu.VMEM((rows * qrows, LANES), F32),
            pltpu.VMEM((rows * qrows, LANES), F32),
            pltpu.VMEM((rows * qrows, LANES), F32),
            pltpu.SemaphoreType.DMA((heads + 2 * kvs,)),
            pltpu.SemaphoreType.DMA((n_blocks,)),
            pltpu.SemaphoreType.DMA((n_blocks,)),
            pltpu.SemaphoreType.DMA((2,)),
        ],
        compiler_params=pltpu.CompilerParams(vmem_limit_bytes=60 << 20),
        name="attention_part",
    )(positions, tokens, gain, w_q, w_k, w_v, rows_k, rows_v)


CHUNKS = 2
MESH = pl.DeviceIdType.MESH


def combine(mine, theirs):
    left = lax.broadcasted_iota(jnp.int32, mine[2].shape, mine[2].ndim - 1) < LANES // 2
    axis = mine[2].ndim - 1

    def unpack(stats):
        turned = pltpu.roll(stats, LANES // 2, axis)
        return jnp.where(left, stats, turned), jnp.where(left, turned, stats)

    (m_a, l_a), (m_b, l_b) = unpack(mine[2]), unpack(theirs[2])
    top = jnp.maximum(m_a, m_b)
    f_a = jnp.where(m_a == -jnp.inf, 0.0, jnp.exp(m_a - top))
    f_b = jnp.where(m_b == -jnp.inf, 0.0, jnp.exp(m_b - top))
    return mine[0] * f_a + theirs[0] * f_b, mine[1] * f_a + theirs[1] * f_b, top, l_a * f_a + l_b * f_b


def tail_kernel(
    part_ref, x_ref, gain_ref, wo_hbm, wg_hbm, wu_hbm, wd_hbm,
    out_ref,
    wo, wg, wu, wd, rd, sx, rx, po, ro, so, yo, hb, act, pm, rm, sm, ym, ob,
    w_sem, g_sem, u_sem, d_sem, send_sem, recv_sem,
):
    heads, _, rows, _ = part_ref.shape
    width = x_ref.shape[1]
    mine_h = heads // 2
    half, quarter = rows // 2, rows // 4
    sp, tp = lax.axis_index("sp"), lax.axis_index("tp")
    x, k = sp // 2, lax.rem(sp, 2)
    d_dev, x_dev, y_dev = {"sp": x * 2 + 1 - k}, {"sp": (1 - x) * 2 + k}, {"tp": 1 - tp}
    o_rows, n_gate = wo.shape[0], wg.shape[0]
    g_cols = wg.shape[2]
    m_cols = n_gate * g_cols
    n_down = wd.shape[0]
    d_rows = wd.shape[1]
    span = width // CHUNKS

    def weight_copies():
        yield pltpu.make_async_copy(wo_hbm.at[pl.ds(k * o_rows, o_rows)], wo, w_sem)
        for c in range(n_gate):
            cols = pl.ds(pl.multiple_of(k * m_cols + c * g_cols, LANES), g_cols)
            yield pltpu.make_async_copy(wg_hbm.at[:, cols], wg.at[c], g_sem.at[c])
            yield pltpu.make_async_copy(wu_hbm.at[:, cols], wu.at[c], u_sem.at[c])
        for c in range(n_down):
            yield pltpu.make_async_copy(
                wd_hbm.at[pl.ds(pl.multiple_of(k * m_cols + c * d_rows, 8), d_rows)], wd.at[c], d_sem.at[c]
            )

    for copy in weight_copies():
        copy.start()

    barrier = pltpu.get_barrier_semaphore()
    for dev in (d_dev, x_dev, y_dev):
        pl.semaphore_signal(barrier, inc=1, device_id=dev, device_id_type=MESH)
    pl.semaphore_wait(barrier, 3)

    counter = [0]

    def remote(src, dst, dev):
        n = counter[0]
        counter[0] += 1
        return pltpu.make_async_remote_copy(
            src_ref=src, dst_ref=dst, send_sem=send_sem.at[n], recv_sem=recv_sem.at[n],
            device_id=dev, device_id_type=MESH,
        )

    far_rows, near_rows = pl.ds((1 - x) * half, half), pl.ds(x * half, half)
    swap = remote(part_ref.at[pl.ds((1 - k) * mine_h, mine_h)], rd, d_dev)
    swap.start()
    swap.wait_recv()
    my_heads = pl.ds(k * mine_h, mine_h)

    def chip_part(at):
        return combine(
            [part_ref[my_heads, i, at] for i in range(3)], [rd[:, i, at] for i in range(3)]
        )

    left = lax.broadcasted_iota(jnp.int32, (mine_h, half, LANES), 2) < LANES // 2
    o_a, o_b, m, l = chip_part(far_rows)
    sx[:, 0], sx[:, 1], sx[:, 2] = o_a, o_b, jnp.where(left, m, l)
    cross = remote(sx, rx, x_dev)
    cross.start()
    o_a, o_b, m, l = chip_part(near_rows)
    cross.wait_recv()
    o_a, o_b, _, l = combine([o_a, o_b, jnp.where(left, m, l)], [rx[:, i] for i in range(3)])
    o_a, o_b = (o_a / l).astype(BF16), (o_b / l).astype(BF16)
    attended = jnp.concatenate([v[h] for h in range(mine_h) for v in (o_a, o_b)], axis=-1)

    own, other = pl.ds(k * quarter, quarter), pl.ds((1 - k) * quarter, quarter)
    my_rows = pl.ds(pl.multiple_of(x * half + k * quarter, quarter), quarter)
    x_peer_rows = pl.ds(pl.multiple_of((1 - x) * half + k * quarter, quarter), quarter)
    cols = [pl.ds(c * span, span) for c in range(CHUNKS)]

    def staged(stages):
        for t in range(CHUNKS + len(stages) - 1):
            for s in reversed(range(len(stages))):
                if 0 <= t - s < CHUNKS:
                    stages[s](t - s)

    swaps = [remote(po.at[other, c], ro.at[:, c], d_dev) for c in cols]
    crosses = [remote(so.at[:, c], yo.at[:, c], y_dev) for c in cols]
    gathers = [remote(hb.at[own, c], hb.at[own, c], d_dev) for c in cols]
    weights = weight_copies()
    next(weights).wait()

    def o_dot(c):
        po[:, cols[c]] = jnp.dot(attended, wo[:, cols[c]], preferred_element_type=F32)
        swaps[c].start()

    def o_swap(c):
        swaps[c].wait_recv()
        so[:, cols[c]] = po[own, cols[c]] + ro[:, cols[c]]
        crosses[c].start()

    def o_cross(c):
        crosses[c].wait_recv()
        total = so[:, cols[c]] + yo[:, cols[c]]
        hb[own, cols[c]] = (x_ref[my_rows, cols[c]].astype(F32) + total).astype(BF16).astype(F32)
        gathers[c].start()

    def o_gather(c):
        gathers[c].wait_recv()

    staged([o_dot, o_swap, o_cross, o_gather])

    normed = rms_norm(hb[...], gain_ref[...])
    for c in range(n_gate):
        next(weights).wait()
        next(weights).wait()
        gate = jnp.dot(normed, wg[c], preferred_element_type=F32)
        up = jnp.dot(normed, wu[c], preferred_element_type=F32)
        act[:, c * g_cols : (c + 1) * g_cols] = (jax.nn.silu(gate) * up).astype(BF16)
    for copy in weights:
        copy.wait()

    swaps_m = [remote(pm.at[other, c], rm.at[:, c], d_dev) for c in cols]
    crosses_m = [remote(sm.at[:, c], ym.at[:, c], y_dev) for c in cols]
    to_core = [remote(ob.at[my_rows, c], ob.at[my_rows, c], d_dev) for c in cols]
    to_x = [remote(ob.at[my_rows, c], ob.at[my_rows, c], x_dev) for c in cols]
    onward = [remote(ob.at[x_peer_rows, c], ob.at[x_peer_rows, c], d_dev) for c in cols]

    def m_dot(c):
        total = None
        for r in range(n_down):
            piece = jnp.dot(
                act[:, r * d_rows : (r + 1) * d_rows], wd[r, :, cols[c]], preferred_element_type=F32
            )
            total = piece if total is None else total + piece
        pm[:, cols[c]] = total
        swaps_m[c].start()

    def m_swap(c):
        swaps_m[c].wait_recv()
        sm[:, cols[c]] = pm[own, cols[c]] + rm[:, cols[c]]
        crosses_m[c].start()

    def m_cross(c):
        crosses_m[c].wait_recv()
        total = sm[:, cols[c]] + ym[:, cols[c]]
        ob[my_rows, cols[c]] = (hb[own, cols[c]] + total).astype(BF16).astype(F32)
        to_x[c].start()
        to_core[c].start()

    def m_gather(c):
        to_x[c].wait_recv()
        onward[c].start()

    def m_last(c):
        to_core[c].wait_recv()
        onward[c].wait_recv()
        out_ref[:, cols[c]] = ob[:, cols[c]].astype(BF16)

    staged([m_dot, m_swap, m_cross, m_gather, m_last])
    for copy in [swap, cross, *swaps, *crosses, *gathers, *swaps_m, *crosses_m, *to_core, *to_x, *onward]:
        copy.wait_send()


def tail(part, tokens, gain, w_o, w_gate, w_up, w_down):
    heads, _, rows, _ = part.shape
    width = tokens.shape[1]
    half, quarter = rows // 2, rows // 4
    cut = w_gate.shape[1] // 2
    n_gate, n_down = cut // 256, 4
    vmem = pl.BlockSpec(memory_space=pltpu.VMEM)
    hbm = pl.BlockSpec(memory_space=pl.ANY)
    flat = lambda n: pltpu.VMEM((n, width), F32)
    stats = lambda n: pltpu.VMEM((heads // 2, 3, n, LANES), F32)
    n_remote = 2 + 8 * CHUNKS
    return pl.pallas_call(
        tail_kernel,
        out_shape=jax.ShapeDtypeStruct(tokens.shape, BF16),
        in_specs=[vmem, vmem, vmem] + [hbm] * 4,
        out_specs=vmem,
        scratch_shapes=[
            pltpu.VMEM((w_o.shape[0] // 2, width), BF16),
            pltpu.VMEM((n_gate, width, 256), BF16),
            pltpu.VMEM((n_gate, width, 256), BF16),
            pltpu.VMEM((n_down, cut // n_down, width), BF16),
            stats(rows), stats(half), stats(half),
            flat(half), flat(quarter), flat(quarter), flat(quarter), flat(half),
            pltpu.VMEM((half, cut), BF16),
            flat(half), flat(quarter), flat(quarter), flat(quarter), flat(rows),
            pltpu.SemaphoreType.DMA,
            pltpu.SemaphoreType.DMA((n_gate,)),
            pltpu.SemaphoreType.DMA((n_gate,)),
            pltpu.SemaphoreType.DMA((n_down,)),
            pltpu.SemaphoreType.DMA((n_remote,)),
            pltpu.SemaphoreType.DMA((n_remote,)),
        ],
        compiler_params=pltpu.CompilerParams(
            vmem_limit_bytes=60 << 20, collective_id=0, has_side_effects=True
        ),
        name="tail",
    )(part, tokens, gain, w_o, w_gate, w_up, w_down)


def to_rows(cache):
    b, s, kv, d = cache.shape
    return cache.reshape(b, s, kv, d // LANES, LANES).transpose(0, 1, 3, 2, 4).reshape(b, -1, LANES)


def from_rows(rows, shape):
    b, s, kv, d = shape
    return rows.reshape(b, s, d // LANES, kv, LANES).transpose(0, 1, 3, 2, 4).reshape(shape)


def solution(mesh):
    cache_spec = P("dp", "sp", "tp", None)
    row_spec = P("dp", None)
    col_spec = P(None, "tp")
    in_specs = (row_spec, P("dp"), cache_spec, cache_spec, P(None), col_spec, col_spec, col_spec, P("tp", None), P(None), col_spec, col_spec, P("tp", None))
    out_specs = (row_spec, cache_spec, cache_spec)

    def local_step(tokens, positions, cache_k, cache_v, attn_gain, w_q, w_k, w_v, w_o, mlp_gain, w_gate, w_up, w_down):
        part, rows_k, rows_v = attention(
            positions, tokens, attn_gain, w_q, w_k, w_v, to_rows(cache_k), to_rows(cache_v)
        )
        new_k = from_rows(rows_k, cache_k.shape)
        new_v = from_rows(rows_v, cache_v.shape)
        layer_out = tail(part, tokens, mlp_gain, w_o, w_gate, w_up, w_down)
        return layer_out, new_k, new_v

    return jax.shard_map(local_step, mesh=mesh, in_specs=in_specs, out_specs=out_specs, check_vma=False)
```

```python
import functools
import itertools
import math

import jax
import jax.numpy as jnp
from jax import lax
from jax.experimental import pallas as pl
from jax.experimental.pallas import tpu as pltpu
from jax.sharding import PartitionSpec as P

NORM_EPS = 1e-5
ROPE_THETA = 10000.0
LANES = 128
F32 = jnp.float32
BF16 = jnp.bfloat16
FAR = 1 << 28
BLOCK = 4
AHEAD = 5


def rms_norm(values, gain):
    wide = values.astype(F32)
    inv_rms = lax.rsqrt(jnp.mean(wide * wide, axis=-1, keepdims=True) + NORM_EPS)
    return (wide * inv_rms * gain.astype(F32)).astype(BF16)


def attention_kernel(
    pos_hbm, x_hbm, gain_hbm, wq_hbm, wk_hbm, wv_hbm, ck_hbm, cv_hbm,
    part_ref, nk_hbm, nv_hbm,
    wbuf, kbuf, vbuf, q_s, kn_s, vn_s, ang_s, o_s, m_s, l_s,
    pos, x_ref, gain_ref, w_sem, k_sem, v_sem, out_sem, x_sem,
):
    rows = x_ref.shape[0]
    head_dim = 2 * LANES
    heads = wq_hbm.shape[1] // head_dim
    kvs = wk_hbm.shape[1] // head_dim
    group = heads // kvs
    per_slot = 2 * kvs
    qrows = 2 * heads
    key_rows = ck_hbm.shape[1]
    local_slots = key_rows // per_slot
    slots = local_slots * lax.axis_size("sp")
    slices = key_rows // LANES
    n_blocks = rows // BLOCK
    base = lax.axis_index("sp") * local_slots

    def w_copy(n):
        src, col = (
            (wk_hbm, n) if n < kvs else (wv_hbm, n - kvs) if n < 2 * kvs else (wq_hbm, n - 2 * kvs)
        )
        return pltpu.make_async_copy(src.at[:, pl.ds(col * head_dim, head_dim)], wbuf.at[n], w_sem.at[n])

    def in_copies(j):
        span = pl.ds(j * BLOCK, BLOCK)
        return (
            pltpu.make_async_copy(ck_hbm.at[span], kbuf.at[span], k_sem.at[j]),
            pltpu.make_async_copy(cv_hbm.at[span], vbuf.at[span], v_sem.at[j]),
        )

    def out_copies(j):
        span = pl.ds(j * BLOCK, BLOCK)
        return (
            pltpu.make_async_copy(kbuf.at[span], nk_hbm.at[span], out_sem.at[0]),
            pltpu.make_async_copy(vbuf.at[span], nv_hbm.at[span], out_sem.at[1]),
        )

    small = [
        pltpu.make_async_copy(src, dst, x_sem.at[i])
        for i, (src, dst) in enumerate(((pos_hbm, pos), (x_hbm, x_ref), (gain_hbm, gain_ref)))
    ]
    for copy in small:
        copy.start()
    n_w = heads + 2 * kvs
    for n in range(n_w):
        w_copy(n).start()
    for j in range(AHEAD):
        for copy in in_copies(j):
            copy.start()

    lane = lax.broadcasted_iota(jnp.int32, (1, LANES), 1).astype(F32)
    freq = jnp.exp2(lane * (-math.log2(ROPE_THETA) / LANES))

    for copy in small:
        copy.wait()

    def angle_row(b, carry):
        ang_s[pl.ds(b, 1), :] = freq * pos[b].astype(F32)
        return carry

    lax.fori_loop(0, rows, angle_row, 0, unroll=8)
    angles = ang_s[...]
    cos_t, sin_t = jnp.cos(angles), jnp.sin(angles)
    normed = rms_norm(x_ref[...], gain_ref[...])

    for n in range(n_w):
        w_copy(n).wait()
        lin = jnp.dot(normed, wbuf[n], preferred_element_type=F32)
        first, second = lin[:, :LANES], lin[:, LANES:]
        if not kvs <= n < 2 * kvs:
            first, second = first * cos_t - second * sin_t, second * cos_t + first * sin_t
        if n >= 2 * kvs:
            h = n - 2 * kvs
            q_s[pl.ds(h, rows, stride=qrows), :] = first
            q_s[pl.ds(heads + h, rows, stride=qrows), :] = second
        else:
            dst, kv = (kn_s, n) if n < kvs else (vn_s, n - kvs)
            for rep in range(16 // per_slot):
                dst[pl.ds(rep * per_slot + kv, rows, stride=16), :] = first
                dst[pl.ds(rep * per_slot + kvs + kv, rows, stride=16), :] = second

    row = lax.broadcasted_iota(jnp.int32, (qrows, LANES), 0)
    col = lax.broadcasted_iota(jnp.int32, (qrows, LANES), 1)
    half_of_col = (col // kvs) % 2
    fits = (half_of_col == row // heads) & (col % kvs == (row % heads) // group)
    slot_of_col = jnp.where(fits, col // per_slot, FAR)
    low_half = half_of_col == 0
    patch_row = lax.broadcasted_iota(jnp.int32, (16, LANES), 0) // per_slot
    scale = 1.0 / math.sqrt(head_dim)

    def block_step(j, carry):
        @pl.when(j + AHEAD < n_blocks)
        def _():
            for copy in in_copies(j + AHEAD):
                copy.start()

        for copy in in_copies(j):
            copy.wait()
        for i in range(BLOCK):
            b = j * BLOCK + i
            local = lax.rem(pos[b], slots) - base
            owned = (local >= 0) & (local < local_slots)
            safe = jnp.where(owned, local, 0)
            hit = jnp.where(owned, lax.rem(safe, 16 // per_slot), -1)
            span = pl.ds(pl.multiple_of((safe // (16 // per_slot)) * 16, 16), 16)
            for buf, new in ((kbuf, kn_s), (vbuf, vn_s)):
                old = buf[b, span, :].astype(F32)
                fresh = new[pl.ds(pl.multiple_of(b * 16, 16), 16), :]
                buf[b, span, :] = jnp.where(patch_row == hit, fresh, old).astype(BF16)
        scores = []
        for i in range(BLOCK):
            b = j * BLOCK + i
            q = q_s[pl.ds(pl.multiple_of(b * qrows, qrows), qrows), :].astype(BF16)
            scores.append(
                lax.dot_general(q, kbuf[b], (((1,), (1,)), ((), ())), preferred_element_type=F32)
            )
        probs = []
        for i in range(BLOCK):
            b = j * BLOCK + i
            limit = jnp.where(pos[b] >= slots - 1, FAR // 2, pos[b]) - base
            parts = []
            for t in range(slices):
                own = scores[i][:, t * LANES : (t + 1) * LANES]
                other = pltpu.roll(own, heads, 0)
                other = jnp.where(
                    low_half, pltpu.roll(other, LANES - kvs, 1), pltpu.roll(other, kvs, 1)
                )
                ok = slot_of_col <= limit - t * (LANES // per_slot)
                parts.append(jnp.where(ok, (own + other) * scale, -jnp.inf))
            top = functools.reduce(jnp.maximum, parts)
            top = jnp.max(top, axis=1, keepdims=True)
            floor = jnp.where(top == -jnp.inf, 0.0, top)
            parts = [jnp.exp(part - floor) for part in parts]
            total = jnp.sum(functools.reduce(jnp.add, parts), axis=1, keepdims=True)
            span = pl.ds(pl.multiple_of(b * qrows, qrows), qrows)
            m_s[span, :] = jnp.broadcast_to(top, (qrows, LANES))
            l_s[span, :] = jnp.broadcast_to(total, (qrows, LANES))
            probs.append(jnp.concatenate([part.astype(BF16) for part in parts], axis=1))
        for i in range(BLOCK):
            b = j * BLOCK + i
            span = pl.ds(pl.multiple_of(b * qrows, qrows), qrows)
            o_s[span, :] = jnp.dot(probs[i], vbuf[b], preferred_element_type=F32)
        for copy in out_copies(j):
            copy.start()
        return carry

    lax.fori_loop(0, n_blocks, block_step, 0)

    left = lax.broadcasted_iota(jnp.int32, (rows, LANES), 1) < LANES // 2
    for h in range(heads):
        part_ref[h, 0] = o_s[pl.ds(h, rows, stride=qrows), :]
        part_ref[h, 1] = o_s[pl.ds(heads + h, rows, stride=qrows), :]
        part_ref[h, 2] = jnp.where(
            left, m_s[pl.ds(h, rows, stride=qrows), :], l_s[pl.ds(h, rows, stride=qrows), :]
        )
    for j in range(n_blocks):
        for copy in out_copies(j):
            copy.wait()


def attention(positions, tokens, gain, w_q, w_k, w_v, rows_k, rows_v):
    rows, width = tokens.shape
    head_dim = 2 * LANES
    heads = w_q.shape[1] // head_dim
    kvs = w_k.shape[1] // head_dim
    qrows = 2 * heads
    vmem = pl.BlockSpec(memory_space=pltpu.VMEM)
    hbm = pl.BlockSpec(memory_space=pltpu.HBM)
    n_blocks = rows // BLOCK
    return pl.pallas_call(
        attention_kernel,
        out_shape=(
            pltpu.VMEM((heads, 3, rows, LANES), F32),
            jax.ShapeDtypeStruct(rows_k.shape, BF16),
            jax.ShapeDtypeStruct(rows_v.shape, BF16),
        ),
        in_specs=[hbm] * 8,
        out_specs=(vmem, hbm, hbm),
        scratch_shapes=[
            pltpu.VMEM((heads + 2 * kvs, width, head_dim), BF16),
            pltpu.VMEM(rows_k.shape, BF16),
            pltpu.VMEM(rows_v.shape, BF16),
            pltpu.VMEM((rows * qrows, LANES), F32),
            pltpu.VMEM((rows * 16, LANES), F32),
            pltpu.VMEM((rows * 16, LANES), F32),
            pltpu.VMEM((rows, LANES), F32),
            pltpu.VMEM((rows * qrows, LANES), F32),
            pltpu.VMEM((rows * qrows, LANES), F32),
            pltpu.VMEM((rows * qrows, LANES), F32),
            pltpu.SMEM((rows,), jnp.int32),
            pltpu.VMEM(tokens.shape, BF16),
            pltpu.VMEM(gain.shape, BF16),
            pltpu.SemaphoreType.DMA((heads + 2 * kvs,)),
            pltpu.SemaphoreType.DMA((n_blocks,)),
            pltpu.SemaphoreType.DMA((n_blocks,)),
            pltpu.SemaphoreType.DMA((2,)),
            pltpu.SemaphoreType.DMA((3,)),
        ],
        compiler_params=pltpu.CompilerParams(vmem_limit_bytes=52 << 20),
        name="attention_part",
    )(*(pltpu.with_memory_space_constraint(v, pltpu.HBM) for v in (positions, tokens, gain)), w_q, w_k, w_v, rows_k, rows_v)


CHUNKS = 5
MESH = pl.DeviceIdType.MESH


def combine(mine, theirs):
    left = lax.broadcasted_iota(jnp.int32, mine[2].shape, mine[2].ndim - 1) < LANES // 2
    axis = mine[2].ndim - 1

    def unpack(stats):
        turned = pltpu.roll(stats, LANES // 2, axis)
        return jnp.where(left, stats, turned), jnp.where(left, turned, stats)

    (m_a, l_a), (m_b, l_b) = unpack(mine[2]), unpack(theirs[2])
    top = jnp.maximum(m_a, m_b)
    f_a = jnp.where(m_a == -jnp.inf, 0.0, jnp.exp(m_a - top))
    f_b = jnp.where(m_b == -jnp.inf, 0.0, jnp.exp(m_b - top))
    return mine[0] * f_a + theirs[0] * f_b, mine[1] * f_a + theirs[1] * f_b, top, l_a * f_a + l_b * f_b


def tail_kernel(
    part_ref, x_ref, gain_ref, wo_hbm, wg_hbm, wu_hbm, wd_hbm,
    out_ref,
    wo, wg, wu, wd, rd, sx, rx, po, ro, so, yo, hb, act, pm, rm, sm, ym, ob,
    w_sem, g_sem, u_sem, d_sem, send_sem, recv_sem,
):
    heads, _, rows, _ = part_ref.shape
    width = x_ref.shape[1]
    mine_h = heads // 2
    half, quarter = rows // 2, rows // 4
    sp, tp = lax.axis_index("sp"), lax.axis_index("tp")
    x, k = sp // 2, lax.rem(sp, 2)
    d_dev, x_dev, y_dev = {"sp": x * 2 + 1 - k}, {"sp": (1 - x) * 2 + k}, {"tp": 1 - tp}
    o_rows, n_gate = wo.shape[0], wg.shape[0]
    g_cols = wg.shape[2]
    m_cols = n_gate * g_cols
    d_rows = g_cols
    n_down = wd.shape[0] // d_rows
    span = width // CHUNKS

    barrier = pltpu.get_barrier_semaphore()
    for dev in (d_dev, x_dev, y_dev):
        pl.semaphore_signal(barrier, inc=1, device_id=dev, device_id_type=MESH)

    o_copy = pltpu.make_async_copy(wo_hbm.at[pl.ds(k * o_rows, o_rows)], wo, w_sem)
    g_copies, d_copies = [], []
    for c in range(n_gate):
        at = pl.ds(pl.multiple_of(k * m_cols + c * g_cols, LANES), g_cols)
        g_copies.append(pltpu.make_async_copy(wg_hbm.at[:, at], wg.at[c], g_sem.at[c]))
        g_copies.append(pltpu.make_async_copy(wu_hbm.at[:, at], wu.at[c], u_sem.at[c]))
    for c in range(n_down):
        at = pl.ds(pl.multiple_of(k * m_cols + c * d_rows, LANES), d_rows)
        d_copies.append(pltpu.make_async_copy(wd_hbm.at[at], wd.at[pl.ds(c * d_rows, d_rows)], d_sem.at[c]))
    queue = iter(g_copies + d_copies)

    def fetch(n):
        for copy in itertools.islice(queue, n):
            copy.start()

    o_copy.start()
    pl.semaphore_wait(barrier, 3)

    counter = [0]

    def remote(src, dst, dev):
        n = counter[0]
        counter[0] += 1
        return pltpu.make_async_remote_copy(
            src_ref=src, dst_ref=dst, send_sem=send_sem.at[n], recv_sem=recv_sem.at[n],
            device_id=dev, device_id_type=MESH,
        )

    far_rows, near_rows = pl.ds((1 - x) * half, half), pl.ds(x * half, half)
    swap = remote(part_ref.at[pl.ds((1 - k) * mine_h, mine_h)], rd, d_dev)
    swap.start()
    fetch(2)
    swap.wait_recv()
    my_heads = pl.ds(k * mine_h, mine_h)

    def chip_part(at):
        return combine(
            [part_ref[my_heads, i, at] for i in range(3)], [rd[:, i, at] for i in range(3)]
        )

    left = lax.broadcasted_iota(jnp.int32, (mine_h, half, LANES), 2) < LANES // 2
    o_a, o_b, m, l = chip_part(far_rows)
    sx[:, 0], sx[:, 1], sx[:, 2] = o_a, o_b, jnp.where(left, m, l)
    cross = remote(sx, rx, x_dev)
    cross.start()
    fetch(8)
    o_a, o_b, m, l = chip_part(near_rows)
    cross.wait_recv()
    o_a, o_b, _, l = combine([o_a, o_b, jnp.where(left, m, l)], [rx[:, i] for i in range(3)])
    o_a, o_b = (o_a / l).astype(BF16), (o_b / l).astype(BF16)
    attended = jnp.concatenate([v[h] for h in range(mine_h) for v in (o_a, o_b)], axis=-1)

    own, other = pl.ds(k * quarter, quarter), pl.ds((1 - k) * quarter, quarter)
    my_rows = pl.ds(pl.multiple_of(x * half + k * quarter, quarter), quarter)
    x_peer_rows = pl.ds(pl.multiple_of((1 - x) * half + k * quarter, quarter), quarter)
    cols = [pl.ds(c * span, span) for c in range(CHUNKS)]

    def staged(dot, swap, cross, *rest):
        for c in range(CHUNKS + 2):
            if c < CHUNKS:
                dot(c)
            if c >= 2:
                swap(c - 2)
        for c in range(CHUNKS):
            cross(c)
        for c in range(CHUNKS + len(rest) - 1):
            for s, stage in enumerate(rest):
                if 0 <= c - s < CHUNKS:
                    stage(c - s)

    swaps = [remote(po.at[other, c], ro.at[:, c], d_dev) for c in cols]
    crosses = [remote(so.at[:, c], yo.at[:, c], y_dev) for c in cols]
    gathers = [remote(hb.at[own, c], hb.at[own, c], d_dev) for c in cols]
    o_copy.wait()

    def o_dot(c):
        po[:, cols[c]] = jnp.dot(attended, wo[:, cols[c]], preferred_element_type=F32)
        swaps[c].start()

    def o_swap(c):
        swaps[c].wait_recv()
        so[:, cols[c]] = po[own, cols[c]] + ro[:, cols[c]]
        crosses[c].start()
        fetch(3)

    def o_cross(c):
        crosses[c].wait_recv()
        total = so[:, cols[c]] + yo[:, cols[c]]
        hb[own, cols[c]] = (x_ref[my_rows, cols[c]].astype(F32) + total).astype(BF16).astype(F32)
        gathers[c].start()

    def o_gather(c):
        gathers[c].wait_recv()

    staged(o_dot, o_swap, o_cross, o_gather)
    fetch(len(g_copies) + len(d_copies))

    normed = rms_norm(hb[...], gain_ref[...])
    for c in range(n_gate):
        g_copies[2 * c].wait()
        g_copies[2 * c + 1].wait()
        gate = jnp.dot(normed, wg[c], preferred_element_type=F32)
        up = jnp.dot(normed, wu[c], preferred_element_type=F32)
        act[:, c * g_cols : (c + 1) * g_cols] = (jax.nn.silu(gate) * up).astype(BF16)
    for copy in d_copies:
        copy.wait()

    swaps_m = [remote(pm.at[other, c], rm.at[:, c], d_dev) for c in cols]
    crosses_m = [remote(sm.at[:, c], ym.at[:, c], y_dev) for c in cols]
    to_core = [remote(ob.at[my_rows, c], ob.at[my_rows, c], d_dev) for c in cols]
    to_x = [remote(ob.at[my_rows, c], ob.at[my_rows, c], x_dev) for c in cols]
    onward = [remote(ob.at[x_peer_rows, c], ob.at[x_peer_rows, c], d_dev) for c in cols]

    def m_dot(c):
        pm[:, cols[c]] = jnp.dot(act[...], wd[:, cols[c]], preferred_element_type=F32)
        swaps_m[c].start()

    def m_swap(c):
        swaps_m[c].wait_recv()
        sm[:, cols[c]] = pm[own, cols[c]] + rm[:, cols[c]]
        crosses_m[c].start()

    def m_cross(c):
        crosses_m[c].wait_recv()
        total = sm[:, cols[c]] + ym[:, cols[c]]
        ob[my_rows, cols[c]] = (hb[own, cols[c]] + total).astype(BF16).astype(F32)
        to_x[c].start()
        to_core[c].start()

    def m_gather(c):
        to_x[c].wait_recv()
        onward[c].start()

    def m_last(c):
        to_core[c].wait_recv()
        onward[c].wait_recv()
        out_ref[:, cols[c]] = ob[:, cols[c]].astype(BF16)

    staged(m_dot, m_swap, m_cross, m_gather, m_last)
    for copy in [swap, cross, *swaps, *crosses, *gathers, *swaps_m, *crosses_m, *to_core, *to_x, *onward]:
        copy.wait_send()


def tail(part, tokens, gain, w_o, w_gate, w_up, w_down):
    heads, _, rows, _ = part.shape
    width = tokens.shape[1]
    half, quarter = rows // 2, rows // 4
    cut = w_gate.shape[1] // 2
    n_gate = cut // 256
    vmem = pl.BlockSpec(memory_space=pltpu.VMEM)
    hbm = pl.BlockSpec(memory_space=pltpu.HBM)
    flat = lambda n: pltpu.VMEM((n, width), F32)
    stats = lambda n: pltpu.VMEM((heads // 2, 3, n, LANES), F32)
    n_remote = 2 + 8 * CHUNKS
    return pl.pallas_call(
        tail_kernel,
        out_shape=pltpu.VMEM(tokens.shape, BF16),
        in_specs=[vmem, vmem, vmem] + [hbm] * 4,
        out_specs=vmem,
        scratch_shapes=[
            pltpu.VMEM((w_o.shape[0] // 2, width), BF16),
            pltpu.VMEM((n_gate, width, 256), BF16),
            pltpu.VMEM((n_gate, width, 256), BF16),
            pltpu.VMEM((cut, width), BF16),
            stats(rows), stats(half), stats(half),
            flat(half), flat(quarter), flat(quarter), flat(quarter), flat(half),
            pltpu.VMEM((half, cut), BF16),
            flat(half), flat(quarter), flat(quarter), flat(quarter), flat(rows),
            pltpu.SemaphoreType.DMA,
            pltpu.SemaphoreType.DMA((n_gate,)),
            pltpu.SemaphoreType.DMA((n_gate,)),
            pltpu.SemaphoreType.DMA((n_gate,)),
            pltpu.SemaphoreType.DMA((n_remote,)),
            pltpu.SemaphoreType.DMA((n_remote,)),
        ],
        compiler_params=pltpu.CompilerParams(
            vmem_limit_bytes=50 << 20, collective_id=0, has_side_effects=True
        ),
        name="tail",
    )(part, tokens, gain, w_o, w_gate, w_up, w_down)


def to_rows(cache):
    b, s, kv, d = cache.shape
    return cache.reshape(b, s, kv, d // LANES, LANES).transpose(0, 1, 3, 2, 4).reshape(b, -1, LANES)


def from_rows(rows, shape):
    b, s, kv, d = shape
    return rows.reshape(b, s, d // LANES, kv, LANES).transpose(0, 1, 3, 2, 4).reshape(shape)


def solution(mesh):
    cache_spec = P("dp", "sp", "tp", None)
    row_spec = P("dp", None)
    col_spec = P(None, "tp")
    in_specs = (row_spec, P("dp"), cache_spec, cache_spec, P(None), col_spec, col_spec, col_spec, P("tp", None), P(None), col_spec, col_spec, P("tp", None))
    out_specs = (row_spec, cache_spec, cache_spec)

    def local_step(tokens, positions, cache_k, cache_v, attn_gain, w_q, w_k, w_v, w_o, mlp_gain, w_gate, w_up, w_down):
        part, rows_k, rows_v = attention(
            positions, tokens, attn_gain, w_q, w_k, w_v, to_rows(cache_k), to_rows(cache_v)
        )
        new_k = from_rows(rows_k, cache_k.shape)
        new_v = from_rows(rows_v, cache_v.shape)
        layer_out = tail(part, tokens, mlp_gain, w_o, w_gate, w_up, w_down)
        return layer_out, new_k, new_v

    return jax.shard_map(local_step, mesh=mesh, in_specs=in_specs, out_specs=out_specs, check_vma=False)
```

```python
import functools
import itertools
import math

import jax
import jax.numpy as jnp
from jax import lax
from jax.experimental import pallas as pl
from jax.experimental.pallas import tpu as pltpu
from jax.sharding import PartitionSpec as P

NORM_EPS = 1e-5
ROPE_THETA = 10000.0
LANES = 128
F32 = jnp.float32
BF16 = jnp.bfloat16
FAR = 1 << 28
BLOCK = 4
FIRST = 4


def rms_norm(values, gain):
    wide = values.astype(F32)
    inv_rms = lax.rsqrt(jnp.mean(wide * wide, axis=-1, keepdims=True) + NORM_EPS)
    return (wide * inv_rms * gain.astype(F32)).astype(BF16)


def attention_kernel(
    pos_hbm, x_hbm, gain_hbm, wq_hbm, wk_hbm, wv_hbm, ck_hbm, cv_hbm,
    part_ref, nk_hbm, nv_hbm,
    wbuf, kbuf, vbuf, q_s, kn_s, vn_s, ang_s, o_s, m_s, l_s,
    pos, x_ref, gain_ref, w_sem, k_sem, v_sem, out_sem, x_sem,
):
    rows = x_ref.shape[0]
    head_dim = 2 * LANES
    heads = wq_hbm.shape[1] // head_dim
    kvs = wk_hbm.shape[1] // head_dim
    group = heads // kvs
    per_slot = 2 * kvs
    qrows = 2 * heads
    key_rows = ck_hbm.shape[1]
    local_slots = key_rows // per_slot
    slots = local_slots * lax.axis_size("sp")
    slices = key_rows // LANES
    n_blocks = rows // BLOCK
    base = lax.axis_index("sp") * local_slots

    def w_copy(n):
        src, col = (
            (wk_hbm, n) if n < kvs else (wv_hbm, n - kvs) if n < 2 * kvs else (wq_hbm, n - 2 * kvs)
        )
        return pltpu.make_async_copy(src.at[:, pl.ds(col * head_dim, head_dim)], wbuf.at[n], w_sem.at[n])

    def in_copies(j):
        span = pl.ds(j * BLOCK, BLOCK)
        return (
            pltpu.make_async_copy(ck_hbm.at[span], kbuf.at[span], k_sem.at[j]),
            pltpu.make_async_copy(cv_hbm.at[span], vbuf.at[span], v_sem.at[j]),
        )

    def out_copies(j):
        span = pl.ds(j * BLOCK, BLOCK)
        return (
            pltpu.make_async_copy(kbuf.at[span], nk_hbm.at[span], out_sem.at[0]),
            pltpu.make_async_copy(vbuf.at[span], nv_hbm.at[span], out_sem.at[1]),
        )

    small = [
        pltpu.make_async_copy(src, dst, x_sem.at[i])
        for i, (src, dst) in enumerate(((pos_hbm, pos), (x_hbm, x_ref), (gain_hbm, gain_ref)))
    ]
    for copy in small:
        copy.start()
    n_w = heads + 2 * kvs
    ahead = FIRST + n_w
    for n in range(n_w // 2):
        w_copy(n).start()

    lane = lax.broadcasted_iota(jnp.int32, (1, LANES), 1).astype(F32)
    freq = jnp.exp2(lane * (-math.log2(ROPE_THETA) / LANES))

    for copy in small:
        copy.wait()
    for n in range(n_w // 2, n_w):
        w_copy(n).start()
    for j in range(FIRST):
        for copy in in_copies(j):
            copy.start()

    def angle_row(b, carry):
        ang_s[pl.ds(b, 1), :] = freq * pos[b].astype(F32)
        return carry

    lax.fori_loop(0, rows, angle_row, 0, unroll=8)
    angles = ang_s[...]
    cos_t, sin_t = jnp.cos(angles), jnp.sin(angles)
    normed = rms_norm(x_ref[...], gain_ref[...])

    for n in range(n_w):
        w_copy(n).wait()
        for copy in in_copies(FIRST + n):
            copy.start()
        lin = jnp.dot(normed, wbuf[n], preferred_element_type=F32)
        first, second = lin[:, :LANES], lin[:, LANES:]
        if not kvs <= n < 2 * kvs:
            first, second = first * cos_t - second * sin_t, second * cos_t + first * sin_t
        if n >= 2 * kvs:
            h = n - 2 * kvs
            q_s[pl.ds(h, rows, stride=qrows), :] = first
            q_s[pl.ds(heads + h, rows, stride=qrows), :] = second
        else:
            dst, kv = (kn_s, n) if n < kvs else (vn_s, n - kvs)
            for rep in range(16 // per_slot):
                dst[pl.ds(rep * per_slot + kv, rows, stride=16), :] = first
                dst[pl.ds(rep * per_slot + kvs + kv, rows, stride=16), :] = second

    row = lax.broadcasted_iota(jnp.int32, (qrows, LANES), 0)
    col = lax.broadcasted_iota(jnp.int32, (qrows, LANES), 1)
    half_of_col = (col // kvs) % 2
    fits = (half_of_col == row // heads) & (col % kvs == (row % heads) // group)
    slot_of_col = jnp.where(fits, col // per_slot, FAR)
    low_half = half_of_col == 0
    patch_row = lax.broadcasted_iota(jnp.int32, (16, LANES), 0) // per_slot
    scale = 1.0 / math.sqrt(head_dim)

    def block_step(j, carry):
        @pl.when(j + ahead < n_blocks)
        def _():
            for copy in in_copies(j + ahead):
                copy.start()

        for copy in in_copies(j):
            copy.wait()
        for i in range(BLOCK):
            b = j * BLOCK + i
            local = lax.rem(pos[b], slots) - base
            owned = (local >= 0) & (local < local_slots)
            safe = jnp.where(owned, local, 0)
            hit = jnp.where(owned, lax.rem(safe, 16 // per_slot), -1)
            span = pl.ds(pl.multiple_of((safe // (16 // per_slot)) * 16, 16), 16)
            for buf, new in ((kbuf, kn_s), (vbuf, vn_s)):
                old = buf[b, span, :].astype(F32)
                fresh = new[pl.ds(pl.multiple_of(b * 16, 16), 16), :]
                buf[b, span, :] = jnp.where(patch_row == hit, fresh, old).astype(BF16)
        scores = []
        for i in range(BLOCK):
            b = j * BLOCK + i
            q = q_s[pl.ds(pl.multiple_of(b * qrows, qrows), qrows), :].astype(BF16)
            scores.append(
                lax.dot_general(q, kbuf[b], (((1,), (1,)), ((), ())), preferred_element_type=F32)
            )
        probs = []
        for i in range(BLOCK):
            b = j * BLOCK + i
            limit = jnp.where(pos[b] >= slots - 1, FAR // 2, pos[b]) - base
            parts = []
            for t in range(slices):
                own = scores[i][:, t * LANES : (t + 1) * LANES]
                other = pltpu.roll(own, heads, 0)
                other = jnp.where(
                    low_half, pltpu.roll(other, LANES - kvs, 1), pltpu.roll(other, kvs, 1)
                )
                ok = slot_of_col <= limit - t * (LANES // per_slot)
                parts.append(jnp.where(ok, (own + other) * scale, -jnp.inf))
            top = functools.reduce(jnp.maximum, parts)
            top = jnp.max(top, axis=1, keepdims=True)
            floor = jnp.where(top == -jnp.inf, 0.0, top)
            parts = [jnp.exp(part - floor) for part in parts]
            total = jnp.sum(functools.reduce(jnp.add, parts), axis=1, keepdims=True)
            span = pl.ds(pl.multiple_of(b * qrows, qrows), qrows)
            m_s[span, :] = jnp.broadcast_to(top, (qrows, LANES))
            l_s[span, :] = jnp.broadcast_to(total, (qrows, LANES))
            probs.append(jnp.concatenate([part.astype(BF16) for part in parts], axis=1))
        for i in range(BLOCK):
            b = j * BLOCK + i
            span = pl.ds(pl.multiple_of(b * qrows, qrows), qrows)
            o_s[span, :] = jnp.dot(probs[i], vbuf[b], preferred_element_type=F32)
        for copy in out_copies(j):
            copy.start()
        return carry

    lax.fori_loop(0, n_blocks, block_step, 0)

    left = lax.broadcasted_iota(jnp.int32, (rows, LANES), 1) < LANES // 2
    for h in range(heads):
        part_ref[h, 0] = o_s[pl.ds(h, rows, stride=qrows), :]
        part_ref[h, 1] = o_s[pl.ds(heads + h, rows, stride=qrows), :]
        part_ref[h, 2] = jnp.where(
            left, m_s[pl.ds(h, rows, stride=qrows), :], l_s[pl.ds(h, rows, stride=qrows), :]
        )
    for j in range(n_blocks):
        for copy in out_copies(j):
            copy.wait()


def attention(positions, tokens, gain, w_q, w_k, w_v, rows_k, rows_v):
    rows, width = tokens.shape
    head_dim = 2 * LANES
    heads = w_q.shape[1] // head_dim
    kvs = w_k.shape[1] // head_dim
    qrows = 2 * heads
    vmem = pl.BlockSpec(memory_space=pltpu.VMEM)
    hbm = pl.BlockSpec(memory_space=pltpu.HBM)
    n_blocks = rows // BLOCK
    return pl.pallas_call(
        attention_kernel,
        out_shape=(
            pltpu.VMEM((heads, 3, rows, LANES), F32),
            jax.ShapeDtypeStruct(rows_k.shape, BF16),
            jax.ShapeDtypeStruct(rows_v.shape, BF16),
        ),
        in_specs=[hbm] * 8,
        out_specs=(vmem, hbm, hbm),
        scratch_shapes=[
            pltpu.VMEM((heads + 2 * kvs, width, head_dim), BF16),
            pltpu.VMEM(rows_k.shape, BF16),
            pltpu.VMEM(rows_v.shape, BF16),
            pltpu.VMEM((rows * qrows, LANES), F32),
            pltpu.VMEM((rows * 16, LANES), F32),
            pltpu.VMEM((rows * 16, LANES), F32),
            pltpu.VMEM((rows, LANES), F32),
            pltpu.VMEM((rows * qrows, LANES), F32),
            pltpu.VMEM((rows * qrows, LANES), F32),
            pltpu.VMEM((rows * qrows, LANES), F32),
            pltpu.SMEM((rows,), jnp.int32),
            pltpu.VMEM(tokens.shape, BF16),
            pltpu.VMEM(gain.shape, BF16),
            pltpu.SemaphoreType.DMA((heads + 2 * kvs,)),
            pltpu.SemaphoreType.DMA((n_blocks,)),
            pltpu.SemaphoreType.DMA((n_blocks,)),
            pltpu.SemaphoreType.DMA((2,)),
            pltpu.SemaphoreType.DMA((3,)),
        ],
        compiler_params=pltpu.CompilerParams(vmem_limit_bytes=52 << 20),
        name="attention_part",
    )(*(pltpu.with_memory_space_constraint(v, pltpu.HBM) for v in (positions, tokens, gain)), w_q, w_k, w_v, rows_k, rows_v)


CHUNKS = 5
MESH = pl.DeviceIdType.MESH


def combine(mine, theirs):
    left = lax.broadcasted_iota(jnp.int32, mine[2].shape, mine[2].ndim - 1) < LANES // 2
    axis = mine[2].ndim - 1

    def unpack(stats):
        turned = pltpu.roll(stats, LANES // 2, axis)
        return jnp.where(left, stats, turned), jnp.where(left, turned, stats)

    (m_a, l_a), (m_b, l_b) = unpack(mine[2]), unpack(theirs[2])
    top = jnp.maximum(m_a, m_b)
    f_a = jnp.where(m_a == -jnp.inf, 0.0, jnp.exp(m_a - top))
    f_b = jnp.where(m_b == -jnp.inf, 0.0, jnp.exp(m_b - top))
    return mine[0] * f_a + theirs[0] * f_b, mine[1] * f_a + theirs[1] * f_b, top, l_a * f_a + l_b * f_b


def tail_kernel(
    part_ref, x_ref, gain_ref, wo_hbm, wg_hbm, wu_hbm, wd_hbm,
    out_ref,
    wo, wg, wu, wd, rd, sx, rx, po, ro, so, yo, hb, act, pm, rm, sm, ym, ob,
    w_sem, g_sem, u_sem, d_sem, send_sem, recv_sem,
):
    heads, _, rows, _ = part_ref.shape
    width = x_ref.shape[1]
    mine_h = heads // 2
    half, quarter = rows // 2, rows // 4
    sp, tp = lax.axis_index("sp"), lax.axis_index("tp")
    x, k = sp // 2, lax.rem(sp, 2)
    d_dev, x_dev, y_dev = {"sp": x * 2 + 1 - k}, {"sp": (1 - x) * 2 + k}, {"tp": 1 - tp}
    o_rows, n_gate = wo.shape[0], wg.shape[0]
    g_cols = wg.shape[2]
    m_cols = n_gate * g_cols
    d_rows = g_cols
    n_down = wd.shape[0] // d_rows
    span = width // CHUNKS

    barrier = pltpu.get_barrier_semaphore()
    for dev in (d_dev, x_dev, y_dev):
        pl.semaphore_signal(barrier, inc=1, device_id=dev, device_id_type=MESH)

    o_copy = pltpu.make_async_copy(wo_hbm.at[pl.ds(k * o_rows, o_rows)], wo, w_sem)
    g_copies, d_copies = [], []
    for c in range(n_gate):
        at = pl.ds(pl.multiple_of(k * m_cols + c * g_cols, LANES), g_cols)
        g_copies.append(pltpu.make_async_copy(wg_hbm.at[:, at], wg.at[c], g_sem.at[c]))
        g_copies.append(pltpu.make_async_copy(wu_hbm.at[:, at], wu.at[c], u_sem.at[c]))
    for c in range(n_down):
        at = pl.ds(pl.multiple_of(k * m_cols + c * d_rows, LANES), d_rows)
        d_copies.append(pltpu.make_async_copy(wd_hbm.at[at], wd.at[pl.ds(c * d_rows, d_rows)], d_sem.at[c]))
    queue = iter(g_copies + d_copies)

    def fetch(n):
        for copy in itertools.islice(queue, n):
            copy.start()

    o_copy.start()
    pl.semaphore_wait(barrier, 3)

    counter = [0]

    def remote(src, dst, dev):
        n = counter[0]
        counter[0] += 1
        return pltpu.make_async_remote_copy(
            src_ref=src, dst_ref=dst, send_sem=send_sem.at[n], recv_sem=recv_sem.at[n],
            device_id=dev, device_id_type=MESH,
        )

    far_rows, near_rows = pl.ds((1 - x) * half, half), pl.ds(x * half, half)
    swap = remote(part_ref.at[pl.ds((1 - k) * mine_h, mine_h)], rd, d_dev)
    swap.start()
    fetch(2)
    swap.wait_recv()
    my_heads = pl.ds(k * mine_h, mine_h)

    def chip_part(at):
        return combine(
            [part_ref[my_heads, i, at] for i in range(3)], [rd[:, i, at] for i in range(3)]
        )

    left = lax.broadcasted_iota(jnp.int32, (mine_h, half, LANES), 2) < LANES // 2
    o_a, o_b, m, l = chip_part(far_rows)
    sx[:, 0], sx[:, 1], sx[:, 2] = o_a, o_b, jnp.where(left, m, l)
    cross = remote(sx, rx, x_dev)
    cross.start()
    fetch(8)
    o_a, o_b, m, l = chip_part(near_rows)
    cross.wait_recv()
    o_a, o_b, _, l = combine([o_a, o_b, jnp.where(left, m, l)], [rx[:, i] for i in range(3)])
    o_a, o_b = (o_a / l).astype(BF16), (o_b / l).astype(BF16)
    attended = jnp.concatenate([v[h] for h in range(mine_h) for v in (o_a, o_b)], axis=-1)

    own, other = pl.ds(k * quarter, quarter), pl.ds((1 - k) * quarter, quarter)
    my_rows = pl.ds(pl.multiple_of(x * half + k * quarter, quarter), quarter)
    x_peer_rows = pl.ds(pl.multiple_of((1 - x) * half + k * quarter, quarter), quarter)
    cols = [pl.ds(c * span, span) for c in range(CHUNKS)]

    def staged(dot, swap, cross, *rest):
        for c in range(CHUNKS + 2):
            if c < CHUNKS:
                dot(c)
            if c >= 2:
                swap(c - 2)
        for c in range(CHUNKS):
            cross(c)
        for c in range(CHUNKS + len(rest) - 1):
            for s, stage in enumerate(rest):
                if 0 <= c - s < CHUNKS:
                    stage(c - s)

    swaps = [remote(po.at[other, c], ro.at[:, c], d_dev) for c in cols]
    crosses = [remote(so.at[:, c], yo.at[:, c], y_dev) for c in cols]
    gathers = [remote(hb.at[own, c], hb.at[own, c], d_dev) for c in cols]
    o_copy.wait()

    def o_dot(c):
        po[:, cols[c]] = jnp.dot(attended, wo[:, cols[c]], preferred_element_type=F32)
        swaps[c].start()

    def o_swap(c):
        swaps[c].wait_recv()
        so[:, cols[c]] = po[own, cols[c]] + ro[:, cols[c]]
        crosses[c].start()
        fetch(3)

    def o_cross(c):
        crosses[c].wait_recv()
        total = so[:, cols[c]] + yo[:, cols[c]]
        hb[own, cols[c]] = (x_ref[my_rows, cols[c]].astype(F32) + total).astype(BF16).astype(F32)
        gathers[c].start()

    def o_gather(c):
        gathers[c].wait_recv()

    staged(o_dot, o_swap, o_cross, o_gather)
    fetch(len(g_copies) + len(d_copies))

    normed = rms_norm(hb[...], gain_ref[...])
    for c in range(n_gate):
        g_copies[2 * c].wait()
        g_copies[2 * c + 1].wait()
        gate = jnp.dot(normed, wg[c], preferred_element_type=F32)
        up = jnp.dot(normed, wu[c], preferred_element_type=F32)
        act[:, c * g_cols : (c + 1) * g_cols] = (jax.nn.silu(gate) * up).astype(BF16)
    for copy in d_copies:
        copy.wait()

    swaps_m = [remote(pm.at[other, c], rm.at[:, c], d_dev) for c in cols]
    crosses_m = [remote(sm.at[:, c], ym.at[:, c], y_dev) for c in cols]
    to_core = [remote(ob.at[my_rows, c], ob.at[my_rows, c], d_dev) for c in cols]
    to_x = [remote(ob.at[my_rows, c], ob.at[my_rows, c], x_dev) for c in cols]
    onward = [remote(ob.at[x_peer_rows, c], ob.at[x_peer_rows, c], d_dev) for c in cols]

    def m_dot(c):
        pm[:, cols[c]] = jnp.dot(act[...], wd[:, cols[c]], preferred_element_type=F32)
        swaps_m[c].start()

    def m_swap(c):
        swaps_m[c].wait_recv()
        sm[:, cols[c]] = pm[own, cols[c]] + rm[:, cols[c]]
        crosses_m[c].start()

    def m_cross(c):
        crosses_m[c].wait_recv()
        total = sm[:, cols[c]] + ym[:, cols[c]]
        ob[my_rows, cols[c]] = (hb[own, cols[c]] + total).astype(BF16).astype(F32)
        to_x[c].start()
        to_core[c].start()

    def m_gather(c):
        to_x[c].wait_recv()
        onward[c].start()

    def m_last(c):
        to_core[c].wait_recv()
        onward[c].wait_recv()
        out_ref[:, cols[c]] = ob[:, cols[c]].astype(BF16)

    staged(m_dot, m_swap, m_cross, m_gather, m_last)
    for copy in [swap, cross, *swaps, *crosses, *gathers, *swaps_m, *crosses_m, *to_core, *to_x, *onward]:
        copy.wait_send()


def tail(part, tokens, gain, w_o, w_gate, w_up, w_down):
    heads, _, rows, _ = part.shape
    width = tokens.shape[1]
    half, quarter = rows // 2, rows // 4
    cut = w_gate.shape[1] // 2
    n_gate = cut // 256
    vmem = pl.BlockSpec(memory_space=pltpu.VMEM)
    hbm = pl.BlockSpec(memory_space=pltpu.HBM)
    flat = lambda n: pltpu.VMEM((n, width), F32)
    stats = lambda n: pltpu.VMEM((heads // 2, 3, n, LANES), F32)
    n_remote = 2 + 8 * CHUNKS
    return pl.pallas_call(
        tail_kernel,
        out_shape=pltpu.VMEM(tokens.shape, BF16),
        in_specs=[vmem, vmem, vmem] + [hbm] * 4,
        out_specs=vmem,
        scratch_shapes=[
            pltpu.VMEM((w_o.shape[0] // 2, width), BF16),
            pltpu.VMEM((n_gate, width, 256), BF16),
            pltpu.VMEM((n_gate, width, 256), BF16),
            pltpu.VMEM((cut, width), BF16),
            stats(rows), stats(half), stats(half),
            flat(half), flat(quarter), flat(quarter), flat(quarter), flat(half),
            pltpu.VMEM((half, cut), BF16),
            flat(half), flat(quarter), flat(quarter), flat(quarter), flat(rows),
            pltpu.SemaphoreType.DMA,
            pltpu.SemaphoreType.DMA((n_gate,)),
            pltpu.SemaphoreType.DMA((n_gate,)),
            pltpu.SemaphoreType.DMA((n_gate,)),
            pltpu.SemaphoreType.DMA((n_remote,)),
            pltpu.SemaphoreType.DMA((n_remote,)),
        ],
        compiler_params=pltpu.CompilerParams(
            vmem_limit_bytes=50 << 20, collective_id=0, has_side_effects=True
        ),
        name="tail",
    )(part, tokens, gain, w_o, w_gate, w_up, w_down)


def to_rows(cache):
    b, s, kv, d = cache.shape
    return cache.reshape(b, s, kv, d // LANES, LANES).transpose(0, 1, 3, 2, 4).reshape(b, -1, LANES)


def from_rows(rows, shape):
    b, s, kv, d = shape
    return rows.reshape(b, s, d // LANES, kv, LANES).transpose(0, 1, 3, 2, 4).reshape(shape)


def solution(mesh):
    cache_spec = P("dp", "sp", "tp", None)
    row_spec = P("dp", None)
    col_spec = P(None, "tp")
    in_specs = (row_spec, P("dp"), cache_spec, cache_spec, P(None), col_spec, col_spec, col_spec, P("tp", None), P(None), col_spec, col_spec, P("tp", None))
    out_specs = (row_spec, cache_spec, cache_spec)

    def local_step(tokens, positions, cache_k, cache_v, attn_gain, w_q, w_k, w_v, w_o, mlp_gain, w_gate, w_up, w_down):
        part, rows_k, rows_v = attention(
            positions, tokens, attn_gain, w_q, w_k, w_v, to_rows(cache_k), to_rows(cache_v)
        )
        new_k = from_rows(rows_k, cache_k.shape)
        new_v = from_rows(rows_v, cache_v.shape)
        layer_out = tail(part, tokens, mlp_gain, w_o, w_gate, w_up, w_down)
        return layer_out, new_k, new_v

    return jax.shard_map(local_step, mesh=mesh, in_specs=in_specs, out_specs=out_specs, check_vma=False)
```

```python
import functools
import itertools
import math

import jax
import jax.numpy as jnp
from jax import lax
from jax.experimental import pallas as pl
from jax.experimental.pallas import tpu as pltpu
from jax.sharding import PartitionSpec as P

NORM_EPS = 1e-5
ROPE_THETA = 10000.0
LANES = 128
F32 = jnp.float32
BF16 = jnp.bfloat16
FAR = 1 << 28
BLOCK = 4
AHEAD = 3
FIRST = 4
SLOTS = 22
LAYER_VMEM = 35
CHUNKS = 5
GROUPS = 4
MESH = pl.DeviceIdType.MESH


def rms_norm(values, gain):
    wide = values.astype(F32)
    inv_rms = lax.rsqrt(jnp.mean(wide * wide, axis=-1, keepdims=True) + NORM_EPS)
    return (wide * inv_rms * gain.astype(F32)).astype(BF16)


def first_kernel(
    pos_hbm, x_hbm, gain_hbm, wq_hbm, wk_hbm, wv_hbm, ck_hbm, cv_hbm,
    part_ref, nk_hbm, nv_hbm, q_s, kx_s, vx_s, tiles,
    wbuf, kn_s, vn_s, kbuf, vbuf, ang_s, o_s, m_s, l_s,
    pos, x_ref, gain_ref, w_sem, k_sem, v_sem, out_sem, x_sem, old, t_sem,
):
    rows = x_ref.shape[0]
    head_dim = 2 * LANES
    heads = wq_hbm.shape[1] // head_dim
    kvs = wk_hbm.shape[1] // head_dim
    group = heads // kvs
    per_slot = 2 * kvs
    qrows = 2 * heads
    key_rows = ck_hbm.shape[1]
    local_slots = key_rows // per_slot
    slots = local_slots * lax.axis_size("sp")
    slices = key_rows // LANES
    half = rows // 2
    n_blocks = half // BLOCK
    start = (1 - lax.axis_index("sp") // 2) * half
    base = lax.axis_index("sp") * local_slots

    def w_copy(n):
        src, col = (
            (wk_hbm, n) if n < kvs else (wv_hbm, n - kvs) if n < 2 * kvs else (wq_hbm, n - 2 * kvs)
        )
        return pltpu.make_async_copy(src.at[:, pl.ds(col * head_dim, head_dim)], wbuf.at[n], w_sem.at[n])

    def in_copies(j):
        far, here = pl.ds(start + j * BLOCK, BLOCK), pl.ds(j * BLOCK, BLOCK)
        return (
            pltpu.make_async_copy(ck_hbm.at[far], kbuf.at[here], k_sem.at[j]),
            pltpu.make_async_copy(cv_hbm.at[far], vbuf.at[here], v_sem.at[j]),
        )

    def out_copies(j):
        far, here = pl.ds(start + j * BLOCK, BLOCK), pl.ds(j * BLOCK, BLOCK)
        return (
            pltpu.make_async_copy(kbuf.at[here], nk_hbm.at[far], out_sem.at[0]),
            pltpu.make_async_copy(vbuf.at[here], nv_hbm.at[far], out_sem.at[1]),
        )

    small = [
        pltpu.make_async_copy(src, dst, x_sem.at[i])
        for i, (src, dst) in enumerate(((pos_hbm, pos), (x_hbm, x_ref), (gain_hbm, gain_ref)))
    ]
    for copy in small:
        copy.start()
    n_w = heads + 2 * kvs
    for n in range(n_w // 2):
        w_copy(n).start()

    lane = lax.broadcasted_iota(jnp.int32, (1, LANES), 1).astype(F32)
    freq = jnp.exp2(lane * (-math.log2(ROPE_THETA) / LANES))

    for copy in small:
        copy.wait()
    for n in range(n_w // 2, n_w):
        w_copy(n).start()
    for j in range(FIRST):
        for copy in in_copies(j):
            copy.start()

    per_tile = 16 // per_slot
    near = lax.axis_index("sp") // 2 * half
    tile_row = lax.broadcasted_iota(jnp.int32, (16, LANES), 0) // per_slot

    def target(b):
        local = lax.rem(pos[b], slots) - base
        owned = (local >= 0) & (local < local_slots)
        safe = jnp.where(owned, local, 0)
        hit = jnp.where(owned, lax.rem(safe, per_tile), -1)
        return hit, pl.ds(pl.multiple_of((safe // per_tile) * 16, 16), 16)

    def tile_copies(n):
        at = target(near + n)[1]
        return (
            pltpu.make_async_copy(ck_hbm.at[near + n, at], old.at[0, n], t_sem.at[0]),
            pltpu.make_async_copy(cv_hbm.at[near + n, at], old.at[1, n], t_sem.at[1]),
        )

    def start_tile(n, carry):
        for copy in tile_copies(n):
            copy.start()
        return carry

    def wait_tile(n, carry):
        for copy in tile_copies(n):
            copy.wait()
        return carry

    def make_tile(n, carry):
        hit = target(near + n)[0]
        for i, new in enumerate((kn_s, vn_s)):
            fresh = new[pl.ds(pl.multiple_of((near + n) * 16, 16), 16), :]
            tiles[i, n] = jnp.where(tile_row == hit, fresh, old[i, n].astype(F32)).astype(BF16)
        return carry

    lax.fori_loop(0, half, start_tile, 0, unroll=4)

    def angle_row(b, carry):
        ang_s[pl.ds(b, 1), :] = freq * pos[b].astype(F32)
        return carry

    lax.fori_loop(0, rows, angle_row, 0, unroll=8)
    angles = ang_s[...]
    cos_t, sin_t = jnp.cos(angles), jnp.sin(angles)
    normed = rms_norm(x_ref[...], gain_ref[...])

    for n in range(n_w):
        w_copy(n).wait()
        if FIRST + n < n_blocks:
            for copy in in_copies(FIRST + n):
                copy.start()
        lin = jnp.dot(normed, wbuf[n], preferred_element_type=F32)
        first, second = lin[:, :LANES], lin[:, LANES:]
        if not kvs <= n < 2 * kvs:
            first, second = first * cos_t - second * sin_t, second * cos_t + first * sin_t
        first, second = first.astype(BF16).astype(F32), second.astype(BF16).astype(F32)
        if n >= 2 * kvs:
            h = n - 2 * kvs
            q_s[pl.ds(h, rows, stride=qrows), :] = first
            q_s[pl.ds(heads + h, rows, stride=qrows), :] = second
        else:
            dst, tile, kv = (kn_s, kx_s, n) if n < kvs else (vn_s, vx_s, n - kvs)
            for rep in range(16 // per_slot):
                dst[pl.ds(rep * per_slot + kv, rows, stride=16), :] = first
                dst[pl.ds(rep * per_slot + kvs + kv, rows, stride=16), :] = second
            for g in range(group):
                tile[pl.ds(kv * group + g, rows, stride=qrows), :] = first
                tile[pl.ds(heads + kv * group + g, rows, stride=qrows), :] = second

    row = lax.broadcasted_iota(jnp.int32, (qrows, LANES), 0)
    col = lax.broadcasted_iota(jnp.int32, (qrows, LANES), 1)
    half_of_col = (col // kvs) % 2
    fits = (half_of_col == row // heads) & (col % kvs == (row % heads) // group)
    slot_of_col = jnp.where(fits, col // per_slot, FAR)
    low_half = half_of_col == 0
    patch_row = lax.broadcasted_iota(jnp.int32, (16, LANES), 0) // per_slot
    scale = 1.0 / math.sqrt(head_dim)

    def block_step(j, carry):
        for copy in in_copies(j):
            copy.wait()
        for i in range(BLOCK):
            n = j * BLOCK + i
            b = start + n
            local = lax.rem(pos[b], slots) - base
            owned = (local >= 0) & (local < local_slots)
            safe = jnp.where(owned, local, 0)
            hit = jnp.where(owned, lax.rem(safe, 16 // per_slot), -1)
            span = pl.ds(pl.multiple_of((safe // (16 // per_slot)) * 16, 16), 16)
            for buf, new in ((kbuf, kn_s), (vbuf, vn_s)):
                old = buf[n, span, :].astype(F32)
                fresh = new[pl.ds(pl.multiple_of(b * 16, 16), 16), :]
                buf[n, span, :] = jnp.where(patch_row == hit, fresh, old).astype(BF16)
        scores = []
        for i in range(BLOCK):
            b = start + j * BLOCK + i
            q = q_s[pl.ds(pl.multiple_of(b * qrows, qrows), qrows), :].astype(BF16)
            scores.append(
                lax.dot_general(q, kbuf[j * BLOCK + i], (((1,), (1,)), ((), ())), preferred_element_type=F32)
            )
        probs = []
        for i in range(BLOCK):
            n = j * BLOCK + i
            p = pos[start + n]
            limit = jnp.where(p >= slots - 1, FAR // 2, p) - base
            parts = []
            for t in range(slices):
                own = scores[i][:, t * LANES : (t + 1) * LANES]
                other = pltpu.roll(own, heads, 0)
                other = jnp.where(
                    low_half, pltpu.roll(other, LANES - kvs, 1), pltpu.roll(other, kvs, 1)
                )
                ok = slot_of_col <= limit - t * (LANES // per_slot)
                parts.append(jnp.where(ok, (own + other) * scale, -jnp.inf))
            top = functools.reduce(jnp.maximum, parts)
            top = jnp.max(top, axis=1, keepdims=True)
            floor = jnp.where(top == -jnp.inf, 0.0, top)
            parts = [jnp.exp(part - floor) for part in parts]
            total = jnp.sum(functools.reduce(jnp.add, parts), axis=1, keepdims=True)
            span = pl.ds(pl.multiple_of(n * qrows, qrows), qrows)
            m_s[span, :] = jnp.broadcast_to(top, (qrows, LANES))
            l_s[span, :] = jnp.broadcast_to(total, (qrows, LANES))
            probs.append(jnp.concatenate([part.astype(BF16) for part in parts], axis=1))
        for i in range(BLOCK):
            n = j * BLOCK + i
            span = pl.ds(pl.multiple_of(n * qrows, qrows), qrows)
            o_s[span, :] = jnp.dot(probs[i], vbuf[n], preferred_element_type=F32)
        for copy in out_copies(j):
            copy.start()
        return carry

    lax.fori_loop(0, n_blocks, block_step, 0)

    lax.fori_loop(0, half, wait_tile, 0, unroll=8)
    lax.fori_loop(0, half, make_tile, 0, unroll=4)
    left = lax.broadcasted_iota(jnp.int32, (half, LANES), 1) < LANES // 2
    for h in range(heads):
        lo, hi = pl.ds(h, half, stride=qrows), pl.ds(heads + h, half, stride=qrows)
        part_ref[h, 0], part_ref[h, 1] = o_s[lo, :], o_s[hi, :]
        part_ref[h, 2] = jnp.where(left, m_s[lo, :], l_s[lo, :])
    for j in range(n_blocks):
        for copy in out_copies(j):
            copy.wait()


def first_half(positions, tokens, gain, w_q, w_k, w_v, rows_k, rows_v):
    rows, width = tokens.shape
    head_dim = 2 * LANES
    heads = w_q.shape[1] // head_dim
    kvs = w_k.shape[1] // head_dim
    qrows = 2 * heads
    vmem = pl.BlockSpec(memory_space=pltpu.VMEM)
    hbm = pl.BlockSpec(memory_space=pltpu.HBM)
    n_blocks = rows // 2 // BLOCK
    tile = lambda n: pltpu.VMEM((rows * n, LANES), F32)
    return pl.pallas_call(
        first_kernel,
        out_shape=(
            pltpu.VMEM((heads, 3, rows // 2, LANES), F32),
            jax.ShapeDtypeStruct(rows_k.shape, BF16),
            jax.ShapeDtypeStruct(rows_v.shape, BF16),
            tile(qrows), tile(qrows), tile(qrows),
            pltpu.VMEM((2, rows // 2, 16, LANES), BF16),
        ),
        in_specs=[hbm] * 8,
        out_specs=(vmem, hbm, hbm) + (vmem,) * 4,
        scratch_shapes=[
            pltpu.VMEM((heads + 2 * kvs, width, head_dim), BF16),
            tile(16), tile(16),
            pltpu.VMEM((rows // 2, *rows_k.shape[1:]), BF16),
            pltpu.VMEM((rows // 2, *rows_v.shape[1:]), BF16),
            tile(1),
            pltpu.VMEM((rows // 2 * qrows, LANES), F32),
            pltpu.VMEM((rows // 2 * qrows, LANES), F32),
            pltpu.VMEM((rows // 2 * qrows, LANES), F32),
            pltpu.SMEM((rows,), jnp.int32),
            pltpu.VMEM(tokens.shape, BF16),
            pltpu.VMEM(gain.shape, BF16),
            pltpu.SemaphoreType.DMA((heads + 2 * kvs,)),
            pltpu.SemaphoreType.DMA((n_blocks,)),
            pltpu.SemaphoreType.DMA((n_blocks,)),
            pltpu.SemaphoreType.DMA((2,)),
            pltpu.SemaphoreType.DMA((3,)),
            pltpu.VMEM((2, rows // 2, 16, LANES), BF16),
            pltpu.SemaphoreType.DMA((2,)),
        ],
        compiler_params=pltpu.CompilerParams(vmem_limit_bytes=36 << 20),
        name="first",
    )(*(pltpu.with_memory_space_constraint(v, pltpu.HBM) for v in (positions, tokens, gain, w_q, w_k, w_v, rows_k, rows_v)))


def combine(mine, theirs):
    left = lax.broadcasted_iota(jnp.int32, mine[2].shape, mine[2].ndim - 1) < LANES // 2
    axis = mine[2].ndim - 1

    def unpack(stats):
        turned = pltpu.roll(stats, LANES // 2, axis)
        return jnp.where(left, stats, turned), jnp.where(left, turned, stats)

    (m_a, l_a), (m_b, l_b) = unpack(mine[2]), unpack(theirs[2])
    top = jnp.maximum(m_a, m_b)
    f_a = jnp.where(m_a == -jnp.inf, 0.0, jnp.exp(m_a - top))
    f_b = jnp.where(m_b == -jnp.inf, 0.0, jnp.exp(m_b - top))
    return mine[0] * f_a + theirs[0] * f_b, mine[1] * f_a + theirs[1] * f_b, top, l_a * f_a + l_b * f_b


def layer_kernel(
    kv_heads, pos_hbm, x_hbm, gm_hbm, wo_hbm, wg_hbm, wu_hbm, wd_hbm, ck_hbm, cv_hbm,
    far_ref, q_s, kx_s, vx_s,
    out_ref, kbuf, vbuf,
    ring, o_s, m_s, l_s, part, rd, sx, rx,
    po, ro, so, yo, hb, act, pm, rm, sm, ym, ob,
    pos, x_ref, gm_ref,
    small_sem, k_sem, v_sem, o_sem, c_sem, send_sem, recv_sem,
):
    rows, width = x_ref.shape
    head_dim = ring.shape[2]
    heads = far_ref.shape[0]
    kvs = kv_heads
    group = heads // kvs
    per_slot, qrows = 2 * kvs, 2 * heads
    key_rows = ck_hbm.shape[1]
    local_slots = key_rows // per_slot
    slots = local_slots * lax.axis_size("sp")
    slices = key_rows // LANES
    n_blocks = rows // 2 // BLOCK
    mine_h = heads // 2
    half, quarter = rows // 2, rows // 4
    sp, tp = lax.axis_index("sp"), lax.axis_index("tp")
    x, k = sp // 2, lax.rem(sp, 2)
    d_dev, x_dev, y_dev = {"sp": x * 2 + 1 - k}, {"sp": (1 - x) * 2 + k}, {"tp": 1 - tp}
    base = sp * local_slots
    m_cols = act.shape[1]
    span = width // CHUNKS

    barrier = pltpu.get_barrier_semaphore()
    for dev in (d_dev, x_dev, y_dev):
        pl.semaphore_signal(barrier, inc=1, device_id=dev, device_id_type=MESH)

    counter = [0]

    def remote(src, dst, dev):
        n = counter[0]
        counter[0] += 1
        return pltpu.make_async_remote_copy(
            src_ref=src, dst_ref=dst, send_sem=send_sem.at[n], recv_sem=recv_sem.at[n],
            device_id=dev, device_id_type=MESH,
        )

    def in_copies(j):
        near, here = pl.ds(x * half + j * BLOCK, BLOCK), pl.ds(j * BLOCK, BLOCK)
        return (
            pltpu.make_async_copy(ck_hbm.at[near], kbuf.at[here], k_sem.at[j]),
            pltpu.make_async_copy(cv_hbm.at[near], vbuf.at[here], v_sem.at[j]),
        )

    small = [
        pltpu.make_async_copy(src, dst, small_sem.at[i])
        for i, (src, dst) in enumerate(
            ((pos_hbm, pos), (x_hbm, x_ref), (gm_hbm, gm_ref))
        )
    ]
    for copy in small:
        copy.start()
    for j in range(AHEAD):
        for copy in in_copies(j):
            copy.start()

    n_w = 0
    o_rows = mine_h * head_dim
    per_o = width // o_rows
    o_copies = [
        pltpu.make_async_copy(
            wo_hbm.at[pl.ds(k * o_rows, o_rows), pl.ds(c * head_dim, head_dim)],
            ring.at[n_w + c // per_o, pl.ds((c % per_o) * o_rows, o_rows)],
            o_sem.at[c],
        )
        for c in range(width // head_dim)
    ]
    n_gate = m_cols // head_dim
    ring_at = lambda i: (n_w + 2 + i) % SLOTS
    chunks = []
    for c in range(n_gate):
        at = pl.ds(pl.multiple_of(k * m_cols + c * head_dim, LANES), head_dim)
        chunks += [wg_hbm.at[:, at], wu_hbm.at[:, at]]
    for c in range(width // head_dim):
        chunks.append(wd_hbm.at[pl.ds(pl.multiple_of(k * m_cols, LANES), m_cols), pl.ds(c * head_dim, head_dim)])
    chunks = [
        pltpu.make_async_copy(src, ring.at[ring_at(i)], c_sem.at[i]) for i, src in enumerate(chunks)
    ]
    queue = iter(chunks)

    def fetch(n):
        for copy in itertools.islice(queue, n):
            copy.start()

    for copy in small:
        copy.wait()
    pl.semaphore_wait(barrier, 3)

    row = lax.broadcasted_iota(jnp.int32, (qrows, LANES), 0)
    col = lax.broadcasted_iota(jnp.int32, (qrows, LANES), 1)
    half_of_col = (col // kvs) % 2
    fits = (half_of_col == row // heads) & (col % kvs == (row % heads) // group)
    slot_of_col = jnp.where(fits, col // per_slot, FAR)
    low_half = half_of_col == 0
    scale = 1.0 / math.sqrt(head_dim)

    def block_step(j, carry):
        @pl.when(j + AHEAD < n_blocks)
        def _():
            for copy in in_copies(j + AHEAD):
                copy.start()

        for copy in in_copies(j):
            copy.wait()
        first = x * half + j * BLOCK
        at_rows = [pl.ds(pl.multiple_of((first + i) * qrows, qrows), qrows) for i in range(BLOCK)]
        scores = []
        for i in range(BLOCK):
            scores.append(
                lax.dot_general(
                    q_s[at_rows[i], :].astype(BF16), kbuf[j * BLOCK + i], (((1,), (1,)), ((), ())),
                    preferred_element_type=F32,
                )
            )
        probs, news = [], []
        for i in range(BLOCK):
            p = pos[first + i]
            local = lax.rem(p, slots) - base
            owned = (local >= 0) & (local < local_slots)
            hidden = jnp.where(owned, local, -FAR)
            limit = jnp.where(p >= slots - 1, FAR // 2, p) - base
            fresh = q_s[at_rows[i], :] * kx_s[at_rows[i], :]
            fresh = jnp.sum(fresh + pltpu.roll(fresh, heads, 0), axis=1, keepdims=True) * scale
            fresh = jnp.where(jnp.broadcast_to(owned, fresh.shape), fresh, -jnp.inf)
            parts = []
            for t in range(slices):
                own = scores[i][:, t * LANES : (t + 1) * LANES]
                other = pltpu.roll(own, heads, 0)
                other = jnp.where(
                    low_half, pltpu.roll(other, LANES - kvs, 1), pltpu.roll(other, kvs, 1)
                )
                shift = t * (LANES // per_slot)
                ok = (slot_of_col <= limit - shift) & (slot_of_col != hidden - shift)
                parts.append(jnp.where(ok, (own + other) * scale, -jnp.inf))
            top = functools.reduce(jnp.maximum, parts)
            top = jnp.maximum(jnp.max(top, axis=1, keepdims=True), fresh)
            floor = jnp.where(top == -jnp.inf, 0.0, top)
            parts = [jnp.exp(part_t - floor) for part_t in parts]
            new = jnp.exp(fresh - floor)
            total = jnp.sum(functools.reduce(jnp.add, parts), axis=1, keepdims=True) + new
            at = pl.ds(pl.multiple_of((j * BLOCK + i) * qrows, qrows), qrows)
            m_s[at, :] = jnp.broadcast_to(top, (qrows, LANES))
            l_s[at, :] = jnp.broadcast_to(total, (qrows, LANES))
            news.append(new)
            probs.append(jnp.concatenate([part_t.astype(BF16) for part_t in parts], axis=1))
        for i in range(BLOCK):
            at = pl.ds(pl.multiple_of((j * BLOCK + i) * qrows, qrows), qrows)
            o_s[at, :] = (
                jnp.dot(probs[i], vbuf[j * BLOCK + i], preferred_element_type=F32) + news[i] * vx_s[at_rows[i], :]
            )
        return carry

    size = rows // GROUPS
    my_heads, their_heads = pl.ds(k * mine_h, mine_h), pl.ds((1 - k) * mine_h, mine_h)
    spans = [pl.ds(g * size, size) for g in range(GROUPS)]
    near = GROUPS // 2
    sources = [far_ref.at[their_heads, :, spans[g]] for g in range(near)]
    sources += [part.at[their_heads, :, spans[g]] for g in range(near)]
    swaps_a = [remote(src, rd.at[:, :, at], d_dev) for src, at in zip(sources, spans)]
    cross_a = [remote(sx.at[:, :, at], rx.at[:, :, at], x_dev) for at in spans[: GROUPS // 2]]
    left = lax.broadcasted_iota(jnp.int32, (mine_h, size, LANES), 2) < LANES // 2
    joined = [None] * GROUPS

    def publish(g):
        at = spans[g - near]
        for h in range(heads):
            lo = pl.ds((g - near) * size * qrows + h, size, stride=qrows)
            hi = pl.ds((g - near) * size * qrows + heads + h, size, stride=qrows)
            part[h, 0, at], part[h, 1, at] = o_s[lo, :], o_s[hi, :]
            part[h, 2, at] = jnp.where(left[0], m_s[lo, :], l_s[lo, :])
        swaps_a[g].start()

    def chip(g):
        swaps_a[g].wait_recv()
        at = spans[g]
        here, local = (far_ref, at) if g < near else (part, spans[g - near])
        o_a, o_b, m, l = combine(
            [here[my_heads, i, local] for i in range(3)], [rd[:, i, at] for i in range(3)]
        )
        value = [o_a, o_b, jnp.where(left, m, l)]
        if g < GROUPS // 2:
            for i in range(3):
                sx[:, i, at] = value[i]
            cross_a[g].start()
        joined[g] = value

    for g in range(near):
        swaps_a[g].start()
    step = n_blocks // GROUPS
    for g in range(GROUPS):
        lax.fori_loop(g * step, (g + 1) * step, block_step, 0)
        if g == 0:
            for n in range(near):
                chip(n)
        elif g == 1:
            publish(near)
        elif g == 2:
            chip(near)
            for copy in o_copies:
                copy.start()
    publish(GROUPS - 1)
    fetch(3)
    chip(GROUPS - 1)
    pieces = []
    for g in range(GROUPS // 2):
        cross_a[g].wait_recv()
        o_a, o_b, _, l = combine(joined[GROUPS // 2 + g], [rx[:, i, spans[g]] for i in range(3)])
        o_a, o_b = (o_a / l).astype(BF16), (o_b / l).astype(BF16)
        pieces.append(jnp.concatenate([v[h] for h in range(mine_h) for v in (o_a, o_b)], axis=-1))
    attended = jnp.concatenate(pieces, axis=0)

    own, other = pl.ds(k * quarter, quarter), pl.ds((1 - k) * quarter, quarter)
    my_rows = pl.ds(pl.multiple_of(x * half + k * quarter, quarter), quarter)
    x_peer_rows = pl.ds(pl.multiple_of((1 - x) * half + k * quarter, quarter), quarter)
    cols = [pl.ds(c * span, span) for c in range(CHUNKS)]
    per_span = span // head_dim

    def staged(dot, swap, cross, *rest):
        for c in range(CHUNKS + 2):
            if c < CHUNKS:
                dot(c)
            if c >= 2:
                swap(c - 2)
        for c in range(CHUNKS):
            cross(c)
        for c in range(CHUNKS + len(rest) - 1):
            for s, stage in enumerate(rest):
                if 0 <= c - s < CHUNKS:
                    stage(c - s)

    swaps = [remote(po.at[other, c], ro.at[:, c], d_dev) for c in cols]
    crosses = [remote(so.at[:, c], yo.at[:, c], y_dev) for c in cols]
    gathers = [remote(hb.at[own, c], hb.at[own, c], d_dev) for c in cols]

    def o_dot(c):
        for i in range(c * per_span, (c + 1) * per_span):
            o_copies[i].wait()
            w = ring[n_w + i // per_o, (i % per_o) * o_rows : (i % per_o + 1) * o_rows, :]
            po[:, i * head_dim : (i + 1) * head_dim] = jnp.dot(attended, w, preferred_element_type=F32)
        swaps[c].start()

    def o_swap(c):
        swaps[c].wait_recv()
        so[:, cols[c]] = po[own, cols[c]] + ro[:, cols[c]]
        crosses[c].start()
        fetch(3)

    def o_cross(c):
        crosses[c].wait_recv()
        total = so[:, cols[c]] + yo[:, cols[c]]
        hb[own, cols[c]] = (x_ref[my_rows, cols[c]].astype(F32) + total).astype(BF16).astype(F32)
        gathers[c].start()

    def o_gather(c):
        gathers[c].wait_recv()

    staged(o_dot, o_swap, o_cross, o_gather)

    normed_m = rms_norm(hb[...], gm_ref[...])
    for c in range(n_gate):
        chunks[2 * c].wait()
        chunks[2 * c + 1].wait()
        gate = jnp.dot(normed_m, ring[ring_at(2 * c)], preferred_element_type=F32)
        up = jnp.dot(normed_m, ring[ring_at(2 * c + 1)], preferred_element_type=F32)
        act[:, c * head_dim : (c + 1) * head_dim] = (jax.nn.silu(gate) * up).astype(BF16)
        fetch(2)

    swaps_m = [remote(pm.at[other, c], rm.at[:, c], d_dev) for c in cols]
    crosses_m = [remote(sm.at[:, c], ym.at[:, c], y_dev) for c in cols]
    to_core = [remote(ob.at[my_rows, c], ob.at[my_rows, c], d_dev) for c in cols]
    to_x = [remote(ob.at[my_rows, c], ob.at[my_rows, c], x_dev) for c in cols]
    onward = [remote(ob.at[x_peer_rows, c], ob.at[x_peer_rows, c], d_dev) for c in cols]

    def m_dot(c):
        for i in range(c * per_span, (c + 1) * per_span):
            chunks[2 * n_gate + i].wait()
            pm[:, i * head_dim : (i + 1) * head_dim] = jnp.dot(
                act[...], ring[ring_at(2 * n_gate + i)], preferred_element_type=F32
            )
        swaps_m[c].start()

    def m_swap(c):
        swaps_m[c].wait_recv()
        sm[:, cols[c]] = pm[own, cols[c]] + rm[:, cols[c]]
        crosses_m[c].start()

    def m_cross(c):
        crosses_m[c].wait_recv()
        total = sm[:, cols[c]] + ym[:, cols[c]]
        ob[my_rows, cols[c]] = (hb[own, cols[c]] + total).astype(BF16).astype(F32)
        to_x[c].start()
        to_core[c].start()

    def m_gather(c):
        to_x[c].wait_recv()
        onward[c].start()

    def m_last(c):
        to_core[c].wait_recv()
        onward[c].wait_recv()
        out_ref[:, cols[c]] = ob[:, cols[c]].astype(BF16)

    staged(m_dot, m_swap, m_cross, m_gather, m_last)
    for copy in [*swaps_a, *cross_a, *swaps, *crosses, *gathers, *swaps_m, *crosses_m, *to_core, *to_x, *onward]:
        copy.wait_send()


def layer(positions, tokens, gain, w_o, w_gate, w_up, w_down, rows_k, rows_v, kvs, carried):
    rows, width = tokens.shape
    head_dim = 2 * LANES
    heads = carried[0].shape[0]
    qrows = 2 * heads
    half, quarter = rows // 2, rows // 4
    cut = w_gate.shape[1] // 2
    n_blocks = half // BLOCK
    vmem = pl.BlockSpec(memory_space=pltpu.VMEM)
    hbm = pl.BlockSpec(memory_space=pltpu.HBM)
    flat = lambda n: pltpu.VMEM((n, width), F32)
    stats = lambda h, n: pltpu.VMEM((h, 3, n, LANES), F32)
    dma = lambda n: pltpu.SemaphoreType.DMA((n,))
    n_remote = GROUPS + GROUPS // 2 + 8 * CHUNKS
    args = (positions, tokens, gain, w_o, w_gate, w_up, w_down, rows_k, rows_v)
    shape = (half, *rows_k.shape[1:])
    return pl.pallas_call(
        functools.partial(layer_kernel, kvs),
        out_shape=(
            pltpu.VMEM(tokens.shape, BF16),
            pltpu.VMEM(shape, BF16),
            pltpu.VMEM(shape, BF16),
        ),
        in_specs=[hbm] * len(args) + [vmem] * len(carried),
        out_specs=(vmem,) * 3,
        scratch_shapes=[
            pltpu.VMEM((SLOTS, width, head_dim), BF16),
            *(pltpu.VMEM((half * qrows, LANES), F32) for _ in range(3)),
            stats(heads, half), stats(heads // 2, rows), stats(heads // 2, half), stats(heads // 2, half),
            flat(half), flat(quarter), flat(quarter), flat(quarter), flat(half),
            pltpu.VMEM((half, cut), BF16),
            flat(half), flat(quarter), flat(quarter), flat(quarter), flat(rows),
            pltpu.SMEM((rows,), jnp.int32),
            pltpu.VMEM(tokens.shape, BF16),
            pltpu.VMEM(gain.shape, BF16),
            dma(3), dma(n_blocks), dma(n_blocks), dma(width // head_dim),
            dma(2 * (cut // head_dim) + width // head_dim), dma(n_remote), dma(n_remote),
        ],
        compiler_params=pltpu.CompilerParams(
            vmem_limit_bytes=LAYER_VMEM << 20, collective_id=0, has_side_effects=True
        ),
        name="layer",
    )(*(pltpu.with_memory_space_constraint(v, pltpu.HBM) for v in args), *carried)


def write_kernel(pos_hbm, t_ref, tiles, kbuf, vbuf, _k, _v, out_ref, nk_hbm, nv_hbm, pos, sem, tile_sem, pos_sem):
    rows, key_rows, _ = kbuf.shape
    per_slot = 4
    local_slots = key_rows // per_slot
    slots = local_slots * lax.axis_size("sp")
    base = lax.axis_index("sp") * local_slots
    start = lax.axis_index("sp") // 2 * rows
    per_tile = 16 // per_slot
    n_blocks = rows // BLOCK

    def copies(j):
        here, near = pl.ds(j * BLOCK, BLOCK), pl.ds(start + j * BLOCK, BLOCK)
        return (
            pltpu.make_async_copy(kbuf.at[here], nk_hbm.at[near], sem.at[0, j]),
            pltpu.make_async_copy(vbuf.at[here], nv_hbm.at[near], sem.at[1, j]),
        )

    def where(b):
        local = lax.rem(pos[b], slots) - base
        owned = (local >= 0) & (local < local_slots)
        safe = jnp.where(owned, local, 0)
        return pl.ds(pl.multiple_of((safe // per_tile) * 16, 16), 16)

    def tile_copies(b):
        at = where(start + b)
        return (
            pltpu.make_async_copy(tiles.at[0, b], nk_hbm.at[start + b, at], tile_sem.at[0]),
            pltpu.make_async_copy(tiles.at[1, b], nv_hbm.at[start + b, at], tile_sem.at[1]),
        )

    pos_copy = pltpu.make_async_copy(pos_hbm, pos, pos_sem)
    pos_copy.start()
    for j in range(n_blocks):
        for copy in copies(j):
            copy.start()
    pos_copy.wait()

    out_ref[...] = t_ref[...]

    def place_tiles(j, carry):
        for copy in copies(j):
            copy.wait()
        for i in range(BLOCK):
            for copy in tile_copies(j * BLOCK + i):
                copy.start()
        return carry

    lax.fori_loop(0, n_blocks, place_tiles, 0)

    def finish(b, carry):
        for copy in tile_copies(b):
            copy.wait()
        return carry

    lax.fori_loop(0, rows, finish, 0, unroll=8)


def write(positions, layer_out, tiles, buf_k, buf_v, new_k, new_v):
    vmem = pl.BlockSpec(memory_space=pltpu.VMEM)
    hbm = pl.BlockSpec(memory_space=pltpu.HBM)
    rows = buf_k.shape[0]
    any_space = pl.BlockSpec(memory_space=pl.ANY)
    return pl.pallas_call(
        write_kernel,
        out_shape=tuple(jax.ShapeDtypeStruct(v.shape, BF16) for v in (layer_out, new_k, new_v)),
        in_specs=[hbm, vmem, vmem] + [any_space] * 2 + [hbm] * 2,
        out_specs=(vmem, hbm, hbm),
        input_output_aliases={5: 1, 6: 2},
        scratch_shapes=[
            pltpu.SMEM(positions.shape, jnp.int32),
            pltpu.SemaphoreType.DMA((2, rows // BLOCK)),
            pltpu.SemaphoreType.DMA((2,)),
            pltpu.SemaphoreType.DMA,
        ],
        compiler_params=pltpu.CompilerParams(vmem_limit_bytes=LAYER_VMEM << 20),
        name="write",
    )(pltpu.with_memory_space_constraint(positions, pltpu.HBM), layer_out, tiles, buf_k, buf_v, new_k, new_v)


def to_rows(cache):
    b, s, kv, d = cache.shape
    return cache.reshape(b, s, kv, d // LANES, LANES).transpose(0, 1, 3, 2, 4).reshape(b, -1, LANES)


def from_rows(rows, shape):
    b, s, kv, d = shape
    return rows.reshape(b, s, d // LANES, kv, LANES).transpose(0, 1, 3, 2, 4).reshape(shape)


def solution(mesh):
    cache_spec = P("dp", "sp", "tp", None)
    row_spec = P("dp", None)
    col_spec = P(None, "tp")
    in_specs = (row_spec, P("dp"), cache_spec, cache_spec, P(None), col_spec, col_spec, col_spec, P("tp", None), P(None), col_spec, col_spec, P("tp", None))
    out_specs = (row_spec, cache_spec, cache_spec)

    def local_step(tokens, positions, cache_k, cache_v, attn_gain, w_q, w_k, w_v, w_o, mlp_gain, w_gate, w_up, w_down):
        old_k, old_v = to_rows(cache_k), to_rows(cache_v)
        far, rows_k, rows_v, *carried, tiles = first_half(
            positions, tokens, attn_gain, w_q, w_k, w_v, old_k, old_v
        )
        out, buf_k, buf_v = layer(
            positions, tokens, mlp_gain, w_o, w_gate, w_up, w_down, old_k, old_v, cache_k.shape[2], (far, *carried)
        )
        layer_out, rows_k, rows_v = write(positions, out, tiles, buf_k, buf_v, rows_k, rows_v)
        new_k = from_rows(rows_k, cache_k.shape)
        new_v = from_rows(rows_v, cache_v.shape)
        return layer_out, new_k, new_v

    return jax.shard_map(local_step, mesh=mesh, in_specs=in_specs, out_specs=out_specs, check_vma=False)
```

```python
import functools
import itertools
import math

import jax
import jax.numpy as jnp
from jax import lax
from jax.experimental import pallas as pl
from jax.experimental.pallas import tpu as pltpu
from jax.sharding import PartitionSpec as P

NORM_EPS = 1e-5
ROPE_THETA = 10000.0
LANES = 128
F32 = jnp.float32
BF16 = jnp.bfloat16
FAR = 1 << 28
BLOCK = 4
AHEAD = 2
FIRST = 4
SLOTS = 22
LAYER_VMEM = 35
CHUNKS = 5
GROUPS = 4
MESH = pl.DeviceIdType.MESH


def rms_norm(values, gain):
    wide = values.astype(F32)
    inv_rms = lax.rsqrt(jnp.mean(wide * wide, axis=-1, keepdims=True) + NORM_EPS)
    return (wide * inv_rms * gain.astype(F32)).astype(BF16)


def first_kernel(
    pos_hbm, x_hbm, gain_hbm, wq_hbm, wk_hbm, wv_hbm, ck_hbm, cv_hbm,
    part_ref, nk_hbm, nv_hbm, q_s, kx_s, vx_s, kn_s, vn_s,
    wbuf, kbuf, vbuf, ang_s, o_s, m_s, l_s,
    pos, x_ref, gain_ref, w_sem, k_sem, v_sem, out_sem, x_sem,
):
    rows = x_ref.shape[0]
    head_dim = 2 * LANES
    heads = wq_hbm.shape[1] // head_dim
    kvs = wk_hbm.shape[1] // head_dim
    group = heads // kvs
    per_slot = 2 * kvs
    qrows = 2 * heads
    key_rows = ck_hbm.shape[1]
    local_slots = key_rows // per_slot
    slots = local_slots * lax.axis_size("sp")
    slices = key_rows // LANES
    half = rows // 2
    n_blocks = half // BLOCK
    start = (1 - lax.axis_index("sp") // 2) * half
    base = lax.axis_index("sp") * local_slots

    def w_copy(n):
        src, col = (
            (wk_hbm, n) if n < kvs else (wv_hbm, n - kvs) if n < 2 * kvs else (wq_hbm, n - 2 * kvs)
        )
        return pltpu.make_async_copy(src.at[:, pl.ds(col * head_dim, head_dim)], wbuf.at[n], w_sem.at[n])

    def in_copies(j):
        far, here = pl.ds(start + j * BLOCK, BLOCK), pl.ds(j * BLOCK, BLOCK)
        return (
            pltpu.make_async_copy(ck_hbm.at[far], kbuf.at[here], k_sem.at[j]),
            pltpu.make_async_copy(cv_hbm.at[far], vbuf.at[here], v_sem.at[j]),
        )

    def out_copies(j):
        far, here = pl.ds(start + j * BLOCK, BLOCK), pl.ds(j * BLOCK, BLOCK)
        return (
            pltpu.make_async_copy(kbuf.at[here], nk_hbm.at[far], out_sem.at[0]),
            pltpu.make_async_copy(vbuf.at[here], nv_hbm.at[far], out_sem.at[1]),
        )

    small = [
        pltpu.make_async_copy(src, dst, x_sem.at[i])
        for i, (src, dst) in enumerate(((pos_hbm, pos), (x_hbm, x_ref), (gain_hbm, gain_ref)))
    ]
    for copy in small:
        copy.start()
    n_w = heads + 2 * kvs
    for n in range(n_w // 2):
        w_copy(n).start()

    lane = lax.broadcasted_iota(jnp.int32, (1, LANES), 1).astype(F32)
    freq = jnp.exp2(lane * (-math.log2(ROPE_THETA) / LANES))

    for copy in small:
        copy.wait()
    for n in range(n_w // 2, n_w):
        w_copy(n).start()
    for j in range(FIRST):
        for copy in in_copies(j):
            copy.start()

    def angle_row(b, carry):
        ang_s[pl.ds(b, 1), :] = freq * pos[b].astype(F32)
        return carry

    lax.fori_loop(0, rows, angle_row, 0, unroll=8)
    angles = ang_s[...]
    cos_t, sin_t = jnp.cos(angles), jnp.sin(angles)
    normed = rms_norm(x_ref[...], gain_ref[...])

    for n in range(n_w):
        w_copy(n).wait()
        if FIRST + n < n_blocks:
            for copy in in_copies(FIRST + n):
                copy.start()
        lin = jnp.dot(normed, wbuf[n], preferred_element_type=F32)
        first, second = lin[:, :LANES], lin[:, LANES:]
        if not kvs <= n < 2 * kvs:
            first, second = first * cos_t - second * sin_t, second * cos_t + first * sin_t
        first, second = first.astype(BF16).astype(F32), second.astype(BF16).astype(F32)
        if n >= 2 * kvs:
            h = n - 2 * kvs
            q_s[pl.ds(h, rows, stride=qrows), :] = first
            q_s[pl.ds(heads + h, rows, stride=qrows), :] = second
        else:
            dst, tile, kv = (kn_s, kx_s, n) if n < kvs else (vn_s, vx_s, n - kvs)
            for rep in range(16 // per_slot):
                dst[pl.ds(rep * per_slot + kv, rows, stride=16), :] = first
                dst[pl.ds(rep * per_slot + kvs + kv, rows, stride=16), :] = second
            for g in range(group):
                tile[pl.ds(kv * group + g, rows, stride=qrows), :] = first
                tile[pl.ds(heads + kv * group + g, rows, stride=qrows), :] = second

    row = lax.broadcasted_iota(jnp.int32, (qrows, LANES), 0)
    col = lax.broadcasted_iota(jnp.int32, (qrows, LANES), 1)
    half_of_col = (col // kvs) % 2
    fits = (half_of_col == row // heads) & (col % kvs == (row % heads) // group)
    slot_of_col = jnp.where(fits, col // per_slot, FAR)
    low_half = half_of_col == 0
    patch_row = lax.broadcasted_iota(jnp.int32, (16, LANES), 0) // per_slot
    scale = 1.0 / math.sqrt(head_dim)

    def block_step(j, carry):
        for copy in in_copies(j):
            copy.wait()
        for i in range(BLOCK):
            n = j * BLOCK + i
            b = start + n
            local = lax.rem(pos[b], slots) - base
            owned = (local >= 0) & (local < local_slots)
            safe = jnp.where(owned, local, 0)
            hit = jnp.where(owned, lax.rem(safe, 16 // per_slot), -1)
            span = pl.ds(pl.multiple_of((safe // (16 // per_slot)) * 16, 16), 16)
            for buf, new in ((kbuf, kn_s), (vbuf, vn_s)):
                old = buf[n, span, :].astype(F32)
                fresh = new[pl.ds(pl.multiple_of(b * 16, 16), 16), :]
                buf[n, span, :] = jnp.where(patch_row == hit, fresh, old).astype(BF16)
        scores = []
        for i in range(BLOCK):
            b = start + j * BLOCK + i
            q = q_s[pl.ds(pl.multiple_of(b * qrows, qrows), qrows), :].astype(BF16)
            scores.append(
                lax.dot_general(q, kbuf[j * BLOCK + i], (((1,), (1,)), ((), ())), preferred_element_type=F32)
            )
        probs = []
        for i in range(BLOCK):
            n = j * BLOCK + i
            p = pos[start + n]
            limit = jnp.where(p >= slots - 1, FAR // 2, p) - base
            parts = []
            for t in range(slices):
                own = scores[i][:, t * LANES : (t + 1) * LANES]
                other = pltpu.roll(own, heads, 0)
                other = jnp.where(
                    low_half, pltpu.roll(other, LANES - kvs, 1), pltpu.roll(other, kvs, 1)
                )
                ok = slot_of_col <= limit - t * (LANES // per_slot)
                parts.append(jnp.where(ok, (own + other) * scale, -jnp.inf))
            top = functools.reduce(jnp.maximum, parts)
            top = jnp.max(top, axis=1, keepdims=True)
            floor = jnp.where(top == -jnp.inf, 0.0, top)
            parts = [jnp.exp(part - floor) for part in parts]
            total = jnp.sum(functools.reduce(jnp.add, parts), axis=1, keepdims=True)
            span = pl.ds(pl.multiple_of(n * qrows, qrows), qrows)
            m_s[span, :] = jnp.broadcast_to(top, (qrows, LANES))
            l_s[span, :] = jnp.broadcast_to(total, (qrows, LANES))
            probs.append(jnp.concatenate([part.astype(BF16) for part in parts], axis=1))
        for i in range(BLOCK):
            n = j * BLOCK + i
            span = pl.ds(pl.multiple_of(n * qrows, qrows), qrows)
            o_s[span, :] = jnp.dot(probs[i], vbuf[n], preferred_element_type=F32)
        for copy in out_copies(j):
            copy.start()
        return carry

    lax.fori_loop(0, n_blocks, block_step, 0)

    left = lax.broadcasted_iota(jnp.int32, (half, LANES), 1) < LANES // 2
    for h in range(heads):
        lo, hi = pl.ds(h, half, stride=qrows), pl.ds(heads + h, half, stride=qrows)
        part_ref[h, 0], part_ref[h, 1] = o_s[lo, :], o_s[hi, :]
        part_ref[h, 2] = jnp.where(left, m_s[lo, :], l_s[lo, :])
    for j in range(n_blocks):
        for copy in out_copies(j):
            copy.wait()


def first_half(positions, tokens, gain, w_q, w_k, w_v, rows_k, rows_v):
    rows, width = tokens.shape
    head_dim = 2 * LANES
    heads = w_q.shape[1] // head_dim
    kvs = w_k.shape[1] // head_dim
    qrows = 2 * heads
    vmem = pl.BlockSpec(memory_space=pltpu.VMEM)
    hbm = pl.BlockSpec(memory_space=pltpu.HBM)
    n_blocks = rows // 2 // BLOCK
    tile = lambda n: pltpu.VMEM((rows * n, LANES), F32)
    return pl.pallas_call(
        first_kernel,
        out_shape=(
            pltpu.VMEM((heads, 3, rows // 2, LANES), F32),
            jax.ShapeDtypeStruct(rows_k.shape, BF16),
            jax.ShapeDtypeStruct(rows_v.shape, BF16),
            tile(qrows), tile(qrows), tile(qrows), tile(16), tile(16),
        ),
        in_specs=[hbm] * 8,
        out_specs=(vmem, hbm, hbm) + (vmem,) * 5,
        scratch_shapes=[
            pltpu.VMEM((heads + 2 * kvs, width, head_dim), BF16),
            pltpu.VMEM((rows // 2, *rows_k.shape[1:]), BF16),
            pltpu.VMEM((rows // 2, *rows_v.shape[1:]), BF16),
            tile(1),
            pltpu.VMEM((rows // 2 * qrows, LANES), F32),
            pltpu.VMEM((rows // 2 * qrows, LANES), F32),
            pltpu.VMEM((rows // 2 * qrows, LANES), F32),
            pltpu.SMEM((rows,), jnp.int32),
            pltpu.VMEM(tokens.shape, BF16),
            pltpu.VMEM(gain.shape, BF16),
            pltpu.SemaphoreType.DMA((heads + 2 * kvs,)),
            pltpu.SemaphoreType.DMA((n_blocks,)),
            pltpu.SemaphoreType.DMA((n_blocks,)),
            pltpu.SemaphoreType.DMA((2,)),
            pltpu.SemaphoreType.DMA((3,)),
        ],
        compiler_params=pltpu.CompilerParams(vmem_limit_bytes=36 << 20),
        name="first",
    )(*(pltpu.with_memory_space_constraint(v, pltpu.HBM) for v in (positions, tokens, gain, w_q, w_k, w_v, rows_k, rows_v)))


def combine(mine, theirs):
    left = lax.broadcasted_iota(jnp.int32, mine[2].shape, mine[2].ndim - 1) < LANES // 2
    axis = mine[2].ndim - 1

    def unpack(stats):
        turned = pltpu.roll(stats, LANES // 2, axis)
        return jnp.where(left, stats, turned), jnp.where(left, turned, stats)

    (m_a, l_a), (m_b, l_b) = unpack(mine[2]), unpack(theirs[2])
    top = jnp.maximum(m_a, m_b)
    f_a = jnp.where(m_a == -jnp.inf, 0.0, jnp.exp(m_a - top))
    f_b = jnp.where(m_b == -jnp.inf, 0.0, jnp.exp(m_b - top))
    return mine[0] * f_a + theirs[0] * f_b, mine[1] * f_a + theirs[1] * f_b, top, l_a * f_a + l_b * f_b


def layer_kernel(
    kv_heads, pos_hbm, x_hbm, gm_hbm, wo_hbm, wg_hbm, wu_hbm, wd_hbm, ck_hbm, cv_hbm,
    far_ref, q_s, kx_s, vx_s,
    out_ref, kbuf, vbuf,
    ring, o_s, m_s, l_s, part, rd, sx, rx,
    po, ro, so, yo, hb, act, pm, rm, sm, ym, ob,
    pos, x_ref, gm_ref,
    small_sem, k_sem, v_sem, o_sem, c_sem, send_sem, recv_sem,
):
    rows, width = x_ref.shape
    head_dim = ring.shape[2]
    heads = far_ref.shape[0]
    kvs = kv_heads
    group = heads // kvs
    per_slot, qrows = 2 * kvs, 2 * heads
    key_rows = ck_hbm.shape[1]
    local_slots = key_rows // per_slot
    slots = local_slots * lax.axis_size("sp")
    slices = key_rows // LANES
    n_blocks = rows // 2 // BLOCK
    mine_h = heads // 2
    half, quarter = rows // 2, rows // 4
    sp, tp = lax.axis_index("sp"), lax.axis_index("tp")
    x, k = sp // 2, lax.rem(sp, 2)
    d_dev, x_dev, y_dev = {"sp": x * 2 + 1 - k}, {"sp": (1 - x) * 2 + k}, {"tp": 1 - tp}
    base = sp * local_slots
    m_cols = act.shape[1]
    span = width // CHUNKS

    barrier = pltpu.get_barrier_semaphore()
    for dev in (d_dev, x_dev, y_dev):
        pl.semaphore_signal(barrier, inc=1, device_id=dev, device_id_type=MESH)

    counter = [0]

    def remote(src, dst, dev):
        n = counter[0]
        counter[0] += 1
        return pltpu.make_async_remote_copy(
            src_ref=src, dst_ref=dst, send_sem=send_sem.at[n], recv_sem=recv_sem.at[n],
            device_id=dev, device_id_type=MESH,
        )

    def in_copies(j):
        near, here = pl.ds(x * half + j * BLOCK, BLOCK), pl.ds(j * BLOCK, BLOCK)
        return (
            pltpu.make_async_copy(ck_hbm.at[near], kbuf.at[here], k_sem.at[j]),
            pltpu.make_async_copy(cv_hbm.at[near], vbuf.at[here], v_sem.at[j]),
        )

    small = [
        pltpu.make_async_copy(src, dst, small_sem.at[i])
        for i, (src, dst) in enumerate(
            ((pos_hbm, pos), (x_hbm, x_ref), (gm_hbm, gm_ref))
        )
    ]
    for copy in small:
        copy.start()
    for j in range(AHEAD):
        for copy in in_copies(j):
            copy.start()

    n_w = 0
    o_rows = mine_h * head_dim
    per_o = width // o_rows
    o_copies = [
        pltpu.make_async_copy(
            wo_hbm.at[pl.ds(k * o_rows, o_rows), pl.ds(c * head_dim, head_dim)],
            ring.at[n_w + c // per_o, pl.ds((c % per_o) * o_rows, o_rows)],
            o_sem.at[c],
        )
        for c in range(width // head_dim)
    ]
    n_gate = m_cols // head_dim
    ring_at = lambda i: (n_w + 2 + i) % SLOTS
    chunks = []
    for c in range(n_gate):
        at = pl.ds(pl.multiple_of(k * m_cols + c * head_dim, LANES), head_dim)
        chunks += [wg_hbm.at[:, at], wu_hbm.at[:, at]]
    for c in range(width // head_dim):
        chunks.append(wd_hbm.at[pl.ds(pl.multiple_of(k * m_cols, LANES), m_cols), pl.ds(c * head_dim, head_dim)])
    chunks = [
        pltpu.make_async_copy(src, ring.at[ring_at(i)], c_sem.at[i]) for i, src in enumerate(chunks)
    ]
    queue = iter(chunks)

    def fetch(n):
        for copy in itertools.islice(queue, n):
            copy.start()

    for copy in small:
        copy.wait()
    pl.semaphore_wait(barrier, 3)

    row = lax.broadcasted_iota(jnp.int32, (qrows, LANES), 0)
    col = lax.broadcasted_iota(jnp.int32, (qrows, LANES), 1)
    half_of_col = (col // kvs) % 2
    fits = (half_of_col == row // heads) & (col % kvs == (row % heads) // group)
    slot_of_col = jnp.where(fits, col // per_slot, FAR)
    low_half = half_of_col == 0
    scale = 1.0 / math.sqrt(head_dim)

    def block_step(j, carry):
        @pl.when(j + AHEAD < n_blocks)
        def _():
            for copy in in_copies(j + AHEAD):
                copy.start()

        for copy in in_copies(j):
            copy.wait()
        first = x * half + j * BLOCK
        at_rows = [pl.ds(pl.multiple_of((first + i) * qrows, qrows), qrows) for i in range(BLOCK)]
        scores = []
        for i in range(BLOCK):
            scores.append(
                lax.dot_general(
                    q_s[at_rows[i], :].astype(BF16), kbuf[j * BLOCK + i], (((1,), (1,)), ((), ())),
                    preferred_element_type=F32,
                )
            )
        probs, news = [], []
        for i in range(BLOCK):
            p = pos[first + i]
            local = lax.rem(p, slots) - base
            owned = (local >= 0) & (local < local_slots)
            hidden = jnp.where(owned, local, -FAR)
            limit = jnp.where(p >= slots - 1, FAR // 2, p) - base
            fresh = q_s[at_rows[i], :] * kx_s[at_rows[i], :]
            fresh = jnp.sum(fresh + pltpu.roll(fresh, heads, 0), axis=1, keepdims=True) * scale
            fresh = jnp.where(jnp.broadcast_to(owned, fresh.shape), fresh, -jnp.inf)
            parts = []
            for t in range(slices):
                own = scores[i][:, t * LANES : (t + 1) * LANES]
                other = pltpu.roll(own, heads, 0)
                other = jnp.where(
                    low_half, pltpu.roll(other, LANES - kvs, 1), pltpu.roll(other, kvs, 1)
                )
                shift = t * (LANES // per_slot)
                ok = (slot_of_col <= limit - shift) & (slot_of_col != hidden - shift)
                parts.append(jnp.where(ok, (own + other) * scale, -jnp.inf))
            top = functools.reduce(jnp.maximum, parts)
            top = jnp.maximum(jnp.max(top, axis=1, keepdims=True), fresh)
            floor = jnp.where(top == -jnp.inf, 0.0, top)
            parts = [jnp.exp(part_t - floor) for part_t in parts]
            new = jnp.exp(fresh - floor)
            total = jnp.sum(functools.reduce(jnp.add, parts), axis=1, keepdims=True) + new
            at = pl.ds(pl.multiple_of((j * BLOCK + i) * qrows, qrows), qrows)
            m_s[at, :] = jnp.broadcast_to(top, (qrows, LANES))
            l_s[at, :] = jnp.broadcast_to(total, (qrows, LANES))
            news.append(new)
            probs.append(jnp.concatenate([part_t.astype(BF16) for part_t in parts], axis=1))
        for i in range(BLOCK):
            at = pl.ds(pl.multiple_of((j * BLOCK + i) * qrows, qrows), qrows)
            o_s[at, :] = (
                jnp.dot(probs[i], vbuf[j * BLOCK + i], preferred_element_type=F32) + news[i] * vx_s[at_rows[i], :]
            )
        return carry

    size = rows // GROUPS
    my_heads, their_heads = pl.ds(k * mine_h, mine_h), pl.ds((1 - k) * mine_h, mine_h)
    spans = [pl.ds(g * size, size) for g in range(GROUPS)]
    near = GROUPS // 2
    sources = [far_ref.at[their_heads, :, spans[g]] for g in range(near)]
    sources += [part.at[their_heads, :, spans[g]] for g in range(near)]
    swaps_a = [remote(src, rd.at[:, :, at], d_dev) for src, at in zip(sources, spans)]
    cross_a = [remote(sx.at[:, :, at], rx.at[:, :, at], x_dev) for at in spans[: GROUPS // 2]]
    left = lax.broadcasted_iota(jnp.int32, (mine_h, size, LANES), 2) < LANES // 2
    joined = [None] * GROUPS

    def publish(g):
        at = spans[g - near]
        for h in range(heads):
            lo = pl.ds((g - near) * size * qrows + h, size, stride=qrows)
            hi = pl.ds((g - near) * size * qrows + heads + h, size, stride=qrows)
            part[h, 0, at], part[h, 1, at] = o_s[lo, :], o_s[hi, :]
            part[h, 2, at] = jnp.where(left[0], m_s[lo, :], l_s[lo, :])
        swaps_a[g].start()

    def chip(g):
        swaps_a[g].wait_recv()
        at = spans[g]
        here, local = (far_ref, at) if g < near else (part, spans[g - near])
        o_a, o_b, m, l = combine(
            [here[my_heads, i, local] for i in range(3)], [rd[:, i, at] for i in range(3)]
        )
        value = [o_a, o_b, jnp.where(left, m, l)]
        if g < GROUPS // 2:
            for i in range(3):
                sx[:, i, at] = value[i]
            cross_a[g].start()
        joined[g] = value

    for g in range(near):
        swaps_a[g].start()
    step = n_blocks // GROUPS
    for g in range(GROUPS):
        lax.fori_loop(g * step, (g + 1) * step, block_step, 0)
        if g == 0:
            for n in range(near):
                chip(n)
        elif g == 1:
            publish(near)
        elif g == 2:
            chip(near)
            for copy in o_copies:
                copy.start()
    publish(GROUPS - 1)
    fetch(3)
    chip(GROUPS - 1)
    pieces = []
    for g in range(GROUPS // 2):
        cross_a[g].wait_recv()
        o_a, o_b, _, l = combine(joined[GROUPS // 2 + g], [rx[:, i, spans[g]] for i in range(3)])
        o_a, o_b = (o_a / l).astype(BF16), (o_b / l).astype(BF16)
        pieces.append(jnp.concatenate([v[h] for h in range(mine_h) for v in (o_a, o_b)], axis=-1))
    attended = jnp.concatenate(pieces, axis=0)

    own, other = pl.ds(k * quarter, quarter), pl.ds((1 - k) * quarter, quarter)
    my_rows = pl.ds(pl.multiple_of(x * half + k * quarter, quarter), quarter)
    x_peer_rows = pl.ds(pl.multiple_of((1 - x) * half + k * quarter, quarter), quarter)
    cols = [pl.ds(c * span, span) for c in range(CHUNKS)]
    per_span = span // head_dim

    def staged(dot, swap, cross, *rest):
        for c in range(CHUNKS + 2):
            if c < CHUNKS:
                dot(c)
            if c >= 2:
                swap(c - 2)
        for c in range(CHUNKS):
            cross(c)
        for c in range(CHUNKS + len(rest) - 1):
            for s, stage in enumerate(rest):
                if 0 <= c - s < CHUNKS:
                    stage(c - s)

    swaps = [remote(po.at[other, c], ro.at[:, c], d_dev) for c in cols]
    crosses = [remote(so.at[:, c], yo.at[:, c], y_dev) for c in cols]
    gathers = [remote(hb.at[own, c], hb.at[own, c], d_dev) for c in cols]

    def o_dot(c):
        for i in range(c * per_span, (c + 1) * per_span):
            o_copies[i].wait()
            w = ring[n_w + i // per_o, (i % per_o) * o_rows : (i % per_o + 1) * o_rows, :]
            po[:, i * head_dim : (i + 1) * head_dim] = jnp.dot(attended, w, preferred_element_type=F32)
        swaps[c].start()

    def o_swap(c):
        swaps[c].wait_recv()
        so[:, cols[c]] = po[own, cols[c]] + ro[:, cols[c]]
        crosses[c].start()
        fetch(3)

    def o_cross(c):
        crosses[c].wait_recv()
        total = so[:, cols[c]] + yo[:, cols[c]]
        hb[own, cols[c]] = (x_ref[my_rows, cols[c]].astype(F32) + total).astype(BF16).astype(F32)
        gathers[c].start()

    def o_gather(c):
        gathers[c].wait_recv()

    staged(o_dot, o_swap, o_cross, o_gather)

    normed_m = rms_norm(hb[...], gm_ref[...])
    for c in range(n_gate):
        chunks[2 * c].wait()
        chunks[2 * c + 1].wait()
        gate = jnp.dot(normed_m, ring[ring_at(2 * c)], preferred_element_type=F32)
        up = jnp.dot(normed_m, ring[ring_at(2 * c + 1)], preferred_element_type=F32)
        act[:, c * head_dim : (c + 1) * head_dim] = (jax.nn.silu(gate) * up).astype(BF16)
        fetch(2)

    swaps_m = [remote(pm.at[other, c], rm.at[:, c], d_dev) for c in cols]
    crosses_m = [remote(sm.at[:, c], ym.at[:, c], y_dev) for c in cols]
    to_core = [remote(ob.at[my_rows, c], ob.at[my_rows, c], d_dev) for c in cols]
    to_x = [remote(ob.at[my_rows, c], ob.at[my_rows, c], x_dev) for c in cols]
    onward = [remote(ob.at[x_peer_rows, c], ob.at[x_peer_rows, c], d_dev) for c in cols]

    def m_dot(c):
        for i in range(c * per_span, (c + 1) * per_span):
            chunks[2 * n_gate + i].wait()
            pm[:, i * head_dim : (i + 1) * head_dim] = jnp.dot(
                act[...], ring[ring_at(2 * n_gate + i)], preferred_element_type=F32
            )
        swaps_m[c].start()

    def m_swap(c):
        swaps_m[c].wait_recv()
        sm[:, cols[c]] = pm[own, cols[c]] + rm[:, cols[c]]
        crosses_m[c].start()

    def m_cross(c):
        crosses_m[c].wait_recv()
        total = sm[:, cols[c]] + ym[:, cols[c]]
        ob[my_rows, cols[c]] = (hb[own, cols[c]] + total).astype(BF16).astype(F32)
        to_x[c].start()
        to_core[c].start()

    def m_gather(c):
        to_x[c].wait_recv()
        onward[c].start()

    def m_last(c):
        to_core[c].wait_recv()
        onward[c].wait_recv()
        out_ref[:, cols[c]] = ob[:, cols[c]].astype(BF16)

    staged(m_dot, m_swap, m_cross, m_gather, m_last)
    for copy in [*swaps_a, *cross_a, *swaps, *crosses, *gathers, *swaps_m, *crosses_m, *to_core, *to_x, *onward]:
        copy.wait_send()


def layer(positions, tokens, gain, w_o, w_gate, w_up, w_down, rows_k, rows_v, kvs, carried):
    rows, width = tokens.shape
    head_dim = 2 * LANES
    heads = carried[0].shape[0]
    qrows = 2 * heads
    half, quarter = rows // 2, rows // 4
    cut = w_gate.shape[1] // 2
    n_blocks = half // BLOCK
    vmem = pl.BlockSpec(memory_space=pltpu.VMEM)
    hbm = pl.BlockSpec(memory_space=pltpu.HBM)
    flat = lambda n: pltpu.VMEM((n, width), F32)
    stats = lambda h, n: pltpu.VMEM((h, 3, n, LANES), F32)
    dma = lambda n: pltpu.SemaphoreType.DMA((n,))
    n_remote = GROUPS + GROUPS // 2 + 8 * CHUNKS
    args = (positions, tokens, gain, w_o, w_gate, w_up, w_down, rows_k, rows_v)
    shape = (half, *rows_k.shape[1:])
    return pl.pallas_call(
        functools.partial(layer_kernel, kvs),
        out_shape=(
            pltpu.VMEM(tokens.shape, BF16),
            pltpu.VMEM(shape, BF16),
            pltpu.VMEM(shape, BF16),
        ),
        in_specs=[hbm] * len(args) + [vmem] * len(carried),
        out_specs=(vmem,) * 3,
        scratch_shapes=[
            pltpu.VMEM((SLOTS, width, head_dim), BF16),
            *(pltpu.VMEM((half * qrows, LANES), F32) for _ in range(3)),
            stats(heads, half), stats(heads // 2, rows), stats(heads // 2, half), stats(heads // 2, half),
            flat(half), flat(quarter), flat(quarter), flat(quarter), flat(half),
            pltpu.VMEM((half, cut), BF16),
            flat(half), flat(quarter), flat(quarter), flat(quarter), flat(rows),
            pltpu.SMEM((rows,), jnp.int32),
            pltpu.VMEM(tokens.shape, BF16),
            pltpu.VMEM(gain.shape, BF16),
            dma(3), dma(n_blocks), dma(n_blocks), dma(width // head_dim),
            dma(2 * (cut // head_dim) + width // head_dim), dma(n_remote), dma(n_remote),
        ],
        compiler_params=pltpu.CompilerParams(
            vmem_limit_bytes=LAYER_VMEM << 20, collective_id=0, has_side_effects=True
        ),
        name="layer",
    )(*(pltpu.with_memory_space_constraint(v, pltpu.HBM) for v in args), *carried)


def write_kernel(pos_hbm, t_ref, kn_s, vn_s, _bk, _bv, _k, _v, out_ref, nk_hbm, nv_hbm, kbuf, vbuf, pos, sem, pos_sem):
    rows, key_rows, _ = kbuf.shape
    per_slot = 4
    local_slots = key_rows // per_slot
    slots = local_slots * lax.axis_size("sp")
    base = lax.axis_index("sp") * local_slots
    start = lax.axis_index("sp") // 2 * rows
    per_tile = 16 // per_slot
    n_blocks = rows // BLOCK
    tile_row = lax.broadcasted_iota(jnp.int32, (16, LANES), 0) // per_slot

    def copies(j):
        here, near = pl.ds(j * BLOCK, BLOCK), pl.ds(start + j * BLOCK, BLOCK)
        return (
            pltpu.make_async_copy(kbuf.at[here], nk_hbm.at[near], sem.at[0]),
            pltpu.make_async_copy(vbuf.at[here], nv_hbm.at[near], sem.at[1]),
        )

    def patch(n):
        b = start + n
        local = lax.rem(pos[b], slots) - base
        owned = (local >= 0) & (local < local_slots)
        safe = jnp.where(owned, local, 0)
        hit = jnp.where(owned, lax.rem(safe, per_tile), -1)
        at = pl.ds(pl.multiple_of((safe // per_tile) * 16, 16), 16)
        for buf, new in ((kbuf, kn_s), (vbuf, vn_s)):
            fresh = new[pl.ds(pl.multiple_of(b * 16, 16), 16), :]
            buf[n, at, :] = jnp.where(tile_row == hit, fresh, buf[n, at, :].astype(F32)).astype(BF16)

    pos_copy = pltpu.make_async_copy(pos_hbm, pos, pos_sem)
    pos_copy.start()
    out_ref[...] = t_ref[...]
    pos_copy.wait()
    for j in range(n_blocks + 1):
        if j < n_blocks:
            for i in range(BLOCK):
                patch(j * BLOCK + i)
        if j:
            for copy in copies(j - 1):
                copy.start()
    for j in range(n_blocks):
        for copy in copies(j):
            copy.wait()


def write(positions, layer_out, fresh_k, fresh_v, buf_k, buf_v, new_k, new_v):
    vmem = pl.BlockSpec(memory_space=pltpu.VMEM)
    hbm = pl.BlockSpec(memory_space=pltpu.HBM)
    return pl.pallas_call(
        write_kernel,
        out_shape=(
            *(jax.ShapeDtypeStruct(v.shape, BF16) for v in (layer_out, new_k, new_v)),
            pltpu.VMEM(buf_k.shape, BF16),
            pltpu.VMEM(buf_v.shape, BF16),
        ),
        in_specs=[hbm] + [vmem] * 5 + [hbm] * 2,
        out_specs=(vmem, hbm, hbm, vmem, vmem),
        input_output_aliases={4: 3, 5: 4, 6: 1, 7: 2},
        scratch_shapes=[
            pltpu.SMEM(positions.shape, jnp.int32),
            pltpu.SemaphoreType.DMA((2,)),
            pltpu.SemaphoreType.DMA,
        ],
        compiler_params=pltpu.CompilerParams(vmem_limit_bytes=LAYER_VMEM << 20),
        name="write",
    )(pltpu.with_memory_space_constraint(positions, pltpu.HBM), layer_out, fresh_k, fresh_v, buf_k, buf_v, new_k, new_v)[:3]


def to_rows(cache):
    b, s, kv, d = cache.shape
    return cache.reshape(b, s, kv, d // LANES, LANES).transpose(0, 1, 3, 2, 4).reshape(b, -1, LANES)


def from_rows(rows, shape):
    b, s, kv, d = shape
    return rows.reshape(b, s, d // LANES, kv, LANES).transpose(0, 1, 3, 2, 4).reshape(shape)


def solution(mesh):
    cache_spec = P("dp", "sp", "tp", None)
    row_spec = P("dp", None)
    col_spec = P(None, "tp")
    in_specs = (row_spec, P("dp"), cache_spec, cache_spec, P(None), col_spec, col_spec, col_spec, P("tp", None), P(None), col_spec, col_spec, P("tp", None))
    out_specs = (row_spec, cache_spec, cache_spec)

    def local_step(tokens, positions, cache_k, cache_v, attn_gain, w_q, w_k, w_v, w_o, mlp_gain, w_gate, w_up, w_down):
        old_k, old_v = to_rows(cache_k), to_rows(cache_v)
        far, rows_k, rows_v, *carried, fresh_k, fresh_v = first_half(
            positions, tokens, attn_gain, w_q, w_k, w_v, old_k, old_v
        )
        out, buf_k, buf_v = layer(
            positions, tokens, mlp_gain, w_o, w_gate, w_up, w_down, old_k, old_v, cache_k.shape[2], (far, *carried)
        )
        layer_out, rows_k, rows_v = write(positions, out, fresh_k, fresh_v, buf_k, buf_v, rows_k, rows_v)
        new_k = from_rows(rows_k, cache_k.shape)
        new_v = from_rows(rows_v, cache_v.shape)
        return layer_out, new_k, new_v

    return jax.shard_map(local_step, mesh=mesh, in_specs=in_specs, out_specs=out_specs, check_vma=False)
```

```python
import functools
import itertools
import math

import jax
import jax.numpy as jnp
from jax import lax
from jax.experimental import pallas as pl
from jax.experimental.pallas import tpu as pltpu
from jax.sharding import PartitionSpec as P

NORM_EPS = 1e-5
ROPE_THETA = 10000.0
LANES = 128
F32 = jnp.float32
BF16 = jnp.bfloat16
FAR = 1 << 28
BLOCK = 4
EARLY = 3
AHEAD = 3
FIRST = 4
SLOTS = 22
LAYER_VMEM = 35
CHUNKS = 5
GROUPS = 4
MESH = pl.DeviceIdType.MESH


def rms_norm(values, gain):
    wide = values.astype(F32)
    inv_rms = lax.rsqrt(jnp.mean(wide * wide, axis=-1, keepdims=True) + NORM_EPS)
    return (wide * inv_rms * gain.astype(F32)).astype(BF16)


def first_kernel(
    pos_hbm, x_hbm, gain_hbm, wq_hbm, wk_hbm, wv_hbm, ck_hbm, cv_hbm,
    part_ref, nk_hbm, nv_hbm, q_s, kx_s, vx_s, lim_s, hid_s, kn_s, vn_s,
    wbuf, kbuf, vbuf, ang_s, o_s, m_s, l_s,
    pos, x_ref, gain_ref, w_sem, k_sem, v_sem, out_sem, x_sem,
):
    rows = x_ref.shape[0]
    head_dim = 2 * LANES
    heads = wq_hbm.shape[1] // head_dim
    kvs = wk_hbm.shape[1] // head_dim
    group = heads // kvs
    per_slot = 2 * kvs
    qrows = 2 * heads
    key_rows = ck_hbm.shape[1]
    local_slots = key_rows // per_slot
    slots = local_slots * lax.axis_size("sp")
    slices = key_rows // LANES
    half = rows // 2
    n_blocks = half // BLOCK
    start = (1 - lax.axis_index("sp") // 2) * half
    base = lax.axis_index("sp") * local_slots

    def w_copy(n):
        src, col = (
            (wk_hbm, n) if n < kvs else (wv_hbm, n - kvs) if n < 2 * kvs else (wq_hbm, n - 2 * kvs)
        )
        return pltpu.make_async_copy(src.at[:, pl.ds(col * head_dim, head_dim)], wbuf.at[n], w_sem.at[n])

    def in_copies(j):
        far, here = pl.ds(start + j * BLOCK, BLOCK), pl.ds(j * BLOCK, BLOCK)
        return (
            pltpu.make_async_copy(ck_hbm.at[far], kbuf.at[here], k_sem.at[j]),
            pltpu.make_async_copy(cv_hbm.at[far], vbuf.at[here], v_sem.at[j]),
        )

    def out_copies(j):
        far, here = pl.ds(start + j * BLOCK, BLOCK), pl.ds(j * BLOCK, BLOCK)
        return (
            pltpu.make_async_copy(kbuf.at[here], nk_hbm.at[far], out_sem.at[0]),
            pltpu.make_async_copy(vbuf.at[here], nv_hbm.at[far], out_sem.at[1]),
        )

    small = [
        pltpu.make_async_copy(src, dst, x_sem.at[i])
        for i, (src, dst) in enumerate(((pos_hbm, pos), (x_hbm, x_ref), (gain_hbm, gain_ref)))
    ]
    for copy in small:
        copy.start()
    n_w = heads + 2 * kvs
    for n in range(n_w // 2):
        w_copy(n).start()

    lane = lax.broadcasted_iota(jnp.int32, (1, LANES), 1).astype(F32)
    freq = jnp.exp2(lane * (-math.log2(ROPE_THETA) / LANES))

    for copy in small:
        copy.wait()
    for n in range(n_w // 2, n_w):
        w_copy(n).start()
    for j in range(FIRST):
        for copy in in_copies(j):
            copy.start()

    def angle_row(b, carry):
        p = pos[b]
        ang_s[pl.ds(b, 1), :] = freq * p.astype(F32)
        local = lax.rem(p, slots) - base
        owned = (local >= 0) & (local < local_slots)
        span = pl.ds(pl.multiple_of(b * qrows, qrows), qrows)
        lim_s[span, :] = jnp.full((qrows, LANES), jnp.where(p >= slots - 1, FAR // 2, p) - base, jnp.int32)
        hid_s[span, :] = jnp.full((qrows, LANES), jnp.where(owned, local, -FAR), jnp.int32)
        return carry

    lax.fori_loop(0, rows, angle_row, 0, unroll=8)
    angles = ang_s[...]
    cos_t, sin_t = jnp.cos(angles), jnp.sin(angles)
    normed = rms_norm(x_ref[...], gain_ref[...])

    for n in range(n_w):
        w_copy(n).wait()
        if FIRST + n < n_blocks:
            for copy in in_copies(FIRST + n):
                copy.start()
        lin = jnp.dot(normed, wbuf[n], preferred_element_type=F32)
        first, second = lin[:, :LANES], lin[:, LANES:]
        if not kvs <= n < 2 * kvs:
            first, second = first * cos_t - second * sin_t, second * cos_t + first * sin_t
        first, second = first.astype(BF16).astype(F32), second.astype(BF16).astype(F32)
        if n >= 2 * kvs:
            h = n - 2 * kvs
            q_s[pl.ds(h, rows, stride=qrows), :] = first
            q_s[pl.ds(heads + h, rows, stride=qrows), :] = second
        else:
            dst, tile, kv = (kn_s, kx_s, n) if n < kvs else (vn_s, vx_s, n - kvs)
            for rep in range(16 // per_slot):
                dst[pl.ds(rep * per_slot + kv, rows, stride=16), :] = first
                dst[pl.ds(rep * per_slot + kvs + kv, rows, stride=16), :] = second
            for g in range(group):
                tile[pl.ds(kv * group + g, rows, stride=qrows), :] = first
                tile[pl.ds(heads + kv * group + g, rows, stride=qrows), :] = second

    row = lax.broadcasted_iota(jnp.int32, (qrows, LANES), 0)
    col = lax.broadcasted_iota(jnp.int32, (qrows, LANES), 1)
    half_of_col = (col // kvs) % 2
    fits = (half_of_col == row // heads) & (col % kvs == (row % heads) // group)
    slot_of_col = jnp.where(fits, col // per_slot, FAR)
    low_half = half_of_col == 0
    patch_row = lax.broadcasted_iota(jnp.int32, (16, LANES), 0) // per_slot
    scale = 1.0 / math.sqrt(head_dim)

    def block_step(j, carry):
        for copy in in_copies(j):
            copy.wait()
        for i in range(BLOCK):
            n = j * BLOCK + i
            b = start + n
            local = lax.rem(pos[b], slots) - base
            owned = (local >= 0) & (local < local_slots)
            safe = jnp.where(owned, local, 0)
            hit = jnp.where(owned, lax.rem(safe, 16 // per_slot), -1)
            span = pl.ds(pl.multiple_of((safe // (16 // per_slot)) * 16, 16), 16)
            for buf, new in ((kbuf, kn_s), (vbuf, vn_s)):
                old = buf[n, span, :].astype(F32)
                fresh = new[pl.ds(pl.multiple_of(b * 16, 16), 16), :]
                buf[n, span, :] = jnp.where(patch_row == hit, fresh, old).astype(BF16)
        scores = []
        for i in range(BLOCK):
            b = start + j * BLOCK + i
            q = q_s[pl.ds(pl.multiple_of(b * qrows, qrows), qrows), :].astype(BF16)
            scores.append(
                lax.dot_general(q, kbuf[j * BLOCK + i], (((1,), (1,)), ((), ())), preferred_element_type=F32)
            )
        probs = []
        for i in range(BLOCK):
            n = j * BLOCK + i
            p = pos[start + n]
            limit = jnp.where(p >= slots - 1, FAR // 2, p) - base
            parts = []
            for t in range(slices):
                own = scores[i][:, t * LANES : (t + 1) * LANES]
                other = pltpu.roll(own, heads, 0)
                other = jnp.where(
                    low_half, pltpu.roll(other, LANES - kvs, 1), pltpu.roll(other, kvs, 1)
                )
                ok = slot_of_col <= limit - t * (LANES // per_slot)
                parts.append(jnp.where(ok, (own + other) * scale, -jnp.inf))
            top = functools.reduce(jnp.maximum, parts)
            top = jnp.max(top, axis=1, keepdims=True)
            floor = jnp.where(top == -jnp.inf, 0.0, top)
            parts = [jnp.exp(part - floor) for part in parts]
            total = jnp.sum(functools.reduce(jnp.add, parts), axis=1, keepdims=True)
            span = pl.ds(pl.multiple_of(n * qrows, qrows), qrows)
            m_s[span, :] = jnp.broadcast_to(top, (qrows, LANES))
            l_s[span, :] = jnp.broadcast_to(total, (qrows, LANES))
            probs.append(jnp.concatenate([part.astype(BF16) for part in parts], axis=1))
        for i in range(BLOCK):
            n = j * BLOCK + i
            span = pl.ds(pl.multiple_of(n * qrows, qrows), qrows)
            o_s[span, :] = jnp.dot(probs[i], vbuf[n], preferred_element_type=F32)
        for copy in out_copies(j):
            copy.start()
        return carry

    lax.fori_loop(0, n_blocks, block_step, 0)

    left = lax.broadcasted_iota(jnp.int32, (half, LANES), 1) < LANES // 2
    for h in range(heads):
        lo, hi = pl.ds(h, half, stride=qrows), pl.ds(heads + h, half, stride=qrows)
        part_ref[h, 0], part_ref[h, 1] = o_s[lo, :], o_s[hi, :]
        part_ref[h, 2] = jnp.where(left, m_s[lo, :], l_s[lo, :])
    for j in range(n_blocks):
        for copy in out_copies(j):
            copy.wait()


def first_half(positions, tokens, gain, w_q, w_k, w_v, rows_k, rows_v):
    rows, width = tokens.shape
    head_dim = 2 * LANES
    heads = w_q.shape[1] // head_dim
    kvs = w_k.shape[1] // head_dim
    qrows = 2 * heads
    vmem = pl.BlockSpec(memory_space=pltpu.VMEM)
    hbm = pl.BlockSpec(memory_space=pltpu.HBM)
    n_blocks = rows // 2 // BLOCK
    tile = lambda n: pltpu.VMEM((rows * n, LANES), F32)
    return pl.pallas_call(
        first_kernel,
        out_shape=(
            pltpu.VMEM((heads, 3, rows // 2, LANES), F32),
            jax.ShapeDtypeStruct(rows_k.shape, BF16),
            jax.ShapeDtypeStruct(rows_v.shape, BF16),
            tile(qrows), tile(qrows), tile(qrows),
            *(pltpu.VMEM((rows * qrows, LANES), jnp.int32) for _ in range(2)),
            tile(16), tile(16),
        ),
        in_specs=[hbm] * 8,
        out_specs=(vmem, hbm, hbm) + (vmem,) * 7,
        scratch_shapes=[
            pltpu.VMEM((heads + 2 * kvs, width, head_dim), BF16),
            pltpu.VMEM((rows // 2, *rows_k.shape[1:]), BF16),
            pltpu.VMEM((rows // 2, *rows_v.shape[1:]), BF16),
            tile(1),
            pltpu.VMEM((rows // 2 * qrows, LANES), F32),
            pltpu.VMEM((rows // 2 * qrows, LANES), F32),
            pltpu.VMEM((rows // 2 * qrows, LANES), F32),
            pltpu.SMEM((rows,), jnp.int32),
            pltpu.VMEM(tokens.shape, BF16),
            pltpu.VMEM(gain.shape, BF16),
            pltpu.SemaphoreType.DMA((heads + 2 * kvs,)),
            pltpu.SemaphoreType.DMA((n_blocks,)),
            pltpu.SemaphoreType.DMA((n_blocks,)),
            pltpu.SemaphoreType.DMA((2,)),
            pltpu.SemaphoreType.DMA((3,)),
        ],
        compiler_params=pltpu.CompilerParams(vmem_limit_bytes=36 << 20),
        name="first",
    )(*(pltpu.with_memory_space_constraint(v, pltpu.HBM) for v in (positions, tokens, gain, w_q, w_k, w_v, rows_k, rows_v)))


def combine(mine, theirs):
    left = lax.broadcasted_iota(jnp.int32, mine[2].shape, mine[2].ndim - 1) < LANES // 2
    axis = mine[2].ndim - 1

    def unpack(stats):
        turned = pltpu.roll(stats, LANES // 2, axis)
        return jnp.where(left, stats, turned), jnp.where(left, turned, stats)

    (m_a, l_a), (m_b, l_b) = unpack(mine[2]), unpack(theirs[2])
    top = jnp.maximum(m_a, m_b)
    f_a = jnp.where(m_a == -jnp.inf, 0.0, jnp.exp(m_a - top))
    f_b = jnp.where(m_b == -jnp.inf, 0.0, jnp.exp(m_b - top))
    return mine[0] * f_a + theirs[0] * f_b, mine[1] * f_a + theirs[1] * f_b, top, l_a * f_a + l_b * f_b


def layer_kernel(
    kv_heads, x_hbm, gm_hbm, wo_hbm, wg_hbm, wu_hbm, wd_hbm, ck_hbm, cv_hbm,
    far_ref, q_s, kx_s, vx_s, lim_s, hid_s,
    out_ref, kbuf, vbuf,
    ring, o_s, m_s, l_s, part, rd, sx, rx,
    po, ro, so, yo, hb, act, pm, rm, sm, ym, ob,
    x_ref, gm_ref,
    small_sem, k_sem, v_sem, o_sem, c_sem, send_sem, recv_sem,
):
    rows, width = x_ref.shape
    head_dim = ring.shape[2]
    heads = far_ref.shape[0]
    kvs = kv_heads
    group = heads // kvs
    per_slot, qrows = 2 * kvs, 2 * heads
    key_rows = ck_hbm.shape[1]
    local_slots = key_rows // per_slot
    slices = key_rows // LANES
    n_blocks = rows // 2 // BLOCK
    mine_h = heads // 2
    half, quarter = rows // 2, rows // 4
    sp, tp = lax.axis_index("sp"), lax.axis_index("tp")
    x, k = sp // 2, lax.rem(sp, 2)
    d_dev, x_dev, y_dev = {"sp": x * 2 + 1 - k}, {"sp": (1 - x) * 2 + k}, {"tp": 1 - tp}
    m_cols = act.shape[1]
    span = width // CHUNKS

    barrier = pltpu.get_barrier_semaphore()
    for dev in (d_dev, x_dev, y_dev):
        pl.semaphore_signal(barrier, inc=1, device_id=dev, device_id_type=MESH)

    counter = [0]

    def remote(src, dst, dev):
        n = counter[0]
        counter[0] += 1
        return pltpu.make_async_remote_copy(
            src_ref=src, dst_ref=dst, send_sem=send_sem.at[n], recv_sem=recv_sem.at[n],
            device_id=dev, device_id_type=MESH,
        )

    def in_copies(j):
        near, here = pl.ds(x * half + j * BLOCK, BLOCK), pl.ds(j * BLOCK, BLOCK)
        return (
            pltpu.make_async_copy(ck_hbm.at[near], kbuf.at[here], k_sem.at[j]),
            pltpu.make_async_copy(cv_hbm.at[near], vbuf.at[here], v_sem.at[j]),
        )

    small = [
        pltpu.make_async_copy(src, dst, small_sem.at[i])
        for i, (src, dst) in enumerate(
            ((x_hbm, x_ref), (gm_hbm, gm_ref))
        )
    ]
    for copy in in_copies(0):
        copy.start()

    n_w = 0
    o_rows = mine_h * head_dim
    per_o = width // o_rows
    o_copies = [
        pltpu.make_async_copy(
            wo_hbm.at[pl.ds(k * o_rows, o_rows), pl.ds(c * head_dim, head_dim)],
            ring.at[n_w + c // per_o, pl.ds((c % per_o) * o_rows, o_rows)],
            o_sem.at[c],
        )
        for c in range(width // head_dim)
    ]
    n_gate = m_cols // head_dim
    ring_at = lambda i: (n_w + 2 + i) % SLOTS
    chunks = []
    for c in range(n_gate):
        at = pl.ds(pl.multiple_of(k * m_cols + c * head_dim, LANES), head_dim)
        chunks += [wg_hbm.at[:, at], wu_hbm.at[:, at]]
    for c in range(width // head_dim):
        chunks.append(wd_hbm.at[pl.ds(pl.multiple_of(k * m_cols, LANES), m_cols), pl.ds(c * head_dim, head_dim)])
    chunks = [
        pltpu.make_async_copy(src, ring.at[ring_at(i)], c_sem.at[i]) for i, src in enumerate(chunks)
    ]
    queue = iter(chunks)

    def fetch(n):
        for copy in itertools.islice(queue, n):
            copy.start()

    row = lax.broadcasted_iota(jnp.int32, (qrows, LANES), 0)
    col = lax.broadcasted_iota(jnp.int32, (qrows, LANES), 1)
    half_of_col = (col // kvs) % 2
    fits = (half_of_col == row // heads) & (col % kvs == (row % heads) // group)
    slot_of_col = jnp.where(fits, col // per_slot, FAR)
    low_half = half_of_col == 0
    scale = 1.0 / math.sqrt(head_dim)

    def block_step(j, carry):
        @pl.when(j + AHEAD < n_blocks)
        def _():
            for copy in in_copies(j + AHEAD):
                copy.start()

        for copy in in_copies(j):
            copy.wait()
        first = x * half + j * BLOCK
        at_rows = [pl.ds(pl.multiple_of((first + i) * qrows, qrows), qrows) for i in range(BLOCK)]
        scores = []
        for i in range(BLOCK):
            scores.append(
                lax.dot_general(
                    q_s[at_rows[i], :].astype(BF16), kbuf[j * BLOCK + i], (((1,), (1,)), ((), ())),
                    preferred_element_type=F32,
                )
            )
        probs, news = [], []
        for i in range(BLOCK):
            limit, hidden = lim_s[at_rows[i], :], hid_s[at_rows[i], :]
            fresh = q_s[at_rows[i], :] * kx_s[at_rows[i], :]
            fresh = jnp.sum(fresh + pltpu.roll(fresh, heads, 0), axis=1, keepdims=True) * scale
            fresh = jnp.where(hidden[:, :1] >= 0, fresh, -jnp.inf)
            parts = []
            for t in range(slices):
                own = scores[i][:, t * LANES : (t + 1) * LANES]
                other = pltpu.roll(own, heads, 0)
                other = jnp.where(
                    low_half, pltpu.roll(other, LANES - kvs, 1), pltpu.roll(other, kvs, 1)
                )
                shift = t * (LANES // per_slot)
                ok = (slot_of_col <= limit - shift) & (slot_of_col != hidden - shift)
                parts.append(jnp.where(ok, (own + other) * scale, -jnp.inf))
            top = functools.reduce(jnp.maximum, parts)
            top = jnp.maximum(jnp.max(top, axis=1, keepdims=True), fresh)
            floor = jnp.where(top == -jnp.inf, 0.0, top)
            parts = [jnp.exp(part_t - floor) for part_t in parts]
            new = jnp.exp(fresh - floor)
            total = jnp.sum(functools.reduce(jnp.add, parts), axis=1, keepdims=True) + new
            at = pl.ds(pl.multiple_of((j * BLOCK + i) * qrows, qrows), qrows)
            m_s[at, :] = jnp.broadcast_to(top, (qrows, LANES))
            l_s[at, :] = jnp.broadcast_to(total, (qrows, LANES))
            news.append(new)
            probs.append(jnp.concatenate([part_t.astype(BF16) for part_t in parts], axis=1))
        for i in range(BLOCK):
            at = pl.ds(pl.multiple_of((j * BLOCK + i) * qrows, qrows), qrows)
            o_s[at, :] = (
                jnp.dot(probs[i], vbuf[j * BLOCK + i], preferred_element_type=F32) + news[i] * vx_s[at_rows[i], :]
            )
        return carry

    size = rows // GROUPS
    my_heads, their_heads = pl.ds(k * mine_h, mine_h), pl.ds((1 - k) * mine_h, mine_h)
    spans = [pl.ds(g * size, size) for g in range(GROUPS)]
    near = GROUPS // 2
    sources = [far_ref.at[their_heads, :, spans[g]] for g in range(near)]
    sources += [part.at[their_heads, :, spans[g]] for g in range(near)]
    swaps_a = [remote(src, rd.at[:, :, at], d_dev) for src, at in zip(sources, spans)]
    cross_a = [remote(sx.at[:, :, at], rx.at[:, :, at], x_dev) for at in spans[: GROUPS // 2]]
    left = lax.broadcasted_iota(jnp.int32, (mine_h, size, LANES), 2) < LANES // 2
    joined = [None] * GROUPS

    def publish(g):
        at = spans[g - near]
        for h in range(heads):
            lo = pl.ds((g - near) * size * qrows + h, size, stride=qrows)
            hi = pl.ds((g - near) * size * qrows + heads + h, size, stride=qrows)
            part[h, 0, at], part[h, 1, at] = o_s[lo, :], o_s[hi, :]
            part[h, 2, at] = jnp.where(left[0], m_s[lo, :], l_s[lo, :])
        swaps_a[g].start()

    def chip(g):
        swaps_a[g].wait_recv()
        at = spans[g]
        here, local = (far_ref, at) if g < near else (part, spans[g - near])
        o_a, o_b, m, l = combine(
            [here[my_heads, i, local] for i in range(3)], [rd[:, i, at] for i in range(3)]
        )
        value = [o_a, o_b, jnp.where(left, m, l)]
        if g < GROUPS // 2:
            for i in range(3):
                sx[:, i, at] = value[i]
            cross_a[g].start()
        joined[g] = value

    pl.semaphore_wait(barrier, 3)
    for g in range(near):
        swaps_a[g].start()
    for j in range(1, AHEAD):
        for copy in in_copies(j):
            copy.start()
    for copy in small:
        copy.start()
    step = n_blocks // GROUPS
    for g in range(GROUPS):
        lax.fori_loop(g * step, (g + 1) * step, block_step, 0)
        if g == 0:
            for n in range(near):
                chip(n)
        elif g == 1:
            publish(near)
        elif g == 2:
            chip(near)
            for copy in o_copies:
                copy.start()
    publish(GROUPS - 1)
    fetch(3)
    chip(GROUPS - 1)
    pieces = []
    for g in range(GROUPS // 2):
        cross_a[g].wait_recv()
        o_a, o_b, _, l = combine(joined[GROUPS // 2 + g], [rx[:, i, spans[g]] for i in range(3)])
        o_a, o_b = (o_a / l).astype(BF16), (o_b / l).astype(BF16)
        pieces.append(jnp.concatenate([v[h] for h in range(mine_h) for v in (o_a, o_b)], axis=-1))
    attended = jnp.concatenate(pieces, axis=0)
    for copy in small:
        copy.wait()

    own, other = pl.ds(k * quarter, quarter), pl.ds((1 - k) * quarter, quarter)
    my_rows = pl.ds(pl.multiple_of(x * half + k * quarter, quarter), quarter)
    x_peer_rows = pl.ds(pl.multiple_of((1 - x) * half + k * quarter, quarter), quarter)
    cols = [pl.ds(c * span, span) for c in range(CHUNKS)]
    per_span = span // head_dim

    def staged(dot, swap, cross, *rest):
        for c in range(CHUNKS + 2):
            if c < CHUNKS:
                dot(c)
            if c >= 2:
                swap(c - 2)
        for c in range(CHUNKS):
            cross(c)
        for c in range(CHUNKS + len(rest) - 1):
            for s, stage in enumerate(rest):
                if 0 <= c - s < CHUNKS:
                    stage(c - s)

    swaps = [remote(po.at[other, c], ro.at[:, c], d_dev) for c in cols]
    crosses = [remote(so.at[:, c], yo.at[:, c], y_dev) for c in cols]
    gathers = [remote(hb.at[own, c], hb.at[own, c], d_dev) for c in cols]

    def o_dot(c):
        for i in range(c * per_span, (c + 1) * per_span):
            o_copies[i].wait()
            w = ring[n_w + i // per_o, (i % per_o) * o_rows : (i % per_o + 1) * o_rows, :]
            po[:, i * head_dim : (i + 1) * head_dim] = jnp.dot(attended, w, preferred_element_type=F32)
        swaps[c].start()

    def o_swap(c):
        swaps[c].wait_recv()
        so[:, cols[c]] = po[own, cols[c]] + ro[:, cols[c]]
        crosses[c].start()
        fetch(3)

    def o_cross(c):
        crosses[c].wait_recv()
        total = so[:, cols[c]] + yo[:, cols[c]]
        hb[own, cols[c]] = (x_ref[my_rows, cols[c]].astype(F32) + total).astype(BF16).astype(F32)
        gathers[c].start()

    def o_gather(c):
        gathers[c].wait_recv()

    staged(o_dot, o_swap, o_cross, o_gather)

    normed_m = rms_norm(hb[...], gm_ref[...])
    for c in range(n_gate):
        chunks[2 * c].wait()
        chunks[2 * c + 1].wait()
        gate = jnp.dot(normed_m, ring[ring_at(2 * c)], preferred_element_type=F32)
        up = jnp.dot(normed_m, ring[ring_at(2 * c + 1)], preferred_element_type=F32)
        act[:, c * head_dim : (c + 1) * head_dim] = (jax.nn.silu(gate) * up).astype(BF16)
        fetch(2)

    swaps_m = [remote(pm.at[other, c], rm.at[:, c], d_dev) for c in cols]
    crosses_m = [remote(sm.at[:, c], ym.at[:, c], y_dev) for c in cols]
    to_core = [remote(ob.at[my_rows, c], ob.at[my_rows, c], d_dev) for c in cols]
    to_x = [remote(ob.at[my_rows, c], ob.at[my_rows, c], x_dev) for c in cols]
    onward = [remote(ob.at[x_peer_rows, c], ob.at[x_peer_rows, c], d_dev) for c in cols]

    def m_dot(c):
        for i in range(c * per_span, (c + 1) * per_span):
            chunks[2 * n_gate + i].wait()
            pm[:, i * head_dim : (i + 1) * head_dim] = jnp.dot(
                act[...], ring[ring_at(2 * n_gate + i)], preferred_element_type=F32
            )
        swaps_m[c].start()

    def m_swap(c):
        swaps_m[c].wait_recv()
        sm[:, cols[c]] = pm[own, cols[c]] + rm[:, cols[c]]
        crosses_m[c].start()

    def m_cross(c):
        crosses_m[c].wait_recv()
        total = sm[:, cols[c]] + ym[:, cols[c]]
        ob[my_rows, cols[c]] = (hb[own, cols[c]] + total).astype(BF16).astype(F32)
        to_x[c].start()
        to_core[c].start()

    def m_gather(c):
        to_x[c].wait_recv()
        onward[c].start()

    def m_last(c):
        to_core[c].wait_recv()
        onward[c].wait_recv()
        out_ref[:, cols[c]] = ob[:, cols[c]].astype(BF16)

    staged(m_dot, m_swap, m_cross, m_gather, m_last)
    for copy in [*swaps_a, *cross_a, *swaps, *crosses, *gathers, *swaps_m, *crosses_m, *to_core, *to_x, *onward]:
        copy.wait_send()


def layer(tokens, gain, w_o, w_gate, w_up, w_down, rows_k, rows_v, kvs, carried):
    rows, width = tokens.shape
    head_dim = 2 * LANES
    heads = carried[0].shape[0]
    qrows = 2 * heads
    half, quarter = rows // 2, rows // 4
    cut = w_gate.shape[1] // 2
    n_blocks = half // BLOCK
    vmem = pl.BlockSpec(memory_space=pltpu.VMEM)
    hbm = pl.BlockSpec(memory_space=pltpu.HBM)
    flat = lambda n: pltpu.VMEM((n, width), F32)
    stats = lambda h, n: pltpu.VMEM((h, 3, n, LANES), F32)
    dma = lambda n: pltpu.SemaphoreType.DMA((n,))
    n_remote = GROUPS + GROUPS // 2 + 8 * CHUNKS
    args = (tokens, gain, w_o, w_gate, w_up, w_down, rows_k, rows_v)
    shape = (half, *rows_k.shape[1:])
    return pl.pallas_call(
        functools.partial(layer_kernel, kvs),
        out_shape=(
            pltpu.VMEM(tokens.shape, BF16),
            pltpu.VMEM(shape, BF16),
            pltpu.VMEM(shape, BF16),
        ),
        in_specs=[hbm] * len(args) + [vmem] * len(carried),
        out_specs=(vmem,) * 3,
        scratch_shapes=[
            pltpu.VMEM((SLOTS, width, head_dim), BF16),
            *(pltpu.VMEM((half * qrows, LANES), F32) for _ in range(3)),
            stats(heads, half), stats(heads // 2, rows), stats(heads // 2, half), stats(heads // 2, half),
            flat(half), flat(quarter), flat(quarter), flat(quarter), flat(half),
            pltpu.VMEM((half, cut), BF16),
            flat(half), flat(quarter), flat(quarter), flat(quarter), flat(rows),
            pltpu.VMEM(tokens.shape, BF16),
            pltpu.VMEM(gain.shape, BF16),
            dma(2), dma(n_blocks), dma(n_blocks), dma(width // head_dim),
            dma(2 * (cut // head_dim) + width // head_dim), dma(n_remote), dma(n_remote),
        ],
        compiler_params=pltpu.CompilerParams(
            vmem_limit_bytes=LAYER_VMEM << 20, collective_id=0, has_side_effects=True
        ),
        name="layer",
    )(*(pltpu.with_memory_space_constraint(v, pltpu.HBM) for v in args), *carried)


def write_kernel(pos_hbm, t_ref, kn_s, vn_s, _bk, _bv, _k, _v, out_ref, nk_hbm, nv_hbm, kbuf, vbuf, pos, sem, tile_sem, pos_sem):
    rows, key_rows, _ = kbuf.shape
    per_slot = 4
    local_slots = key_rows // per_slot
    slots = local_slots * lax.axis_size("sp")
    base = lax.axis_index("sp") * local_slots
    start = lax.axis_index("sp") // 2 * rows
    per_tile = 16 // per_slot
    n_blocks = rows // BLOCK
    tile_row = lax.broadcasted_iota(jnp.int32, (16, LANES), 0) // per_slot

    def copies(j):
        here, near = pl.ds(j * BLOCK, BLOCK), pl.ds(start + j * BLOCK, BLOCK)
        return (
            pltpu.make_async_copy(kbuf.at[here], nk_hbm.at[near], sem.at[0, j]),
            pltpu.make_async_copy(vbuf.at[here], nv_hbm.at[near], sem.at[1, j]),
        )

    def target(b):
        local = lax.rem(pos[b], slots) - base
        owned = (local >= 0) & (local < local_slots)
        safe = jnp.where(owned, local, 0)
        hit = jnp.where(owned, lax.rem(safe, per_tile), -1)
        return hit, pl.ds(pl.multiple_of((safe // per_tile) * 16, 16), 16)

    def tile_copies(n):
        at = target(start + n)[1]
        return (
            pltpu.make_async_copy(kbuf.at[n, at], nk_hbm.at[start + n, at], tile_sem.at[0]),
            pltpu.make_async_copy(vbuf.at[n, at], nv_hbm.at[start + n, at], tile_sem.at[1]),
        )

    def patch(n):
        b = start + n
        hit, at = target(b)
        for buf, new in ((kbuf, kn_s), (vbuf, vn_s)):
            fresh = new[pl.ds(pl.multiple_of(b * 16, 16), 16), :]
            buf[n, at, :] = jnp.where(tile_row == hit, fresh, buf[n, at, :].astype(F32)).astype(BF16)

    pos_copy = pltpu.make_async_copy(pos_hbm, pos, pos_sem)
    pos_copy.start()
    for j in range(EARLY):
        for copy in copies(j):
            copy.start()
    out_ref[...] = t_ref[...]
    pos_copy.wait()
    for j in range(EARLY, n_blocks + 1):
        if j < n_blocks:
            for i in range(BLOCK):
                patch(j * BLOCK + i)
        if j > EARLY:
            for copy in copies(j - 1):
                copy.start()
    for j in range(EARLY):
        for copy in copies(j):
            copy.wait()
        for i in range(BLOCK):
            patch(j * BLOCK + i)
        if j:
            for i in range(BLOCK):
                for copy in tile_copies((j - 1) * BLOCK + i):
                    copy.start()
    for i in range(BLOCK):
        for copy in tile_copies((EARLY - 1) * BLOCK + i):
            copy.start()
    for j in range(EARLY, n_blocks):
        for copy in copies(j):
            copy.wait()
    for n in range(EARLY * BLOCK):
        for copy in tile_copies(n):
            copy.wait()


def write(positions, layer_out, fresh_k, fresh_v, buf_k, buf_v, new_k, new_v):
    vmem = pl.BlockSpec(memory_space=pltpu.VMEM)
    hbm = pl.BlockSpec(memory_space=pltpu.HBM)
    return pl.pallas_call(
        write_kernel,
        out_shape=(
            *(jax.ShapeDtypeStruct(v.shape, BF16) for v in (layer_out, new_k, new_v)),
            pltpu.VMEM(buf_k.shape, BF16),
            pltpu.VMEM(buf_v.shape, BF16),
        ),
        in_specs=[hbm] + [vmem] * 5 + [hbm] * 2,
        out_specs=(vmem, hbm, hbm, vmem, vmem),
        input_output_aliases={4: 3, 5: 4, 6: 1, 7: 2},
        scratch_shapes=[
            pltpu.SMEM(positions.shape, jnp.int32),
            pltpu.SemaphoreType.DMA((2, buf_k.shape[0] // BLOCK)),
            pltpu.SemaphoreType.DMA((2,)),
            pltpu.SemaphoreType.DMA,
        ],
        compiler_params=pltpu.CompilerParams(vmem_limit_bytes=LAYER_VMEM << 20),
        name="write",
    )(pltpu.with_memory_space_constraint(positions, pltpu.HBM), layer_out, fresh_k, fresh_v, buf_k, buf_v, new_k, new_v)[:3]


def to_rows(cache):
    b, s, kv, d = cache.shape
    return cache.reshape(b, s, kv, d // LANES, LANES).transpose(0, 1, 3, 2, 4).reshape(b, -1, LANES)


def from_rows(rows, shape):
    b, s, kv, d = shape
    return rows.reshape(b, s, d // LANES, kv, LANES).transpose(0, 1, 3, 2, 4).reshape(shape)


def solution(mesh):
    cache_spec = P("dp", "sp", "tp", None)
    row_spec = P("dp", None)
    col_spec = P(None, "tp")
    in_specs = (row_spec, P("dp"), cache_spec, cache_spec, P(None), col_spec, col_spec, col_spec, P("tp", None), P(None), col_spec, col_spec, P("tp", None))
    out_specs = (row_spec, cache_spec, cache_spec)

    def local_step(tokens, positions, cache_k, cache_v, attn_gain, w_q, w_k, w_v, w_o, mlp_gain, w_gate, w_up, w_down):
        old_k, old_v = to_rows(cache_k), to_rows(cache_v)
        far, rows_k, rows_v, *carried, fresh_k, fresh_v = first_half(
            positions, tokens, attn_gain, w_q, w_k, w_v, old_k, old_v
        )
        out, buf_k, buf_v = layer(
            tokens, mlp_gain, w_o, w_gate, w_up, w_down, old_k, old_v, cache_k.shape[2], (far, *carried)
        )
        layer_out, rows_k, rows_v = write(positions, out, fresh_k, fresh_v, buf_k, buf_v, rows_k, rows_v)
        new_k = from_rows(rows_k, cache_k.shape)
        new_v = from_rows(rows_v, cache_v.shape)
        return layer_out, new_k, new_v

    return jax.shard_map(local_step, mesh=mesh, in_specs=in_specs, out_specs=out_specs, check_vma=False)
```

```python
import functools
import itertools
import math

import jax
import jax.numpy as jnp
from jax import lax
from jax.experimental import pallas as pl
from jax.experimental.pallas import tpu as pltpu
from jax.sharding import PartitionSpec as P

NORM_EPS = 1e-5
ROPE_THETA = 10000.0
LANES = 128
F32 = jnp.float32
BF16 = jnp.bfloat16
FAR = 1 << 28
BLOCK = 4
EARLY = 3
EAGER = (2, 6)
FIRST = 4
SLOTS = 22
LAYER_VMEM = 35
CHUNKS = 5
GROUPS = 4
MESH = pl.DeviceIdType.MESH


def rms_norm(values, gain):
    wide = values.astype(F32)
    inv_rms = lax.rsqrt(jnp.mean(wide * wide, axis=-1, keepdims=True) + NORM_EPS)
    return (wide * inv_rms * gain.astype(F32)).astype(BF16)


def first_kernel(
    pos_hbm, x_hbm, gain_hbm, wq_hbm, wk_hbm, wv_hbm, ck_hbm, cv_hbm,
    part_ref, nk_hbm, nv_hbm, q_s, kx_s, vx_s, lim_s, hid_s, kn_s, vn_s,
    wbuf, kbuf, vbuf, ang_s, o_s, m_s, l_s,
    pos, x_ref, gain_ref, w_sem, k_sem, v_sem, out_sem, x_sem,
):
    rows = x_ref.shape[0]
    head_dim = 2 * LANES
    heads = wq_hbm.shape[1] // head_dim
    kvs = wk_hbm.shape[1] // head_dim
    group = heads // kvs
    per_slot = 2 * kvs
    qrows = 2 * heads
    key_rows = ck_hbm.shape[1]
    local_slots = key_rows // per_slot
    slots = local_slots * lax.axis_size("sp")
    slices = key_rows // LANES
    half = rows // 2
    n_blocks = half // BLOCK
    start = (1 - lax.axis_index("sp") // 2) * half
    base = lax.axis_index("sp") * local_slots

    def w_copy(n):
        src, col = (
            (wk_hbm, n) if n < kvs else (wv_hbm, n - kvs) if n < 2 * kvs else (wq_hbm, n - 2 * kvs)
        )
        return pltpu.make_async_copy(src.at[:, pl.ds(col * head_dim, head_dim)], wbuf.at[n], w_sem.at[n])

    def in_copies(j):
        far, here = pl.ds(start + j * BLOCK, BLOCK), pl.ds(j * BLOCK, BLOCK)
        return (
            pltpu.make_async_copy(ck_hbm.at[far], kbuf.at[here], k_sem.at[j]),
            pltpu.make_async_copy(cv_hbm.at[far], vbuf.at[here], v_sem.at[j]),
        )

    def out_copies(j):
        far, here = pl.ds(start + j * BLOCK, BLOCK), pl.ds(j * BLOCK, BLOCK)
        return (
            pltpu.make_async_copy(kbuf.at[here], nk_hbm.at[far], out_sem.at[0]),
            pltpu.make_async_copy(vbuf.at[here], nv_hbm.at[far], out_sem.at[1]),
        )

    small = [
        pltpu.make_async_copy(src, dst, x_sem.at[i])
        for i, (src, dst) in enumerate(((pos_hbm, pos), (x_hbm, x_ref), (gain_hbm, gain_ref)))
    ]
    for copy in small:
        copy.start()
    n_w = heads + 2 * kvs
    for n in range(n_w // 2):
        w_copy(n).start()

    lane = lax.broadcasted_iota(jnp.int32, (1, LANES), 1).astype(F32)
    freq = jnp.exp2(lane * (-math.log2(ROPE_THETA) / LANES))

    for copy in small:
        copy.wait()
    for n in range(n_w // 2, n_w):
        w_copy(n).start()
    for j in range(FIRST):
        for copy in in_copies(j):
            copy.start()

    def angle_row(b, carry):
        p = pos[b]
        ang_s[pl.ds(b, 1), :] = freq * p.astype(F32)
        local = lax.rem(p, slots) - base
        owned = (local >= 0) & (local < local_slots)
        span = pl.ds(pl.multiple_of(b * qrows, qrows), qrows)
        lim_s[span, :] = jnp.full((qrows, LANES), jnp.where(p >= slots - 1, FAR // 2, p) - base, jnp.int32)
        hid_s[span, :] = jnp.full((qrows, LANES), jnp.where(owned, local, -FAR), jnp.int32)
        return carry

    lax.fori_loop(0, rows, angle_row, 0, unroll=8)
    angles = ang_s[...]
    cos_t, sin_t = jnp.cos(angles), jnp.sin(angles)
    normed = rms_norm(x_ref[...], gain_ref[...])

    for n in range(n_w):
        w_copy(n).wait()
        if FIRST + n < n_blocks:
            for copy in in_copies(FIRST + n):
                copy.start()
        lin = jnp.dot(normed, wbuf[n], preferred_element_type=F32)
        first, second = lin[:, :LANES], lin[:, LANES:]
        if not kvs <= n < 2 * kvs:
            first, second = first * cos_t - second * sin_t, second * cos_t + first * sin_t
        first, second = first.astype(BF16).astype(F32), second.astype(BF16).astype(F32)
        if n >= 2 * kvs:
            h = n - 2 * kvs
            q_s[pl.ds(h, rows, stride=qrows), :] = first
            q_s[pl.ds(heads + h, rows, stride=qrows), :] = second
        else:
            dst, tile, kv = (kn_s, kx_s, n) if n < kvs else (vn_s, vx_s, n - kvs)
            for rep in range(16 // per_slot):
                dst[pl.ds(rep * per_slot + kv, rows, stride=16), :] = first
                dst[pl.ds(rep * per_slot + kvs + kv, rows, stride=16), :] = second
            for g in range(group):
                tile[pl.ds(kv * group + g, rows, stride=qrows), :] = first
                tile[pl.ds(heads + kv * group + g, rows, stride=qrows), :] = second

    row = lax.broadcasted_iota(jnp.int32, (qrows, LANES), 0)
    col = lax.broadcasted_iota(jnp.int32, (qrows, LANES), 1)
    half_of_col = (col // kvs) % 2
    fits = (half_of_col == row // heads) & (col % kvs == (row % heads) // group)
    slot_of_col = jnp.where(fits, col // per_slot, FAR)
    low_half = half_of_col == 0
    patch_row = lax.broadcasted_iota(jnp.int32, (16, LANES), 0) // per_slot
    scale = 1.0 / math.sqrt(head_dim)

    def block_step(j, carry):
        for copy in in_copies(j):
            copy.wait()
        for i in range(BLOCK):
            n = j * BLOCK + i
            b = start + n
            local = lax.rem(pos[b], slots) - base
            owned = (local >= 0) & (local < local_slots)
            safe = jnp.where(owned, local, 0)
            hit = jnp.where(owned, lax.rem(safe, 16 // per_slot), -1)
            span = pl.ds(pl.multiple_of((safe // (16 // per_slot)) * 16, 16), 16)
            for buf, new in ((kbuf, kn_s), (vbuf, vn_s)):
                old = buf[n, span, :].astype(F32)
                fresh = new[pl.ds(pl.multiple_of(b * 16, 16), 16), :]
                buf[n, span, :] = jnp.where(patch_row == hit, fresh, old).astype(BF16)
        scores = []
        for i in range(BLOCK):
            b = start + j * BLOCK + i
            q = q_s[pl.ds(pl.multiple_of(b * qrows, qrows), qrows), :].astype(BF16)
            scores.append(
                lax.dot_general(q, kbuf[j * BLOCK + i], (((1,), (1,)), ((), ())), preferred_element_type=F32)
            )
        probs = []
        for i in range(BLOCK):
            n = j * BLOCK + i
            p = pos[start + n]
            limit = jnp.where(p >= slots - 1, FAR // 2, p) - base
            parts = []
            for t in range(slices):
                own = scores[i][:, t * LANES : (t + 1) * LANES]
                other = pltpu.roll(own, heads, 0)
                other = jnp.where(
                    low_half, pltpu.roll(other, LANES - kvs, 1), pltpu.roll(other, kvs, 1)
                )
                ok = slot_of_col <= limit - t * (LANES // per_slot)
                parts.append(jnp.where(ok, (own + other) * scale, -jnp.inf))
            top = functools.reduce(jnp.maximum, parts)
            top = jnp.max(top, axis=1, keepdims=True)
            floor = jnp.where(top == -jnp.inf, 0.0, top)
            parts = [jnp.exp(part - floor) for part in parts]
            total = jnp.sum(functools.reduce(jnp.add, parts), axis=1, keepdims=True)
            span = pl.ds(pl.multiple_of(n * qrows, qrows), qrows)
            m_s[span, :] = jnp.broadcast_to(top, (qrows, LANES))
            l_s[span, :] = jnp.broadcast_to(total, (qrows, LANES))
            probs.append(jnp.concatenate([part.astype(BF16) for part in parts], axis=1))
        for i in range(BLOCK):
            n = j * BLOCK + i
            span = pl.ds(pl.multiple_of(n * qrows, qrows), qrows)
            o_s[span, :] = jnp.dot(probs[i], vbuf[n], preferred_element_type=F32)
        for copy in out_copies(j):
            copy.start()
        return carry

    lax.fori_loop(0, n_blocks, block_step, 0)

    left = lax.broadcasted_iota(jnp.int32, (half, LANES), 1) < LANES // 2
    for h in range(heads):
        lo, hi = pl.ds(h, half, stride=qrows), pl.ds(heads + h, half, stride=qrows)
        part_ref[h, 0], part_ref[h, 1] = o_s[lo, :], o_s[hi, :]
        part_ref[h, 2] = jnp.where(left, m_s[lo, :], l_s[lo, :])
    for j in range(n_blocks):
        for copy in out_copies(j):
            copy.wait()


def first_half(positions, tokens, gain, w_q, w_k, w_v, rows_k, rows_v):
    rows, width = tokens.shape
    head_dim = 2 * LANES
    heads = w_q.shape[1] // head_dim
    kvs = w_k.shape[1] // head_dim
    qrows = 2 * heads
    vmem = pl.BlockSpec(memory_space=pltpu.VMEM)
    hbm = pl.BlockSpec(memory_space=pltpu.HBM)
    n_blocks = rows // 2 // BLOCK
    tile = lambda n: pltpu.VMEM((rows * n, LANES), F32)
    return pl.pallas_call(
        first_kernel,
        out_shape=(
            pltpu.VMEM((heads, 3, rows // 2, LANES), F32),
            jax.ShapeDtypeStruct(rows_k.shape, BF16),
            jax.ShapeDtypeStruct(rows_v.shape, BF16),
            tile(qrows), tile(qrows), tile(qrows),
            *(pltpu.VMEM((rows * qrows, LANES), jnp.int32) for _ in range(2)),
            tile(16), tile(16),
        ),
        in_specs=[hbm] * 8,
        out_specs=(vmem, hbm, hbm) + (vmem,) * 7,
        scratch_shapes=[
            pltpu.VMEM((heads + 2 * kvs, width, head_dim), BF16),
            pltpu.VMEM((rows // 2, *rows_k.shape[1:]), BF16),
            pltpu.VMEM((rows // 2, *rows_v.shape[1:]), BF16),
            tile(1),
            pltpu.VMEM((rows // 2 * qrows, LANES), F32),
            pltpu.VMEM((rows // 2 * qrows, LANES), F32),
            pltpu.VMEM((rows // 2 * qrows, LANES), F32),
            pltpu.SMEM((rows,), jnp.int32),
            pltpu.VMEM(tokens.shape, BF16),
            pltpu.VMEM(gain.shape, BF16),
            pltpu.SemaphoreType.DMA((heads + 2 * kvs,)),
            pltpu.SemaphoreType.DMA((n_blocks,)),
            pltpu.SemaphoreType.DMA((n_blocks,)),
            pltpu.SemaphoreType.DMA((2,)),
            pltpu.SemaphoreType.DMA((3,)),
        ],
        compiler_params=pltpu.CompilerParams(vmem_limit_bytes=36 << 20),
        name="first",
    )(*(pltpu.with_memory_space_constraint(v, pltpu.HBM) for v in (positions, tokens, gain, w_q, w_k, w_v, rows_k, rows_v)))


def combine(mine, theirs):
    left = lax.broadcasted_iota(jnp.int32, mine[2].shape, mine[2].ndim - 1) < LANES // 2
    axis = mine[2].ndim - 1

    def unpack(stats):
        turned = pltpu.roll(stats, LANES // 2, axis)
        return jnp.where(left, stats, turned), jnp.where(left, turned, stats)

    (m_a, l_a), (m_b, l_b) = unpack(mine[2]), unpack(theirs[2])
    top = jnp.maximum(m_a, m_b)
    f_a = jnp.where(m_a == -jnp.inf, 0.0, jnp.exp(m_a - top))
    f_b = jnp.where(m_b == -jnp.inf, 0.0, jnp.exp(m_b - top))
    return mine[0] * f_a + theirs[0] * f_b, mine[1] * f_a + theirs[1] * f_b, top, l_a * f_a + l_b * f_b


def layer_kernel(
    kv_heads, x_hbm, gm_hbm, wo_hbm, wg_hbm, wu_hbm, wd_hbm, ck_hbm, cv_hbm,
    far_ref, q_s, kx_s, vx_s, lim_s, hid_s,
    out_ref, kbuf, vbuf,
    ring, o_s, m_s, l_s, part, rd, sx, rx,
    po, ro, so, yo, hb, act, pm, rm, sm, ym, ob,
    x_ref, gm_ref,
    small_sem, k_sem, v_sem, o_sem, c_sem, send_sem, recv_sem,
):
    rows, width = x_ref.shape
    head_dim = ring.shape[2]
    heads = far_ref.shape[0]
    kvs = kv_heads
    group = heads // kvs
    per_slot, qrows = 2 * kvs, 2 * heads
    key_rows = ck_hbm.shape[1]
    local_slots = key_rows // per_slot
    slices = key_rows // LANES
    n_blocks = rows // 2 // BLOCK
    mine_h = heads // 2
    half, quarter = rows // 2, rows // 4
    sp, tp = lax.axis_index("sp"), lax.axis_index("tp")
    x, k = sp // 2, lax.rem(sp, 2)
    d_dev, x_dev, y_dev = {"sp": x * 2 + 1 - k}, {"sp": (1 - x) * 2 + k}, {"tp": 1 - tp}
    m_cols = act.shape[1]
    span = width // CHUNKS

    barrier = pltpu.get_barrier_semaphore()
    for dev in (d_dev, x_dev, y_dev):
        pl.semaphore_signal(barrier, inc=1, device_id=dev, device_id_type=MESH)

    counter = [0]

    def remote(src, dst, dev):
        n = counter[0]
        counter[0] += 1
        return pltpu.make_async_remote_copy(
            src_ref=src, dst_ref=dst, send_sem=send_sem.at[n], recv_sem=recv_sem.at[n],
            device_id=dev, device_id_type=MESH,
        )

    def in_copies(j):
        near, here = pl.ds(x * half + j * BLOCK, BLOCK), pl.ds(j * BLOCK, BLOCK)
        return (
            pltpu.make_async_copy(ck_hbm.at[near], kbuf.at[here], k_sem.at[j]),
            pltpu.make_async_copy(cv_hbm.at[near], vbuf.at[here], v_sem.at[j]),
        )

    small = [
        pltpu.make_async_copy(src, dst, small_sem.at[i])
        for i, (src, dst) in enumerate(
            ((x_hbm, x_ref), (gm_hbm, gm_ref))
        )
    ]
    def read(blocks):
        for j in blocks:
            for copy in in_copies(j):
                copy.start()

    read(range(EAGER[0]))

    n_w = 0
    o_rows = mine_h * head_dim
    per_o = width // o_rows
    o_copies = [
        pltpu.make_async_copy(
            wo_hbm.at[pl.ds(k * o_rows, o_rows), pl.ds(c * head_dim, head_dim)],
            ring.at[n_w + c // per_o, pl.ds((c % per_o) * o_rows, o_rows)],
            o_sem.at[c],
        )
        for c in range(width // head_dim)
    ]
    n_gate = m_cols // head_dim
    ring_at = lambda i: (n_w + 2 + i) % SLOTS
    chunks = []
    for c in range(n_gate):
        at = pl.ds(pl.multiple_of(k * m_cols + c * head_dim, LANES), head_dim)
        chunks += [wg_hbm.at[:, at], wu_hbm.at[:, at]]
    for c in range(width // head_dim):
        chunks.append(wd_hbm.at[pl.ds(pl.multiple_of(k * m_cols, LANES), m_cols), pl.ds(c * head_dim, head_dim)])
    chunks = [
        pltpu.make_async_copy(src, ring.at[ring_at(i)], c_sem.at[i]) for i, src in enumerate(chunks)
    ]
    queue = iter(chunks)

    def fetch(n):
        for copy in itertools.islice(queue, n):
            copy.start()

    row = lax.broadcasted_iota(jnp.int32, (qrows, LANES), 0)
    col = lax.broadcasted_iota(jnp.int32, (qrows, LANES), 1)
    half_of_col = (col // kvs) % 2
    fits = (half_of_col == row // heads) & (col % kvs == (row % heads) // group)
    slot_of_col = jnp.where(fits, col // per_slot, FAR)
    low_half = half_of_col == 0
    scale = 1.0 / math.sqrt(head_dim)

    def block_step(j, carry):
        for copy in in_copies(j):
            copy.wait()
        first = x * half + j * BLOCK
        at_rows = [pl.ds(pl.multiple_of((first + i) * qrows, qrows), qrows) for i in range(BLOCK)]
        scores = []
        for i in range(BLOCK):
            scores.append(
                lax.dot_general(
                    q_s[at_rows[i], :].astype(BF16), kbuf[j * BLOCK + i], (((1,), (1,)), ((), ())),
                    preferred_element_type=F32,
                )
            )
        probs, news = [], []
        for i in range(BLOCK):
            limit, hidden = lim_s[at_rows[i], :], hid_s[at_rows[i], :]
            fresh = q_s[at_rows[i], :] * kx_s[at_rows[i], :]
            fresh = jnp.sum(fresh + pltpu.roll(fresh, heads, 0), axis=1, keepdims=True) * scale
            fresh = jnp.where(hidden[:, :1] >= 0, fresh, -jnp.inf)
            parts = []
            for t in range(slices):
                own = scores[i][:, t * LANES : (t + 1) * LANES]
                other = pltpu.roll(own, heads, 0)
                other = jnp.where(
                    low_half, pltpu.roll(other, LANES - kvs, 1), pltpu.roll(other, kvs, 1)
                )
                shift = t * (LANES // per_slot)
                ok = (slot_of_col <= limit - shift) & (slot_of_col != hidden - shift)
                parts.append(jnp.where(ok, (own + other) * scale, -jnp.inf))
            top = functools.reduce(jnp.maximum, parts)
            top = jnp.maximum(jnp.max(top, axis=1, keepdims=True), fresh)
            floor = jnp.where(top == -jnp.inf, 0.0, top)
            parts = [jnp.exp(part_t - floor) for part_t in parts]
            new = jnp.exp(fresh - floor)
            total = jnp.sum(functools.reduce(jnp.add, parts), axis=1, keepdims=True) + new
            at = pl.ds(pl.multiple_of((j * BLOCK + i) * qrows, qrows), qrows)
            m_s[at, :] = jnp.broadcast_to(top, (qrows, LANES))
            l_s[at, :] = jnp.broadcast_to(total, (qrows, LANES))
            news.append(new)
            probs.append(jnp.concatenate([part_t.astype(BF16) for part_t in parts], axis=1))
        for i in range(BLOCK):
            at = pl.ds(pl.multiple_of((j * BLOCK + i) * qrows, qrows), qrows)
            o_s[at, :] = (
                jnp.dot(probs[i], vbuf[j * BLOCK + i], preferred_element_type=F32) + news[i] * vx_s[at_rows[i], :]
            )
        return carry

    size = rows // GROUPS
    my_heads, their_heads = pl.ds(k * mine_h, mine_h), pl.ds((1 - k) * mine_h, mine_h)
    spans = [pl.ds(g * size, size) for g in range(GROUPS)]
    near = GROUPS // 2
    sources = [far_ref.at[their_heads, :, spans[g]] for g in range(near)]
    sources += [part.at[their_heads, :, spans[g]] for g in range(near)]
    swaps_a = [remote(src, rd.at[:, :, at], d_dev) for src, at in zip(sources, spans)]
    cross_a = [remote(sx.at[:, :, at], rx.at[:, :, at], x_dev) for at in spans[: GROUPS // 2]]
    left = lax.broadcasted_iota(jnp.int32, (mine_h, size, LANES), 2) < LANES // 2
    joined = [None] * GROUPS

    def publish(g):
        at = spans[g - near]
        for h in range(heads):
            lo = pl.ds((g - near) * size * qrows + h, size, stride=qrows)
            hi = pl.ds((g - near) * size * qrows + heads + h, size, stride=qrows)
            part[h, 0, at], part[h, 1, at] = o_s[lo, :], o_s[hi, :]
            part[h, 2, at] = jnp.where(left[0], m_s[lo, :], l_s[lo, :])
        swaps_a[g].start()

    def chip(g):
        swaps_a[g].wait_recv()
        at = spans[g]
        here, local = (far_ref, at) if g < near else (part, spans[g - near])
        o_a, o_b, m, l = combine(
            [here[my_heads, i, local] for i in range(3)], [rd[:, i, at] for i in range(3)]
        )
        value = [o_a, o_b, jnp.where(left, m, l)]
        if g < GROUPS // 2:
            for i in range(3):
                sx[:, i, at] = value[i]
            cross_a[g].start()
        joined[g] = value

    pl.semaphore_wait(barrier, 3)
    for g in range(near):
        swaps_a[g].start()
    read(range(*EAGER))
    for copy in small:
        copy.start()
    step = n_blocks // near
    lax.fori_loop(0, step, block_step, 0)
    for g in range(near):
        chip(g)
    read(range(EAGER[1], n_blocks))
    publish(near)
    for copy in o_copies:
        copy.start()
    lax.fori_loop(step, n_blocks, block_step, 0)
    publish(GROUPS - 1)
    fetch(3)
    for g in range(near, GROUPS):
        chip(g)
    pieces = []
    for g in range(GROUPS // 2):
        cross_a[g].wait_recv()
        o_a, o_b, _, l = combine(joined[GROUPS // 2 + g], [rx[:, i, spans[g]] for i in range(3)])
        o_a, o_b = (o_a / l).astype(BF16), (o_b / l).astype(BF16)
        pieces.append(jnp.concatenate([v[h] for h in range(mine_h) for v in (o_a, o_b)], axis=-1))
    attended = jnp.concatenate(pieces, axis=0)
    for copy in small:
        copy.wait()

    own, other = pl.ds(k * quarter, quarter), pl.ds((1 - k) * quarter, quarter)
    my_rows = pl.ds(pl.multiple_of(x * half + k * quarter, quarter), quarter)
    x_peer_rows = pl.ds(pl.multiple_of((1 - x) * half + k * quarter, quarter), quarter)
    cols = [pl.ds(c * span, span) for c in range(CHUNKS)]
    per_span = span // head_dim

    def staged(dot, swap, cross, *rest):
        for c in range(CHUNKS + 2):
            if c < CHUNKS:
                dot(c)
            if c >= 2:
                swap(c - 2)
        for c in range(CHUNKS):
            cross(c)
        for c in range(CHUNKS + len(rest) - 1):
            for s, stage in enumerate(rest):
                if 0 <= c - s < CHUNKS:
                    stage(c - s)

    swaps = [remote(po.at[other, c], ro.at[:, c], d_dev) for c in cols]
    crosses = [remote(so.at[:, c], yo.at[:, c], y_dev) for c in cols]
    gathers = [remote(hb.at[own, c], hb.at[own, c], d_dev) for c in cols]

    def o_dot(c):
        for i in range(c * per_span, (c + 1) * per_span):
            o_copies[i].wait()
            w = ring[n_w + i // per_o, (i % per_o) * o_rows : (i % per_o + 1) * o_rows, :]
            po[:, i * head_dim : (i + 1) * head_dim] = jnp.dot(attended, w, preferred_element_type=F32)
        swaps[c].start()

    def o_swap(c):
        swaps[c].wait_recv()
        so[:, cols[c]] = po[own, cols[c]] + ro[:, cols[c]]
        crosses[c].start()
        fetch(3)

    def o_cross(c):
        crosses[c].wait_recv()
        total = so[:, cols[c]] + yo[:, cols[c]]
        hb[own, cols[c]] = (x_ref[my_rows, cols[c]].astype(F32) + total).astype(BF16).astype(F32)
        gathers[c].start()

    def o_gather(c):
        gathers[c].wait_recv()

    staged(o_dot, o_swap, o_cross, o_gather)

    normed_m = rms_norm(hb[...], gm_ref[...])
    for c in range(n_gate):
        chunks[2 * c].wait()
        chunks[2 * c + 1].wait()
        gate = jnp.dot(normed_m, ring[ring_at(2 * c)], preferred_element_type=F32)
        up = jnp.dot(normed_m, ring[ring_at(2 * c + 1)], preferred_element_type=F32)
        act[:, c * head_dim : (c + 1) * head_dim] = (jax.nn.silu(gate) * up).astype(BF16)
        fetch(2)

    swaps_m = [remote(pm.at[other, c], rm.at[:, c], d_dev) for c in cols]
    crosses_m = [remote(sm.at[:, c], ym.at[:, c], y_dev) for c in cols]
    to_core = [remote(ob.at[my_rows, c], ob.at[my_rows, c], d_dev) for c in cols]
    to_x = [remote(ob.at[my_rows, c], ob.at[my_rows, c], x_dev) for c in cols]
    onward = [remote(ob.at[x_peer_rows, c], ob.at[x_peer_rows, c], d_dev) for c in cols]

    def m_dot(c):
        for i in range(c * per_span, (c + 1) * per_span):
            chunks[2 * n_gate + i].wait()
            pm[:, i * head_dim : (i + 1) * head_dim] = jnp.dot(
                act[...], ring[ring_at(2 * n_gate + i)], preferred_element_type=F32
            )
        swaps_m[c].start()

    def m_swap(c):
        swaps_m[c].wait_recv()
        sm[:, cols[c]] = pm[own, cols[c]] + rm[:, cols[c]]
        crosses_m[c].start()

    def m_cross(c):
        crosses_m[c].wait_recv()
        total = sm[:, cols[c]] + ym[:, cols[c]]
        ob[my_rows, cols[c]] = (hb[own, cols[c]] + total).astype(BF16).astype(F32)
        to_x[c].start()
        to_core[c].start()

    def m_gather(c):
        to_x[c].wait_recv()
        onward[c].start()

    def m_last(c):
        to_core[c].wait_recv()
        onward[c].wait_recv()
        out_ref[:, cols[c]] = ob[:, cols[c]].astype(BF16)

    staged(m_dot, m_swap, m_cross, m_gather, m_last)
    for copy in [*swaps_a, *cross_a, *swaps, *crosses, *gathers, *swaps_m, *crosses_m, *to_core, *to_x, *onward]:
        copy.wait_send()


def layer(tokens, gain, w_o, w_gate, w_up, w_down, rows_k, rows_v, kvs, carried):
    rows, width = tokens.shape
    head_dim = 2 * LANES
    heads = carried[0].shape[0]
    qrows = 2 * heads
    half, quarter = rows // 2, rows // 4
    cut = w_gate.shape[1] // 2
    n_blocks = half // BLOCK
    vmem = pl.BlockSpec(memory_space=pltpu.VMEM)
    hbm = pl.BlockSpec(memory_space=pltpu.HBM)
    flat = lambda n: pltpu.VMEM((n, width), F32)
    stats = lambda h, n: pltpu.VMEM((h, 3, n, LANES), F32)
    dma = lambda n: pltpu.SemaphoreType.DMA((n,))
    n_remote = GROUPS + GROUPS // 2 + 8 * CHUNKS
    args = (tokens, gain, w_o, w_gate, w_up, w_down, rows_k, rows_v)
    shape = (half, *rows_k.shape[1:])
    return pl.pallas_call(
        functools.partial(layer_kernel, kvs),
        out_shape=(
            pltpu.VMEM(tokens.shape, BF16),
            pltpu.VMEM(shape, BF16),
            pltpu.VMEM(shape, BF16),
        ),
        in_specs=[hbm] * len(args) + [vmem] * len(carried),
        out_specs=(vmem,) * 3,
        scratch_shapes=[
            pltpu.VMEM((SLOTS, width, head_dim), BF16),
            *(pltpu.VMEM((half * qrows, LANES), F32) for _ in range(3)),
            stats(heads, half), stats(heads // 2, rows), stats(heads // 2, half), stats(heads // 2, half),
            flat(half), flat(quarter), flat(quarter), flat(quarter), flat(half),
            pltpu.VMEM((half, cut), BF16),
            flat(half), flat(quarter), flat(quarter), flat(quarter), flat(rows),
            pltpu.VMEM(tokens.shape, BF16),
            pltpu.VMEM(gain.shape, BF16),
            dma(2), dma(n_blocks), dma(n_blocks), dma(width // head_dim),
            dma(2 * (cut // head_dim) + width // head_dim), dma(n_remote), dma(n_remote),
        ],
        compiler_params=pltpu.CompilerParams(
            vmem_limit_bytes=LAYER_VMEM << 20, collective_id=0, has_side_effects=True
        ),
        name="layer",
    )(*(pltpu.with_memory_space_constraint(v, pltpu.HBM) for v in args), *carried)


def write_kernel(pos_hbm, t_ref, kn_s, vn_s, _bk, _bv, _k, _v, out_ref, nk_hbm, nv_hbm, kbuf, vbuf, pos, sem, tile_sem, pos_sem):
    rows, key_rows, _ = kbuf.shape
    per_slot = 4
    local_slots = key_rows // per_slot
    slots = local_slots * lax.axis_size("sp")
    base = lax.axis_index("sp") * local_slots
    start = lax.axis_index("sp") // 2 * rows
    per_tile = 16 // per_slot
    n_blocks = rows // BLOCK
    tile_row = lax.broadcasted_iota(jnp.int32, (16, LANES), 0) // per_slot

    def copies(j):
        here, near = pl.ds(j * BLOCK, BLOCK), pl.ds(start + j * BLOCK, BLOCK)
        return (
            pltpu.make_async_copy(kbuf.at[here], nk_hbm.at[near], sem.at[0, j]),
            pltpu.make_async_copy(vbuf.at[here], nv_hbm.at[near], sem.at[1, j]),
        )

    def target(b):
        local = lax.rem(pos[b], slots) - base
        owned = (local >= 0) & (local < local_slots)
        safe = jnp.where(owned, local, 0)
        hit = jnp.where(owned, lax.rem(safe, per_tile), -1)
        return hit, pl.ds(pl.multiple_of((safe // per_tile) * 16, 16), 16)

    def tile_copies(n):
        at = target(start + n)[1]
        return (
            pltpu.make_async_copy(kbuf.at[n, at], nk_hbm.at[start + n, at], tile_sem.at[0]),
            pltpu.make_async_copy(vbuf.at[n, at], nv_hbm.at[start + n, at], tile_sem.at[1]),
        )

    def patch(n):
        b = start + n
        hit, at = target(b)
        for buf, new in ((kbuf, kn_s), (vbuf, vn_s)):
            fresh = new[pl.ds(pl.multiple_of(b * 16, 16), 16), :]
            buf[n, at, :] = jnp.where(tile_row == hit, fresh, buf[n, at, :].astype(F32)).astype(BF16)

    pos_copy = pltpu.make_async_copy(pos_hbm, pos, pos_sem)
    pos_copy.start()
    for j in range(EARLY):
        for copy in copies(j):
            copy.start()
    out_ref[...] = t_ref[...]
    pos_copy.wait()
    for j in range(EARLY, n_blocks + 1):
        if j < n_blocks:
            for i in range(BLOCK):
                patch(j * BLOCK + i)
        if j > EARLY:
            for copy in copies(j - 1):
                copy.start()
    for j in range(EARLY):
        for copy in copies(j):
            copy.wait()
        for i in range(BLOCK):
            patch(j * BLOCK + i)
        if j:
            for i in range(BLOCK):
                for copy in tile_copies((j - 1) * BLOCK + i):
                    copy.start()
    for i in range(BLOCK):
        for copy in tile_copies((EARLY - 1) * BLOCK + i):
            copy.start()
    for j in range(EARLY, n_blocks):
        for copy in copies(j):
            copy.wait()
    for n in range(EARLY * BLOCK):
        for copy in tile_copies(n):
            copy.wait()


def write(positions, layer_out, fresh_k, fresh_v, buf_k, buf_v, new_k, new_v):
    vmem = pl.BlockSpec(memory_space=pltpu.VMEM)
    hbm = pl.BlockSpec(memory_space=pltpu.HBM)
    return pl.pallas_call(
        write_kernel,
        out_shape=(
            *(jax.ShapeDtypeStruct(v.shape, BF16) for v in (layer_out, new_k, new_v)),
            pltpu.VMEM(buf_k.shape, BF16),
            pltpu.VMEM(buf_v.shape, BF16),
        ),
        in_specs=[hbm] + [vmem] * 5 + [hbm] * 2,
        out_specs=(vmem, hbm, hbm, vmem, vmem),
        input_output_aliases={4: 3, 5: 4, 6: 1, 7: 2},
        scratch_shapes=[
            pltpu.SMEM(positions.shape, jnp.int32),
            pltpu.SemaphoreType.DMA((2, buf_k.shape[0] // BLOCK)),
            pltpu.SemaphoreType.DMA((2,)),
            pltpu.SemaphoreType.DMA,
        ],
        compiler_params=pltpu.CompilerParams(vmem_limit_bytes=LAYER_VMEM << 20),
        name="write",
    )(pltpu.with_memory_space_constraint(positions, pltpu.HBM), layer_out, fresh_k, fresh_v, buf_k, buf_v, new_k, new_v)[:3]


def to_rows(cache):
    b, s, kv, d = cache.shape
    return cache.reshape(b, s, kv, d // LANES, LANES).transpose(0, 1, 3, 2, 4).reshape(b, -1, LANES)


def from_rows(rows, shape):
    b, s, kv, d = shape
    return rows.reshape(b, s, d // LANES, kv, LANES).transpose(0, 1, 3, 2, 4).reshape(shape)


def solution(mesh):
    cache_spec = P("dp", "sp", "tp", None)
    row_spec = P("dp", None)
    col_spec = P(None, "tp")
    in_specs = (row_spec, P("dp"), cache_spec, cache_spec, P(None), col_spec, col_spec, col_spec, P("tp", None), P(None), col_spec, col_spec, P("tp", None))
    out_specs = (row_spec, cache_spec, cache_spec)

    def local_step(tokens, positions, cache_k, cache_v, attn_gain, w_q, w_k, w_v, w_o, mlp_gain, w_gate, w_up, w_down):
        old_k, old_v = to_rows(cache_k), to_rows(cache_v)
        far, rows_k, rows_v, *carried, fresh_k, fresh_v = first_half(
            positions, tokens, attn_gain, w_q, w_k, w_v, old_k, old_v
        )
        out, buf_k, buf_v = layer(
            tokens, mlp_gain, w_o, w_gate, w_up, w_down, old_k, old_v, cache_k.shape[2], (far, *carried)
        )
        layer_out, rows_k, rows_v = write(positions, out, fresh_k, fresh_v, buf_k, buf_v, rows_k, rows_v)
        new_k = from_rows(rows_k, cache_k.shape)
        new_v = from_rows(rows_v, cache_v.shape)
        return layer_out, new_k, new_v

    return jax.shard_map(local_step, mesh=mesh, in_specs=in_specs, out_specs=out_specs, check_vma=False)
```

```python
import functools
import itertools
import math

import jax
import jax.numpy as jnp
from jax import lax
from jax.experimental import pallas as pl
from jax.experimental.pallas import tpu as pltpu
from jax.sharding import PartitionSpec as P

NORM_EPS = 1e-5
ROPE_THETA = 10000.0
LANES = 128
F32 = jnp.float32
BF16 = jnp.bfloat16
FAR = 1 << 28
BLOCK = 4
EARLY = 3
EAGER = (2, 5)
FIRST = 4
SLOTS = 22
LAYER_VMEM = 35
CHUNKS = 10
GROUPS = 4
MESH = pl.DeviceIdType.MESH


def rms_norm(values, gain):
    wide = values.astype(F32)
    inv_rms = lax.rsqrt(jnp.mean(wide * wide, axis=-1, keepdims=True) + NORM_EPS)
    return (wide * inv_rms * gain.astype(F32)).astype(BF16)


def first_kernel(
    pos_hbm, x_hbm, gain_hbm, wq_hbm, wk_hbm, wv_hbm, ck_hbm, cv_hbm,
    part_ref, nk_hbm, nv_hbm, q_s, kx_s, vx_s, lim_s, hid_s, kn_s, vn_s,
    wbuf, kbuf, vbuf, ang_s, o_s, m_s, l_s,
    pos, x_ref, gain_ref, w_sem, k_sem, v_sem, out_sem, x_sem,
):
    rows = x_ref.shape[0]
    head_dim = 2 * LANES
    heads = wq_hbm.shape[1] // head_dim
    kvs = wk_hbm.shape[1] // head_dim
    group = heads // kvs
    per_slot = 2 * kvs
    qrows = 2 * heads
    key_rows = ck_hbm.shape[1]
    local_slots = key_rows // per_slot
    slots = local_slots * lax.axis_size("sp")
    slices = key_rows // LANES
    half = rows // 2
    n_blocks = half // BLOCK
    start = (1 - lax.axis_index("sp") // 2) * half
    base = lax.axis_index("sp") * local_slots

    def w_copy(n):
        src, col = (
            (wk_hbm, n) if n < kvs else (wv_hbm, n - kvs) if n < 2 * kvs else (wq_hbm, n - 2 * kvs)
        )
        return pltpu.make_async_copy(src.at[:, pl.ds(col * head_dim, head_dim)], wbuf.at[n], w_sem.at[n])

    def in_copies(j):
        far, here = pl.ds(start + j * BLOCK, BLOCK), pl.ds(j * BLOCK, BLOCK)
        return (
            pltpu.make_async_copy(ck_hbm.at[far], kbuf.at[here], k_sem.at[j]),
            pltpu.make_async_copy(cv_hbm.at[far], vbuf.at[here], v_sem.at[j]),
        )

    def out_copies(j):
        far, here = pl.ds(start + j * BLOCK, BLOCK), pl.ds(j * BLOCK, BLOCK)
        return (
            pltpu.make_async_copy(kbuf.at[here], nk_hbm.at[far], out_sem.at[0]),
            pltpu.make_async_copy(vbuf.at[here], nv_hbm.at[far], out_sem.at[1]),
        )

    small = [
        pltpu.make_async_copy(src, dst, x_sem.at[i])
        for i, (src, dst) in enumerate(((pos_hbm, pos), (x_hbm, x_ref), (gain_hbm, gain_ref)))
    ]
    for copy in small:
        copy.start()
    n_w = heads + 2 * kvs
    for n in range(n_w // 2):
        w_copy(n).start()

    lane = lax.broadcasted_iota(jnp.int32, (1, LANES), 1).astype(F32)
    freq = jnp.exp2(lane * (-math.log2(ROPE_THETA) / LANES))

    for copy in small:
        copy.wait()
    for n in range(n_w // 2, n_w):
        w_copy(n).start()
    for j in range(FIRST):
        for copy in in_copies(j):
            copy.start()

    def angle_row(b, carry):
        p = pos[b]
        ang_s[pl.ds(b, 1), :] = freq * p.astype(F32)
        local = lax.rem(p, slots) - base
        owned = (local >= 0) & (local < local_slots)
        span = pl.ds(pl.multiple_of(b * qrows, qrows), qrows)
        lim_s[span, :] = jnp.full((qrows, LANES), jnp.where(p >= slots - 1, FAR // 2, p) - base, jnp.int32)
        hid_s[span, :] = jnp.full((qrows, LANES), jnp.where(owned, local, -FAR), jnp.int32)
        return carry

    lax.fori_loop(0, rows, angle_row, 0, unroll=8)
    angles = ang_s[...]
    cos_t, sin_t = jnp.cos(angles), jnp.sin(angles)
    normed = rms_norm(x_ref[...], gain_ref[...])

    for n in range(n_w):
        w_copy(n).wait()
        if FIRST + n < n_blocks:
            for copy in in_copies(FIRST + n):
                copy.start()
        lin = jnp.dot(normed, wbuf[n], preferred_element_type=F32)
        first, second = lin[:, :LANES], lin[:, LANES:]
        if not kvs <= n < 2 * kvs:
            first, second = first * cos_t - second * sin_t, second * cos_t + first * sin_t
        first, second = first.astype(BF16).astype(F32), second.astype(BF16).astype(F32)
        if n >= 2 * kvs:
            h = n - 2 * kvs
            q_s[pl.ds(h, rows, stride=qrows), :] = first
            q_s[pl.ds(heads + h, rows, stride=qrows), :] = second
        else:
            dst, tile, kv = (kn_s, kx_s, n) if n < kvs else (vn_s, vx_s, n - kvs)
            for rep in range(16 // per_slot):
                dst[pl.ds(rep * per_slot + kv, rows, stride=16), :] = first
                dst[pl.ds(rep * per_slot + kvs + kv, rows, stride=16), :] = second
            for g in range(group):
                tile[pl.ds(kv * group + g, rows, stride=qrows), :] = first
                tile[pl.ds(heads + kv * group + g, rows, stride=qrows), :] = second

    row = lax.broadcasted_iota(jnp.int32, (qrows, LANES), 0)
    col = lax.broadcasted_iota(jnp.int32, (qrows, LANES), 1)
    half_of_col = (col // kvs) % 2
    fits = (half_of_col == row // heads) & (col % kvs == (row % heads) // group)
    slot_of_col = jnp.where(fits, col // per_slot, FAR)
    low_half = half_of_col == 0
    patch_row = lax.broadcasted_iota(jnp.int32, (16, LANES), 0) // per_slot
    scale = 1.0 / math.sqrt(head_dim)

    def block_step(j, carry):
        for copy in in_copies(j):
            copy.wait()
        for i in range(BLOCK):
            n = j * BLOCK + i
            b = start + n
            local = lax.rem(pos[b], slots) - base
            owned = (local >= 0) & (local < local_slots)
            safe = jnp.where(owned, local, 0)
            hit = jnp.where(owned, lax.rem(safe, 16 // per_slot), -1)
            span = pl.ds(pl.multiple_of((safe // (16 // per_slot)) * 16, 16), 16)
            for buf, new in ((kbuf, kn_s), (vbuf, vn_s)):
                old = buf[n, span, :].astype(F32)
                fresh = new[pl.ds(pl.multiple_of(b * 16, 16), 16), :]
                buf[n, span, :] = jnp.where(patch_row == hit, fresh, old).astype(BF16)
        scores = []
        for i in range(BLOCK):
            b = start + j * BLOCK + i
            q = q_s[pl.ds(pl.multiple_of(b * qrows, qrows), qrows), :].astype(BF16)
            scores.append(
                lax.dot_general(q, kbuf[j * BLOCK + i], (((1,), (1,)), ((), ())), preferred_element_type=F32)
            )
        probs = []
        for i in range(BLOCK):
            n = j * BLOCK + i
            p = pos[start + n]
            limit = jnp.where(p >= slots - 1, FAR // 2, p) - base
            parts = []
            for t in range(slices):
                own = scores[i][:, t * LANES : (t + 1) * LANES]
                other = pltpu.roll(own, heads, 0)
                other = jnp.where(
                    low_half, pltpu.roll(other, LANES - kvs, 1), pltpu.roll(other, kvs, 1)
                )
                ok = slot_of_col <= limit - t * (LANES // per_slot)
                parts.append(jnp.where(ok, (own + other) * scale, -jnp.inf))
            top = functools.reduce(jnp.maximum, parts)
            top = jnp.max(top, axis=1, keepdims=True)
            floor = jnp.where(top == -jnp.inf, 0.0, top)
            parts = [jnp.exp(part - floor) for part in parts]
            total = jnp.sum(functools.reduce(jnp.add, parts), axis=1, keepdims=True)
            span = pl.ds(pl.multiple_of(n * qrows, qrows), qrows)
            m_s[span, :] = jnp.broadcast_to(top, (qrows, LANES))
            l_s[span, :] = jnp.broadcast_to(total, (qrows, LANES))
            probs.append(jnp.concatenate([part.astype(BF16) for part in parts], axis=1))
        for i in range(BLOCK):
            n = j * BLOCK + i
            span = pl.ds(pl.multiple_of(n * qrows, qrows), qrows)
            o_s[span, :] = jnp.dot(probs[i], vbuf[n], preferred_element_type=F32)
        for copy in out_copies(j):
            copy.start()
        return carry

    lax.fori_loop(0, n_blocks, block_step, 0)

    left = lax.broadcasted_iota(jnp.int32, (half, LANES), 1) < LANES // 2
    for h in range(heads):
        lo, hi = pl.ds(h, half, stride=qrows), pl.ds(heads + h, half, stride=qrows)
        part_ref[h, 0], part_ref[h, 1] = o_s[lo, :], o_s[hi, :]
        part_ref[h, 2] = jnp.where(left, m_s[lo, :], l_s[lo, :])
    for j in range(n_blocks):
        for copy in out_copies(j):
            copy.wait()


def first_half(positions, tokens, gain, w_q, w_k, w_v, rows_k, rows_v):
    rows, width = tokens.shape
    head_dim = 2 * LANES
    heads = w_q.shape[1] // head_dim
    kvs = w_k.shape[1] // head_dim
    qrows = 2 * heads
    vmem = pl.BlockSpec(memory_space=pltpu.VMEM)
    hbm = pl.BlockSpec(memory_space=pltpu.HBM)
    n_blocks = rows // 2 // BLOCK
    tile = lambda n: pltpu.VMEM((rows * n, LANES), F32)
    return pl.pallas_call(
        first_kernel,
        out_shape=(
            pltpu.VMEM((heads, 3, rows // 2, LANES), F32),
            jax.ShapeDtypeStruct(rows_k.shape, BF16),
            jax.ShapeDtypeStruct(rows_v.shape, BF16),
            tile(qrows), tile(qrows), tile(qrows),
            *(pltpu.VMEM((rows * qrows, LANES), jnp.int32) for _ in range(2)),
            tile(16), tile(16),
        ),
        in_specs=[hbm] * 8,
        out_specs=(vmem, hbm, hbm) + (vmem,) * 7,
        scratch_shapes=[
            pltpu.VMEM((heads + 2 * kvs, width, head_dim), BF16),
            pltpu.VMEM((rows // 2, *rows_k.shape[1:]), BF16),
            pltpu.VMEM((rows // 2, *rows_v.shape[1:]), BF16),
            tile(1),
            pltpu.VMEM((rows // 2 * qrows, LANES), F32),
            pltpu.VMEM((rows // 2 * qrows, LANES), F32),
            pltpu.VMEM((rows // 2 * qrows, LANES), F32),
            pltpu.SMEM((rows,), jnp.int32),
            pltpu.VMEM(tokens.shape, BF16),
            pltpu.VMEM(gain.shape, BF16),
            pltpu.SemaphoreType.DMA((heads + 2 * kvs,)),
            pltpu.SemaphoreType.DMA((n_blocks,)),
            pltpu.SemaphoreType.DMA((n_blocks,)),
            pltpu.SemaphoreType.DMA((2,)),
            pltpu.SemaphoreType.DMA((3,)),
        ],
        compiler_params=pltpu.CompilerParams(vmem_limit_bytes=36 << 20),
        name="first",
    )(*(pltpu.with_memory_space_constraint(v, pltpu.HBM) for v in (positions, tokens, gain, w_q, w_k, w_v, rows_k, rows_v)))


def combine(mine, theirs):
    left = lax.broadcasted_iota(jnp.int32, mine[2].shape, mine[2].ndim - 1) < LANES // 2
    axis = mine[2].ndim - 1

    def unpack(stats):
        turned = pltpu.roll(stats, LANES // 2, axis)
        return jnp.where(left, stats, turned), jnp.where(left, turned, stats)

    (m_a, l_a), (m_b, l_b) = unpack(mine[2]), unpack(theirs[2])
    top = jnp.maximum(m_a, m_b)
    f_a = jnp.where(m_a == -jnp.inf, 0.0, jnp.exp(m_a - top))
    f_b = jnp.where(m_b == -jnp.inf, 0.0, jnp.exp(m_b - top))
    return mine[0] * f_a + theirs[0] * f_b, mine[1] * f_a + theirs[1] * f_b, top, l_a * f_a + l_b * f_b


def layer_kernel(
    kv_heads, x_hbm, gm_hbm, wo_hbm, wg_hbm, wu_hbm, wd_hbm, ck_hbm, cv_hbm,
    far_ref, q_s, kx_s, vx_s, lim_s, hid_s,
    out_ref, kbuf, vbuf,
    ring, o_s, m_s, l_s, part, rd, sx, rx,
    po, ro, so, yo, hb, act, pm, rm, sm, ym, ob,
    x_ref, gm_ref,
    small_sem, k_sem, v_sem, o_sem, c_sem, send_sem, recv_sem,
):
    rows, width = x_ref.shape
    head_dim = ring.shape[2]
    heads = far_ref.shape[0]
    kvs = kv_heads
    group = heads // kvs
    per_slot, qrows = 2 * kvs, 2 * heads
    key_rows = ck_hbm.shape[1]
    local_slots = key_rows // per_slot
    slices = key_rows // LANES
    n_blocks = rows // 2 // BLOCK
    mine_h = heads // 2
    half, quarter = rows // 2, rows // 4
    sp, tp = lax.axis_index("sp"), lax.axis_index("tp")
    x, k = sp // 2, lax.rem(sp, 2)
    d_dev, x_dev, y_dev = {"sp": x * 2 + 1 - k}, {"sp": (1 - x) * 2 + k}, {"tp": 1 - tp}
    m_cols = act.shape[1]
    span = width // CHUNKS

    barrier = pltpu.get_barrier_semaphore()
    for dev in (d_dev, x_dev, y_dev):
        pl.semaphore_signal(barrier, inc=1, device_id=dev, device_id_type=MESH)

    counter = [0]

    def remote(src, dst, dev):
        n = counter[0]
        counter[0] += 1
        return pltpu.make_async_remote_copy(
            src_ref=src, dst_ref=dst, send_sem=send_sem.at[n], recv_sem=recv_sem.at[n],
            device_id=dev, device_id_type=MESH,
        )

    def in_copies(j):
        near, here = pl.ds(x * half + j * BLOCK, BLOCK), pl.ds(j * BLOCK, BLOCK)
        return (
            pltpu.make_async_copy(ck_hbm.at[near], kbuf.at[here], k_sem.at[j]),
            pltpu.make_async_copy(cv_hbm.at[near], vbuf.at[here], v_sem.at[j]),
        )

    small = [
        pltpu.make_async_copy(src, dst, small_sem.at[i])
        for i, (src, dst) in enumerate(
            ((x_hbm, x_ref), (gm_hbm, gm_ref))
        )
    ]
    def read(blocks):
        for j in blocks:
            for copy in in_copies(j):
                copy.start()

    read(range(EAGER[0]))

    n_w = 0
    o_rows = mine_h * head_dim
    per_o = width // o_rows
    o_copies = [
        pltpu.make_async_copy(
            wo_hbm.at[pl.ds(k * o_rows, o_rows), pl.ds(c * head_dim, head_dim)],
            ring.at[n_w + c // per_o, pl.ds((c % per_o) * o_rows, o_rows)],
            o_sem.at[c],
        )
        for c in range(width // head_dim)
    ]
    n_gate = m_cols // head_dim
    ring_at = lambda i: (n_w + 2 + i) % SLOTS
    chunks = []
    for c in range(n_gate):
        at = pl.ds(pl.multiple_of(k * m_cols + c * head_dim, LANES), head_dim)
        chunks += [wg_hbm.at[:, at], wu_hbm.at[:, at]]
    for c in range(width // head_dim):
        chunks.append(wd_hbm.at[pl.ds(pl.multiple_of(k * m_cols, LANES), m_cols), pl.ds(c * head_dim, head_dim)])
    chunks = [
        pltpu.make_async_copy(src, ring.at[ring_at(i)], c_sem.at[i]) for i, src in enumerate(chunks)
    ]
    queue = iter(chunks)

    started = [0]

    def fetch(n, limit=len(chunks)):
        n = min(n, limit - started[0])
        started[0] += n
        for copy in itertools.islice(queue, n):
            copy.start()

    row = lax.broadcasted_iota(jnp.int32, (qrows, LANES), 0)
    col = lax.broadcasted_iota(jnp.int32, (qrows, LANES), 1)
    half_of_col = (col // kvs) % 2
    fits = (half_of_col == row // heads) & (col % kvs == (row % heads) // group)
    slot_of_col = jnp.where(fits, col // per_slot, FAR)
    low_half = half_of_col == 0
    scale = 1.0 / math.sqrt(head_dim)

    def block_step(j, carry):
        for copy in in_copies(j):
            copy.wait()
        first = x * half + j * BLOCK
        at_rows = [pl.ds(pl.multiple_of((first + i) * qrows, qrows), qrows) for i in range(BLOCK)]
        scores = []
        for i in range(BLOCK):
            scores.append(
                lax.dot_general(
                    q_s[at_rows[i], :].astype(BF16), kbuf[j * BLOCK + i], (((1,), (1,)), ((), ())),
                    preferred_element_type=F32,
                )
            )
        probs, news = [], []
        for i in range(BLOCK):
            limit, hidden = lim_s[at_rows[i], :], hid_s[at_rows[i], :]
            fresh = q_s[at_rows[i], :] * kx_s[at_rows[i], :]
            fresh = jnp.sum(fresh + pltpu.roll(fresh, heads, 0), axis=1, keepdims=True) * scale
            fresh = jnp.where(hidden[:, :1] >= 0, fresh, -jnp.inf)
            parts = []
            for t in range(slices):
                own = scores[i][:, t * LANES : (t + 1) * LANES]
                other = pltpu.roll(own, heads, 0)
                other = jnp.where(
                    low_half, pltpu.roll(other, LANES - kvs, 1), pltpu.roll(other, kvs, 1)
                )
                shift = t * (LANES // per_slot)
                ok = (slot_of_col <= limit - shift) & (slot_of_col != hidden - shift)
                parts.append(jnp.where(ok, (own + other) * scale, -jnp.inf))
            top = functools.reduce(jnp.maximum, parts)
            top = jnp.maximum(jnp.max(top, axis=1, keepdims=True), fresh)
            floor = jnp.where(top == -jnp.inf, 0.0, top)
            parts = [jnp.exp(part_t - floor) for part_t in parts]
            new = jnp.exp(fresh - floor)
            total = jnp.sum(functools.reduce(jnp.add, parts), axis=1, keepdims=True) + new
            at = pl.ds(pl.multiple_of((j * BLOCK + i) * qrows, qrows), qrows)
            m_s[at, :] = jnp.broadcast_to(top, (qrows, LANES))
            l_s[at, :] = jnp.broadcast_to(total, (qrows, LANES))
            news.append(new)
            probs.append(jnp.concatenate([part_t.astype(BF16) for part_t in parts], axis=1))
        for i in range(BLOCK):
            at = pl.ds(pl.multiple_of((j * BLOCK + i) * qrows, qrows), qrows)
            o_s[at, :] = (
                jnp.dot(probs[i], vbuf[j * BLOCK + i], preferred_element_type=F32) + news[i] * vx_s[at_rows[i], :]
            )
        return carry

    size = rows // GROUPS
    my_heads, their_heads = pl.ds(k * mine_h, mine_h), pl.ds((1 - k) * mine_h, mine_h)
    spans = [pl.ds(g * size, size) for g in range(GROUPS)]
    near = GROUPS // 2
    sources = [far_ref.at[their_heads, :, spans[g]] for g in range(near)]
    sources += [part.at[their_heads, :, spans[g]] for g in range(near)]
    swaps_a = [remote(src, rd.at[:, :, at], d_dev) for src, at in zip(sources, spans)]
    cross_a = [remote(sx.at[:, :, at], rx.at[:, :, at], x_dev) for at in spans[: GROUPS // 2]]
    left = lax.broadcasted_iota(jnp.int32, (mine_h, size, LANES), 2) < LANES // 2
    joined = [None] * GROUPS

    def publish(g):
        at = spans[g - near]
        for h in range(heads):
            lo = pl.ds((g - near) * size * qrows + h, size, stride=qrows)
            hi = pl.ds((g - near) * size * qrows + heads + h, size, stride=qrows)
            part[h, 0, at], part[h, 1, at] = o_s[lo, :], o_s[hi, :]
            part[h, 2, at] = jnp.where(left[0], m_s[lo, :], l_s[lo, :])
        swaps_a[g].start()

    def chip(g):
        swaps_a[g].wait_recv()
        at = spans[g]
        here, local = (far_ref, at) if g < near else (part, spans[g - near])
        o_a, o_b, m, l = combine(
            [here[my_heads, i, local] for i in range(3)], [rd[:, i, at] for i in range(3)]
        )
        value = [o_a, o_b, jnp.where(left, m, l)]
        if g < GROUPS // 2:
            for i in range(3):
                sx[:, i, at] = value[i]
            cross_a[g].start()
        joined[g] = value

    pl.semaphore_wait(barrier, 3)
    for g in range(near):
        swaps_a[g].start()
    read(range(*EAGER))
    for copy in small:
        copy.start()
    step = n_blocks // near
    lax.fori_loop(0, step, block_step, 0)
    for g in range(near):
        chip(g)
    read(range(EAGER[1], n_blocks))
    publish(near)
    for copy in o_copies:
        copy.start()
    lax.fori_loop(step, n_blocks, block_step, 0)
    publish(GROUPS - 1)
    fetch(3)
    for g in range(near, GROUPS):
        chip(g)
    pieces = []
    for g in range(GROUPS // 2):
        cross_a[g].wait_recv()
        o_a, o_b, _, l = combine(joined[GROUPS // 2 + g], [rx[:, i, spans[g]] for i in range(3)])
        o_a, o_b = (o_a / l).astype(BF16), (o_b / l).astype(BF16)
        pieces.append(jnp.concatenate([v[h] for h in range(mine_h) for v in (o_a, o_b)], axis=-1))
    attended = jnp.concatenate(pieces, axis=0)
    for copy in small:
        copy.wait()

    own, other = pl.ds(k * quarter, quarter), pl.ds((1 - k) * quarter, quarter)
    my_rows = pl.ds(pl.multiple_of(x * half + k * quarter, quarter), quarter)
    x_peer_rows = pl.ds(pl.multiple_of((1 - x) * half + k * quarter, quarter), quarter)
    cols = [pl.ds(c * span, span) for c in range(CHUNKS)]
    per_span = span // head_dim

    def staged(dot, swap, cross, *rest):
        for c in range(CHUNKS + 2):
            if c < CHUNKS:
                dot(c)
            if c >= 2:
                swap(c - 2)
        for c in range(CHUNKS):
            cross(c)
        for c in range(CHUNKS + len(rest) - 1):
            for s, stage in enumerate(rest):
                if 0 <= c - s < CHUNKS:
                    stage(c - s)

    swaps = [remote(po.at[other, c], ro.at[:, c], d_dev) for c in cols]
    crosses = [remote(so.at[:, c], yo.at[:, c], y_dev) for c in cols]
    gathers = [remote(hb.at[own, c], hb.at[own, c], d_dev) for c in cols]

    def o_dot(c):
        for i in range(c * per_span, (c + 1) * per_span):
            o_copies[i].wait()
            w = ring[n_w + i // per_o, (i % per_o) * o_rows : (i % per_o + 1) * o_rows, :]
            po[:, i * head_dim : (i + 1) * head_dim] = jnp.dot(attended, w, preferred_element_type=F32)
        swaps[c].start()

    def o_swap(c):
        swaps[c].wait_recv()
        so[:, cols[c]] = po[own, cols[c]] + ro[:, cols[c]]
        crosses[c].start()
        fetch(2, SLOTS)

    def o_cross(c):
        crosses[c].wait_recv()
        total = so[:, cols[c]] + yo[:, cols[c]]
        hb[own, cols[c]] = (x_ref[my_rows, cols[c]].astype(F32) + total).astype(BF16).astype(F32)
        gathers[c].start()

    def o_gather(c):
        gathers[c].wait_recv()

    staged(o_dot, o_swap, o_cross, o_gather)

    normed_m = rms_norm(hb[...], gm_ref[...])
    for c in range(n_gate):
        chunks[2 * c].wait()
        chunks[2 * c + 1].wait()
        gate = jnp.dot(normed_m, ring[ring_at(2 * c)], preferred_element_type=F32)
        up = jnp.dot(normed_m, ring[ring_at(2 * c + 1)], preferred_element_type=F32)
        act[:, c * head_dim : (c + 1) * head_dim] = (jax.nn.silu(gate) * up).astype(BF16)
        fetch(2)

    swaps_m = [remote(pm.at[other, c], rm.at[:, c], d_dev) for c in cols]
    crosses_m = [remote(sm.at[:, c], ym.at[:, c], y_dev) for c in cols]
    to_core = [remote(ob.at[my_rows, c], ob.at[my_rows, c], d_dev) for c in cols]
    to_x = [remote(ob.at[my_rows, c], ob.at[my_rows, c], x_dev) for c in cols]
    onward = [remote(ob.at[x_peer_rows, c], ob.at[x_peer_rows, c], d_dev) for c in cols]

    def m_dot(c):
        for i in range(c * per_span, (c + 1) * per_span):
            chunks[2 * n_gate + i].wait()
            pm[:, i * head_dim : (i + 1) * head_dim] = jnp.dot(
                act[...], ring[ring_at(2 * n_gate + i)], preferred_element_type=F32
            )
        swaps_m[c].start()

    def m_swap(c):
        swaps_m[c].wait_recv()
        sm[:, cols[c]] = pm[own, cols[c]] + rm[:, cols[c]]
        crosses_m[c].start()

    def m_cross(c):
        crosses_m[c].wait_recv()
        total = sm[:, cols[c]] + ym[:, cols[c]]
        ob[my_rows, cols[c]] = (hb[own, cols[c]] + total).astype(BF16).astype(F32)
        to_x[c].start()
        to_core[c].start()

    def m_gather(c):
        to_x[c].wait_recv()
        onward[c].start()

    def m_last(c):
        to_core[c].wait_recv()
        onward[c].wait_recv()
        out_ref[:, cols[c]] = ob[:, cols[c]].astype(BF16)

    staged(m_dot, m_swap, m_cross, m_gather, m_last)
    for copy in [*swaps_a, *cross_a, *swaps, *crosses, *gathers, *swaps_m, *crosses_m, *to_core, *to_x, *onward]:
        copy.wait_send()


def layer(tokens, gain, w_o, w_gate, w_up, w_down, rows_k, rows_v, kvs, carried):
    rows, width = tokens.shape
    head_dim = 2 * LANES
    heads = carried[0].shape[0]
    qrows = 2 * heads
    half, quarter = rows // 2, rows // 4
    cut = w_gate.shape[1] // 2
    n_blocks = half // BLOCK
    vmem = pl.BlockSpec(memory_space=pltpu.VMEM)
    hbm = pl.BlockSpec(memory_space=pltpu.HBM)
    flat = lambda n: pltpu.VMEM((n, width), F32)
    stats = lambda h, n: pltpu.VMEM((h, 3, n, LANES), F32)
    dma = lambda n: pltpu.SemaphoreType.DMA((n,))
    n_remote = GROUPS + GROUPS // 2 + 8 * CHUNKS
    args = (tokens, gain, w_o, w_gate, w_up, w_down, rows_k, rows_v)
    shape = (half, *rows_k.shape[1:])
    return pl.pallas_call(
        functools.partial(layer_kernel, kvs),
        out_shape=(
            pltpu.VMEM(tokens.shape, BF16),
            pltpu.VMEM(shape, BF16),
            pltpu.VMEM(shape, BF16),
        ),
        in_specs=[hbm] * len(args) + [vmem] * len(carried),
        out_specs=(vmem,) * 3,
        scratch_shapes=[
            pltpu.VMEM((SLOTS, width, head_dim), BF16),
            *(pltpu.VMEM((half * qrows, LANES), F32) for _ in range(3)),
            stats(heads, half), stats(heads // 2, rows), stats(heads // 2, half), stats(heads // 2, half),
            flat(half), flat(quarter), flat(quarter), flat(quarter), flat(half),
            pltpu.VMEM((half, cut), BF16),
            flat(half), flat(quarter), flat(quarter), flat(quarter), flat(rows),
            pltpu.VMEM(tokens.shape, BF16),
            pltpu.VMEM(gain.shape, BF16),
            dma(2), dma(n_blocks), dma(n_blocks), dma(width // head_dim),
            dma(2 * (cut // head_dim) + width // head_dim), dma(n_remote), dma(n_remote),
        ],
        compiler_params=pltpu.CompilerParams(
            vmem_limit_bytes=LAYER_VMEM << 20, collective_id=0, has_side_effects=True
        ),
        name="layer",
    )(*(pltpu.with_memory_space_constraint(v, pltpu.HBM) for v in args), *carried)


def write_kernel(pos_hbm, t_ref, kn_s, vn_s, _bk, _bv, _k, _v, out_ref, nk_hbm, nv_hbm, kbuf, vbuf, pos, sem, tile_sem, pos_sem):
    rows, key_rows, _ = kbuf.shape
    per_slot = 4
    local_slots = key_rows // per_slot
    slots = local_slots * lax.axis_size("sp")
    base = lax.axis_index("sp") * local_slots
    start = lax.axis_index("sp") // 2 * rows
    per_tile = 16 // per_slot
    n_blocks = rows // BLOCK
    tile_row = lax.broadcasted_iota(jnp.int32, (16, LANES), 0) // per_slot

    def copies(j):
        here, near = pl.ds(j * BLOCK, BLOCK), pl.ds(start + j * BLOCK, BLOCK)
        return (
            pltpu.make_async_copy(kbuf.at[here], nk_hbm.at[near], sem.at[0, j]),
            pltpu.make_async_copy(vbuf.at[here], nv_hbm.at[near], sem.at[1, j]),
        )

    def target(b):
        local = lax.rem(pos[b], slots) - base
        owned = (local >= 0) & (local < local_slots)
        safe = jnp.where(owned, local, 0)
        hit = jnp.where(owned, lax.rem(safe, per_tile), -1)
        return hit, pl.ds(pl.multiple_of((safe // per_tile) * 16, 16), 16)

    def tile_copies(n):
        at = target(start + n)[1]
        return (
            pltpu.make_async_copy(kbuf.at[n, at], nk_hbm.at[start + n, at], tile_sem.at[0]),
            pltpu.make_async_copy(vbuf.at[n, at], nv_hbm.at[start + n, at], tile_sem.at[1]),
        )

    def patch(n):
        b = start + n
        hit, at = target(b)
        for buf, new in ((kbuf, kn_s), (vbuf, vn_s)):
            fresh = new[pl.ds(pl.multiple_of(b * 16, 16), 16), :]
            buf[n, at, :] = jnp.where(tile_row == hit, fresh, buf[n, at, :].astype(F32)).astype(BF16)

    pos_copy = pltpu.make_async_copy(pos_hbm, pos, pos_sem)
    pos_copy.start()
    for j in range(EARLY):
        for copy in copies(j):
            copy.start()
    out_ref[...] = t_ref[...]
    pos_copy.wait()
    for j in range(EARLY, n_blocks + 1):
        if j < n_blocks:
            for i in range(BLOCK):
                patch(j * BLOCK + i)
        if j > EARLY:
            for copy in copies(j - 1):
                copy.start()
    for j in range(EARLY):
        for copy in copies(j):
            copy.wait()
        for i in range(BLOCK):
            patch(j * BLOCK + i)
        if j:
            for i in range(BLOCK):
                for copy in tile_copies((j - 1) * BLOCK + i):
                    copy.start()
    for i in range(BLOCK):
        for copy in tile_copies((EARLY - 1) * BLOCK + i):
            copy.start()
    for j in range(EARLY, n_blocks):
        for copy in copies(j):
            copy.wait()
    for n in range(EARLY * BLOCK):
        for copy in tile_copies(n):
            copy.wait()


def write(positions, layer_out, fresh_k, fresh_v, buf_k, buf_v, new_k, new_v):
    vmem = pl.BlockSpec(memory_space=pltpu.VMEM)
    hbm = pl.BlockSpec(memory_space=pltpu.HBM)
    return pl.pallas_call(
        write_kernel,
        out_shape=(
            *(jax.ShapeDtypeStruct(v.shape, BF16) for v in (layer_out, new_k, new_v)),
            pltpu.VMEM(buf_k.shape, BF16),
            pltpu.VMEM(buf_v.shape, BF16),
        ),
        in_specs=[hbm] + [vmem] * 5 + [hbm] * 2,
        out_specs=(vmem, hbm, hbm, vmem, vmem),
        input_output_aliases={4: 3, 5: 4, 6: 1, 7: 2},
        scratch_shapes=[
            pltpu.SMEM(positions.shape, jnp.int32),
            pltpu.SemaphoreType.DMA((2, buf_k.shape[0] // BLOCK)),
            pltpu.SemaphoreType.DMA((2,)),
            pltpu.SemaphoreType.DMA,
        ],
        compiler_params=pltpu.CompilerParams(vmem_limit_bytes=LAYER_VMEM << 20),
        name="write",
    )(pltpu.with_memory_space_constraint(positions, pltpu.HBM), layer_out, fresh_k, fresh_v, buf_k, buf_v, new_k, new_v)[:3]


def to_rows(cache):
    b, s, kv, d = cache.shape
    return cache.reshape(b, s, kv, d // LANES, LANES).transpose(0, 1, 3, 2, 4).reshape(b, -1, LANES)


def from_rows(rows, shape):
    b, s, kv, d = shape
    return rows.reshape(b, s, d // LANES, kv, LANES).transpose(0, 1, 3, 2, 4).reshape(shape)


def solution(mesh):
    cache_spec = P("dp", "sp", "tp", None)
    row_spec = P("dp", None)
    col_spec = P(None, "tp")
    in_specs = (row_spec, P("dp"), cache_spec, cache_spec, P(None), col_spec, col_spec, col_spec, P("tp", None), P(None), col_spec, col_spec, P("tp", None))
    out_specs = (row_spec, cache_spec, cache_spec)

    def local_step(tokens, positions, cache_k, cache_v, attn_gain, w_q, w_k, w_v, w_o, mlp_gain, w_gate, w_up, w_down):
        old_k, old_v = to_rows(cache_k), to_rows(cache_v)
        far, rows_k, rows_v, *carried, fresh_k, fresh_v = first_half(
            positions, tokens, attn_gain, w_q, w_k, w_v, old_k, old_v
        )
        out, buf_k, buf_v = layer(
            tokens, mlp_gain, w_o, w_gate, w_up, w_down, old_k, old_v, cache_k.shape[2], (far, *carried)
        )
        layer_out, rows_k, rows_v = write(positions, out, fresh_k, fresh_v, buf_k, buf_v, rows_k, rows_v)
        new_k = from_rows(rows_k, cache_k.shape)
        new_v = from_rows(rows_v, cache_v.shape)
        return layer_out, new_k, new_v

    return jax.shard_map(local_step, mesh=mesh, in_specs=in_specs, out_specs=out_specs, check_vma=False)
```

```python
import functools
import itertools
import math

import jax
import jax.numpy as jnp
from jax import lax
from jax.experimental import pallas as pl
from jax.experimental.pallas import tpu as pltpu
from jax.sharding import PartitionSpec as P

NORM_EPS = 1e-5
ROPE_THETA = 10000.0
LANES = 128
F32 = jnp.float32
BF16 = jnp.bfloat16
FAR = 1 << 28
BLOCK = 4
EARLY = 3
EAGER = (2, 5)
FIRST = 4
SLOTS = 22
LAYER_VMEM = 35
CHUNKS = 2
GROUPS = 4
MESH = pl.DeviceIdType.MESH


def rms_norm(values, gain):
    wide = values.astype(F32)
    inv_rms = lax.rsqrt(jnp.mean(wide * wide, axis=-1, keepdims=True) + NORM_EPS)
    return (wide * inv_rms * gain.astype(F32)).astype(BF16)


def first_kernel(
    pos_hbm, x_hbm, gain_hbm, wq_hbm, wk_hbm, wv_hbm, ck_hbm, cv_hbm,
    part_ref, nk_hbm, nv_hbm, q_s, kx_s, vx_s, lim_s, hid_s, kn_s, vn_s,
    wbuf, kbuf, vbuf, ang_s, o_s, m_s, l_s,
    pos, x_ref, gain_ref, w_sem, k_sem, v_sem, out_sem, x_sem,
):
    rows = x_ref.shape[0]
    head_dim = 2 * LANES
    heads = wq_hbm.shape[1] // head_dim
    kvs = wk_hbm.shape[1] // head_dim
    group = heads // kvs
    per_slot = 2 * kvs
    qrows = 2 * heads
    key_rows = ck_hbm.shape[1]
    local_slots = key_rows // per_slot
    slots = local_slots * lax.axis_size("sp")
    slices = key_rows // LANES
    half = rows // 2
    n_blocks = half // BLOCK
    start = (1 - lax.axis_index("sp") // 2) * half
    base = lax.axis_index("sp") * local_slots

    def w_copy(n):
        src, col = (
            (wk_hbm, n) if n < kvs else (wv_hbm, n - kvs) if n < 2 * kvs else (wq_hbm, n - 2 * kvs)
        )
        return pltpu.make_async_copy(src.at[:, pl.ds(col * head_dim, head_dim)], wbuf.at[n], w_sem.at[n])

    def in_copies(j):
        far, here = pl.ds(start + j * BLOCK, BLOCK), pl.ds(j * BLOCK, BLOCK)
        return (
            pltpu.make_async_copy(ck_hbm.at[far], kbuf.at[here], k_sem.at[j]),
            pltpu.make_async_copy(cv_hbm.at[far], vbuf.at[here], v_sem.at[j]),
        )

    def out_copies(j):
        far, here = pl.ds(start + j * BLOCK, BLOCK), pl.ds(j * BLOCK, BLOCK)
        return (
            pltpu.make_async_copy(kbuf.at[here], nk_hbm.at[far], out_sem.at[0]),
            pltpu.make_async_copy(vbuf.at[here], nv_hbm.at[far], out_sem.at[1]),
        )

    small = [
        pltpu.make_async_copy(src, dst, x_sem.at[i])
        for i, (src, dst) in enumerate(((pos_hbm, pos), (x_hbm, x_ref), (gain_hbm, gain_ref)))
    ]
    for copy in small:
        copy.start()
    n_w = heads + 2 * kvs
    for n in range(n_w // 2):
        w_copy(n).start()

    lane = lax.broadcasted_iota(jnp.int32, (1, LANES), 1).astype(F32)
    freq = jnp.exp2(lane * (-math.log2(ROPE_THETA) / LANES))

    for copy in small:
        copy.wait()
    for n in range(n_w // 2, n_w):
        w_copy(n).start()
    for j in range(FIRST):
        for copy in in_copies(j):
            copy.start()

    def angle_row(b, carry):
        p = pos[b]
        ang_s[pl.ds(b, 1), :] = freq * p.astype(F32)
        local = lax.rem(p, slots) - base
        owned = (local >= 0) & (local < local_slots)
        span = pl.ds(pl.multiple_of(b * qrows, qrows), qrows)
        lim_s[span, :] = jnp.full((qrows, LANES), jnp.where(p >= slots - 1, FAR // 2, p) - base, jnp.int32)
        hid_s[span, :] = jnp.full((qrows, LANES), jnp.where(owned, local, -FAR), jnp.int32)
        return carry

    lax.fori_loop(0, rows, angle_row, 0, unroll=8)
    angles = ang_s[...]
    cos_t, sin_t = jnp.cos(angles), jnp.sin(angles)
    normed = rms_norm(x_ref[...], gain_ref[...])

    for n in range(n_w):
        w_copy(n).wait()
        if FIRST + n < n_blocks:
            for copy in in_copies(FIRST + n):
                copy.start()
        lin = jnp.dot(normed, wbuf[n], preferred_element_type=F32)
        first, second = lin[:, :LANES], lin[:, LANES:]
        if not kvs <= n < 2 * kvs:
            first, second = first * cos_t - second * sin_t, second * cos_t + first * sin_t
        first, second = first.astype(BF16).astype(F32), second.astype(BF16).astype(F32)
        if n >= 2 * kvs:
            h = n - 2 * kvs
            q_s[pl.ds(h, rows, stride=qrows), :] = first
            q_s[pl.ds(heads + h, rows, stride=qrows), :] = second
        else:
            dst, tile, kv = (kn_s, kx_s, n) if n < kvs else (vn_s, vx_s, n - kvs)
            for rep in range(16 // per_slot):
                dst[pl.ds(rep * per_slot + kv, rows, stride=16), :] = first
                dst[pl.ds(rep * per_slot + kvs + kv, rows, stride=16), :] = second
            for g in range(group):
                tile[pl.ds(kv * group + g, rows, stride=qrows), :] = first
                tile[pl.ds(heads + kv * group + g, rows, stride=qrows), :] = second

    row = lax.broadcasted_iota(jnp.int32, (qrows, LANES), 0)
    col = lax.broadcasted_iota(jnp.int32, (qrows, LANES), 1)
    half_of_col = (col // kvs) % 2
    fits = (half_of_col == row // heads) & (col % kvs == (row % heads) // group)
    slot_of_col = jnp.where(fits, col // per_slot, FAR)
    low_half = half_of_col == 0
    patch_row = lax.broadcasted_iota(jnp.int32, (16, LANES), 0) // per_slot
    scale = 1.0 / math.sqrt(head_dim)

    def block_step(j, carry):
        for copy in in_copies(j):
            copy.wait()
        for i in range(BLOCK):
            n = j * BLOCK + i
            b = start + n
            local = lax.rem(pos[b], slots) - base
            owned = (local >= 0) & (local < local_slots)
            safe = jnp.where(owned, local, 0)
            hit = jnp.where(owned, lax.rem(safe, 16 // per_slot), -1)
            span = pl.ds(pl.multiple_of((safe // (16 // per_slot)) * 16, 16), 16)
            for buf, new in ((kbuf, kn_s), (vbuf, vn_s)):
                old = buf[n, span, :].astype(F32)
                fresh = new[pl.ds(pl.multiple_of(b * 16, 16), 16), :]
                buf[n, span, :] = jnp.where(patch_row == hit, fresh, old).astype(BF16)
        scores = []
        for i in range(BLOCK):
            b = start + j * BLOCK + i
            q = q_s[pl.ds(pl.multiple_of(b * qrows, qrows), qrows), :].astype(BF16)
            scores.append(
                lax.dot_general(q, kbuf[j * BLOCK + i], (((1,), (1,)), ((), ())), preferred_element_type=F32)
            )
        probs = []
        for i in range(BLOCK):
            n = j * BLOCK + i
            p = pos[start + n]
            limit = jnp.where(p >= slots - 1, FAR // 2, p) - base
            parts = []
            for t in range(slices):
                own = scores[i][:, t * LANES : (t + 1) * LANES]
                other = pltpu.roll(own, heads, 0)
                other = jnp.where(
                    low_half, pltpu.roll(other, LANES - kvs, 1), pltpu.roll(other, kvs, 1)
                )
                ok = slot_of_col <= limit - t * (LANES // per_slot)
                parts.append(jnp.where(ok, (own + other) * scale, -jnp.inf))
            top = functools.reduce(jnp.maximum, parts)
            top = jnp.max(top, axis=1, keepdims=True)
            floor = jnp.where(top == -jnp.inf, 0.0, top)
            parts = [jnp.exp(part - floor) for part in parts]
            total = jnp.sum(functools.reduce(jnp.add, parts), axis=1, keepdims=True)
            span = pl.ds(pl.multiple_of(n * qrows, qrows), qrows)
            m_s[span, :] = jnp.broadcast_to(top, (qrows, LANES))
            l_s[span, :] = jnp.broadcast_to(total, (qrows, LANES))
            probs.append(jnp.concatenate([part.astype(BF16) for part in parts], axis=1))
        for i in range(BLOCK):
            n = j * BLOCK + i
            span = pl.ds(pl.multiple_of(n * qrows, qrows), qrows)
            o_s[span, :] = jnp.dot(probs[i], vbuf[n], preferred_element_type=F32)
        for copy in out_copies(j):
            copy.start()
        return carry

    lax.fori_loop(0, n_blocks, block_step, 0)

    left = lax.broadcasted_iota(jnp.int32, (half, LANES), 1) < LANES // 2
    for h in range(heads):
        lo, hi = pl.ds(h, half, stride=qrows), pl.ds(heads + h, half, stride=qrows)
        part_ref[h, 0], part_ref[h, 1] = o_s[lo, :], o_s[hi, :]
        part_ref[h, 2] = jnp.where(left, m_s[lo, :], l_s[lo, :])
    for j in range(n_blocks):
        for copy in out_copies(j):
            copy.wait()


def first_half(positions, tokens, gain, w_q, w_k, w_v, rows_k, rows_v):
    rows, width = tokens.shape
    head_dim = 2 * LANES
    heads = w_q.shape[1] // head_dim
    kvs = w_k.shape[1] // head_dim
    qrows = 2 * heads
    vmem = pl.BlockSpec(memory_space=pltpu.VMEM)
    hbm = pl.BlockSpec(memory_space=pltpu.HBM)
    n_blocks = rows // 2 // BLOCK
    tile = lambda n: pltpu.VMEM((rows * n, LANES), F32)
    return pl.pallas_call(
        first_kernel,
        out_shape=(
            pltpu.VMEM((heads, 3, rows // 2, LANES), F32),
            jax.ShapeDtypeStruct(rows_k.shape, BF16),
            jax.ShapeDtypeStruct(rows_v.shape, BF16),
            tile(qrows), tile(qrows), tile(qrows),
            *(pltpu.VMEM((rows * qrows, LANES), jnp.int32) for _ in range(2)),
            tile(16), tile(16),
        ),
        in_specs=[hbm] * 8,
        out_specs=(vmem, hbm, hbm) + (vmem,) * 7,
        scratch_shapes=[
            pltpu.VMEM((heads + 2 * kvs, width, head_dim), BF16),
            pltpu.VMEM((rows // 2, *rows_k.shape[1:]), BF16),
            pltpu.VMEM((rows // 2, *rows_v.shape[1:]), BF16),
            tile(1),
            pltpu.VMEM((rows // 2 * qrows, LANES), F32),
            pltpu.VMEM((rows // 2 * qrows, LANES), F32),
            pltpu.VMEM((rows // 2 * qrows, LANES), F32),
            pltpu.SMEM((rows,), jnp.int32),
            pltpu.VMEM(tokens.shape, BF16),
            pltpu.VMEM(gain.shape, BF16),
            pltpu.SemaphoreType.DMA((heads + 2 * kvs,)),
            pltpu.SemaphoreType.DMA((n_blocks,)),
            pltpu.SemaphoreType.DMA((n_blocks,)),
            pltpu.SemaphoreType.DMA((2,)),
            pltpu.SemaphoreType.DMA((3,)),
        ],
        compiler_params=pltpu.CompilerParams(vmem_limit_bytes=36 << 20),
        name="first",
    )(*(pltpu.with_memory_space_constraint(v, pltpu.HBM) for v in (positions, tokens, gain, w_q, w_k, w_v, rows_k, rows_v)))


def combine(mine, theirs):
    left = lax.broadcasted_iota(jnp.int32, mine[2].shape, mine[2].ndim - 1) < LANES // 2
    axis = mine[2].ndim - 1

    def unpack(stats):
        turned = pltpu.roll(stats, LANES // 2, axis)
        return jnp.where(left, stats, turned), jnp.where(left, turned, stats)

    (m_a, l_a), (m_b, l_b) = unpack(mine[2]), unpack(theirs[2])
    top = jnp.maximum(m_a, m_b)
    f_a = jnp.where(m_a == -jnp.inf, 0.0, jnp.exp(m_a - top))
    f_b = jnp.where(m_b == -jnp.inf, 0.0, jnp.exp(m_b - top))
    return mine[0] * f_a + theirs[0] * f_b, mine[1] * f_a + theirs[1] * f_b, top, l_a * f_a + l_b * f_b


def layer_kernel(
    kv_heads, x_hbm, gm_hbm, wo_hbm, wg_hbm, wu_hbm, wd_hbm, ck_hbm, cv_hbm,
    far_ref, q_s, kx_s, vx_s, lim_s, hid_s,
    out_ref, kbuf, vbuf,
    ring, o_s, m_s, l_s, part, rd, sx, rx,
    po, ro, so, yo, hb, act, pm, rm, sm, ym, ob,
    x_ref, gm_ref,
    small_sem, k_sem, v_sem, o_sem, c_sem, send_sem, recv_sem,
):
    rows, width = x_ref.shape
    head_dim = ring.shape[2]
    heads = far_ref.shape[0]
    kvs = kv_heads
    group = heads // kvs
    per_slot, qrows = 2 * kvs, 2 * heads
    key_rows = ck_hbm.shape[1]
    local_slots = key_rows // per_slot
    slices = key_rows // LANES
    n_blocks = rows // 2 // BLOCK
    mine_h = heads // 2
    half, quarter = rows // 2, rows // 4
    sp, tp = lax.axis_index("sp"), lax.axis_index("tp")
    x, k = sp // 2, lax.rem(sp, 2)
    d_dev, x_dev, y_dev = {"sp": x * 2 + 1 - k}, {"sp": (1 - x) * 2 + k}, {"tp": 1 - tp}
    m_cols = act.shape[1]
    span = width // CHUNKS

    barrier = pltpu.get_barrier_semaphore()
    for dev in (d_dev, x_dev, y_dev):
        pl.semaphore_signal(barrier, inc=1, device_id=dev, device_id_type=MESH)

    counter = [0]

    def remote(src, dst, dev):
        n = counter[0]
        counter[0] += 1
        return pltpu.make_async_remote_copy(
            src_ref=src, dst_ref=dst, send_sem=send_sem.at[n], recv_sem=recv_sem.at[n],
            device_id=dev, device_id_type=MESH,
        )

    def in_copies(j):
        near, here = pl.ds(x * half + j * BLOCK, BLOCK), pl.ds(j * BLOCK, BLOCK)
        return (
            pltpu.make_async_copy(ck_hbm.at[near], kbuf.at[here], k_sem.at[j]),
            pltpu.make_async_copy(cv_hbm.at[near], vbuf.at[here], v_sem.at[j]),
        )

    small = [
        pltpu.make_async_copy(src, dst, small_sem.at[i])
        for i, (src, dst) in enumerate(
            ((x_hbm, x_ref), (gm_hbm, gm_ref))
        )
    ]
    def read(blocks):
        for j in blocks:
            for copy in in_copies(j):
                copy.start()

    read(range(EAGER[0]))

    n_w = 0
    o_rows = mine_h * head_dim
    per_o = width // o_rows
    o_copies = [
        pltpu.make_async_copy(
            wo_hbm.at[pl.ds(k * o_rows, o_rows), pl.ds(c * head_dim, head_dim)],
            ring.at[n_w + c // per_o, pl.ds((c % per_o) * o_rows, o_rows)],
            o_sem.at[c],
        )
        for c in range(width // head_dim)
    ]
    n_gate = m_cols // head_dim
    ring_at = lambda i: (n_w + 2 + i) % SLOTS
    chunks = []
    for c in range(n_gate):
        at = pl.ds(pl.multiple_of(k * m_cols + c * head_dim, LANES), head_dim)
        chunks += [wg_hbm.at[:, at], wu_hbm.at[:, at]]
    for c in range(width // head_dim):
        chunks.append(wd_hbm.at[pl.ds(pl.multiple_of(k * m_cols, LANES), m_cols), pl.ds(c * head_dim, head_dim)])
    chunks = [
        pltpu.make_async_copy(src, ring.at[ring_at(i)], c_sem.at[i]) for i, src in enumerate(chunks)
    ]
    queue = iter(chunks)

    started = [0]

    def fetch(n, limit=len(chunks)):
        n = min(n, limit - started[0])
        started[0] += n
        for copy in itertools.islice(queue, n):
            copy.start()

    row = lax.broadcasted_iota(jnp.int32, (qrows, LANES), 0)
    col = lax.broadcasted_iota(jnp.int32, (qrows, LANES), 1)
    half_of_col = (col // kvs) % 2
    fits = (half_of_col == row // heads) & (col % kvs == (row % heads) // group)
    slot_of_col = jnp.where(fits, col // per_slot, FAR)
    low_half = half_of_col == 0
    scale = 1.0 / math.sqrt(head_dim)

    def block_step(j, carry):
        for copy in in_copies(j):
            copy.wait()
        first = x * half + j * BLOCK
        at_rows = [pl.ds(pl.multiple_of((first + i) * qrows, qrows), qrows) for i in range(BLOCK)]
        scores = []
        for i in range(BLOCK):
            scores.append(
                lax.dot_general(
                    q_s[at_rows[i], :].astype(BF16), kbuf[j * BLOCK + i], (((1,), (1,)), ((), ())),
                    preferred_element_type=F32,
                )
            )
        probs, news = [], []
        for i in range(BLOCK):
            limit, hidden = lim_s[at_rows[i], :], hid_s[at_rows[i], :]
            fresh = q_s[at_rows[i], :] * kx_s[at_rows[i], :]
            fresh = jnp.sum(fresh + pltpu.roll(fresh, heads, 0), axis=1, keepdims=True) * scale
            fresh = jnp.where(hidden[:, :1] >= 0, fresh, -jnp.inf)
            parts = []
            for t in range(slices):
                own = scores[i][:, t * LANES : (t + 1) * LANES]
                other = pltpu.roll(own, heads, 0)
                other = jnp.where(
                    low_half, pltpu.roll(other, LANES - kvs, 1), pltpu.roll(other, kvs, 1)
                )
                shift = t * (LANES // per_slot)
                ok = (slot_of_col <= limit - shift) & (slot_of_col != hidden - shift)
                parts.append(jnp.where(ok, (own + other) * scale, -jnp.inf))
            top = functools.reduce(jnp.maximum, parts)
            top = jnp.maximum(jnp.max(top, axis=1, keepdims=True), fresh)
            floor = jnp.where(top == -jnp.inf, 0.0, top)
            parts = [jnp.exp(part_t - floor) for part_t in parts]
            new = jnp.exp(fresh - floor)
            total = jnp.sum(functools.reduce(jnp.add, parts), axis=1, keepdims=True) + new
            at = pl.ds(pl.multiple_of((j * BLOCK + i) * qrows, qrows), qrows)
            m_s[at, :] = jnp.broadcast_to(top, (qrows, LANES))
            l_s[at, :] = jnp.broadcast_to(total, (qrows, LANES))
            news.append(new)
            probs.append(jnp.concatenate([part_t.astype(BF16) for part_t in parts], axis=1))
        for i in range(BLOCK):
            at = pl.ds(pl.multiple_of((j * BLOCK + i) * qrows, qrows), qrows)
            o_s[at, :] = (
                jnp.dot(probs[i], vbuf[j * BLOCK + i], preferred_element_type=F32) + news[i] * vx_s[at_rows[i], :]
            )
        return carry

    size = rows // GROUPS
    my_heads, their_heads = pl.ds(k * mine_h, mine_h), pl.ds((1 - k) * mine_h, mine_h)
    spans = [pl.ds(g * size, size) for g in range(GROUPS)]
    near = GROUPS // 2
    sources = [far_ref.at[their_heads, :, spans[g]] for g in range(near)]
    sources += [part.at[their_heads, :, spans[g]] for g in range(near)]
    swaps_a = [remote(src, rd.at[:, :, at], d_dev) for src, at in zip(sources, spans)]
    cross_a = [remote(sx.at[:, :, at], rx.at[:, :, at], x_dev) for at in spans[: GROUPS // 2]]
    left = lax.broadcasted_iota(jnp.int32, (mine_h, size, LANES), 2) < LANES // 2
    joined = [None] * GROUPS

    def publish(g):
        at = spans[g - near]
        for h in range(heads):
            lo = pl.ds((g - near) * size * qrows + h, size, stride=qrows)
            hi = pl.ds((g - near) * size * qrows + heads + h, size, stride=qrows)
            part[h, 0, at], part[h, 1, at] = o_s[lo, :], o_s[hi, :]
            part[h, 2, at] = jnp.where(left[0], m_s[lo, :], l_s[lo, :])
        swaps_a[g].start()

    def chip(g):
        swaps_a[g].wait_recv()
        at = spans[g]
        here, local = (far_ref, at) if g < near else (part, spans[g - near])
        o_a, o_b, m, l = combine(
            [here[my_heads, i, local] for i in range(3)], [rd[:, i, at] for i in range(3)]
        )
        value = [o_a, o_b, jnp.where(left, m, l)]
        if g < GROUPS // 2:
            for i in range(3):
                sx[:, i, at] = value[i]
            cross_a[g].start()
        joined[g] = value

    pl.semaphore_wait(barrier, 3)
    for g in range(near):
        swaps_a[g].start()
    read(range(*EAGER))
    for copy in small:
        copy.start()
    step = n_blocks // near
    lax.fori_loop(0, step, block_step, 0)
    for g in range(near):
        chip(g)
    read(range(EAGER[1], n_blocks))
    publish(near)
    for copy in o_copies:
        copy.start()
    lax.fori_loop(step, n_blocks, block_step, 0)
    publish(GROUPS - 1)
    fetch(3)
    for g in range(near, GROUPS):
        chip(g)
    pieces = []
    for g in range(GROUPS // 2):
        cross_a[g].wait_recv()
        o_a, o_b, _, l = combine(joined[GROUPS // 2 + g], [rx[:, i, spans[g]] for i in range(3)])
        o_a, o_b = (o_a / l).astype(BF16), (o_b / l).astype(BF16)
        pieces.append(jnp.concatenate([v[h] for h in range(mine_h) for v in (o_a, o_b)], axis=-1))
    attended = jnp.concatenate(pieces, axis=0)
    for copy in small:
        copy.wait()

    own, other = pl.ds(k * quarter, quarter), pl.ds((1 - k) * quarter, quarter)
    my_rows = pl.ds(pl.multiple_of(x * half + k * quarter, quarter), quarter)
    x_peer_rows = pl.ds(pl.multiple_of((1 - x) * half + k * quarter, quarter), quarter)
    cols = [pl.ds(c * span, span) for c in range(CHUNKS)]
    per_span = span // head_dim

    def staged(dot, swap, cross, *rest):
        for c in range(CHUNKS + 2):
            if c < CHUNKS:
                dot(c)
            if c >= 2:
                swap(c - 2)
        for c in range(CHUNKS):
            cross(c)
        for c in range(CHUNKS + len(rest) - 1):
            for s, stage in enumerate(rest):
                if 0 <= c - s < CHUNKS:
                    stage(c - s)

    swaps = [remote(po.at[other, c], ro.at[:, c], d_dev) for c in cols]
    crosses = [remote(so.at[:, c], yo.at[:, c], y_dev) for c in cols]
    gathers = [remote(hb.at[own, c], hb.at[own, c], d_dev) for c in cols]

    def o_dot(c):
        for i in range(c * per_span, (c + 1) * per_span):
            o_copies[i].wait()
            w = ring[n_w + i // per_o, (i % per_o) * o_rows : (i % per_o + 1) * o_rows, :]
            po[:, i * head_dim : (i + 1) * head_dim] = jnp.dot(attended, w, preferred_element_type=F32)
        swaps[c].start()

    def o_swap(c):
        swaps[c].wait_recv()
        so[:, cols[c]] = po[own, cols[c]] + ro[:, cols[c]]
        crosses[c].start()
        fetch(-(-SLOTS // CHUNKS), SLOTS)

    def o_cross(c):
        crosses[c].wait_recv()
        total = so[:, cols[c]] + yo[:, cols[c]]
        hb[own, cols[c]] = (x_ref[my_rows, cols[c]].astype(F32) + total).astype(BF16).astype(F32)
        gathers[c].start()

    def o_gather(c):
        gathers[c].wait_recv()

    staged(o_dot, o_swap, o_cross, o_gather)

    normed_m = rms_norm(hb[...], gm_ref[...])
    for c in range(n_gate):
        chunks[2 * c].wait()
        chunks[2 * c + 1].wait()
        gate = jnp.dot(normed_m, ring[ring_at(2 * c)], preferred_element_type=F32)
        up = jnp.dot(normed_m, ring[ring_at(2 * c + 1)], preferred_element_type=F32)
        act[:, c * head_dim : (c + 1) * head_dim] = (jax.nn.silu(gate) * up).astype(BF16)
        fetch(2)

    swaps_m = [remote(pm.at[other, c], rm.at[:, c], d_dev) for c in cols]
    crosses_m = [remote(sm.at[:, c], ym.at[:, c], y_dev) for c in cols]
    to_core = [remote(ob.at[my_rows, c], ob.at[my_rows, c], d_dev) for c in cols]
    to_x = [remote(ob.at[my_rows, c], ob.at[my_rows, c], x_dev) for c in cols]
    onward = [remote(ob.at[x_peer_rows, c], ob.at[x_peer_rows, c], d_dev) for c in cols]

    def m_dot(c):
        for i in range(c * per_span, (c + 1) * per_span):
            chunks[2 * n_gate + i].wait()
            pm[:, i * head_dim : (i + 1) * head_dim] = jnp.dot(
                act[...], ring[ring_at(2 * n_gate + i)], preferred_element_type=F32
            )
        swaps_m[c].start()

    def m_swap(c):
        swaps_m[c].wait_recv()
        sm[:, cols[c]] = pm[own, cols[c]] + rm[:, cols[c]]
        crosses_m[c].start()

    def m_cross(c):
        crosses_m[c].wait_recv()
        total = sm[:, cols[c]] + ym[:, cols[c]]
        ob[my_rows, cols[c]] = (hb[own, cols[c]] + total).astype(BF16).astype(F32)
        to_x[c].start()
        to_core[c].start()

    def m_gather(c):
        to_x[c].wait_recv()
        onward[c].start()

    def m_last(c):
        to_core[c].wait_recv()
        onward[c].wait_recv()
        out_ref[:, cols[c]] = ob[:, cols[c]].astype(BF16)

    staged(m_dot, m_swap, m_cross, m_gather, m_last)
    for copy in [*swaps_a, *cross_a, *swaps, *crosses, *gathers, *swaps_m, *crosses_m, *to_core, *to_x, *onward]:
        copy.wait_send()


def layer(tokens, gain, w_o, w_gate, w_up, w_down, rows_k, rows_v, kvs, carried):
    rows, width = tokens.shape
    head_dim = 2 * LANES
    heads = carried[0].shape[0]
    qrows = 2 * heads
    half, quarter = rows // 2, rows // 4
    cut = w_gate.shape[1] // 2
    n_blocks = half // BLOCK
    vmem = pl.BlockSpec(memory_space=pltpu.VMEM)
    hbm = pl.BlockSpec(memory_space=pltpu.HBM)
    flat = lambda n: pltpu.VMEM((n, width), F32)
    stats = lambda h, n: pltpu.VMEM((h, 3, n, LANES), F32)
    dma = lambda n: pltpu.SemaphoreType.DMA((n,))
    n_remote = GROUPS + GROUPS // 2 + 8 * CHUNKS
    args = (tokens, gain, w_o, w_gate, w_up, w_down, rows_k, rows_v)
    shape = (half, *rows_k.shape[1:])
    return pl.pallas_call(
        functools.partial(layer_kernel, kvs),
        out_shape=(
            pltpu.VMEM(tokens.shape, BF16),
            pltpu.VMEM(shape, BF16),
            pltpu.VMEM(shape, BF16),
        ),
        in_specs=[hbm] * len(args) + [vmem] * len(carried),
        out_specs=(vmem,) * 3,
        scratch_shapes=[
            pltpu.VMEM((SLOTS, width, head_dim), BF16),
            *(pltpu.VMEM((half * qrows, LANES), F32) for _ in range(3)),
            stats(heads, half), stats(heads // 2, rows), stats(heads // 2, half), stats(heads // 2, half),
            flat(half), flat(quarter), flat(quarter), flat(quarter), flat(half),
            pltpu.VMEM((half, cut), BF16),
            flat(half), flat(quarter), flat(quarter), flat(quarter), flat(rows),
            pltpu.VMEM(tokens.shape, BF16),
            pltpu.VMEM(gain.shape, BF16),
            dma(2), dma(n_blocks), dma(n_blocks), dma(width // head_dim),
            dma(2 * (cut // head_dim) + width // head_dim), dma(n_remote), dma(n_remote),
        ],
        compiler_params=pltpu.CompilerParams(
            vmem_limit_bytes=LAYER_VMEM << 20, collective_id=0, has_side_effects=True
        ),
        name="layer",
    )(*(pltpu.with_memory_space_constraint(v, pltpu.HBM) for v in args), *carried)


def write_kernel(pos_hbm, t_ref, kn_s, vn_s, _bk, _bv, _k, _v, out_ref, nk_hbm, nv_hbm, kbuf, vbuf, pos, sem, tile_sem, pos_sem):
    rows, key_rows, _ = kbuf.shape
    per_slot = 4
    local_slots = key_rows // per_slot
    slots = local_slots * lax.axis_size("sp")
    base = lax.axis_index("sp") * local_slots
    start = lax.axis_index("sp") // 2 * rows
    per_tile = 16 // per_slot
    n_blocks = rows // BLOCK
    tile_row = lax.broadcasted_iota(jnp.int32, (16, LANES), 0) // per_slot

    def copies(j):
        here, near = pl.ds(j * BLOCK, BLOCK), pl.ds(start + j * BLOCK, BLOCK)
        return (
            pltpu.make_async_copy(kbuf.at[here], nk_hbm.at[near], sem.at[0, j]),
            pltpu.make_async_copy(vbuf.at[here], nv_hbm.at[near], sem.at[1, j]),
        )

    def target(b):
        local = lax.rem(pos[b], slots) - base
        owned = (local >= 0) & (local < local_slots)
        safe = jnp.where(owned, local, 0)
        hit = jnp.where(owned, lax.rem(safe, per_tile), -1)
        return hit, pl.ds(pl.multiple_of((safe // per_tile) * 16, 16), 16)

    def tile_copies(n):
        at = target(start + n)[1]
        return (
            pltpu.make_async_copy(kbuf.at[n, at], nk_hbm.at[start + n, at], tile_sem.at[0]),
            pltpu.make_async_copy(vbuf.at[n, at], nv_hbm.at[start + n, at], tile_sem.at[1]),
        )

    def patch(n):
        b = start + n
        hit, at = target(b)
        for buf, new in ((kbuf, kn_s), (vbuf, vn_s)):
            fresh = new[pl.ds(pl.multiple_of(b * 16, 16), 16), :]
            buf[n, at, :] = jnp.where(tile_row == hit, fresh, buf[n, at, :].astype(F32)).astype(BF16)

    pos_copy = pltpu.make_async_copy(pos_hbm, pos, pos_sem)
    pos_copy.start()
    for j in range(EARLY):
        for copy in copies(j):
            copy.start()
    out_ref[...] = t_ref[...]
    pos_copy.wait()
    for j in range(EARLY, n_blocks + 1):
        if j < n_blocks:
            for i in range(BLOCK):
                patch(j * BLOCK + i)
        if j > EARLY:
            for copy in copies(j - 1):
                copy.start()
    for j in range(EARLY):
        for copy in copies(j):
            copy.wait()
        for i in range(BLOCK):
            patch(j * BLOCK + i)
        if j:
            for i in range(BLOCK):
                for copy in tile_copies((j - 1) * BLOCK + i):
                    copy.start()
    for i in range(BLOCK):
        for copy in tile_copies((EARLY - 1) * BLOCK + i):
            copy.start()
    for j in range(EARLY, n_blocks):
        for copy in copies(j):
            copy.wait()
    for n in range(EARLY * BLOCK):
        for copy in tile_copies(n):
            copy.wait()


def write(positions, layer_out, fresh_k, fresh_v, buf_k, buf_v, new_k, new_v):
    vmem = pl.BlockSpec(memory_space=pltpu.VMEM)
    hbm = pl.BlockSpec(memory_space=pltpu.HBM)
    return pl.pallas_call(
        write_kernel,
        out_shape=(
            *(jax.ShapeDtypeStruct(v.shape, BF16) for v in (layer_out, new_k, new_v)),
            pltpu.VMEM(buf_k.shape, BF16),
            pltpu.VMEM(buf_v.shape, BF16),
        ),
        in_specs=[hbm] + [vmem] * 5 + [hbm] * 2,
        out_specs=(vmem, hbm, hbm, vmem, vmem),
        input_output_aliases={4: 3, 5: 4, 6: 1, 7: 2},
        scratch_shapes=[
            pltpu.SMEM(positions.shape, jnp.int32),
            pltpu.SemaphoreType.DMA((2, buf_k.shape[0] // BLOCK)),
            pltpu.SemaphoreType.DMA((2,)),
            pltpu.SemaphoreType.DMA,
        ],
        compiler_params=pltpu.CompilerParams(vmem_limit_bytes=LAYER_VMEM << 20),
        name="write",
    )(pltpu.with_memory_space_constraint(positions, pltpu.HBM), layer_out, fresh_k, fresh_v, buf_k, buf_v, new_k, new_v)[:3]


def to_rows(cache):
    b, s, kv, d = cache.shape
    return cache.reshape(b, s, kv, d // LANES, LANES).transpose(0, 1, 3, 2, 4).reshape(b, -1, LANES)


def from_rows(rows, shape):
    b, s, kv, d = shape
    return rows.reshape(b, s, d // LANES, kv, LANES).transpose(0, 1, 3, 2, 4).reshape(shape)


def solution(mesh):
    cache_spec = P("dp", "sp", "tp", None)
    row_spec = P("dp", None)
    col_spec = P(None, "tp")
    in_specs = (row_spec, P("dp"), cache_spec, cache_spec, P(None), col_spec, col_spec, col_spec, P("tp", None), P(None), col_spec, col_spec, P("tp", None))
    out_specs = (row_spec, cache_spec, cache_spec)

    def local_step(tokens, positions, cache_k, cache_v, attn_gain, w_q, w_k, w_v, w_o, mlp_gain, w_gate, w_up, w_down):
        old_k, old_v = to_rows(cache_k), to_rows(cache_v)
        far, rows_k, rows_v, *carried, fresh_k, fresh_v = first_half(
            positions, tokens, attn_gain, w_q, w_k, w_v, old_k, old_v
        )
        out, buf_k, buf_v = layer(
            tokens, mlp_gain, w_o, w_gate, w_up, w_down, old_k, old_v, cache_k.shape[2], (far, *carried)
        )
        layer_out, rows_k, rows_v = write(positions, out, fresh_k, fresh_v, buf_k, buf_v, rows_k, rows_v)
        new_k = from_rows(rows_k, cache_k.shape)
        new_v = from_rows(rows_v, cache_v.shape)
        return layer_out, new_k, new_v

    return jax.shard_map(local_step, mesh=mesh, in_specs=in_specs, out_specs=out_specs, check_vma=False)
```

```python
import functools
import itertools
import math

import jax
import jax.numpy as jnp
from jax import lax
from jax.experimental import pallas as pl
from jax.experimental.pallas import tpu as pltpu
from jax.sharding import PartitionSpec as P

NORM_EPS = 1e-5
ROPE_THETA = 10000.0
LANES = 128
F32 = jnp.float32
BF16 = jnp.bfloat16
FAR = 1 << 28
BLOCK = 4
EARLY = 3
EAGER = (2, 6)
FIRST = 4
SLOTS = 22
LAYER_VMEM = 35
CHUNKS = 5
GROUPS = 4
MESH = pl.DeviceIdType.MESH


def rms_norm(values, gain):
    wide = values.astype(F32)
    inv_rms = lax.rsqrt(jnp.mean(wide * wide, axis=-1, keepdims=True) + NORM_EPS)
    return (wide * inv_rms * gain.astype(F32)).astype(BF16)


def first_kernel(
    pos_hbm, x_hbm, gain_hbm, wq_hbm, wk_hbm, wv_hbm, ck_hbm, cv_hbm,
    part_ref, nk_hbm, nv_hbm, q_s, kx_s, vx_s, lim_s, hid_s, kn_s, vn_s,
    wbuf, kbuf, vbuf, ang_s, o_s, m_s, l_s,
    pos, x_ref, gain_ref, w_sem, k_sem, v_sem, out_sem, x_sem,
):
    rows = x_ref.shape[0]
    head_dim = 2 * LANES
    heads = wq_hbm.shape[1] // head_dim
    kvs = wk_hbm.shape[1] // head_dim
    group = heads // kvs
    per_slot = 2 * kvs
    qrows = 2 * heads
    key_rows = ck_hbm.shape[1]
    local_slots = key_rows // per_slot
    slots = local_slots * lax.axis_size("sp")
    slices = key_rows // LANES
    half = rows // 2
    n_blocks = half // BLOCK
    start = (1 - lax.axis_index("sp") // 2) * half
    base = lax.axis_index("sp") * local_slots

    def w_copy(n):
        src, col = (
            (wk_hbm, n) if n < kvs else (wv_hbm, n - kvs) if n < 2 * kvs else (wq_hbm, n - 2 * kvs)
        )
        return pltpu.make_async_copy(src.at[:, pl.ds(col * head_dim, head_dim)], wbuf.at[n], w_sem.at[n])

    def in_copies(j):
        far, here = pl.ds(start + j * BLOCK, BLOCK), pl.ds(j * BLOCK, BLOCK)
        return (
            pltpu.make_async_copy(ck_hbm.at[far], kbuf.at[here], k_sem.at[j]),
            pltpu.make_async_copy(cv_hbm.at[far], vbuf.at[here], v_sem.at[j]),
        )

    def out_copies(j):
        far, here = pl.ds(start + j * BLOCK, BLOCK), pl.ds(j * BLOCK, BLOCK)
        return (
            pltpu.make_async_copy(kbuf.at[here], nk_hbm.at[far], out_sem.at[0]),
            pltpu.make_async_copy(vbuf.at[here], nv_hbm.at[far], out_sem.at[1]),
        )

    small = [
        pltpu.make_async_copy(src, dst, x_sem.at[i])
        for i, (src, dst) in enumerate(((pos_hbm, pos), (x_hbm, x_ref), (gain_hbm, gain_ref)))
    ]
    for copy in small:
        copy.start()
    n_w = heads + 2 * kvs
    for n in range(n_w // 2):
        w_copy(n).start()

    lane = lax.broadcasted_iota(jnp.int32, (1, LANES), 1).astype(F32)
    freq = jnp.exp2(lane * (-math.log2(ROPE_THETA) / LANES))

    for copy in small:
        copy.wait()
    for n in range(n_w // 2, n_w):
        w_copy(n).start()
    for j in range(FIRST):
        for copy in in_copies(j):
            copy.start()

    def angle_row(b, carry):
        p = pos[b]
        ang_s[pl.ds(b, 1), :] = freq * p.astype(F32)
        local = lax.rem(p, slots) - base
        owned = (local >= 0) & (local < local_slots)
        span = pl.ds(pl.multiple_of(b * qrows, qrows), qrows)
        lim_s[span, :] = jnp.full((qrows, LANES), jnp.where(p >= slots - 1, FAR // 2, p) - base, jnp.int32)
        hid_s[span, :] = jnp.full((qrows, LANES), jnp.where(owned, local, -FAR), jnp.int32)
        return carry

    lax.fori_loop(0, rows, angle_row, 0, unroll=8)
    angles = ang_s[...]
    cos_t, sin_t = jnp.cos(angles), jnp.sin(angles)
    normed = rms_norm(x_ref[...], gain_ref[...])

    for n in range(n_w):
        w_copy(n).wait()
        if FIRST + n < n_blocks:
            for copy in in_copies(FIRST + n):
                copy.start()
        lin = jnp.dot(normed, wbuf[n], preferred_element_type=F32)
        first, second = lin[:, :LANES], lin[:, LANES:]
        if not kvs <= n < 2 * kvs:
            first, second = first * cos_t - second * sin_t, second * cos_t + first * sin_t
        first, second = first.astype(BF16).astype(F32), second.astype(BF16).astype(F32)
        if n >= 2 * kvs:
            h = n - 2 * kvs
            q_s[pl.ds(h, rows, stride=qrows), :] = first
            q_s[pl.ds(heads + h, rows, stride=qrows), :] = second
        else:
            dst, tile, kv = (kn_s, kx_s, n) if n < kvs else (vn_s, vx_s, n - kvs)
            for rep in range(16 // per_slot):
                dst[pl.ds(rep * per_slot + kv, rows, stride=16), :] = first
                dst[pl.ds(rep * per_slot + kvs + kv, rows, stride=16), :] = second
            for g in range(group):
                tile[pl.ds(kv * group + g, rows, stride=qrows), :] = first
                tile[pl.ds(heads + kv * group + g, rows, stride=qrows), :] = second

    row = lax.broadcasted_iota(jnp.int32, (qrows, LANES), 0)
    col = lax.broadcasted_iota(jnp.int32, (qrows, LANES), 1)
    half_of_col = (col // kvs) % 2
    fits = (half_of_col == row // heads) & (col % kvs == (row % heads) // group)
    slot_of_col = jnp.where(fits, col // per_slot, FAR)
    low_half = half_of_col == 0
    patch_row = lax.broadcasted_iota(jnp.int32, (16, LANES), 0) // per_slot
    scale = 1.0 / math.sqrt(head_dim)

    def block_step(j, carry):
        for copy in in_copies(j):
            copy.wait()
        for i in range(BLOCK):
            n = j * BLOCK + i
            b = start + n
            local = lax.rem(pos[b], slots) - base
            owned = (local >= 0) & (local < local_slots)
            safe = jnp.where(owned, local, 0)
            hit = jnp.where(owned, lax.rem(safe, 16 // per_slot), -1)
            span = pl.ds(pl.multiple_of((safe // (16 // per_slot)) * 16, 16), 16)
            for buf, new in ((kbuf, kn_s), (vbuf, vn_s)):
                old = buf[n, span, :].astype(F32)
                fresh = new[pl.ds(pl.multiple_of(b * 16, 16), 16), :]
                buf[n, span, :] = jnp.where(patch_row == hit, fresh, old).astype(BF16)
        scores = []
        for i in range(BLOCK):
            b = start + j * BLOCK + i
            q = q_s[pl.ds(pl.multiple_of(b * qrows, qrows), qrows), :].astype(BF16)
            scores.append(
                lax.dot_general(q, kbuf[j * BLOCK + i], (((1,), (1,)), ((), ())), preferred_element_type=F32)
            )
        probs = []
        for i in range(BLOCK):
            n = j * BLOCK + i
            p = pos[start + n]
            limit = jnp.where(p >= slots - 1, FAR // 2, p) - base
            parts = []
            for t in range(slices):
                own = scores[i][:, t * LANES : (t + 1) * LANES]
                other = pltpu.roll(own, heads, 0)
                other = jnp.where(
                    low_half, pltpu.roll(other, LANES - kvs, 1), pltpu.roll(other, kvs, 1)
                )
                ok = slot_of_col <= limit - t * (LANES // per_slot)
                parts.append(jnp.where(ok, (own + other) * scale, -jnp.inf))
            top = functools.reduce(jnp.maximum, parts)
            top = jnp.max(top, axis=1, keepdims=True)
            floor = jnp.where(top == -jnp.inf, 0.0, top)
            parts = [jnp.exp(part - floor) for part in parts]
            total = jnp.sum(functools.reduce(jnp.add, parts), axis=1, keepdims=True)
            span = pl.ds(pl.multiple_of(n * qrows, qrows), qrows)
            m_s[span, :] = jnp.broadcast_to(top, (qrows, LANES))
            l_s[span, :] = jnp.broadcast_to(total, (qrows, LANES))
            probs.append(jnp.concatenate([part.astype(BF16) for part in parts], axis=1))
        for i in range(BLOCK):
            n = j * BLOCK + i
            span = pl.ds(pl.multiple_of(n * qrows, qrows), qrows)
            o_s[span, :] = jnp.dot(probs[i], vbuf[n], preferred_element_type=F32)
        for copy in out_copies(j):
            copy.start()
        return carry

    lax.fori_loop(0, n_blocks, block_step, 0)

    left = lax.broadcasted_iota(jnp.int32, (half, LANES), 1) < LANES // 2
    for h in range(heads):
        lo, hi = pl.ds(h, half, stride=qrows), pl.ds(heads + h, half, stride=qrows)
        part_ref[h, 0], part_ref[h, 1] = o_s[lo, :], o_s[hi, :]
        part_ref[h, 2] = jnp.where(left, m_s[lo, :], l_s[lo, :])
    for j in range(n_blocks):
        for copy in out_copies(j):
            copy.wait()


def first_half(positions, tokens, gain, w_q, w_k, w_v, rows_k, rows_v):
    rows, width = tokens.shape
    head_dim = 2 * LANES
    heads = w_q.shape[1] // head_dim
    kvs = w_k.shape[1] // head_dim
    qrows = 2 * heads
    vmem = pl.BlockSpec(memory_space=pltpu.VMEM)
    hbm = pl.BlockSpec(memory_space=pltpu.HBM)
    n_blocks = rows // 2 // BLOCK
    tile = lambda n: pltpu.VMEM((rows * n, LANES), F32)
    return pl.pallas_call(
        first_kernel,
        out_shape=(
            pltpu.VMEM((heads, 3, rows // 2, LANES), F32),
            jax.ShapeDtypeStruct(rows_k.shape, BF16),
            jax.ShapeDtypeStruct(rows_v.shape, BF16),
            tile(qrows), tile(qrows), tile(qrows),
            *(pltpu.VMEM((rows * qrows, LANES), jnp.int32) for _ in range(2)),
            tile(16), tile(16),
        ),
        in_specs=[hbm] * 8,
        out_specs=(vmem, hbm, hbm) + (vmem,) * 7,
        scratch_shapes=[
            pltpu.VMEM((heads + 2 * kvs, width, head_dim), BF16),
            pltpu.VMEM((rows // 2, *rows_k.shape[1:]), BF16),
            pltpu.VMEM((rows // 2, *rows_v.shape[1:]), BF16),
            tile(1),
            pltpu.VMEM((rows // 2 * qrows, LANES), F32),
            pltpu.VMEM((rows // 2 * qrows, LANES), F32),
            pltpu.VMEM((rows // 2 * qrows, LANES), F32),
            pltpu.SMEM((rows,), jnp.int32),
            pltpu.VMEM(tokens.shape, BF16),
            pltpu.VMEM(gain.shape, BF16),
            pltpu.SemaphoreType.DMA((heads + 2 * kvs,)),
            pltpu.SemaphoreType.DMA((n_blocks,)),
            pltpu.SemaphoreType.DMA((n_blocks,)),
            pltpu.SemaphoreType.DMA((2,)),
            pltpu.SemaphoreType.DMA((3,)),
        ],
        compiler_params=pltpu.CompilerParams(vmem_limit_bytes=36 << 20),
        name="first",
    )(*(pltpu.with_memory_space_constraint(v, pltpu.HBM) for v in (positions, tokens, gain, w_q, w_k, w_v, rows_k, rows_v)))


def combine(mine, theirs):
    left = lax.broadcasted_iota(jnp.int32, mine[2].shape, mine[2].ndim - 1) < LANES // 2
    axis = mine[2].ndim - 1

    def unpack(stats):
        turned = pltpu.roll(stats, LANES // 2, axis)
        return jnp.where(left, stats, turned), jnp.where(left, turned, stats)

    (m_a, l_a), (m_b, l_b) = unpack(mine[2]), unpack(theirs[2])
    top = jnp.maximum(m_a, m_b)
    f_a = jnp.where(m_a == -jnp.inf, 0.0, jnp.exp(m_a - top))
    f_b = jnp.where(m_b == -jnp.inf, 0.0, jnp.exp(m_b - top))
    return mine[0] * f_a + theirs[0] * f_b, mine[1] * f_a + theirs[1] * f_b, top, l_a * f_a + l_b * f_b


def layer_kernel(
    kv_heads, x_hbm, gm_hbm, wo_hbm, wg_hbm, wu_hbm, wd_hbm, ck_hbm, cv_hbm,
    far_ref, q_s, kx_s, vx_s, lim_s, hid_s,
    out_ref, kbuf, vbuf,
    ring, o_s, m_s, l_s, part, rd, sx, rx,
    po, ro, so, yo, hb, act, pm, rm, sm, ym, ob,
    x_ref, gm_ref,
    small_sem, k_sem, v_sem, o_sem, c_sem, send_sem, recv_sem,
):
    rows, width = x_ref.shape
    head_dim = ring.shape[2]
    heads = far_ref.shape[0]
    kvs = kv_heads
    group = heads // kvs
    per_slot, qrows = 2 * kvs, 2 * heads
    key_rows = ck_hbm.shape[1]
    local_slots = key_rows // per_slot
    slices = key_rows // LANES
    n_blocks = rows // 2 // BLOCK
    mine_h = heads // 2
    half, quarter = rows // 2, rows // 4
    sp, tp = lax.axis_index("sp"), lax.axis_index("tp")
    x, k = sp // 2, lax.rem(sp, 2)
    d_dev, x_dev, y_dev = {"sp": x * 2 + 1 - k}, {"sp": (1 - x) * 2 + k}, {"tp": 1 - tp}
    m_cols = act.shape[1]
    span = width // CHUNKS

    barrier = pltpu.get_barrier_semaphore()
    for dev in (d_dev, x_dev, y_dev):
        pl.semaphore_signal(barrier, inc=1, device_id=dev, device_id_type=MESH)

    counter = [0]

    def remote(src, dst, dev):
        n = counter[0]
        counter[0] += 1
        return pltpu.make_async_remote_copy(
            src_ref=src, dst_ref=dst, send_sem=send_sem.at[n], recv_sem=recv_sem.at[n],
            device_id=dev, device_id_type=MESH,
        )

    def in_copies(j):
        near, here = pl.ds(x * half + j * BLOCK, BLOCK), pl.ds(j * BLOCK, BLOCK)
        return (
            pltpu.make_async_copy(ck_hbm.at[near], kbuf.at[here], k_sem.at[j]),
            pltpu.make_async_copy(cv_hbm.at[near], vbuf.at[here], v_sem.at[j]),
        )

    small = [
        pltpu.make_async_copy(src, dst, small_sem.at[i])
        for i, (src, dst) in enumerate(
            ((x_hbm, x_ref), (gm_hbm, gm_ref))
        )
    ]
    def read(blocks):
        for j in blocks:
            for copy in in_copies(j):
                copy.start()

    read(range(EAGER[0]))

    n_w = 0
    o_rows = mine_h * head_dim
    per_o = width // o_rows
    o_copies = [
        pltpu.make_async_copy(
            wo_hbm.at[pl.ds(k * o_rows, o_rows), pl.ds(c * head_dim, head_dim)],
            ring.at[n_w + c // per_o, pl.ds((c % per_o) * o_rows, o_rows)],
            o_sem.at[c],
        )
        for c in range(width // head_dim)
    ]
    n_gate = m_cols // head_dim
    ring_at = lambda i: (n_w + 2 + i) % SLOTS
    chunks = []
    for c in range(n_gate):
        at = pl.ds(pl.multiple_of(k * m_cols + c * head_dim, LANES), head_dim)
        chunks += [wg_hbm.at[:, at], wu_hbm.at[:, at]]
    for c in range(width // head_dim):
        chunks.append(wd_hbm.at[pl.ds(pl.multiple_of(k * m_cols, LANES), m_cols), pl.ds(c * head_dim, head_dim)])
    chunks = [
        pltpu.make_async_copy(src, ring.at[ring_at(i)], c_sem.at[i]) for i, src in enumerate(chunks)
    ]
    queue = iter(chunks)

    started = [0]

    def fetch(n, limit=len(chunks)):
        n = min(n, limit - started[0])
        started[0] += n
        for copy in itertools.islice(queue, n):
            copy.start()

    row = lax.broadcasted_iota(jnp.int32, (qrows, LANES), 0)
    col = lax.broadcasted_iota(jnp.int32, (qrows, LANES), 1)
    half_of_col = (col // kvs) % 2
    fits = (half_of_col == row // heads) & (col % kvs == (row % heads) // group)
    slot_of_col = jnp.where(fits, col // per_slot, FAR)
    low_half = half_of_col == 0
    scale = 1.0 / math.sqrt(head_dim)

    def block_step(j, carry):
        for copy in in_copies(j):
            copy.wait()
        first = x * half + j * BLOCK
        at_rows = [pl.ds(pl.multiple_of((first + i) * qrows, qrows), qrows) for i in range(BLOCK)]
        scores = []
        for i in range(BLOCK):
            scores.append(
                lax.dot_general(
                    q_s[at_rows[i], :].astype(BF16), kbuf[j * BLOCK + i], (((1,), (1,)), ((), ())),
                    preferred_element_type=F32,
                )
            )
        probs, news = [], []
        for i in range(BLOCK):
            limit, hidden = lim_s[at_rows[i], :], hid_s[at_rows[i], :]
            fresh = q_s[at_rows[i], :] * kx_s[at_rows[i], :]
            fresh = jnp.sum(fresh + pltpu.roll(fresh, heads, 0), axis=1, keepdims=True) * scale
            fresh = jnp.where(hidden[:, :1] >= 0, fresh, -jnp.inf)
            parts = []
            for t in range(slices):
                own = scores[i][:, t * LANES : (t + 1) * LANES]
                other = pltpu.roll(own, heads, 0)
                other = jnp.where(
                    low_half, pltpu.roll(other, LANES - kvs, 1), pltpu.roll(other, kvs, 1)
                )
                shift = t * (LANES // per_slot)
                ok = (slot_of_col <= limit - shift) & (slot_of_col != hidden - shift)
                parts.append(jnp.where(ok, (own + other) * scale, -jnp.inf))
            top = functools.reduce(jnp.maximum, parts)
            top = jnp.maximum(jnp.max(top, axis=1, keepdims=True), fresh)
            floor = jnp.where(top == -jnp.inf, 0.0, top)
            parts = [jnp.exp(part_t - floor) for part_t in parts]
            new = jnp.exp(fresh - floor)
            total = jnp.sum(functools.reduce(jnp.add, parts), axis=1, keepdims=True) + new
            at = pl.ds(pl.multiple_of((j * BLOCK + i) * qrows, qrows), qrows)
            m_s[at, :] = jnp.broadcast_to(top, (qrows, LANES))
            l_s[at, :] = jnp.broadcast_to(total, (qrows, LANES))
            news.append(new)
            probs.append(jnp.concatenate([part_t.astype(BF16) for part_t in parts], axis=1))
        for i in range(BLOCK):
            at = pl.ds(pl.multiple_of((j * BLOCK + i) * qrows, qrows), qrows)
            o_s[at, :] = (
                jnp.dot(probs[i], vbuf[j * BLOCK + i], preferred_element_type=F32) + news[i] * vx_s[at_rows[i], :]
            )
        return carry

    size = rows // GROUPS
    my_heads, their_heads = pl.ds(k * mine_h, mine_h), pl.ds((1 - k) * mine_h, mine_h)
    spans = [pl.ds(g * size, size) for g in range(GROUPS)]
    near = GROUPS // 2
    sources = [far_ref.at[their_heads, :, spans[g]] for g in range(near)]
    sources += [part.at[their_heads, :, spans[g]] for g in range(near)]
    swaps_a = [remote(src, rd.at[:, :, at], d_dev) for src, at in zip(sources, spans)]
    cross_a = [remote(sx.at[:, :, at], rx.at[:, :, at], x_dev) for at in spans[: GROUPS // 2]]
    left = lax.broadcasted_iota(jnp.int32, (mine_h, size, LANES), 2) < LANES // 2
    joined = [None] * GROUPS

    def publish(g):
        at = spans[g - near]
        for h in range(heads):
            lo = pl.ds((g - near) * size * qrows + h, size, stride=qrows)
            hi = pl.ds((g - near) * size * qrows + heads + h, size, stride=qrows)
            part[h, 0, at], part[h, 1, at] = o_s[lo, :], o_s[hi, :]
            part[h, 2, at] = jnp.where(left[0], m_s[lo, :], l_s[lo, :])
        swaps_a[g].start()

    def chip(g):
        swaps_a[g].wait_recv()
        at = spans[g]
        here, local = (far_ref, at) if g < near else (part, spans[g - near])
        o_a, o_b, m, l = combine(
            [here[my_heads, i, local] for i in range(3)], [rd[:, i, at] for i in range(3)]
        )
        value = [o_a, o_b, jnp.where(left, m, l)]
        if g < GROUPS // 2:
            for i in range(3):
                sx[:, i, at] = value[i]
            cross_a[g].start()
        joined[g] = value

    pl.semaphore_wait(barrier, 3)
    for g in range(near):
        swaps_a[g].start()
    read(range(*EAGER))
    for copy in small:
        copy.start()
    step = n_blocks // near
    lax.fori_loop(0, step, block_step, 0)
    for g in range(near):
        chip(g)
    read(range(EAGER[1], n_blocks))
    publish(near)
    for copy in o_copies:
        copy.start()
    lax.fori_loop(step, n_blocks, block_step, 0)
    publish(GROUPS - 1)
    fetch(3)
    for g in range(near, GROUPS):
        chip(g)
    pieces = []
    for g in range(GROUPS // 2):
        cross_a[g].wait_recv()
        o_a, o_b, _, l = combine(joined[GROUPS // 2 + g], [rx[:, i, spans[g]] for i in range(3)])
        o_a, o_b = (o_a / l).astype(BF16), (o_b / l).astype(BF16)
        pieces.append(jnp.concatenate([v[h] for h in range(mine_h) for v in (o_a, o_b)], axis=-1))
    attended = jnp.concatenate(pieces, axis=0)
    for copy in small:
        copy.wait()

    own, other = pl.ds(k * quarter, quarter), pl.ds((1 - k) * quarter, quarter)
    my_rows = pl.ds(pl.multiple_of(x * half + k * quarter, quarter), quarter)
    x_peer_rows = pl.ds(pl.multiple_of((1 - x) * half + k * quarter, quarter), quarter)
    cols = [pl.ds(c * span, span) for c in range(CHUNKS)]
    per_span = span // head_dim

    def staged(dot, swap, cross, *rest):
        for c in range(CHUNKS + 2):
            if c < CHUNKS:
                dot(c)
            if c >= 2:
                swap(c - 2)
        for c in range(CHUNKS):
            cross(c)
        for c in range(CHUNKS + len(rest) - 1):
            for s, stage in enumerate(rest):
                if 0 <= c - s < CHUNKS:
                    stage(c - s)

    swaps = [remote(po.at[other, c], ro.at[:, c], d_dev) for c in cols]
    crosses = [remote(so.at[:, c], yo.at[:, c], y_dev) for c in cols]
    gathers = [remote(hb.at[own, c], hb.at[own, c], d_dev) for c in cols]

    def o_dot(c):
        for i in range(c * per_span, (c + 1) * per_span):
            o_copies[i].wait()
            w = ring[n_w + i // per_o, (i % per_o) * o_rows : (i % per_o + 1) * o_rows, :]
            po[:, i * head_dim : (i + 1) * head_dim] = jnp.dot(attended, w, preferred_element_type=F32)
        swaps[c].start()

    def o_swap(c):
        swaps[c].wait_recv()
        so[:, cols[c]] = po[own, cols[c]] + ro[:, cols[c]]
        crosses[c].start()
        if c == CHUNKS - 1:
            fetch(15)

    def o_cross(c):
        crosses[c].wait_recv()
        total = so[:, cols[c]] + yo[:, cols[c]]
        hb[own, cols[c]] = (x_ref[my_rows, cols[c]].astype(F32) + total).astype(BF16).astype(F32)
        gathers[c].start()

    def o_gather(c):
        gathers[c].wait_recv()

    staged(o_dot, o_swap, o_cross, o_gather)
    fetch(SLOTS, SLOTS)

    normed_m = rms_norm(hb[...], gm_ref[...])
    for c in range(n_gate):
        chunks[2 * c].wait()
        chunks[2 * c + 1].wait()
        gate = jnp.dot(normed_m, ring[ring_at(2 * c)], preferred_element_type=F32)
        up = jnp.dot(normed_m, ring[ring_at(2 * c + 1)], preferred_element_type=F32)
        act[:, c * head_dim : (c + 1) * head_dim] = (jax.nn.silu(gate) * up).astype(BF16)
        fetch(2)

    swaps_m = [remote(pm.at[other, c], rm.at[:, c], d_dev) for c in cols]
    crosses_m = [remote(sm.at[:, c], ym.at[:, c], y_dev) for c in cols]
    to_core = [remote(ob.at[my_rows, c], ob.at[my_rows, c], d_dev) for c in cols]
    to_x = [remote(ob.at[my_rows, c], ob.at[my_rows, c], x_dev) for c in cols]
    onward = [remote(ob.at[x_peer_rows, c], ob.at[x_peer_rows, c], d_dev) for c in cols]

    def m_dot(c):
        for i in range(c * per_span, (c + 1) * per_span):
            chunks[2 * n_gate + i].wait()
            pm[:, i * head_dim : (i + 1) * head_dim] = jnp.dot(
                act[...], ring[ring_at(2 * n_gate + i)], preferred_element_type=F32
            )
        swaps_m[c].start()

    def m_swap(c):
        swaps_m[c].wait_recv()
        sm[:, cols[c]] = pm[own, cols[c]] + rm[:, cols[c]]
        crosses_m[c].start()

    def m_cross(c):
        crosses_m[c].wait_recv()
        total = sm[:, cols[c]] + ym[:, cols[c]]
        ob[my_rows, cols[c]] = (hb[own, cols[c]] + total).astype(BF16).astype(F32)
        to_x[c].start()
        to_core[c].start()

    def m_gather(c):
        to_x[c].wait_recv()
        onward[c].start()

    def m_last(c):
        to_core[c].wait_recv()
        onward[c].wait_recv()
        out_ref[:, cols[c]] = ob[:, cols[c]].astype(BF16)

    staged(m_dot, m_swap, m_cross, m_gather, m_last)
    for copy in [*swaps_a, *cross_a, *swaps, *crosses, *gathers, *swaps_m, *crosses_m, *to_core, *to_x, *onward]:
        copy.wait_send()


def layer(tokens, gain, w_o, w_gate, w_up, w_down, rows_k, rows_v, kvs, carried):
    rows, width = tokens.shape
    head_dim = 2 * LANES
    heads = carried[0].shape[0]
    qrows = 2 * heads
    half, quarter = rows // 2, rows // 4
    cut = w_gate.shape[1] // 2
    n_blocks = half // BLOCK
    vmem = pl.BlockSpec(memory_space=pltpu.VMEM)
    hbm = pl.BlockSpec(memory_space=pltpu.HBM)
    flat = lambda n: pltpu.VMEM((n, width), F32)
    stats = lambda h, n: pltpu.VMEM((h, 3, n, LANES), F32)
    dma = lambda n: pltpu.SemaphoreType.DMA((n,))
    n_remote = GROUPS + GROUPS // 2 + 8 * CHUNKS
    args = (tokens, gain, w_o, w_gate, w_up, w_down, rows_k, rows_v)
    shape = (half, *rows_k.shape[1:])
    return pl.pallas_call(
        functools.partial(layer_kernel, kvs),
        out_shape=(
            pltpu.VMEM(tokens.shape, BF16),
            pltpu.VMEM(shape, BF16),
            pltpu.VMEM(shape, BF16),
        ),
        in_specs=[hbm] * len(args) + [vmem] * len(carried),
        out_specs=(vmem,) * 3,
        scratch_shapes=[
            pltpu.VMEM((SLOTS, width, head_dim), BF16),
            *(pltpu.VMEM((half * qrows, LANES), F32) for _ in range(3)),
            stats(heads, half), stats(heads // 2, rows), stats(heads // 2, half), stats(heads // 2, half),
            flat(half), flat(quarter), flat(quarter), flat(quarter), flat(half),
            pltpu.VMEM((half, cut), BF16),
            flat(half), flat(quarter), flat(quarter), flat(quarter), flat(rows),
            pltpu.VMEM(tokens.shape, BF16),
            pltpu.VMEM(gain.shape, BF16),
            dma(2), dma(n_blocks), dma(n_blocks), dma(width // head_dim),
            dma(2 * (cut // head_dim) + width // head_dim), dma(n_remote), dma(n_remote),
        ],
        compiler_params=pltpu.CompilerParams(
            vmem_limit_bytes=LAYER_VMEM << 20, collective_id=0, has_side_effects=True
        ),
        name="layer",
    )(*(pltpu.with_memory_space_constraint(v, pltpu.HBM) for v in args), *carried)


def write_kernel(pos_hbm, t_ref, kn_s, vn_s, _bk, _bv, _k, _v, out_ref, nk_hbm, nv_hbm, kbuf, vbuf, pos, sem, tile_sem, pos_sem):
    rows, key_rows, _ = kbuf.shape
    per_slot = 4
    local_slots = key_rows // per_slot
    slots = local_slots * lax.axis_size("sp")
    base = lax.axis_index("sp") * local_slots
    start = lax.axis_index("sp") // 2 * rows
    per_tile = 16 // per_slot
    n_blocks = rows // BLOCK
    tile_row = lax.broadcasted_iota(jnp.int32, (16, LANES), 0) // per_slot

    def copies(j):
        here, near = pl.ds(j * BLOCK, BLOCK), pl.ds(start + j * BLOCK, BLOCK)
        return (
            pltpu.make_async_copy(kbuf.at[here], nk_hbm.at[near], sem.at[0, j]),
            pltpu.make_async_copy(vbuf.at[here], nv_hbm.at[near], sem.at[1, j]),
        )

    def target(b):
        local = lax.rem(pos[b], slots) - base
        owned = (local >= 0) & (local < local_slots)
        safe = jnp.where(owned, local, 0)
        hit = jnp.where(owned, lax.rem(safe, per_tile), -1)
        return hit, pl.ds(pl.multiple_of((safe // per_tile) * 16, 16), 16)

    def tile_copies(n):
        at = target(start + n)[1]
        return (
            pltpu.make_async_copy(kbuf.at[n, at], nk_hbm.at[start + n, at], tile_sem.at[0]),
            pltpu.make_async_copy(vbuf.at[n, at], nv_hbm.at[start + n, at], tile_sem.at[1]),
        )

    def patch(n):
        b = start + n
        hit, at = target(b)
        for buf, new in ((kbuf, kn_s), (vbuf, vn_s)):
            fresh = new[pl.ds(pl.multiple_of(b * 16, 16), 16), :]
            buf[n, at, :] = jnp.where(tile_row == hit, fresh, buf[n, at, :].astype(F32)).astype(BF16)

    pos_copy = pltpu.make_async_copy(pos_hbm, pos, pos_sem)
    pos_copy.start()
    for j in range(EARLY):
        for copy in copies(j):
            copy.start()
    out_ref[...] = t_ref[...]
    pos_copy.wait()
    for j in range(EARLY, n_blocks + 1):
        if j < n_blocks:
            for i in range(BLOCK):
                patch(j * BLOCK + i)
        if j > EARLY:
            for copy in copies(j - 1):
                copy.start()
    for j in range(EARLY):
        for copy in copies(j):
            copy.wait()
        for i in range(BLOCK):
            patch(j * BLOCK + i)
        if j:
            for i in range(BLOCK):
                for copy in tile_copies((j - 1) * BLOCK + i):
                    copy.start()
    for i in range(BLOCK):
        for copy in tile_copies((EARLY - 1) * BLOCK + i):
            copy.start()
    for j in range(EARLY, n_blocks):
        for copy in copies(j):
            copy.wait()
    for n in range(EARLY * BLOCK):
        for copy in tile_copies(n):
            copy.wait()


def write(positions, layer_out, fresh_k, fresh_v, buf_k, buf_v, new_k, new_v):
    vmem = pl.BlockSpec(memory_space=pltpu.VMEM)
    hbm = pl.BlockSpec(memory_space=pltpu.HBM)
    return pl.pallas_call(
        write_kernel,
        out_shape=(
            *(jax.ShapeDtypeStruct(v.shape, BF16) for v in (layer_out, new_k, new_v)),
            pltpu.VMEM(buf_k.shape, BF16),
            pltpu.VMEM(buf_v.shape, BF16),
        ),
        in_specs=[hbm] + [vmem] * 5 + [hbm] * 2,
        out_specs=(vmem, hbm, hbm, vmem, vmem),
        input_output_aliases={4: 3, 5: 4, 6: 1, 7: 2},
        scratch_shapes=[
            pltpu.SMEM(positions.shape, jnp.int32),
            pltpu.SemaphoreType.DMA((2, buf_k.shape[0] // BLOCK)),
            pltpu.SemaphoreType.DMA((2,)),
            pltpu.SemaphoreType.DMA,
        ],
        compiler_params=pltpu.CompilerParams(vmem_limit_bytes=LAYER_VMEM << 20),
        name="write",
    )(pltpu.with_memory_space_constraint(positions, pltpu.HBM), layer_out, fresh_k, fresh_v, buf_k, buf_v, new_k, new_v)[:3]


def to_rows(cache):
    b, s, kv, d = cache.shape
    return cache.reshape(b, s, kv, d // LANES, LANES).transpose(0, 1, 3, 2, 4).reshape(b, -1, LANES)


def from_rows(rows, shape):
    b, s, kv, d = shape
    return rows.reshape(b, s, d // LANES, kv, LANES).transpose(0, 1, 3, 2, 4).reshape(shape)


def solution(mesh):
    cache_spec = P("dp", "sp", "tp", None)
    row_spec = P("dp", None)
    col_spec = P(None, "tp")
    in_specs = (row_spec, P("dp"), cache_spec, cache_spec, P(None), col_spec, col_spec, col_spec, P("tp", None), P(None), col_spec, col_spec, P("tp", None))
    out_specs = (row_spec, cache_spec, cache_spec)

    def local_step(tokens, positions, cache_k, cache_v, attn_gain, w_q, w_k, w_v, w_o, mlp_gain, w_gate, w_up, w_down):
        old_k, old_v = to_rows(cache_k), to_rows(cache_v)
        far, rows_k, rows_v, *carried, fresh_k, fresh_v = first_half(
            positions, tokens, attn_gain, w_q, w_k, w_v, old_k, old_v
        )
        out, buf_k, buf_v = layer(
            tokens, mlp_gain, w_o, w_gate, w_up, w_down, old_k, old_v, cache_k.shape[2], (far, *carried)
        )
        layer_out, rows_k, rows_v = write(positions, out, fresh_k, fresh_v, buf_k, buf_v, rows_k, rows_v)
        new_k = from_rows(rows_k, cache_k.shape)
        new_v = from_rows(rows_v, cache_v.shape)
        return layer_out, new_k, new_v

    return jax.shard_map(local_step, mesh=mesh, in_specs=in_specs, out_specs=out_specs, check_vma=False)
```

```python
import functools
import itertools
import math

import jax
import jax.numpy as jnp
from jax import lax
from jax.experimental import pallas as pl
from jax.experimental.pallas import tpu as pltpu
from jax.sharding import PartitionSpec as P

NORM_EPS = 1e-5
ROPE_THETA = 10000.0
LANES = 128
F32 = jnp.float32
BF16 = jnp.bfloat16
FAR = 1 << 28
BLOCK = 4
EARLY = 3
EAGER = (3, 8)
FIRST = 4
SLOTS = 22
LAYER_VMEM = 35
CHUNKS = 5
GROUPS = 4
MESH = pl.DeviceIdType.MESH


def rms_norm(values, gain):
    wide = values.astype(F32)
    inv_rms = lax.rsqrt(jnp.mean(wide * wide, axis=-1, keepdims=True) + NORM_EPS)
    return (wide * inv_rms * gain.astype(F32)).astype(BF16)


def first_kernel(
    pos_hbm, x_hbm, gain_hbm, wq_hbm, wk_hbm, wv_hbm, ck_hbm, cv_hbm,
    part_ref, nk_hbm, nv_hbm, q_s, kx_s, vx_s, lim_s, hid_s, kn_s, vn_s,
    wbuf, kbuf, vbuf, ang_s, o_s, m_s, l_s,
    pos, x_ref, gain_ref, w_sem, k_sem, v_sem, out_sem, x_sem,
):
    rows = x_ref.shape[0]
    head_dim = 2 * LANES
    heads = wq_hbm.shape[1] // head_dim
    kvs = wk_hbm.shape[1] // head_dim
    group = heads // kvs
    per_slot = 2 * kvs
    qrows = 2 * heads
    key_rows = ck_hbm.shape[1]
    local_slots = key_rows // per_slot
    slots = local_slots * lax.axis_size("sp")
    slices = key_rows // LANES
    half = rows // 2
    n_blocks = half // BLOCK
    start = (1 - lax.axis_index("sp") // 2) * half
    base = lax.axis_index("sp") * local_slots

    def w_copy(n):
        src, col = (
            (wk_hbm, n) if n < kvs else (wv_hbm, n - kvs) if n < 2 * kvs else (wq_hbm, n - 2 * kvs)
        )
        return pltpu.make_async_copy(src.at[:, pl.ds(col * head_dim, head_dim)], wbuf.at[n], w_sem.at[n])

    def in_copies(j):
        far, here = pl.ds(start + j * BLOCK, BLOCK), pl.ds(j * BLOCK, BLOCK)
        return (
            pltpu.make_async_copy(ck_hbm.at[far], kbuf.at[here], k_sem.at[j]),
            pltpu.make_async_copy(cv_hbm.at[far], vbuf.at[here], v_sem.at[j]),
        )

    def out_copies(j):
        far, here = pl.ds(start + j * BLOCK, BLOCK), pl.ds(j * BLOCK, BLOCK)
        return (
            pltpu.make_async_copy(kbuf.at[here], nk_hbm.at[far], out_sem.at[0]),
            pltpu.make_async_copy(vbuf.at[here], nv_hbm.at[far], out_sem.at[1]),
        )

    small = [
        pltpu.make_async_copy(src, dst, x_sem.at[i])
        for i, (src, dst) in enumerate(((pos_hbm, pos), (x_hbm, x_ref), (gain_hbm, gain_ref)))
    ]
    for copy in small:
        copy.start()
    n_w = heads + 2 * kvs
    for n in range(n_w // 2):
        w_copy(n).start()

    lane = lax.broadcasted_iota(jnp.int32, (1, LANES), 1).astype(F32)
    freq = jnp.exp2(lane * (-math.log2(ROPE_THETA) / LANES))

    for copy in small:
        copy.wait()
    for n in range(n_w // 2, n_w):
        w_copy(n).start()
    for j in range(FIRST):
        for copy in in_copies(j):
            copy.start()

    def angle_row(b, carry):
        p = pos[b]
        ang_s[pl.ds(b, 1), :] = freq * p.astype(F32)
        local = lax.rem(p, slots) - base
        owned = (local >= 0) & (local < local_slots)
        span = pl.ds(pl.multiple_of(b * qrows, qrows), qrows)
        lim_s[span, :] = jnp.full((qrows, LANES), jnp.where(p >= slots - 1, FAR // 2, p) - base, jnp.int32)
        hid_s[span, :] = jnp.full((qrows, LANES), jnp.where(owned, local, -FAR), jnp.int32)
        return carry

    lax.fori_loop(0, rows, angle_row, 0, unroll=8)
    angles = ang_s[...]
    cos_t, sin_t = jnp.cos(angles), jnp.sin(angles)
    normed = rms_norm(x_ref[...], gain_ref[...])

    for n in range(n_w):
        w_copy(n).wait()
        if FIRST + n < n_blocks:
            for copy in in_copies(FIRST + n):
                copy.start()
        lin = jnp.dot(normed, wbuf[n], preferred_element_type=F32)
        first, second = lin[:, :LANES], lin[:, LANES:]
        if not kvs <= n < 2 * kvs:
            first, second = first * cos_t - second * sin_t, second * cos_t + first * sin_t
        first, second = first.astype(BF16).astype(F32), second.astype(BF16).astype(F32)
        if n >= 2 * kvs:
            h = n - 2 * kvs
            q_s[pl.ds(h, rows, stride=qrows), :] = first
            q_s[pl.ds(heads + h, rows, stride=qrows), :] = second
        else:
            dst, tile, kv = (kn_s, kx_s, n) if n < kvs else (vn_s, vx_s, n - kvs)
            for rep in range(16 // per_slot):
                dst[pl.ds(rep * per_slot + kv, rows, stride=16), :] = first
                dst[pl.ds(rep * per_slot + kvs + kv, rows, stride=16), :] = second
            for g in range(group):
                tile[pl.ds(kv * group + g, rows, stride=qrows), :] = first
                tile[pl.ds(heads + kv * group + g, rows, stride=qrows), :] = second

    row = lax.broadcasted_iota(jnp.int32, (qrows, LANES), 0)
    col = lax.broadcasted_iota(jnp.int32, (qrows, LANES), 1)
    half_of_col = (col // kvs) % 2
    fits = (half_of_col == row // heads) & (col % kvs == (row % heads) // group)
    slot_of_col = jnp.where(fits, col // per_slot, FAR)
    low_half = half_of_col == 0
    patch_row = lax.broadcasted_iota(jnp.int32, (16, LANES), 0) // per_slot
    scale = 1.0 / math.sqrt(head_dim)

    def block_step(j, carry):
        for copy in in_copies(j):
            copy.wait()
        for i in range(BLOCK):
            n = j * BLOCK + i
            b = start + n
            local = lax.rem(pos[b], slots) - base
            owned = (local >= 0) & (local < local_slots)
            safe = jnp.where(owned, local, 0)
            hit = jnp.where(owned, lax.rem(safe, 16 // per_slot), -1)
            span = pl.ds(pl.multiple_of((safe // (16 // per_slot)) * 16, 16), 16)
            for buf, new in ((kbuf, kn_s), (vbuf, vn_s)):
                old = buf[n, span, :].astype(F32)
                fresh = new[pl.ds(pl.multiple_of(b * 16, 16), 16), :]
                buf[n, span, :] = jnp.where(patch_row == hit, fresh, old).astype(BF16)
        scores = []
        for i in range(BLOCK):
            b = start + j * BLOCK + i
            q = q_s[pl.ds(pl.multiple_of(b * qrows, qrows), qrows), :].astype(BF16)
            scores.append(
                lax.dot_general(q, kbuf[j * BLOCK + i], (((1,), (1,)), ((), ())), preferred_element_type=F32)
            )
        probs = []
        for i in range(BLOCK):
            n = j * BLOCK + i
            p = pos[start + n]
            limit = jnp.where(p >= slots - 1, FAR // 2, p) - base
            parts = []
            for t in range(slices):
                own = scores[i][:, t * LANES : (t + 1) * LANES]
                other = pltpu.roll(own, heads, 0)
                other = jnp.where(
                    low_half, pltpu.roll(other, LANES - kvs, 1), pltpu.roll(other, kvs, 1)
                )
                ok = slot_of_col <= limit - t * (LANES // per_slot)
                parts.append(jnp.where(ok, (own + other) * scale, -jnp.inf))
            top = functools.reduce(jnp.maximum, parts)
            top = jnp.max(top, axis=1, keepdims=True)
            floor = jnp.where(top == -jnp.inf, 0.0, top)
            parts = [jnp.exp(part - floor) for part in parts]
            total = jnp.sum(functools.reduce(jnp.add, parts), axis=1, keepdims=True)
            span = pl.ds(pl.multiple_of(n * qrows, qrows), qrows)
            m_s[span, :] = jnp.broadcast_to(top, (qrows, LANES))
            l_s[span, :] = jnp.broadcast_to(total, (qrows, LANES))
            probs.append(jnp.concatenate([part.astype(BF16) for part in parts], axis=1))
        for i in range(BLOCK):
            n = j * BLOCK + i
            span = pl.ds(pl.multiple_of(n * qrows, qrows), qrows)
            o_s[span, :] = jnp.dot(probs[i], vbuf[n], preferred_element_type=F32)
        for copy in out_copies(j):
            copy.start()
        return carry

    lax.fori_loop(0, n_blocks, block_step, 0)

    left = lax.broadcasted_iota(jnp.int32, (half, LANES), 1) < LANES // 2
    for h in range(heads):
        lo, hi = pl.ds(h, half, stride=qrows), pl.ds(heads + h, half, stride=qrows)
        part_ref[h, 0], part_ref[h, 1] = o_s[lo, :], o_s[hi, :]
        part_ref[h, 2] = jnp.where(left, m_s[lo, :], l_s[lo, :])
    for j in range(n_blocks):
        for copy in out_copies(j):
            copy.wait()


def first_half(positions, tokens, gain, w_q, w_k, w_v, rows_k, rows_v):
    rows, width = tokens.shape
    head_dim = 2 * LANES
    heads = w_q.shape[1] // head_dim
    kvs = w_k.shape[1] // head_dim
    qrows = 2 * heads
    vmem = pl.BlockSpec(memory_space=pltpu.VMEM)
    hbm = pl.BlockSpec(memory_space=pltpu.HBM)
    n_blocks = rows // 2 // BLOCK
    tile = lambda n: pltpu.VMEM((rows * n, LANES), F32)
    return pl.pallas_call(
        first_kernel,
        out_shape=(
            pltpu.VMEM((heads, 3, rows // 2, LANES), F32),
            jax.ShapeDtypeStruct(rows_k.shape, BF16),
            jax.ShapeDtypeStruct(rows_v.shape, BF16),
            tile(qrows), tile(qrows), tile(qrows),
            *(pltpu.VMEM((rows * qrows, LANES), jnp.int32) for _ in range(2)),
            tile(16), tile(16),
        ),
        in_specs=[hbm] * 8,
        out_specs=(vmem, hbm, hbm) + (vmem,) * 7,
        scratch_shapes=[
            pltpu.VMEM((heads + 2 * kvs, width, head_dim), BF16),
            pltpu.VMEM((rows // 2, *rows_k.shape[1:]), BF16),
            pltpu.VMEM((rows // 2, *rows_v.shape[1:]), BF16),
            tile(1),
            pltpu.VMEM((rows // 2 * qrows, LANES), F32),
            pltpu.VMEM((rows // 2 * qrows, LANES), F32),
            pltpu.VMEM((rows // 2 * qrows, LANES), F32),
            pltpu.SMEM((rows,), jnp.int32),
            pltpu.VMEM(tokens.shape, BF16),
            pltpu.VMEM(gain.shape, BF16),
            pltpu.SemaphoreType.DMA((heads + 2 * kvs,)),
            pltpu.SemaphoreType.DMA((n_blocks,)),
            pltpu.SemaphoreType.DMA((n_blocks,)),
            pltpu.SemaphoreType.DMA((2,)),
            pltpu.SemaphoreType.DMA((3,)),
        ],
        compiler_params=pltpu.CompilerParams(vmem_limit_bytes=36 << 20),
        name="first",
    )(*(pltpu.with_memory_space_constraint(v, pltpu.HBM) for v in (positions, tokens, gain, w_q, w_k, w_v, rows_k, rows_v)))


def combine(mine, theirs):
    left = lax.broadcasted_iota(jnp.int32, mine[2].shape, mine[2].ndim - 1) < LANES // 2
    axis = mine[2].ndim - 1

    def unpack(stats):
        turned = pltpu.roll(stats, LANES // 2, axis)
        return jnp.where(left, stats, turned), jnp.where(left, turned, stats)

    (m_a, l_a), (m_b, l_b) = unpack(mine[2]), unpack(theirs[2])
    top = jnp.maximum(m_a, m_b)
    f_a = jnp.where(m_a == -jnp.inf, 0.0, jnp.exp(m_a - top))
    f_b = jnp.where(m_b == -jnp.inf, 0.0, jnp.exp(m_b - top))
    return mine[0] * f_a + theirs[0] * f_b, mine[1] * f_a + theirs[1] * f_b, top, l_a * f_a + l_b * f_b


def layer_kernel(
    kv_heads, x_hbm, gm_hbm, wo_hbm, wg_hbm, wu_hbm, wd_hbm, ck_hbm, cv_hbm,
    far_ref, q_s, kx_s, vx_s, lim_s, hid_s,
    out_ref, kbuf, vbuf,
    ring, o_s, m_s, l_s, part, rd, sx, rx,
    po, ro, so, yo, hb, act, pm, rm, sm, ym, ob,
    x_ref, gm_ref,
    small_sem, k_sem, v_sem, o_sem, c_sem, send_sem, recv_sem,
):
    rows, width = x_ref.shape
    head_dim = ring.shape[2]
    heads = far_ref.shape[0]
    kvs = kv_heads
    group = heads // kvs
    per_slot, qrows = 2 * kvs, 2 * heads
    key_rows = ck_hbm.shape[1]
    local_slots = key_rows // per_slot
    slices = key_rows // LANES
    n_blocks = rows // 2 // BLOCK
    mine_h = heads // 2
    half, quarter = rows // 2, rows // 4
    sp, tp = lax.axis_index("sp"), lax.axis_index("tp")
    x, k = sp // 2, lax.rem(sp, 2)
    d_dev, x_dev, y_dev = {"sp": x * 2 + 1 - k}, {"sp": (1 - x) * 2 + k}, {"tp": 1 - tp}
    m_cols = act.shape[1]
    span = width // CHUNKS

    barrier = pltpu.get_barrier_semaphore()
    for dev in (d_dev, x_dev, y_dev):
        pl.semaphore_signal(barrier, inc=1, device_id=dev, device_id_type=MESH)

    counter = [0]

    def remote(src, dst, dev):
        n = counter[0]
        counter[0] += 1
        return pltpu.make_async_remote_copy(
            src_ref=src, dst_ref=dst, send_sem=send_sem.at[n], recv_sem=recv_sem.at[n],
            device_id=dev, device_id_type=MESH,
        )

    def in_copies(j):
        near, here = pl.ds(x * half + j * BLOCK, BLOCK), pl.ds(j * BLOCK, BLOCK)
        return (
            pltpu.make_async_copy(ck_hbm.at[near], kbuf.at[here], k_sem.at[j]),
            pltpu.make_async_copy(cv_hbm.at[near], vbuf.at[here], v_sem.at[j]),
        )

    small = [
        pltpu.make_async_copy(src, dst, small_sem.at[i])
        for i, (src, dst) in enumerate(
            ((x_hbm, x_ref), (gm_hbm, gm_ref))
        )
    ]
    def read(blocks):
        for j in blocks:
            for copy in in_copies(j):
                copy.start()

    read(range(EAGER[0]))

    n_w = 0
    o_rows = mine_h * head_dim
    per_o = width // o_rows
    o_copies = [
        pltpu.make_async_copy(
            wo_hbm.at[pl.ds(k * o_rows, o_rows), pl.ds(c * head_dim, head_dim)],
            ring.at[n_w + c // per_o, pl.ds((c % per_o) * o_rows, o_rows)],
            o_sem.at[c],
        )
        for c in range(width // head_dim)
    ]
    n_gate = m_cols // head_dim
    ring_at = lambda i: (n_w + 2 + i) % SLOTS
    chunks = []
    for c in range(n_gate):
        at = pl.ds(pl.multiple_of(k * m_cols + c * head_dim, LANES), head_dim)
        chunks += [wg_hbm.at[:, at], wu_hbm.at[:, at]]
    for c in range(width // head_dim):
        chunks.append(wd_hbm.at[pl.ds(pl.multiple_of(k * m_cols, LANES), m_cols), pl.ds(c * head_dim, head_dim)])
    chunks = [
        pltpu.make_async_copy(src, ring.at[ring_at(i)], c_sem.at[i]) for i, src in enumerate(chunks)
    ]
    queue = iter(chunks)

    started = [0]

    def fetch(n, limit=len(chunks)):
        n = min(n, limit - started[0])
        started[0] += n
        for copy in itertools.islice(queue, n):
            copy.start()

    row = lax.broadcasted_iota(jnp.int32, (qrows, LANES), 0)
    col = lax.broadcasted_iota(jnp.int32, (qrows, LANES), 1)
    half_of_col = (col // kvs) % 2
    fits = (half_of_col == row // heads) & (col % kvs == (row % heads) // group)
    slot_of_col = jnp.where(fits, col // per_slot, FAR)
    low_half = half_of_col == 0
    scale = 1.0 / math.sqrt(head_dim)

    def block_step(j, carry):
        for copy in in_copies(j):
            copy.wait()
        first = x * half + j * BLOCK
        at_rows = [pl.ds(pl.multiple_of((first + i) * qrows, qrows), qrows) for i in range(BLOCK)]
        scores = []
        for i in range(BLOCK):
            scores.append(
                lax.dot_general(
                    q_s[at_rows[i], :].astype(BF16), kbuf[j * BLOCK + i], (((1,), (1,)), ((), ())),
                    preferred_element_type=F32,
                )
            )
        probs, news = [], []
        for i in range(BLOCK):
            limit, hidden = lim_s[at_rows[i], :], hid_s[at_rows[i], :]
            fresh = q_s[at_rows[i], :] * kx_s[at_rows[i], :]
            fresh = jnp.sum(fresh + pltpu.roll(fresh, heads, 0), axis=1, keepdims=True) * scale
            fresh = jnp.where(hidden[:, :1] >= 0, fresh, -jnp.inf)
            parts = []
            for t in range(slices):
                own = scores[i][:, t * LANES : (t + 1) * LANES]
                other = pltpu.roll(own, heads, 0)
                other = jnp.where(
                    low_half, pltpu.roll(other, LANES - kvs, 1), pltpu.roll(other, kvs, 1)
                )
                shift = t * (LANES // per_slot)
                ok = (slot_of_col <= limit - shift) & (slot_of_col != hidden - shift)
                parts.append(jnp.where(ok, (own + other) * scale, -jnp.inf))
            top = functools.reduce(jnp.maximum, parts)
            top = jnp.maximum(jnp.max(top, axis=1, keepdims=True), fresh)
            floor = jnp.where(top == -jnp.inf, 0.0, top)
            parts = [jnp.exp(part_t - floor) for part_t in parts]
            new = jnp.exp(fresh - floor)
            total = jnp.sum(functools.reduce(jnp.add, parts), axis=1, keepdims=True) + new
            at = pl.ds(pl.multiple_of((j * BLOCK + i) * qrows, qrows), qrows)
            m_s[at, :] = jnp.broadcast_to(top, (qrows, LANES))
            l_s[at, :] = jnp.broadcast_to(total, (qrows, LANES))
            news.append(new)
            probs.append(jnp.concatenate([part_t.astype(BF16) for part_t in parts], axis=1))
        for i in range(BLOCK):
            at = pl.ds(pl.multiple_of((j * BLOCK + i) * qrows, qrows), qrows)
            o_s[at, :] = (
                jnp.dot(probs[i], vbuf[j * BLOCK + i], preferred_element_type=F32) + news[i] * vx_s[at_rows[i], :]
            )
        return carry

    size = rows // GROUPS
    my_heads, their_heads = pl.ds(k * mine_h, mine_h), pl.ds((1 - k) * mine_h, mine_h)
    spans = [pl.ds(g * size, size) for g in range(GROUPS)]
    near = GROUPS // 2
    sources = [far_ref.at[their_heads, :, spans[g]] for g in range(near)]
    sources += [part.at[their_heads, :, spans[g]] for g in range(near)]
    swaps_a = [remote(src, rd.at[:, :, at], d_dev) for src, at in zip(sources, spans)]
    cross_a = [remote(sx.at[:, :, at], rx.at[:, :, at], x_dev) for at in spans[: GROUPS // 2]]
    left = lax.broadcasted_iota(jnp.int32, (mine_h, size, LANES), 2) < LANES // 2
    joined = [None] * GROUPS

    def publish(g):
        at = spans[g - near]
        for h in range(heads):
            lo = pl.ds((g - near) * size * qrows + h, size, stride=qrows)
            hi = pl.ds((g - near) * size * qrows + heads + h, size, stride=qrows)
            part[h, 0, at], part[h, 1, at] = o_s[lo, :], o_s[hi, :]
            part[h, 2, at] = jnp.where(left[0], m_s[lo, :], l_s[lo, :])
        swaps_a[g].start()

    def chip(g):
        swaps_a[g].wait_recv()
        at = spans[g]
        here, local = (far_ref, at) if g < near else (part, spans[g - near])
        o_a, o_b, m, l = combine(
            [here[my_heads, i, local] for i in range(3)], [rd[:, i, at] for i in range(3)]
        )
        value = [o_a, o_b, jnp.where(left, m, l)]
        if g < GROUPS // 2:
            for i in range(3):
                sx[:, i, at] = value[i]
            cross_a[g].start()
        joined[g] = value

    pl.semaphore_wait(barrier, 3)
    for g in range(near):
        swaps_a[g].start()
    read(range(*EAGER))
    for copy in small:
        copy.start()
    step = n_blocks // near
    lax.fori_loop(0, step, block_step, 0)
    for g in range(near):
        chip(g)
    read(range(EAGER[1], n_blocks))
    publish(near)
    for copy in o_copies:
        copy.start()
    lax.fori_loop(step, n_blocks, block_step, 0)
    publish(GROUPS - 1)
    fetch(3)
    for g in range(near, GROUPS):
        chip(g)
    pieces = []
    for g in range(GROUPS // 2):
        cross_a[g].wait_recv()
        o_a, o_b, _, l = combine(joined[GROUPS // 2 + g], [rx[:, i, spans[g]] for i in range(3)])
        o_a, o_b = (o_a / l).astype(BF16), (o_b / l).astype(BF16)
        pieces.append(jnp.concatenate([v[h] for h in range(mine_h) for v in (o_a, o_b)], axis=-1))
    attended = jnp.concatenate(pieces, axis=0)
    for copy in small:
        copy.wait()

    own, other = pl.ds(k * quarter, quarter), pl.ds((1 - k) * quarter, quarter)
    my_rows = pl.ds(pl.multiple_of(x * half + k * quarter, quarter), quarter)
    x_peer_rows = pl.ds(pl.multiple_of((1 - x) * half + k * quarter, quarter), quarter)
    cols = [pl.ds(c * span, span) for c in range(CHUNKS)]
    per_span = span // head_dim

    def staged(dot, swap, cross, *rest):
        for c in range(CHUNKS + 2):
            if c < CHUNKS:
                dot(c)
            if c >= 2:
                swap(c - 2)
        for c in range(CHUNKS):
            cross(c)
        for c in range(CHUNKS + len(rest) - 1):
            for s, stage in enumerate(rest):
                if 0 <= c - s < CHUNKS:
                    stage(c - s)

    swaps = [remote(po.at[other, c], ro.at[:, c], d_dev) for c in cols]
    crosses = [remote(so.at[:, c], yo.at[:, c], y_dev) for c in cols]
    gathers = [remote(hb.at[own, c], hb.at[own, c], d_dev) for c in cols]

    def o_dot(c):
        for i in range(c * per_span, (c + 1) * per_span):
            o_copies[i].wait()
            w = ring[n_w + i // per_o, (i % per_o) * o_rows : (i % per_o + 1) * o_rows, :]
            po[:, i * head_dim : (i + 1) * head_dim] = jnp.dot(attended, w, preferred_element_type=F32)
        swaps[c].start()

    def o_swap(c):
        swaps[c].wait_recv()
        so[:, cols[c]] = po[own, cols[c]] + ro[:, cols[c]]
        crosses[c].start()
        if c == CHUNKS - 1:
            fetch(15)

    def o_cross(c):
        crosses[c].wait_recv()
        total = so[:, cols[c]] + yo[:, cols[c]]
        hb[own, cols[c]] = (x_ref[my_rows, cols[c]].astype(F32) + total).astype(BF16).astype(F32)
        gathers[c].start()

    def o_gather(c):
        gathers[c].wait_recv()

    staged(o_dot, o_swap, o_cross, o_gather)
    fetch(SLOTS, SLOTS)

    normed_m = rms_norm(hb[...], gm_ref[...])
    for c in range(n_gate):
        chunks[2 * c].wait()
        chunks[2 * c + 1].wait()
        gate = jnp.dot(normed_m, ring[ring_at(2 * c)], preferred_element_type=F32)
        up = jnp.dot(normed_m, ring[ring_at(2 * c + 1)], preferred_element_type=F32)
        act[:, c * head_dim : (c + 1) * head_dim] = (jax.nn.silu(gate) * up).astype(BF16)
        fetch(2)

    swaps_m = [remote(pm.at[other, c], rm.at[:, c], d_dev) for c in cols]
    crosses_m = [remote(sm.at[:, c], ym.at[:, c], y_dev) for c in cols]
    to_core = [remote(ob.at[my_rows, c], ob.at[my_rows, c], d_dev) for c in cols]
    to_x = [remote(ob.at[my_rows, c], ob.at[my_rows, c], x_dev) for c in cols]
    onward = [remote(ob.at[x_peer_rows, c], ob.at[x_peer_rows, c], d_dev) for c in cols]

    def m_dot(c):
        for i in range(c * per_span, (c + 1) * per_span):
            chunks[2 * n_gate + i].wait()
            pm[:, i * head_dim : (i + 1) * head_dim] = jnp.dot(
                act[...], ring[ring_at(2 * n_gate + i)], preferred_element_type=F32
            )
        swaps_m[c].start()

    def m_swap(c):
        swaps_m[c].wait_recv()
        sm[:, cols[c]] = pm[own, cols[c]] + rm[:, cols[c]]
        crosses_m[c].start()

    def m_cross(c):
        crosses_m[c].wait_recv()
        total = sm[:, cols[c]] + ym[:, cols[c]]
        ob[my_rows, cols[c]] = (hb[own, cols[c]] + total).astype(BF16).astype(F32)
        to_x[c].start()
        to_core[c].start()

    def m_gather(c):
        to_x[c].wait_recv()
        onward[c].start()

    def m_last(c):
        to_core[c].wait_recv()
        onward[c].wait_recv()
        out_ref[:, cols[c]] = ob[:, cols[c]].astype(BF16)

    staged(m_dot, m_swap, m_cross, m_gather, m_last)
    for copy in [*swaps_a, *cross_a, *swaps, *crosses, *gathers, *swaps_m, *crosses_m, *to_core, *to_x, *onward]:
        copy.wait_send()


def layer(tokens, gain, w_o, w_gate, w_up, w_down, rows_k, rows_v, kvs, carried):
    rows, width = tokens.shape
    head_dim = 2 * LANES
    heads = carried[0].shape[0]
    qrows = 2 * heads
    half, quarter = rows // 2, rows // 4
    cut = w_gate.shape[1] // 2
    n_blocks = half // BLOCK
    vmem = pl.BlockSpec(memory_space=pltpu.VMEM)
    hbm = pl.BlockSpec(memory_space=pltpu.HBM)
    flat = lambda n: pltpu.VMEM((n, width), F32)
    stats = lambda h, n: pltpu.VMEM((h, 3, n, LANES), F32)
    dma = lambda n: pltpu.SemaphoreType.DMA((n,))
    n_remote = GROUPS + GROUPS // 2 + 8 * CHUNKS
    args = (tokens, gain, w_o, w_gate, w_up, w_down, rows_k, rows_v)
    shape = (half, *rows_k.shape[1:])
    return pl.pallas_call(
        functools.partial(layer_kernel, kvs),
        out_shape=(
            pltpu.VMEM(tokens.shape, BF16),
            pltpu.VMEM(shape, BF16),
            pltpu.VMEM(shape, BF16),
        ),
        in_specs=[hbm] * len(args) + [vmem] * len(carried),
        out_specs=(vmem,) * 3,
        scratch_shapes=[
            pltpu.VMEM((SLOTS, width, head_dim), BF16),
            *(pltpu.VMEM((half * qrows, LANES), F32) for _ in range(3)),
            stats(heads, half), stats(heads // 2, rows), stats(heads // 2, half), stats(heads // 2, half),
            flat(half), flat(quarter), flat(quarter), flat(quarter), flat(half),
            pltpu.VMEM((half, cut), BF16),
            flat(half), flat(quarter), flat(quarter), flat(quarter), flat(rows),
            pltpu.VMEM(tokens.shape, BF16),
            pltpu.VMEM(gain.shape, BF16),
            dma(2), dma(n_blocks), dma(n_blocks), dma(width // head_dim),
            dma(2 * (cut // head_dim) + width // head_dim), dma(n_remote), dma(n_remote),
        ],
        compiler_params=pltpu.CompilerParams(
            vmem_limit_bytes=LAYER_VMEM << 20, collective_id=0, has_side_effects=True
        ),
        name="layer",
    )(*(pltpu.with_memory_space_constraint(v, pltpu.HBM) for v in args), *carried)


def write_kernel(pos_hbm, t_ref, kn_s, vn_s, _bk, _bv, _k, _v, out_ref, nk_hbm, nv_hbm, kbuf, vbuf, pos, sem, tile_sem, pos_sem):
    rows, key_rows, _ = kbuf.shape
    per_slot = 4
    local_slots = key_rows // per_slot
    slots = local_slots * lax.axis_size("sp")
    base = lax.axis_index("sp") * local_slots
    start = lax.axis_index("sp") // 2 * rows
    per_tile = 16 // per_slot
    n_blocks = rows // BLOCK
    tile_row = lax.broadcasted_iota(jnp.int32, (16, LANES), 0) // per_slot

    def copies(j):
        here, near = pl.ds(j * BLOCK, BLOCK), pl.ds(start + j * BLOCK, BLOCK)
        return (
            pltpu.make_async_copy(kbuf.at[here], nk_hbm.at[near], sem.at[0, j]),
            pltpu.make_async_copy(vbuf.at[here], nv_hbm.at[near], sem.at[1, j]),
        )

    def target(b):
        local = lax.rem(pos[b], slots) - base
        owned = (local >= 0) & (local < local_slots)
        safe = jnp.where(owned, local, 0)
        hit = jnp.where(owned, lax.rem(safe, per_tile), -1)
        return hit, pl.ds(pl.multiple_of((safe // per_tile) * 16, 16), 16)

    def tile_copies(n):
        at = target(start + n)[1]
        return (
            pltpu.make_async_copy(kbuf.at[n, at], nk_hbm.at[start + n, at], tile_sem.at[0]),
            pltpu.make_async_copy(vbuf.at[n, at], nv_hbm.at[start + n, at], tile_sem.at[1]),
        )

    def patch(n):
        b = start + n
        hit, at = target(b)
        for buf, new in ((kbuf, kn_s), (vbuf, vn_s)):
            fresh = new[pl.ds(pl.multiple_of(b * 16, 16), 16), :]
            buf[n, at, :] = jnp.where(tile_row == hit, fresh, buf[n, at, :].astype(F32)).astype(BF16)

    pos_copy = pltpu.make_async_copy(pos_hbm, pos, pos_sem)
    pos_copy.start()
    for j in range(EARLY):
        for copy in copies(j):
            copy.start()
    out_ref[...] = t_ref[...]
    pos_copy.wait()
    for j in range(EARLY, n_blocks + 1):
        if j < n_blocks:
            for i in range(BLOCK):
                patch(j * BLOCK + i)
        if j > EARLY:
            for copy in copies(j - 1):
                copy.start()
    for j in range(EARLY):
        for copy in copies(j):
            copy.wait()
        for i in range(BLOCK):
            patch(j * BLOCK + i)
        if j:
            for i in range(BLOCK):
                for copy in tile_copies((j - 1) * BLOCK + i):
                    copy.start()
    for i in range(BLOCK):
        for copy in tile_copies((EARLY - 1) * BLOCK + i):
            copy.start()
    for j in range(EARLY, n_blocks):
        for copy in copies(j):
            copy.wait()
    for n in range(EARLY * BLOCK):
        for copy in tile_copies(n):
            copy.wait()


def write(positions, layer_out, fresh_k, fresh_v, buf_k, buf_v, new_k, new_v):
    vmem = pl.BlockSpec(memory_space=pltpu.VMEM)
    hbm = pl.BlockSpec(memory_space=pltpu.HBM)
    return pl.pallas_call(
        write_kernel,
        out_shape=(
            *(jax.ShapeDtypeStruct(v.shape, BF16) for v in (layer_out, new_k, new_v)),
            pltpu.VMEM(buf_k.shape, BF16),
            pltpu.VMEM(buf_v.shape, BF16),
        ),
        in_specs=[hbm] + [vmem] * 5 + [hbm] * 2,
        out_specs=(vmem, hbm, hbm, vmem, vmem),
        input_output_aliases={4: 3, 5: 4, 6: 1, 7: 2},
        scratch_shapes=[
            pltpu.SMEM(positions.shape, jnp.int32),
            pltpu.SemaphoreType.DMA((2, buf_k.shape[0] // BLOCK)),
            pltpu.SemaphoreType.DMA((2,)),
            pltpu.SemaphoreType.DMA,
        ],
        compiler_params=pltpu.CompilerParams(vmem_limit_bytes=LAYER_VMEM << 20),
        name="write",
    )(pltpu.with_memory_space_constraint(positions, pltpu.HBM), layer_out, fresh_k, fresh_v, buf_k, buf_v, new_k, new_v)[:3]


def to_rows(cache):
    b, s, kv, d = cache.shape
    return cache.reshape(b, s, kv, d // LANES, LANES).transpose(0, 1, 3, 2, 4).reshape(b, -1, LANES)


def from_rows(rows, shape):
    b, s, kv, d = shape
    return rows.reshape(b, s, d // LANES, kv, LANES).transpose(0, 1, 3, 2, 4).reshape(shape)


def solution(mesh):
    cache_spec = P("dp", "sp", "tp", None)
    row_spec = P("dp", None)
    col_spec = P(None, "tp")
    in_specs = (row_spec, P("dp"), cache_spec, cache_spec, P(None), col_spec, col_spec, col_spec, P("tp", None), P(None), col_spec, col_spec, P("tp", None))
    out_specs = (row_spec, cache_spec, cache_spec)

    def local_step(tokens, positions, cache_k, cache_v, attn_gain, w_q, w_k, w_v, w_o, mlp_gain, w_gate, w_up, w_down):
        old_k, old_v = to_rows(cache_k), to_rows(cache_v)
        far, rows_k, rows_v, *carried, fresh_k, fresh_v = first_half(
            positions, tokens, attn_gain, w_q, w_k, w_v, old_k, old_v
        )
        out, buf_k, buf_v = layer(
            tokens, mlp_gain, w_o, w_gate, w_up, w_down, old_k, old_v, cache_k.shape[2], (far, *carried)
        )
        layer_out, rows_k, rows_v = write(positions, out, fresh_k, fresh_v, buf_k, buf_v, rows_k, rows_v)
        new_k = from_rows(rows_k, cache_k.shape)
        new_v = from_rows(rows_v, cache_v.shape)
        return layer_out, new_k, new_v

    return jax.shard_map(local_step, mesh=mesh, in_specs=in_specs, out_specs=out_specs, check_vma=False)
```

```python
import functools
import itertools
import math

import jax
import jax.numpy as jnp
from jax import lax
from jax.experimental import pallas as pl
from jax.experimental.pallas import tpu as pltpu
from jax.sharding import PartitionSpec as P

NORM_EPS = 1e-5
ROPE_THETA = 10000.0
LANES = 128
F32 = jnp.float32
BF16 = jnp.bfloat16
FAR = 1 << 28
BLOCK = 4
EARLY = 3
EAGER = (3, 8)
FIRST = 4
SLOTS = 22
LAYER_VMEM = 35
CHUNKS = 5
GROUPS = 4
MESH = pl.DeviceIdType.MESH


def rms_norm(values, gain):
    wide = values.astype(F32)
    inv_rms = lax.rsqrt(jnp.mean(wide * wide, axis=-1, keepdims=True) + NORM_EPS)
    return (wide * inv_rms * gain.astype(F32)).astype(BF16)


def first_kernel(
    pos_hbm, x_hbm, gain_hbm, wq_hbm, wk_hbm, wv_hbm, ck_hbm, cv_hbm,
    part_ref, nk_hbm, nv_hbm, q_s, kx_s, vx_s, lim_s, hid_s, kn_s, vn_s,
    wbuf, kbuf, vbuf, ang_s, o_s, m_s, l_s,
    pos, x_ref, gain_ref, w_sem, k_sem, v_sem, out_sem, x_sem,
):
    rows = x_ref.shape[0]
    head_dim = 2 * LANES
    heads = wq_hbm.shape[1] // head_dim
    kvs = wk_hbm.shape[1] // head_dim
    group = heads // kvs
    per_slot = 2 * kvs
    qrows = 2 * heads
    key_rows = ck_hbm.shape[1]
    local_slots = key_rows // per_slot
    slots = local_slots * lax.axis_size("sp")
    slices = key_rows // LANES
    half = rows // 2
    n_blocks = half // BLOCK
    start = (1 - lax.axis_index("sp") // 2) * half
    base = lax.axis_index("sp") * local_slots

    def w_copy(n):
        src, col = (
            (wk_hbm, n) if n < kvs else (wv_hbm, n - kvs) if n < 2 * kvs else (wq_hbm, n - 2 * kvs)
        )
        return pltpu.make_async_copy(src.at[:, pl.ds(col * head_dim, head_dim)], wbuf.at[n], w_sem.at[n])

    def in_copies(j):
        far, here = pl.ds(start + j * BLOCK, BLOCK), pl.ds(j * BLOCK, BLOCK)
        return (
            pltpu.make_async_copy(ck_hbm.at[far], kbuf.at[here], k_sem.at[j]),
            pltpu.make_async_copy(cv_hbm.at[far], vbuf.at[here], v_sem.at[j]),
        )

    def out_copies(j):
        far, here = pl.ds(start + j * BLOCK, BLOCK), pl.ds(j * BLOCK, BLOCK)
        return (
            pltpu.make_async_copy(kbuf.at[here], nk_hbm.at[far], out_sem.at[0]),
            pltpu.make_async_copy(vbuf.at[here], nv_hbm.at[far], out_sem.at[1]),
        )

    small = [
        pltpu.make_async_copy(src, dst, x_sem.at[i])
        for i, (src, dst) in enumerate(((pos_hbm, pos), (x_hbm, x_ref), (gain_hbm, gain_ref)))
    ]
    for copy in small:
        copy.start()
    n_w = heads + 2 * kvs
    for n in range(n_w // 2):
        w_copy(n).start()

    lane = lax.broadcasted_iota(jnp.int32, (1, LANES), 1).astype(F32)
    freq = jnp.exp2(lane * (-math.log2(ROPE_THETA) / LANES))

    for copy in small:
        copy.wait()
    for n in range(n_w // 2, n_w):
        w_copy(n).start()
    for j in range(FIRST):
        for copy in in_copies(j):
            copy.start()

    def angle_row(b, carry):
        p = pos[b]
        ang_s[pl.ds(b, 1), :] = freq * p.astype(F32)
        local = lax.rem(p, slots) - base
        owned = (local >= 0) & (local < local_slots)
        span = pl.ds(pl.multiple_of(b * qrows, qrows), qrows)
        lim_s[span, :] = jnp.full((qrows, LANES), jnp.where(p >= slots - 1, FAR // 2, p) - base, jnp.int32)
        hid_s[span, :] = jnp.full((qrows, LANES), jnp.where(owned, local, -FAR), jnp.int32)
        return carry

    lax.fori_loop(0, rows, angle_row, 0, unroll=8)
    angles = ang_s[...]
    cos_t, sin_t = jnp.cos(angles), jnp.sin(angles)
    normed = rms_norm(x_ref[...], gain_ref[...])

    for n in range(n_w):
        w_copy(n).wait()
        if FIRST + n < n_blocks:
            for copy in in_copies(FIRST + n):
                copy.start()
        lin = jnp.dot(normed, wbuf[n], preferred_element_type=F32)
        first, second = lin[:, :LANES], lin[:, LANES:]
        if not kvs <= n < 2 * kvs:
            first, second = first * cos_t - second * sin_t, second * cos_t + first * sin_t
        first, second = first.astype(BF16).astype(F32), second.astype(BF16).astype(F32)
        if n >= 2 * kvs:
            h = n - 2 * kvs
            q_s[pl.ds(h, rows, stride=qrows), :] = first
            q_s[pl.ds(heads + h, rows, stride=qrows), :] = second
        else:
            dst, tile, kv = (kn_s, kx_s, n) if n < kvs else (vn_s, vx_s, n - kvs)
            for rep in range(16 // per_slot):
                dst[pl.ds(rep * per_slot + kv, rows, stride=16), :] = first
                dst[pl.ds(rep * per_slot + kvs + kv, rows, stride=16), :] = second
            for g in range(group):
                tile[pl.ds(kv * group + g, rows, stride=qrows), :] = first
                tile[pl.ds(heads + kv * group + g, rows, stride=qrows), :] = second

    row = lax.broadcasted_iota(jnp.int32, (qrows, LANES), 0)
    col = lax.broadcasted_iota(jnp.int32, (qrows, LANES), 1)
    half_of_col = (col // kvs) % 2
    fits = (half_of_col == row // heads) & (col % kvs == (row % heads) // group)
    slot_of_col = jnp.where(fits, col // per_slot, FAR)
    low_half = half_of_col == 0
    patch_row = lax.broadcasted_iota(jnp.int32, (16, LANES), 0) // per_slot
    scale = 1.0 / math.sqrt(head_dim)

    def block_step(j, carry):
        for copy in in_copies(j):
            copy.wait()
        for i in range(BLOCK):
            n = j * BLOCK + i
            b = start + n
            local = lax.rem(pos[b], slots) - base
            owned = (local >= 0) & (local < local_slots)
            safe = jnp.where(owned, local, 0)
            hit = jnp.where(owned, lax.rem(safe, 16 // per_slot), -1)
            span = pl.ds(pl.multiple_of((safe // (16 // per_slot)) * 16, 16), 16)
            for buf, new in ((kbuf, kn_s), (vbuf, vn_s)):
                old = buf[n, span, :].astype(F32)
                fresh = new[pl.ds(pl.multiple_of(b * 16, 16), 16), :]
                buf[n, span, :] = jnp.where(patch_row == hit, fresh, old).astype(BF16)
        scores = []
        for i in range(BLOCK):
            b = start + j * BLOCK + i
            q = q_s[pl.ds(pl.multiple_of(b * qrows, qrows), qrows), :].astype(BF16)
            scores.append(
                lax.dot_general(q, kbuf[j * BLOCK + i], (((1,), (1,)), ((), ())), preferred_element_type=F32)
            )
        probs = []
        for i in range(BLOCK):
            n = j * BLOCK + i
            p = pos[start + n]
            limit = jnp.where(p >= slots - 1, FAR // 2, p) - base
            parts = []
            for t in range(slices):
                own = scores[i][:, t * LANES : (t + 1) * LANES]
                other = pltpu.roll(own, heads, 0)
                other = jnp.where(
                    low_half, pltpu.roll(other, LANES - kvs, 1), pltpu.roll(other, kvs, 1)
                )
                ok = slot_of_col <= limit - t * (LANES // per_slot)
                parts.append(jnp.where(ok, (own + other) * scale, -jnp.inf))
            top = functools.reduce(jnp.maximum, parts)
            top = jnp.max(top, axis=1, keepdims=True)
            floor = jnp.where(top == -jnp.inf, 0.0, top)
            parts = [jnp.exp(part - floor) for part in parts]
            total = jnp.sum(functools.reduce(jnp.add, parts), axis=1, keepdims=True)
            span = pl.ds(pl.multiple_of(n * qrows, qrows), qrows)
            m_s[span, :] = jnp.broadcast_to(top, (qrows, LANES))
            l_s[span, :] = jnp.broadcast_to(total, (qrows, LANES))
            probs.append(jnp.concatenate([part.astype(BF16) for part in parts], axis=1))
        for i in range(BLOCK):
            n = j * BLOCK + i
            span = pl.ds(pl.multiple_of(n * qrows, qrows), qrows)
            o_s[span, :] = jnp.dot(probs[i], vbuf[n], preferred_element_type=F32)
        for copy in out_copies(j):
            copy.start()
        return carry

    lax.fori_loop(0, n_blocks, block_step, 0)

    left = lax.broadcasted_iota(jnp.int32, (half, LANES), 1) < LANES // 2
    for h in range(heads):
        lo, hi = pl.ds(h, half, stride=qrows), pl.ds(heads + h, half, stride=qrows)
        part_ref[h, 0], part_ref[h, 1] = o_s[lo, :], o_s[hi, :]
        part_ref[h, 2] = jnp.where(left, m_s[lo, :], l_s[lo, :])
    for j in range(n_blocks):
        for copy in out_copies(j):
            copy.wait()


def first_half(positions, tokens, gain, w_q, w_k, w_v, rows_k, rows_v):
    rows, width = tokens.shape
    head_dim = 2 * LANES
    heads = w_q.shape[1] // head_dim
    kvs = w_k.shape[1] // head_dim
    qrows = 2 * heads
    vmem = pl.BlockSpec(memory_space=pltpu.VMEM)
    hbm = pl.BlockSpec(memory_space=pltpu.HBM)
    n_blocks = rows // 2 // BLOCK
    tile = lambda n: pltpu.VMEM((rows * n, LANES), F32)
    return pl.pallas_call(
        first_kernel,
        out_shape=(
            pltpu.VMEM((heads, 3, rows // 2, LANES), F32),
            jax.ShapeDtypeStruct(rows_k.shape, BF16),
            jax.ShapeDtypeStruct(rows_v.shape, BF16),
            tile(qrows), tile(qrows), tile(qrows),
            *(pltpu.VMEM((rows * qrows, LANES), jnp.int32) for _ in range(2)),
            tile(16), tile(16),
        ),
        in_specs=[hbm] * 8,
        out_specs=(vmem, hbm, hbm) + (vmem,) * 7,
        scratch_shapes=[
            pltpu.VMEM((heads + 2 * kvs, width, head_dim), BF16),
            pltpu.VMEM((rows // 2, *rows_k.shape[1:]), BF16),
            pltpu.VMEM((rows // 2, *rows_v.shape[1:]), BF16),
            tile(1),
            pltpu.VMEM((rows // 2 * qrows, LANES), F32),
            pltpu.VMEM((rows // 2 * qrows, LANES), F32),
            pltpu.VMEM((rows // 2 * qrows, LANES), F32),
            pltpu.SMEM((rows,), jnp.int32),
            pltpu.VMEM(tokens.shape, BF16),
            pltpu.VMEM(gain.shape, BF16),
            pltpu.SemaphoreType.DMA((heads + 2 * kvs,)),
            pltpu.SemaphoreType.DMA((n_blocks,)),
            pltpu.SemaphoreType.DMA((n_blocks,)),
            pltpu.SemaphoreType.DMA((2,)),
            pltpu.SemaphoreType.DMA((3,)),
        ],
        compiler_params=pltpu.CompilerParams(vmem_limit_bytes=36 << 20),
        name="first",
    )(*(pltpu.with_memory_space_constraint(v, pltpu.HBM) for v in (positions, tokens, gain, w_q, w_k, w_v, rows_k, rows_v)))


def combine(mine, theirs):
    left = lax.broadcasted_iota(jnp.int32, mine[2].shape, mine[2].ndim - 1) < LANES // 2
    axis = mine[2].ndim - 1

    def unpack(stats):
        turned = pltpu.roll(stats, LANES // 2, axis)
        return jnp.where(left, stats, turned), jnp.where(left, turned, stats)

    (m_a, l_a), (m_b, l_b) = unpack(mine[2]), unpack(theirs[2])
    top = jnp.maximum(m_a, m_b)
    f_a = jnp.where(m_a == -jnp.inf, 0.0, jnp.exp(m_a - top))
    f_b = jnp.where(m_b == -jnp.inf, 0.0, jnp.exp(m_b - top))
    return mine[0] * f_a + theirs[0] * f_b, mine[1] * f_a + theirs[1] * f_b, top, l_a * f_a + l_b * f_b


def layer_kernel(
    kv_heads, x_hbm, gm_hbm, wo_hbm, wg_hbm, wu_hbm, wd_hbm, ck_hbm, cv_hbm,
    far_ref, q_s, kx_s, vx_s, lim_s, hid_s,
    out_ref, kbuf, vbuf,
    ring, o_s, m_s, l_s, part, rd, sx, rx,
    po, ro, so, yo, hb, act, pm, rm, sm, ym, ob,
    x_ref, gm_ref,
    small_sem, k_sem, v_sem, o_sem, c_sem, send_sem, recv_sem,
):
    rows, width = x_ref.shape
    head_dim = ring.shape[2]
    heads = far_ref.shape[0]
    kvs = kv_heads
    group = heads // kvs
    per_slot, qrows = 2 * kvs, 2 * heads
    key_rows = ck_hbm.shape[1]
    local_slots = key_rows // per_slot
    slices = key_rows // LANES
    n_blocks = rows // 2 // BLOCK
    mine_h = heads // 2
    half, quarter = rows // 2, rows // 4
    sp, tp = lax.axis_index("sp"), lax.axis_index("tp")
    x, k = sp // 2, lax.rem(sp, 2)
    d_dev, x_dev, y_dev = {"sp": x * 2 + 1 - k}, {"sp": (1 - x) * 2 + k}, {"tp": 1 - tp}
    m_cols = act.shape[1]
    span = width // CHUNKS

    barrier = pltpu.get_barrier_semaphore()
    for dev in (d_dev, x_dev, y_dev):
        pl.semaphore_signal(barrier, inc=1, device_id=dev, device_id_type=MESH)

    counter = [0]

    def remote(src, dst, dev):
        n = counter[0]
        counter[0] += 1
        return pltpu.make_async_remote_copy(
            src_ref=src, dst_ref=dst, send_sem=send_sem.at[n], recv_sem=recv_sem.at[n],
            device_id=dev, device_id_type=MESH,
        )

    def in_copies(j):
        near, here = pl.ds(x * half + j * BLOCK, BLOCK), pl.ds(j * BLOCK, BLOCK)
        return (
            pltpu.make_async_copy(ck_hbm.at[near], kbuf.at[here], k_sem.at[j]),
            pltpu.make_async_copy(cv_hbm.at[near], vbuf.at[here], v_sem.at[j]),
        )

    small = [
        pltpu.make_async_copy(src, dst, small_sem.at[i])
        for i, (src, dst) in enumerate(
            ((x_hbm, x_ref), (gm_hbm, gm_ref))
        )
    ]
    def read(blocks):
        for j in blocks:
            for copy in in_copies(j):
                copy.start()

    read(range(EAGER[0]))

    n_w = 0
    o_rows = mine_h * head_dim
    per_o = width // o_rows
    o_copies = [
        pltpu.make_async_copy(
            wo_hbm.at[pl.ds(k * o_rows, o_rows), pl.ds(c * head_dim, head_dim)],
            ring.at[n_w + c // per_o, pl.ds((c % per_o) * o_rows, o_rows)],
            o_sem.at[c],
        )
        for c in range(width // head_dim)
    ]
    n_gate = m_cols // head_dim
    ring_at = lambda i: (n_w + 2 + i) % SLOTS
    chunks = []
    for c in range(n_gate):
        at = pl.ds(pl.multiple_of(k * m_cols + c * head_dim, LANES), head_dim)
        chunks += [wg_hbm.at[:, at], wu_hbm.at[:, at]]
    for c in range(width // head_dim):
        chunks.append(wd_hbm.at[pl.ds(pl.multiple_of(k * m_cols, LANES), m_cols), pl.ds(c * head_dim, head_dim)])
    chunks = [
        pltpu.make_async_copy(src, ring.at[ring_at(i)], c_sem.at[i]) for i, src in enumerate(chunks)
    ]
    queue = iter(chunks)

    started = [0]

    def fetch(n, limit=len(chunks)):
        n = min(n, limit - started[0])
        started[0] += n
        for copy in itertools.islice(queue, n):
            copy.start()

    row = lax.broadcasted_iota(jnp.int32, (qrows, LANES), 0)
    col = lax.broadcasted_iota(jnp.int32, (qrows, LANES), 1)
    half_of_col = (col // kvs) % 2
    fits = (half_of_col == row // heads) & (col % kvs == (row % heads) // group)
    slot_of_col = jnp.where(fits, col // per_slot, FAR)
    low_half = half_of_col == 0
    scale = 1.0 / math.sqrt(head_dim)

    def block_step(j, carry):
        for copy in in_copies(j):
            copy.wait()
        first = x * half + j * BLOCK
        at_rows = [pl.ds(pl.multiple_of((first + i) * qrows, qrows), qrows) for i in range(BLOCK)]
        scores = []
        for i in range(BLOCK):
            scores.append(
                lax.dot_general(
                    q_s[at_rows[i], :].astype(BF16), kbuf[j * BLOCK + i], (((1,), (1,)), ((), ())),
                    preferred_element_type=F32,
                )
            )
        probs, news = [], []
        for i in range(BLOCK):
            limit, hidden = lim_s[at_rows[i], :], hid_s[at_rows[i], :]
            fresh = q_s[at_rows[i], :] * kx_s[at_rows[i], :]
            fresh = jnp.sum(fresh + pltpu.roll(fresh, heads, 0), axis=1, keepdims=True) * scale
            fresh = jnp.where(hidden[:, :1] >= 0, fresh, -jnp.inf)
            parts = []
            for t in range(slices):
                own = scores[i][:, t * LANES : (t + 1) * LANES]
                other = pltpu.roll(own, heads, 0)
                other = jnp.where(
                    low_half, pltpu.roll(other, LANES - kvs, 1), pltpu.roll(other, kvs, 1)
                )
                shift = t * (LANES // per_slot)
                ok = (slot_of_col <= limit - shift) & (slot_of_col != hidden - shift)
                parts.append(jnp.where(ok, (own + other) * scale, -jnp.inf))
            top = functools.reduce(jnp.maximum, parts)
            top = jnp.maximum(jnp.max(top, axis=1, keepdims=True), fresh)
            floor = jnp.where(top == -jnp.inf, 0.0, top)
            parts = [jnp.exp(part_t - floor) for part_t in parts]
            new = jnp.exp(fresh - floor)
            total = jnp.sum(functools.reduce(jnp.add, parts), axis=1, keepdims=True) + new
            at = pl.ds(pl.multiple_of((j * BLOCK + i) * qrows, qrows), qrows)
            m_s[at, :] = jnp.broadcast_to(top, (qrows, LANES))
            l_s[at, :] = jnp.broadcast_to(total, (qrows, LANES))
            news.append(new)
            probs.append(jnp.concatenate([part_t.astype(BF16) for part_t in parts], axis=1))
        for i in range(BLOCK):
            at = pl.ds(pl.multiple_of((j * BLOCK + i) * qrows, qrows), qrows)
            o_s[at, :] = (
                jnp.dot(probs[i], vbuf[j * BLOCK + i], preferred_element_type=F32) + news[i] * vx_s[at_rows[i], :]
            )
        return carry

    size = rows // GROUPS
    my_heads, their_heads = pl.ds(k * mine_h, mine_h), pl.ds((1 - k) * mine_h, mine_h)
    spans = [pl.ds(g * size, size) for g in range(GROUPS)]
    near = GROUPS // 2
    sources = [far_ref.at[their_heads, :, spans[g]] for g in range(near)]
    sources += [part.at[their_heads, :, spans[g]] for g in range(near)]
    swaps_a = [remote(src, rd.at[:, :, at], d_dev) for src, at in zip(sources, spans)]
    cross_a = [remote(sx.at[:, :, at], rx.at[:, :, at], x_dev) for at in spans[: GROUPS // 2]]
    left = lax.broadcasted_iota(jnp.int32, (mine_h, size, LANES), 2) < LANES // 2
    joined = [None] * GROUPS

    def publish(g):
        at = spans[g - near]
        for h in range(heads):
            lo = pl.ds((g - near) * size * qrows + h, size, stride=qrows)
            hi = pl.ds((g - near) * size * qrows + heads + h, size, stride=qrows)
            part[h, 0, at], part[h, 1, at] = o_s[lo, :], o_s[hi, :]
            part[h, 2, at] = jnp.where(left[0], m_s[lo, :], l_s[lo, :])
        swaps_a[g].start()

    def chip(g):
        swaps_a[g].wait_recv()
        at = spans[g]
        here, local = (far_ref, at) if g < near else (part, spans[g - near])
        o_a, o_b, m, l = combine(
            [here[my_heads, i, local] for i in range(3)], [rd[:, i, at] for i in range(3)]
        )
        value = [o_a, o_b, jnp.where(left, m, l)]
        if g < GROUPS // 2:
            for i in range(3):
                sx[:, i, at] = value[i]
            cross_a[g].start()
        joined[g] = value

    pl.semaphore_wait(barrier, 3)
    for g in range(near):
        swaps_a[g].start()
    read(range(*EAGER))
    for copy in small:
        copy.start()
    step = n_blocks // near
    lax.fori_loop(0, step, block_step, 0)
    for g in range(near):
        chip(g)
    read(range(EAGER[1], n_blocks))
    publish(near)
    for copy in o_copies:
        copy.start()
    lax.fori_loop(step, n_blocks, block_step, 0)
    publish(GROUPS - 1)
    fetch(3)
    for g in range(near, GROUPS):
        chip(g)
    pieces = []
    for g in range(GROUPS // 2):
        cross_a[g].wait_recv()
        o_a, o_b, _, l = combine(joined[GROUPS // 2 + g], [rx[:, i, spans[g]] for i in range(3)])
        o_a, o_b = (o_a / l).astype(BF16), (o_b / l).astype(BF16)
        pieces.append(jnp.concatenate([v[h] for h in range(mine_h) for v in (o_a, o_b)], axis=-1))
    attended = jnp.concatenate(pieces, axis=0)
    for copy in small:
        copy.wait()

    own, other = pl.ds(k * quarter, quarter), pl.ds((1 - k) * quarter, quarter)
    my_rows = pl.ds(pl.multiple_of(x * half + k * quarter, quarter), quarter)
    x_peer_rows = pl.ds(pl.multiple_of((1 - x) * half + k * quarter, quarter), quarter)
    cols = [pl.ds(c * span, span) for c in range(CHUNKS)]
    per_span = span // head_dim
    cuts = (0, 3, CHUNKS)
    joint = [pl.ds(a * span, (b - a) * span) for a, b in zip(cuts, cuts[1:])]
    last_of = {b - 1: i for i, b in enumerate(cuts[1:])}

    def staged(dot, swap, cross, *rest):
        for c in range(CHUNKS + 2):
            if c < CHUNKS:
                dot(c)
            if c >= 2:
                swap(c - 2)
        for c in range(CHUNKS):
            cross(c)
        for c in range(CHUNKS + len(rest) - 1):
            for s, stage in enumerate(rest):
                if 0 <= c - s < CHUNKS:
                    stage(c - s)

    swaps = [remote(po.at[other, c], ro.at[:, c], d_dev) for c in cols]
    crosses = [remote(so.at[:, c], yo.at[:, c], y_dev) for c in cols]
    gathers = [remote(hb.at[own, c], hb.at[own, c], d_dev) for c in joint]

    def o_dot(c):
        for i in range(c * per_span, (c + 1) * per_span):
            o_copies[i].wait()
            w = ring[n_w + i // per_o, (i % per_o) * o_rows : (i % per_o + 1) * o_rows, :]
            po[:, i * head_dim : (i + 1) * head_dim] = jnp.dot(attended, w, preferred_element_type=F32)
        swaps[c].start()

    def o_swap(c):
        swaps[c].wait_recv()
        so[:, cols[c]] = po[own, cols[c]] + ro[:, cols[c]]
        crosses[c].start()
        if c == CHUNKS - 1:
            fetch(15)

    def o_cross(c):
        crosses[c].wait_recv()
        total = so[:, cols[c]] + yo[:, cols[c]]
        hb[own, cols[c]] = (x_ref[my_rows, cols[c]].astype(F32) + total).astype(BF16).astype(F32)
        if c in last_of:
            gathers[last_of[c]].start()

    def o_gather(c):
        if c in last_of:
            gathers[last_of[c]].wait_recv()

    staged(o_dot, o_swap, o_cross, o_gather)
    fetch(SLOTS, SLOTS)

    normed_m = rms_norm(hb[...], gm_ref[...])
    for c in range(n_gate):
        chunks[2 * c].wait()
        chunks[2 * c + 1].wait()
        gate = jnp.dot(normed_m, ring[ring_at(2 * c)], preferred_element_type=F32)
        up = jnp.dot(normed_m, ring[ring_at(2 * c + 1)], preferred_element_type=F32)
        act[:, c * head_dim : (c + 1) * head_dim] = (jax.nn.silu(gate) * up).astype(BF16)
        fetch(2)

    swaps_m = [remote(pm.at[other, c], rm.at[:, c], d_dev) for c in cols]
    crosses_m = [remote(sm.at[:, c], ym.at[:, c], y_dev) for c in cols]
    to_core = [remote(ob.at[my_rows], ob.at[my_rows], d_dev)]
    to_x = [remote(ob.at[my_rows, c], ob.at[my_rows, c], x_dev) for c in cols]
    onward = [remote(ob.at[x_peer_rows, c], ob.at[x_peer_rows, c], d_dev) for c in joint]

    def m_dot(c):
        for i in range(c * per_span, (c + 1) * per_span):
            chunks[2 * n_gate + i].wait()
            pm[:, i * head_dim : (i + 1) * head_dim] = jnp.dot(
                act[...], ring[ring_at(2 * n_gate + i)], preferred_element_type=F32
            )
        swaps_m[c].start()

    def m_swap(c):
        swaps_m[c].wait_recv()
        sm[:, cols[c]] = pm[own, cols[c]] + rm[:, cols[c]]
        crosses_m[c].start()

    def m_cross(c):
        crosses_m[c].wait_recv()
        total = sm[:, cols[c]] + ym[:, cols[c]]
        ob[my_rows, cols[c]] = (hb[own, cols[c]] + total).astype(BF16).astype(F32)
        to_x[c].start()
        if c == CHUNKS - 1:
            to_core[0].start()

    def m_gather(c):
        to_x[c].wait_recv()
        if c in last_of:
            onward[last_of[c]].start()

    def m_last(c):
        if c == 0:
            to_core[0].wait_recv()
        if c in last_of:
            at = joint[last_of[c]]
            onward[last_of[c]].wait_recv()
            out_ref[:, at] = ob[:, at].astype(BF16)

    staged(m_dot, m_swap, m_cross, m_gather, m_last)
    for copy in [*swaps_a, *cross_a, *swaps, *crosses, *gathers, *swaps_m, *crosses_m, *to_core, *to_x, *onward]:
        copy.wait_send()


def layer(tokens, gain, w_o, w_gate, w_up, w_down, rows_k, rows_v, kvs, carried):
    rows, width = tokens.shape
    head_dim = 2 * LANES
    heads = carried[0].shape[0]
    qrows = 2 * heads
    half, quarter = rows // 2, rows // 4
    cut = w_gate.shape[1] // 2
    n_blocks = half // BLOCK
    vmem = pl.BlockSpec(memory_space=pltpu.VMEM)
    hbm = pl.BlockSpec(memory_space=pltpu.HBM)
    flat = lambda n: pltpu.VMEM((n, width), F32)
    stats = lambda h, n: pltpu.VMEM((h, 3, n, LANES), F32)
    dma = lambda n: pltpu.SemaphoreType.DMA((n,))
    n_remote = GROUPS + GROUPS // 2 + 5 * CHUNKS + 5
    args = (tokens, gain, w_o, w_gate, w_up, w_down, rows_k, rows_v)
    shape = (half, *rows_k.shape[1:])
    return pl.pallas_call(
        functools.partial(layer_kernel, kvs),
        out_shape=(
            pltpu.VMEM(tokens.shape, BF16),
            pltpu.VMEM(shape, BF16),
            pltpu.VMEM(shape, BF16),
        ),
        in_specs=[hbm] * len(args) + [vmem] * len(carried),
        out_specs=(vmem,) * 3,
        scratch_shapes=[
            pltpu.VMEM((SLOTS, width, head_dim), BF16),
            *(pltpu.VMEM((half * qrows, LANES), F32) for _ in range(3)),
            stats(heads, half), stats(heads // 2, rows), stats(heads // 2, half), stats(heads // 2, half),
            flat(half), flat(quarter), flat(quarter), flat(quarter), flat(half),
            pltpu.VMEM((half, cut), BF16),
            flat(half), flat(quarter), flat(quarter), flat(quarter), flat(rows),
            pltpu.VMEM(tokens.shape, BF16),
            pltpu.VMEM(gain.shape, BF16),
            dma(2), dma(n_blocks), dma(n_blocks), dma(width // head_dim),
            dma(2 * (cut // head_dim) + width // head_dim), dma(n_remote), dma(n_remote),
        ],
        compiler_params=pltpu.CompilerParams(
            vmem_limit_bytes=LAYER_VMEM << 20, collective_id=0, has_side_effects=True
        ),
        name="layer",
    )(*(pltpu.with_memory_space_constraint(v, pltpu.HBM) for v in args), *carried)


def write_kernel(pos_hbm, t_ref, kn_s, vn_s, _bk, _bv, _k, _v, out_ref, nk_hbm, nv_hbm, kbuf, vbuf, pos, sem, tile_sem, pos_sem):
    rows, key_rows, _ = kbuf.shape
    per_slot = 4
    local_slots = key_rows // per_slot
    slots = local_slots * lax.axis_size("sp")
    base = lax.axis_index("sp") * local_slots
    start = lax.axis_index("sp") // 2 * rows
    per_tile = 16 // per_slot
    n_blocks = rows // BLOCK
    tile_row = lax.broadcasted_iota(jnp.int32, (16, LANES), 0) // per_slot

    def copies(j):
        here, near = pl.ds(j * BLOCK, BLOCK), pl.ds(start + j * BLOCK, BLOCK)
        return (
            pltpu.make_async_copy(kbuf.at[here], nk_hbm.at[near], sem.at[0, j]),
            pltpu.make_async_copy(vbuf.at[here], nv_hbm.at[near], sem.at[1, j]),
        )

    def target(b):
        local = lax.rem(pos[b], slots) - base
        owned = (local >= 0) & (local < local_slots)
        safe = jnp.where(owned, local, 0)
        hit = jnp.where(owned, lax.rem(safe, per_tile), -1)
        return hit, pl.ds(pl.multiple_of((safe // per_tile) * 16, 16), 16)

    def tile_copies(n):
        at = target(start + n)[1]
        return (
            pltpu.make_async_copy(kbuf.at[n, at], nk_hbm.at[start + n, at], tile_sem.at[0]),
            pltpu.make_async_copy(vbuf.at[n, at], nv_hbm.at[start + n, at], tile_sem.at[1]),
        )

    def patch(n):
        b = start + n
        hit, at = target(b)
        for buf, new in ((kbuf, kn_s), (vbuf, vn_s)):
            fresh = new[pl.ds(pl.multiple_of(b * 16, 16), 16), :]
            buf[n, at, :] = jnp.where(tile_row == hit, fresh, buf[n, at, :].astype(F32)).astype(BF16)

    pos_copy = pltpu.make_async_copy(pos_hbm, pos, pos_sem)
    pos_copy.start()
    for j in range(EARLY):
        for copy in copies(j):
            copy.start()
    out_ref[...] = t_ref[...]
    pos_copy.wait()
    for j in range(EARLY, n_blocks + 1):
        if j < n_blocks:
            for i in range(BLOCK):
                patch(j * BLOCK + i)
        if j > EARLY:
            for copy in copies(j - 1):
                copy.start()
    for j in range(EARLY):
        for copy in copies(j):
            copy.wait()
        for i in range(BLOCK):
            patch(j * BLOCK + i)
        if j:
            for i in range(BLOCK):
                for copy in tile_copies((j - 1) * BLOCK + i):
                    copy.start()
    for i in range(BLOCK):
        for copy in tile_copies((EARLY - 1) * BLOCK + i):
            copy.start()
    for j in range(EARLY, n_blocks):
        for copy in copies(j):
            copy.wait()
    for n in range(EARLY * BLOCK):
        for copy in tile_copies(n):
            copy.wait()


def write(positions, layer_out, fresh_k, fresh_v, buf_k, buf_v, new_k, new_v):
    vmem = pl.BlockSpec(memory_space=pltpu.VMEM)
    hbm = pl.BlockSpec(memory_space=pltpu.HBM)
    return pl.pallas_call(
        write_kernel,
        out_shape=(
            *(jax.ShapeDtypeStruct(v.shape, BF16) for v in (layer_out, new_k, new_v)),
            pltpu.VMEM(buf_k.shape, BF16),
            pltpu.VMEM(buf_v.shape, BF16),
        ),
        in_specs=[hbm] + [vmem] * 5 + [hbm] * 2,
        out_specs=(vmem, hbm, hbm, vmem, vmem),
        input_output_aliases={4: 3, 5: 4, 6: 1, 7: 2},
        scratch_shapes=[
            pltpu.SMEM(positions.shape, jnp.int32),
            pltpu.SemaphoreType.DMA((2, buf_k.shape[0] // BLOCK)),
            pltpu.SemaphoreType.DMA((2,)),
            pltpu.SemaphoreType.DMA,
        ],
        compiler_params=pltpu.CompilerParams(vmem_limit_bytes=LAYER_VMEM << 20),
        name="write",
    )(pltpu.with_memory_space_constraint(positions, pltpu.HBM), layer_out, fresh_k, fresh_v, buf_k, buf_v, new_k, new_v)[:3]


def to_rows(cache):
    b, s, kv, d = cache.shape
    return cache.reshape(b, s, kv, d // LANES, LANES).transpose(0, 1, 3, 2, 4).reshape(b, -1, LANES)


def from_rows(rows, shape):
    b, s, kv, d = shape
    return rows.reshape(b, s, d // LANES, kv, LANES).transpose(0, 1, 3, 2, 4).reshape(shape)


def solution(mesh):
    cache_spec = P("dp", "sp", "tp", None)
    row_spec = P("dp", None)
    col_spec = P(None, "tp")
    in_specs = (row_spec, P("dp"), cache_spec, cache_spec, P(None), col_spec, col_spec, col_spec, P("tp", None), P(None), col_spec, col_spec, P("tp", None))
    out_specs = (row_spec, cache_spec, cache_spec)

    def local_step(tokens, positions, cache_k, cache_v, attn_gain, w_q, w_k, w_v, w_o, mlp_gain, w_gate, w_up, w_down):
        old_k, old_v = to_rows(cache_k), to_rows(cache_v)
        far, rows_k, rows_v, *carried, fresh_k, fresh_v = first_half(
            positions, tokens, attn_gain, w_q, w_k, w_v, old_k, old_v
        )
        out, buf_k, buf_v = layer(
            tokens, mlp_gain, w_o, w_gate, w_up, w_down, old_k, old_v, cache_k.shape[2], (far, *carried)
        )
        layer_out, rows_k, rows_v = write(positions, out, fresh_k, fresh_v, buf_k, buf_v, rows_k, rows_v)
        new_k = from_rows(rows_k, cache_k.shape)
        new_v = from_rows(rows_v, cache_v.shape)
        return layer_out, new_k, new_v

    return jax.shard_map(local_step, mesh=mesh, in_specs=in_specs, out_specs=out_specs, check_vma=False)
```

```python
import functools
import itertools
import math

import jax
import jax.numpy as jnp
from jax import lax
from jax.experimental import pallas as pl
from jax.experimental.pallas import tpu as pltpu
from jax.sharding import PartitionSpec as P

NORM_EPS = 1e-5
ROPE_THETA = 10000.0
LANES = 128
F32 = jnp.float32
BF16 = jnp.bfloat16
FAR = 1 << 28
BLOCK = 4
EARLY = 3
EAGER = (3, 8)
FIRST = 4
SLOTS = 22
LAYER_VMEM = 35
CHUNKS = 5
GROUPS = 4
MESH = pl.DeviceIdType.MESH


def rms_norm(values, gain):
    wide = values.astype(F32)
    inv_rms = lax.rsqrt(jnp.mean(wide * wide, axis=-1, keepdims=True) + NORM_EPS)
    return (wide * inv_rms * gain.astype(F32)).astype(BF16)


def first_kernel(
    pos_hbm, x_hbm, gain_hbm, wq_hbm, wk_hbm, wv_hbm, ck_hbm, cv_hbm,
    part_ref, nk_hbm, nv_hbm, q_s, kx_s, vx_s, lim_s, hid_s, kn_s, vn_s,
    wbuf, kbuf, vbuf, ang_s, o_s, m_s, l_s,
    pos, x_ref, gain_ref, w_sem, k_sem, v_sem, out_sem, x_sem,
):
    rows = x_ref.shape[0]
    head_dim = 2 * LANES
    heads = wq_hbm.shape[1] // head_dim
    kvs = wk_hbm.shape[1] // head_dim
    group = heads // kvs
    per_slot = 2 * kvs
    qrows = 2 * heads
    key_rows = ck_hbm.shape[1]
    local_slots = key_rows // per_slot
    slots = local_slots * lax.axis_size("sp")
    slices = key_rows // LANES
    half = rows // 2
    n_blocks = half // BLOCK
    start = (1 - lax.axis_index("sp") // 2) * half
    base = lax.axis_index("sp") * local_slots

    def w_copy(n):
        src, col = (
            (wk_hbm, n) if n < kvs else (wv_hbm, n - kvs) if n < 2 * kvs else (wq_hbm, n - 2 * kvs)
        )
        return pltpu.make_async_copy(src.at[:, pl.ds(col * head_dim, head_dim)], wbuf.at[n], w_sem.at[n])

    def in_copies(j):
        far, here = pl.ds(start + j * BLOCK, BLOCK), pl.ds(j * BLOCK, BLOCK)
        return (
            pltpu.make_async_copy(ck_hbm.at[far], kbuf.at[here], k_sem.at[j]),
            pltpu.make_async_copy(cv_hbm.at[far], vbuf.at[here], v_sem.at[j]),
        )

    def out_copies(j):
        far, here = pl.ds(start + j * BLOCK, BLOCK), pl.ds(j * BLOCK, BLOCK)
        return (
            pltpu.make_async_copy(kbuf.at[here], nk_hbm.at[far], out_sem.at[0]),
            pltpu.make_async_copy(vbuf.at[here], nv_hbm.at[far], out_sem.at[1]),
        )

    small = [
        pltpu.make_async_copy(src, dst, x_sem.at[i])
        for i, (src, dst) in enumerate(((pos_hbm, pos), (x_hbm, x_ref), (gain_hbm, gain_ref)))
    ]
    for copy in small:
        copy.start()
    n_w = heads + 2 * kvs
    for n in range(n_w // 2):
        w_copy(n).start()

    lane = lax.broadcasted_iota(jnp.int32, (1, LANES), 1).astype(F32)
    freq = jnp.exp2(lane * (-math.log2(ROPE_THETA) / LANES))

    for copy in small:
        copy.wait()
    for n in range(n_w // 2, n_w):
        w_copy(n).start()
    for j in range(FIRST):
        for copy in in_copies(j):
            copy.start()

    def angle_row(b, carry):
        p = pos[b]
        ang_s[pl.ds(b, 1), :] = freq * p.astype(F32)
        local = lax.rem(p, slots) - base
        owned = (local >= 0) & (local < local_slots)
        span = pl.ds(pl.multiple_of(b * qrows, qrows), qrows)
        lim_s[span, :] = jnp.full((qrows, LANES), jnp.where(p >= slots - 1, FAR // 2, p) - base, jnp.int32)
        hid_s[span, :] = jnp.full((qrows, LANES), jnp.where(owned, local, -FAR), jnp.int32)
        return carry

    lax.fori_loop(0, rows, angle_row, 0, unroll=8)
    angles = ang_s[...]
    cos_t, sin_t = jnp.cos(angles), jnp.sin(angles)
    normed = rms_norm(x_ref[...], gain_ref[...])

    for n in range(n_w):
        w_copy(n).wait()
        if FIRST + n < n_blocks:
            for copy in in_copies(FIRST + n):
                copy.start()
        lin = jnp.dot(normed, wbuf[n], preferred_element_type=F32)
        first, second = lin[:, :LANES], lin[:, LANES:]
        if not kvs <= n < 2 * kvs:
            first, second = first * cos_t - second * sin_t, second * cos_t + first * sin_t
        first, second = first.astype(BF16).astype(F32), second.astype(BF16).astype(F32)
        if n >= 2 * kvs:
            h = n - 2 * kvs
            q_s[pl.ds(h, rows, stride=qrows), :] = first
            q_s[pl.ds(heads + h, rows, stride=qrows), :] = second
        else:
            dst, tile, kv = (kn_s, kx_s, n) if n < kvs else (vn_s, vx_s, n - kvs)
            for rep in range(16 // per_slot):
                dst[pl.ds(rep * per_slot + kv, rows, stride=16), :] = first
                dst[pl.ds(rep * per_slot + kvs + kv, rows, stride=16), :] = second
            for g in range(group):
                tile[pl.ds(kv * group + g, rows, stride=qrows), :] = first
                tile[pl.ds(heads + kv * group + g, rows, stride=qrows), :] = second

    row = lax.broadcasted_iota(jnp.int32, (qrows, LANES), 0)
    col = lax.broadcasted_iota(jnp.int32, (qrows, LANES), 1)
    half_of_col = (col // kvs) % 2
    fits = (half_of_col == row // heads) & (col % kvs == (row % heads) // group)
    slot_of_col = jnp.where(fits, col // per_slot, FAR)
    low_half = half_of_col == 0
    patch_row = lax.broadcasted_iota(jnp.int32, (16, LANES), 0) // per_slot
    scale = 1.0 / math.sqrt(head_dim)

    def block_step(j, carry):
        for copy in in_copies(j):
            copy.wait()
        for i in range(BLOCK):
            n = j * BLOCK + i
            b = start + n
            local = lax.rem(pos[b], slots) - base
            owned = (local >= 0) & (local < local_slots)
            safe = jnp.where(owned, local, 0)
            hit = jnp.where(owned, lax.rem(safe, 16 // per_slot), -1)
            span = pl.ds(pl.multiple_of((safe // (16 // per_slot)) * 16, 16), 16)
            for buf, new in ((kbuf, kn_s), (vbuf, vn_s)):
                old = buf[n, span, :].astype(F32)
                fresh = new[pl.ds(pl.multiple_of(b * 16, 16), 16), :]
                buf[n, span, :] = jnp.where(patch_row == hit, fresh, old).astype(BF16)
        scores = []
        for i in range(BLOCK):
            b = start + j * BLOCK + i
            q = q_s[pl.ds(pl.multiple_of(b * qrows, qrows), qrows), :].astype(BF16)
            scores.append(
                lax.dot_general(q, kbuf[j * BLOCK + i], (((1,), (1,)), ((), ())), preferred_element_type=F32)
            )
        probs = []
        for i in range(BLOCK):
            n = j * BLOCK + i
            p = pos[start + n]
            limit = jnp.where(p >= slots - 1, FAR // 2, p) - base
            parts = []
            for t in range(slices):
                own = scores[i][:, t * LANES : (t + 1) * LANES]
                other = pltpu.roll(own, heads, 0)
                other = jnp.where(
                    low_half, pltpu.roll(other, LANES - kvs, 1), pltpu.roll(other, kvs, 1)
                )
                ok = slot_of_col <= limit - t * (LANES // per_slot)
                parts.append(jnp.where(ok, (own + other) * scale, -jnp.inf))
            top = functools.reduce(jnp.maximum, parts)
            top = jnp.max(top, axis=1, keepdims=True)
            floor = jnp.where(top == -jnp.inf, 0.0, top)
            parts = [jnp.exp(part - floor) for part in parts]
            total = jnp.sum(functools.reduce(jnp.add, parts), axis=1, keepdims=True)
            span = pl.ds(pl.multiple_of(n * qrows, qrows), qrows)
            m_s[span, :] = jnp.broadcast_to(top, (qrows, LANES))
            l_s[span, :] = jnp.broadcast_to(total, (qrows, LANES))
            probs.append(jnp.concatenate([part.astype(BF16) for part in parts], axis=1))
        for i in range(BLOCK):
            n = j * BLOCK + i
            span = pl.ds(pl.multiple_of(n * qrows, qrows), qrows)
            o_s[span, :] = jnp.dot(probs[i], vbuf[n], preferred_element_type=F32)
        for copy in out_copies(j):
            copy.start()
        return carry

    lax.fori_loop(0, n_blocks, block_step, 0)

    left = lax.broadcasted_iota(jnp.int32, (half, LANES), 1) < LANES // 2
    for h in range(heads):
        lo, hi = pl.ds(h, half, stride=qrows), pl.ds(heads + h, half, stride=qrows)
        part_ref[h, 0], part_ref[h, 1] = o_s[lo, :], o_s[hi, :]
        part_ref[h, 2] = jnp.where(left, m_s[lo, :], l_s[lo, :])
    for j in range(n_blocks):
        for copy in out_copies(j):
            copy.wait()


def first_half(positions, tokens, gain, w_q, w_k, w_v, rows_k, rows_v):
    rows, width = tokens.shape
    head_dim = 2 * LANES
    heads = w_q.shape[1] // head_dim
    kvs = w_k.shape[1] // head_dim
    qrows = 2 * heads
    vmem = pl.BlockSpec(memory_space=pltpu.VMEM)
    hbm = pl.BlockSpec(memory_space=pltpu.HBM)
    n_blocks = rows // 2 // BLOCK
    tile = lambda n: pltpu.VMEM((rows * n, LANES), F32)
    return pl.pallas_call(
        first_kernel,
        out_shape=(
            pltpu.VMEM((heads, 3, rows // 2, LANES), F32),
            jax.ShapeDtypeStruct(rows_k.shape, BF16),
            jax.ShapeDtypeStruct(rows_v.shape, BF16),
            tile(qrows), tile(qrows), tile(qrows),
            *(pltpu.VMEM((rows * qrows, LANES), jnp.int32) for _ in range(2)),
            tile(16), tile(16),
        ),
        in_specs=[hbm] * 8,
        out_specs=(vmem, hbm, hbm) + (vmem,) * 7,
        scratch_shapes=[
            pltpu.VMEM((heads + 2 * kvs, width, head_dim), BF16),
            pltpu.VMEM((rows // 2, *rows_k.shape[1:]), BF16),
            pltpu.VMEM((rows // 2, *rows_v.shape[1:]), BF16),
            tile(1),
            pltpu.VMEM((rows // 2 * qrows, LANES), F32),
            pltpu.VMEM((rows // 2 * qrows, LANES), F32),
            pltpu.VMEM((rows // 2 * qrows, LANES), F32),
            pltpu.SMEM((rows,), jnp.int32),
            pltpu.VMEM(tokens.shape, BF16),
            pltpu.VMEM(gain.shape, BF16),
            pltpu.SemaphoreType.DMA((heads + 2 * kvs,)),
            pltpu.SemaphoreType.DMA((n_blocks,)),
            pltpu.SemaphoreType.DMA((n_blocks,)),
            pltpu.SemaphoreType.DMA((2,)),
            pltpu.SemaphoreType.DMA((3,)),
        ],
        compiler_params=pltpu.CompilerParams(vmem_limit_bytes=36 << 20),
        name="first",
    )(*(pltpu.with_memory_space_constraint(v, pltpu.HBM) for v in (positions, tokens, gain, w_q, w_k, w_v, rows_k, rows_v)))


def combine(mine, theirs):
    left = lax.broadcasted_iota(jnp.int32, mine[2].shape, mine[2].ndim - 1) < LANES // 2
    axis = mine[2].ndim - 1

    def unpack(stats):
        turned = pltpu.roll(stats, LANES // 2, axis)
        return jnp.where(left, stats, turned), jnp.where(left, turned, stats)

    (m_a, l_a), (m_b, l_b) = unpack(mine[2]), unpack(theirs[2])
    top = jnp.maximum(m_a, m_b)
    f_a = jnp.where(m_a == -jnp.inf, 0.0, jnp.exp(m_a - top))
    f_b = jnp.where(m_b == -jnp.inf, 0.0, jnp.exp(m_b - top))
    return mine[0] * f_a + theirs[0] * f_b, mine[1] * f_a + theirs[1] * f_b, top, l_a * f_a + l_b * f_b


def layer_kernel(
    kv_heads, x_hbm, gm_hbm, wo_hbm, wg_hbm, wu_hbm, wd_hbm, ck_hbm, cv_hbm,
    far_ref, q_s, kx_s, vx_s, lim_s, hid_s,
    out_ref, kbuf, vbuf,
    ring, o_s, m_s, l_s, part, rd, sx, rx,
    po, ro, so, yo, hb, act, pm, rm, sm, ym, ob,
    x_ref, gm_ref,
    small_sem, k_sem, v_sem, o_sem, c_sem, send_sem, recv_sem,
):
    rows, width = x_ref.shape
    head_dim = ring.shape[2]
    heads = far_ref.shape[0]
    kvs = kv_heads
    group = heads // kvs
    per_slot, qrows = 2 * kvs, 2 * heads
    key_rows = ck_hbm.shape[1]
    local_slots = key_rows // per_slot
    slices = key_rows // LANES
    n_blocks = rows // 2 // BLOCK
    mine_h = heads // 2
    half, quarter = rows // 2, rows // 4
    sp, tp = lax.axis_index("sp"), lax.axis_index("tp")
    x, k = sp // 2, lax.rem(sp, 2)
    d_dev, x_dev, y_dev = {"sp": x * 2 + 1 - k}, {"sp": (1 - x) * 2 + k}, {"tp": 1 - tp}
    m_cols = act.shape[1]
    span = width // CHUNKS

    barrier = pltpu.get_barrier_semaphore()
    for dev in (d_dev, x_dev, y_dev):
        pl.semaphore_signal(barrier, inc=1, device_id=dev, device_id_type=MESH)

    counter = [0]

    def remote(src, dst, dev):
        n = counter[0]
        counter[0] += 1
        return pltpu.make_async_remote_copy(
            src_ref=src, dst_ref=dst, send_sem=send_sem.at[n], recv_sem=recv_sem.at[n],
            device_id=dev, device_id_type=MESH,
        )

    def in_copies(j):
        near, here = pl.ds(x * half + j * BLOCK, BLOCK), pl.ds(j * BLOCK, BLOCK)
        return (
            pltpu.make_async_copy(ck_hbm.at[near], kbuf.at[here], k_sem.at[j]),
            pltpu.make_async_copy(cv_hbm.at[near], vbuf.at[here], v_sem.at[j]),
        )

    small = [
        pltpu.make_async_copy(src, dst, small_sem.at[i])
        for i, (src, dst) in enumerate(
            ((x_hbm, x_ref), (gm_hbm, gm_ref))
        )
    ]
    def read(blocks):
        for j in blocks:
            for copy in in_copies(j):
                copy.start()

    read(range(EAGER[0]))

    n_w = 0
    o_rows = mine_h * head_dim
    per_o = width // o_rows
    o_copies = [
        pltpu.make_async_copy(
            wo_hbm.at[pl.ds(k * o_rows, o_rows), pl.ds(c * head_dim, head_dim)],
            ring.at[n_w + c // per_o, pl.ds((c % per_o) * o_rows, o_rows)],
            o_sem.at[c],
        )
        for c in range(width // head_dim)
    ]
    n_gate = m_cols // head_dim
    ring_at = lambda i: (n_w + 2 + i) % SLOTS
    chunks = []
    for c in range(n_gate):
        at = pl.ds(pl.multiple_of(k * m_cols + c * head_dim, LANES), head_dim)
        chunks += [wg_hbm.at[:, at], wu_hbm.at[:, at]]
    for c in range(width // head_dim):
        chunks.append(wd_hbm.at[pl.ds(pl.multiple_of(k * m_cols, LANES), m_cols), pl.ds(c * head_dim, head_dim)])
    chunks = [
        pltpu.make_async_copy(src, ring.at[ring_at(i)], c_sem.at[i]) for i, src in enumerate(chunks)
    ]
    queue = iter(chunks)

    started = [0]

    def fetch(n, limit=len(chunks)):
        n = min(n, limit - started[0])
        started[0] += n
        for copy in itertools.islice(queue, n):
            copy.start()

    row = lax.broadcasted_iota(jnp.int32, (qrows, LANES), 0)
    col = lax.broadcasted_iota(jnp.int32, (qrows, LANES), 1)
    half_of_col = (col // kvs) % 2
    fits = (half_of_col == row // heads) & (col % kvs == (row % heads) // group)
    slot_of_col = jnp.where(fits, col // per_slot, FAR)
    low_half = half_of_col == 0
    scale = 1.0 / math.sqrt(head_dim)

    def block_step(j, carry):
        for copy in in_copies(j):
            copy.wait()
        first = x * half + j * BLOCK
        at_rows = [pl.ds(pl.multiple_of((first + i) * qrows, qrows), qrows) for i in range(BLOCK)]
        scores = []
        for i in range(BLOCK):
            scores.append(
                lax.dot_general(
                    q_s[at_rows[i], :].astype(BF16), kbuf[j * BLOCK + i], (((1,), (1,)), ((), ())),
                    preferred_element_type=F32,
                )
            )
        probs, news = [], []
        for i in range(BLOCK):
            limit, hidden = lim_s[at_rows[i], :], hid_s[at_rows[i], :]
            fresh = q_s[at_rows[i], :] * kx_s[at_rows[i], :]
            fresh = jnp.sum(fresh + pltpu.roll(fresh, heads, 0), axis=1, keepdims=True) * scale
            fresh = jnp.where(hidden[:, :1] >= 0, fresh, -jnp.inf)
            parts = []
            for t in range(slices):
                own = scores[i][:, t * LANES : (t + 1) * LANES]
                other = pltpu.roll(own, heads, 0)
                other = jnp.where(
                    low_half, pltpu.roll(other, LANES - kvs, 1), pltpu.roll(other, kvs, 1)
                )
                shift = t * (LANES // per_slot)
                ok = (slot_of_col <= limit - shift) & (slot_of_col != hidden - shift)
                parts.append(jnp.where(ok, (own + other) * scale, -jnp.inf))
            top = functools.reduce(jnp.maximum, parts)
            top = jnp.maximum(jnp.max(top, axis=1, keepdims=True), fresh)
            floor = jnp.where(top == -jnp.inf, 0.0, top)
            parts = [jnp.exp(part_t - floor) for part_t in parts]
            new = jnp.exp(fresh - floor)
            total = jnp.sum(functools.reduce(jnp.add, parts), axis=1, keepdims=True) + new
            at = pl.ds(pl.multiple_of((j * BLOCK + i) * qrows, qrows), qrows)
            m_s[at, :] = jnp.broadcast_to(top, (qrows, LANES))
            l_s[at, :] = jnp.broadcast_to(total, (qrows, LANES))
            news.append(new)
            probs.append(jnp.concatenate([part_t.astype(BF16) for part_t in parts], axis=1))
        for i in range(BLOCK):
            at = pl.ds(pl.multiple_of((j * BLOCK + i) * qrows, qrows), qrows)
            o_s[at, :] = (
                jnp.dot(probs[i], vbuf[j * BLOCK + i], preferred_element_type=F32) + news[i] * vx_s[at_rows[i], :]
            )
        return carry

    size = rows // GROUPS
    my_heads, their_heads = pl.ds(k * mine_h, mine_h), pl.ds((1 - k) * mine_h, mine_h)
    near = 1
    spans = [pl.ds(0, half)] + [pl.ds(half + g * size, size) for g in range(GROUPS // 2)]
    inner = [pl.ds(g * size, size) for g in range(GROUPS // 2)]
    sources = [far_ref.at[their_heads]] + [part.at[their_heads, :, at] for at in inner]
    swaps_a = [remote(src, rd.at[:, :, at], d_dev) for src, at in zip(sources, spans)]
    cross_a = remote(sx, rx, x_dev)
    left = lambda n: lax.broadcasted_iota(jnp.int32, (mine_h, n, LANES), 2) < LANES // 2
    joined = [None] * len(spans)

    def publish(g):
        at = inner[g - near]
        for h in range(heads):
            lo = pl.ds((g - near) * size * qrows + h, size, stride=qrows)
            hi = pl.ds((g - near) * size * qrows + heads + h, size, stride=qrows)
            part[h, 0, at], part[h, 1, at] = o_s[lo, :], o_s[hi, :]
            part[h, 2, at] = jnp.where(left(size)[0], m_s[lo, :], l_s[lo, :])
        swaps_a[g].start()

    def chip(g):
        swaps_a[g].wait_recv()
        at = spans[g]
        here, local = (far_ref, at) if g < near else (part, inner[g - near])
        o_a, o_b, m, l = combine(
            [here[my_heads, i, local] for i in range(3)], [rd[:, i, at] for i in range(3)]
        )
        value = [o_a, o_b, jnp.where(left(m.shape[1]), m, l)]
        if g < near:
            for i in range(3):
                sx[:, i] = value[i]
            cross_a.start()
        joined[g] = value

    pl.semaphore_wait(barrier, 3)
    for g in range(near):
        swaps_a[g].start()
    read(range(*EAGER))
    for copy in small:
        copy.start()
    step = n_blocks // 2
    lax.fori_loop(0, step, block_step, 0)
    for g in range(near):
        chip(g)
    read(range(EAGER[1], n_blocks))
    publish(near)
    for copy in o_copies:
        copy.start()
    lax.fori_loop(step, n_blocks, block_step, 0)
    publish(near + 1)
    fetch(3)
    for g in range(near, len(spans)):
        chip(g)
    cross_a.wait_recv()
    pieces = []
    for g in range(GROUPS // 2):
        o_a, o_b, _, l = combine(joined[near + g], [rx[:, i, inner[g]] for i in range(3)])
        o_a, o_b = (o_a / l).astype(BF16), (o_b / l).astype(BF16)
        pieces.append(jnp.concatenate([v[h] for h in range(mine_h) for v in (o_a, o_b)], axis=-1))
    attended = jnp.concatenate(pieces, axis=0)
    for copy in small:
        copy.wait()

    own, other = pl.ds(k * quarter, quarter), pl.ds((1 - k) * quarter, quarter)
    my_rows = pl.ds(pl.multiple_of(x * half + k * quarter, quarter), quarter)
    x_peer_rows = pl.ds(pl.multiple_of((1 - x) * half + k * quarter, quarter), quarter)
    cols = [pl.ds(c * span, span) for c in range(CHUNKS)]
    per_span = span // head_dim
    cuts = (0, 3, CHUNKS)
    joint = [pl.ds(a * span, (b - a) * span) for a, b in zip(cuts, cuts[1:])]
    last_of = {b - 1: i for i, b in enumerate(cuts[1:])}

    def staged(dot, swap, cross, *rest):
        for c in range(CHUNKS + 2):
            if c < CHUNKS:
                dot(c)
            if c >= 2:
                swap(c - 2)
        for c in range(CHUNKS):
            cross(c)
        for c in range(CHUNKS + len(rest) - 1):
            for s, stage in enumerate(rest):
                if 0 <= c - s < CHUNKS:
                    stage(c - s)

    swaps = [remote(po.at[other, c], ro.at[:, c], d_dev) for c in cols]
    crosses = [remote(so.at[:, c], yo.at[:, c], y_dev) for c in cols]
    gathers = [remote(hb.at[own, c], hb.at[own, c], d_dev) for c in joint]

    def o_dot(c):
        for i in range(c * per_span, (c + 1) * per_span):
            o_copies[i].wait()
            w = ring[n_w + i // per_o, (i % per_o) * o_rows : (i % per_o + 1) * o_rows, :]
            po[:, i * head_dim : (i + 1) * head_dim] = jnp.dot(attended, w, preferred_element_type=F32)
        swaps[c].start()

    def o_swap(c):
        swaps[c].wait_recv()
        so[:, cols[c]] = po[own, cols[c]] + ro[:, cols[c]]
        crosses[c].start()
        if c == CHUNKS - 1:
            fetch(15)

    def o_cross(c):
        crosses[c].wait_recv()
        total = so[:, cols[c]] + yo[:, cols[c]]
        hb[own, cols[c]] = (x_ref[my_rows, cols[c]].astype(F32) + total).astype(BF16).astype(F32)
        if c in last_of:
            gathers[last_of[c]].start()

    def o_gather(c):
        if c in last_of:
            gathers[last_of[c]].wait_recv()

    staged(o_dot, o_swap, o_cross, o_gather)
    fetch(SLOTS, SLOTS)

    normed_m = rms_norm(hb[...], gm_ref[...])
    for c in range(n_gate):
        chunks[2 * c].wait()
        chunks[2 * c + 1].wait()
        gate = jnp.dot(normed_m, ring[ring_at(2 * c)], preferred_element_type=F32)
        up = jnp.dot(normed_m, ring[ring_at(2 * c + 1)], preferred_element_type=F32)
        act[:, c * head_dim : (c + 1) * head_dim] = (jax.nn.silu(gate) * up).astype(BF16)
        fetch(2)

    swaps_m = [remote(pm.at[other, c], rm.at[:, c], d_dev) for c in cols]
    crosses_m = [remote(sm.at[:, c], ym.at[:, c], y_dev) for c in cols]
    to_core = [remote(ob.at[my_rows], ob.at[my_rows], d_dev)]
    to_x = [remote(ob.at[my_rows, c], ob.at[my_rows, c], x_dev) for c in cols]
    onward = [remote(ob.at[x_peer_rows, c], ob.at[x_peer_rows, c], d_dev) for c in joint]

    def m_dot(c):
        for i in range(c * per_span, (c + 1) * per_span):
            chunks[2 * n_gate + i].wait()
            pm[:, i * head_dim : (i + 1) * head_dim] = jnp.dot(
                act[...], ring[ring_at(2 * n_gate + i)], preferred_element_type=F32
            )
        swaps_m[c].start()

    def m_swap(c):
        swaps_m[c].wait_recv()
        sm[:, cols[c]] = pm[own, cols[c]] + rm[:, cols[c]]
        crosses_m[c].start()

    def m_cross(c):
        crosses_m[c].wait_recv()
        total = sm[:, cols[c]] + ym[:, cols[c]]
        ob[my_rows, cols[c]] = (hb[own, cols[c]] + total).astype(BF16).astype(F32)
        to_x[c].start()
        if c == CHUNKS - 1:
            to_core[0].start()

    def m_gather(c):
        to_x[c].wait_recv()
        if c in last_of:
            onward[last_of[c]].start()

    def m_last(c):
        if c == 0:
            to_core[0].wait_recv()
        if c in last_of:
            at = joint[last_of[c]]
            onward[last_of[c]].wait_recv()
            out_ref[:, at] = ob[:, at].astype(BF16)

    staged(m_dot, m_swap, m_cross, m_gather, m_last)
    for copy in [*swaps_a, cross_a, *swaps, *crosses, *gathers, *swaps_m, *crosses_m, *to_core, *to_x, *onward]:
        copy.wait_send()


def layer(tokens, gain, w_o, w_gate, w_up, w_down, rows_k, rows_v, kvs, carried):
    rows, width = tokens.shape
    head_dim = 2 * LANES
    heads = carried[0].shape[0]
    qrows = 2 * heads
    half, quarter = rows // 2, rows // 4
    cut = w_gate.shape[1] // 2
    n_blocks = half // BLOCK
    vmem = pl.BlockSpec(memory_space=pltpu.VMEM)
    hbm = pl.BlockSpec(memory_space=pltpu.HBM)
    flat = lambda n: pltpu.VMEM((n, width), F32)
    stats = lambda h, n: pltpu.VMEM((h, 3, n, LANES), F32)
    dma = lambda n: pltpu.SemaphoreType.DMA((n,))
    n_remote = GROUPS // 2 + 2 + 5 * CHUNKS + 5
    args = (tokens, gain, w_o, w_gate, w_up, w_down, rows_k, rows_v)
    shape = (half, *rows_k.shape[1:])
    return pl.pallas_call(
        functools.partial(layer_kernel, kvs),
        out_shape=(
            pltpu.VMEM(tokens.shape, BF16),
            pltpu.VMEM(shape, BF16),
            pltpu.VMEM(shape, BF16),
        ),
        in_specs=[hbm] * len(args) + [vmem] * len(carried),
        out_specs=(vmem,) * 3,
        scratch_shapes=[
            pltpu.VMEM((SLOTS, width, head_dim), BF16),
            *(pltpu.VMEM((half * qrows, LANES), F32) for _ in range(3)),
            stats(heads, half), stats(heads // 2, rows), stats(heads // 2, half), stats(heads // 2, half),
            flat(half), flat(quarter), flat(quarter), flat(quarter), flat(half),
            pltpu.VMEM((half, cut), BF16),
            flat(half), flat(quarter), flat(quarter), flat(quarter), flat(rows),
            pltpu.VMEM(tokens.shape, BF16),
            pltpu.VMEM(gain.shape, BF16),
            dma(2), dma(n_blocks), dma(n_blocks), dma(width // head_dim),
            dma(2 * (cut // head_dim) + width // head_dim), dma(n_remote), dma(n_remote),
        ],
        compiler_params=pltpu.CompilerParams(
            vmem_limit_bytes=LAYER_VMEM << 20, collective_id=0, has_side_effects=True
        ),
        name="layer",
    )(*(pltpu.with_memory_space_constraint(v, pltpu.HBM) for v in args), *carried)


def write_kernel(pos_hbm, t_ref, kn_s, vn_s, _bk, _bv, _k, _v, out_hbm, nk_hbm, nv_hbm, kbuf, vbuf, pos, sem, tile_sem, pos_sem, out_sem):
    rows, key_rows, _ = kbuf.shape
    per_slot = 4
    local_slots = key_rows // per_slot
    slots = local_slots * lax.axis_size("sp")
    base = lax.axis_index("sp") * local_slots
    start = lax.axis_index("sp") // 2 * rows
    per_tile = 16 // per_slot
    n_blocks = rows // BLOCK
    tile_row = lax.broadcasted_iota(jnp.int32, (16, LANES), 0) // per_slot

    def copies(j):
        here, near = pl.ds(j * BLOCK, BLOCK), pl.ds(start + j * BLOCK, BLOCK)
        return (
            pltpu.make_async_copy(kbuf.at[here], nk_hbm.at[near], sem.at[0, j]),
            pltpu.make_async_copy(vbuf.at[here], nv_hbm.at[near], sem.at[1, j]),
        )

    def target(b):
        local = lax.rem(pos[b], slots) - base
        owned = (local >= 0) & (local < local_slots)
        safe = jnp.where(owned, local, 0)
        hit = jnp.where(owned, lax.rem(safe, per_tile), -1)
        return hit, pl.ds(pl.multiple_of((safe // per_tile) * 16, 16), 16)

    def tile_copies(n):
        at = target(start + n)[1]
        return (
            pltpu.make_async_copy(kbuf.at[n, at], nk_hbm.at[start + n, at], tile_sem.at[0]),
            pltpu.make_async_copy(vbuf.at[n, at], nv_hbm.at[start + n, at], tile_sem.at[1]),
        )

    def patch(n):
        b = start + n
        hit, at = target(b)
        for buf, new in ((kbuf, kn_s), (vbuf, vn_s)):
            fresh = new[pl.ds(pl.multiple_of(b * 16, 16), 16), :]
            buf[n, at, :] = jnp.where(tile_row == hit, fresh, buf[n, at, :].astype(F32)).astype(BF16)

    pos_copy = pltpu.make_async_copy(pos_hbm, pos, pos_sem)
    pos_copy.start()
    for j in range(EARLY):
        for copy in copies(j):
            copy.start()
    out_copy = pltpu.make_async_copy(t_ref, out_hbm, out_sem)
    out_copy.start()
    pos_copy.wait()
    for j in range(EARLY, n_blocks + 1):
        if j < n_blocks:
            for i in range(BLOCK):
                patch(j * BLOCK + i)
        if j > EARLY:
            for copy in copies(j - 1):
                copy.start()
    for j in range(EARLY):
        for copy in copies(j):
            copy.wait()
        for i in range(BLOCK):
            patch(j * BLOCK + i)
        if j:
            for i in range(BLOCK):
                for copy in tile_copies((j - 1) * BLOCK + i):
                    copy.start()
    for i in range(BLOCK):
        for copy in tile_copies((EARLY - 1) * BLOCK + i):
            copy.start()
    for j in range(EARLY, n_blocks):
        for copy in copies(j):
            copy.wait()
    for n in range(EARLY * BLOCK):
        for copy in tile_copies(n):
            copy.wait()
    out_copy.wait()


def write(positions, layer_out, fresh_k, fresh_v, buf_k, buf_v, new_k, new_v):
    vmem = pl.BlockSpec(memory_space=pltpu.VMEM)
    hbm = pl.BlockSpec(memory_space=pltpu.HBM)
    return pl.pallas_call(
        write_kernel,
        out_shape=(
            *(jax.ShapeDtypeStruct(v.shape, BF16) for v in (layer_out, new_k, new_v)),
            pltpu.VMEM(buf_k.shape, BF16),
            pltpu.VMEM(buf_v.shape, BF16),
        ),
        in_specs=[hbm] + [vmem] * 5 + [hbm] * 2,
        out_specs=(hbm, hbm, hbm, vmem, vmem),
        input_output_aliases={4: 3, 5: 4, 6: 1, 7: 2},
        scratch_shapes=[
            pltpu.SMEM(positions.shape, jnp.int32),
            pltpu.SemaphoreType.DMA((2, buf_k.shape[0] // BLOCK)),
            pltpu.SemaphoreType.DMA((2,)),
            pltpu.SemaphoreType.DMA,
            pltpu.SemaphoreType.DMA,
        ],
        compiler_params=pltpu.CompilerParams(vmem_limit_bytes=LAYER_VMEM << 20),
        name="write",
    )(pltpu.with_memory_space_constraint(positions, pltpu.HBM), layer_out, fresh_k, fresh_v, buf_k, buf_v, new_k, new_v)[:3]


def to_rows(cache):
    b, s, kv, d = cache.shape
    return cache.reshape(b, s, kv, d // LANES, LANES).transpose(0, 1, 3, 2, 4).reshape(b, -1, LANES)


def from_rows(rows, shape):
    b, s, kv, d = shape
    return rows.reshape(b, s, d // LANES, kv, LANES).transpose(0, 1, 3, 2, 4).reshape(shape)


def solution(mesh):
    cache_spec = P("dp", "sp", "tp", None)
    row_spec = P("dp", None)
    col_spec = P(None, "tp")
    in_specs = (row_spec, P("dp"), cache_spec, cache_spec, P(None), col_spec, col_spec, col_spec, P("tp", None), P(None), col_spec, col_spec, P("tp", None))
    out_specs = (row_spec, cache_spec, cache_spec)

    def local_step(tokens, positions, cache_k, cache_v, attn_gain, w_q, w_k, w_v, w_o, mlp_gain, w_gate, w_up, w_down):
        old_k, old_v = to_rows(cache_k), to_rows(cache_v)
        far, rows_k, rows_v, *carried, fresh_k, fresh_v = first_half(
            positions, tokens, attn_gain, w_q, w_k, w_v, old_k, old_v
        )
        out, buf_k, buf_v = layer(
            tokens, mlp_gain, w_o, w_gate, w_up, w_down, old_k, old_v, cache_k.shape[2], (far, *carried)
        )
        layer_out, rows_k, rows_v = write(positions, out, fresh_k, fresh_v, buf_k, buf_v, rows_k, rows_v)
        new_k = from_rows(rows_k, cache_k.shape)
        new_v = from_rows(rows_v, cache_v.shape)
        return layer_out, new_k, new_v

    return jax.shard_map(local_step, mesh=mesh, in_specs=in_specs, out_specs=out_specs, check_vma=False)
```

```python
import functools
import itertools
import math

import jax
import jax.numpy as jnp
from jax import lax
from jax.experimental import pallas as pl
from jax.experimental.pallas import tpu as pltpu
from jax.sharding import PartitionSpec as P

NORM_EPS = 1e-5
ROPE_THETA = 10000.0
LANES = 128
F32 = jnp.float32
BF16 = jnp.bfloat16
FAR = 1 << 28
BLOCK = 2
EARLY = 6
EAGER = (6, 16)
FIRST = 8
SLOTS = 22
LAYER_VMEM = 35
CUTS = (0, 4, 8, 10)
CHUNKS = len(CUTS) - 1
GROUPS = 4
MESH = pl.DeviceIdType.MESH


def rms_norm(values, gain):
    wide = values.astype(F32)
    inv_rms = lax.rsqrt(jnp.mean(wide * wide, axis=-1, keepdims=True) + NORM_EPS)
    return (wide * inv_rms * gain.astype(F32)).astype(BF16)


def first_kernel(
    pos_hbm, x_hbm, gain_hbm, wq_hbm, wk_hbm, wv_hbm, ck_hbm, cv_hbm,
    part_ref, nk_hbm, nv_hbm, q_s, kx_s, vx_s, lim_s, hid_s, kn_s, vn_s,
    wbuf, kbuf, vbuf, ang_s, o_s, m_s, l_s,
    pos, x_ref, gain_ref, w_sem, k_sem, v_sem, out_sem, x_sem,
):
    rows = x_ref.shape[0]
    head_dim = 2 * LANES
    heads = wq_hbm.shape[1] // head_dim
    kvs = wk_hbm.shape[1] // head_dim
    group = heads // kvs
    per_slot = 2 * kvs
    qrows = 2 * heads
    key_rows = ck_hbm.shape[1]
    local_slots = key_rows // per_slot
    slots = local_slots * lax.axis_size("sp")
    slices = key_rows // LANES
    half = rows // 2
    n_blocks = half // BLOCK
    start = (1 - lax.axis_index("sp") // 2) * half
    base = lax.axis_index("sp") * local_slots

    def w_copy(n):
        src, col = (
            (wk_hbm, n) if n < kvs else (wv_hbm, n - kvs) if n < 2 * kvs else (wq_hbm, n - 2 * kvs)
        )
        return pltpu.make_async_copy(src.at[:, pl.ds(col * head_dim, head_dim)], wbuf.at[n], w_sem.at[n])

    def in_copies(j):
        far, here = pl.ds(start + j * BLOCK, BLOCK), pl.ds(j * BLOCK, BLOCK)
        return (
            pltpu.make_async_copy(ck_hbm.at[far], kbuf.at[here], k_sem.at[j]),
            pltpu.make_async_copy(cv_hbm.at[far], vbuf.at[here], v_sem.at[j]),
        )

    def out_copies(j):
        far, here = pl.ds(start + j * BLOCK, BLOCK), pl.ds(j * BLOCK, BLOCK)
        return (
            pltpu.make_async_copy(kbuf.at[here], nk_hbm.at[far], out_sem.at[0]),
            pltpu.make_async_copy(vbuf.at[here], nv_hbm.at[far], out_sem.at[1]),
        )

    small = [
        pltpu.make_async_copy(src, dst, x_sem.at[i])
        for i, (src, dst) in enumerate(((pos_hbm, pos), (x_hbm, x_ref), (gain_hbm, gain_ref)))
    ]
    for copy in small:
        copy.start()
    n_w = heads + 2 * kvs
    for n in range(n_w // 2):
        w_copy(n).start()

    lane = lax.broadcasted_iota(jnp.int32, (1, LANES), 1).astype(F32)
    freq = jnp.exp2(lane * (-math.log2(ROPE_THETA) / LANES))

    for copy in small:
        copy.wait()
    for n in range(n_w // 2, n_w):
        w_copy(n).start()
    for j in range(FIRST):
        for copy in in_copies(j):
            copy.start()

    def angle_row(b, carry):
        p = pos[b]
        ang_s[pl.ds(b, 1), :] = freq * p.astype(F32)
        local = lax.rem(p, slots) - base
        owned = (local >= 0) & (local < local_slots)
        span = pl.ds(pl.multiple_of(b * qrows, qrows), qrows)
        lim_s[span, :] = jnp.full((qrows, LANES), jnp.where(p >= slots - 1, FAR // 2, p) - base, jnp.int32)
        hid_s[span, :] = jnp.full((qrows, LANES), jnp.where(owned, local, -FAR), jnp.int32)
        return carry

    lax.fori_loop(0, rows, angle_row, 0, unroll=8)
    angles = ang_s[...]
    cos_t, sin_t = jnp.cos(angles), jnp.sin(angles)
    normed = rms_norm(x_ref[...], gain_ref[...])

    for n in range(n_w):
        w_copy(n).wait()
        if FIRST + n < n_blocks:
            for copy in in_copies(FIRST + n):
                copy.start()
        lin = jnp.dot(normed, wbuf[n], preferred_element_type=F32)
        first, second = lin[:, :LANES], lin[:, LANES:]
        if not kvs <= n < 2 * kvs:
            first, second = first * cos_t - second * sin_t, second * cos_t + first * sin_t
        first, second = first.astype(BF16).astype(F32), second.astype(BF16).astype(F32)
        if n >= 2 * kvs:
            h = n - 2 * kvs
            q_s[pl.ds(h, rows, stride=qrows), :] = first
            q_s[pl.ds(heads + h, rows, stride=qrows), :] = second
        else:
            dst, tile, kv = (kn_s, kx_s, n) if n < kvs else (vn_s, vx_s, n - kvs)
            for rep in range(16 // per_slot):
                dst[pl.ds(rep * per_slot + kv, rows, stride=16), :] = first
                dst[pl.ds(rep * per_slot + kvs + kv, rows, stride=16), :] = second
            for g in range(group):
                tile[pl.ds(kv * group + g, rows, stride=qrows), :] = first
                tile[pl.ds(heads + kv * group + g, rows, stride=qrows), :] = second

    row = lax.broadcasted_iota(jnp.int32, (qrows, LANES), 0)
    col = lax.broadcasted_iota(jnp.int32, (qrows, LANES), 1)
    half_of_col = (col // kvs) % 2
    fits = (half_of_col == row // heads) & (col % kvs == (row % heads) // group)
    slot_of_col = jnp.where(fits, col // per_slot, FAR)
    low_half = half_of_col == 0
    patch_row = lax.broadcasted_iota(jnp.int32, (16, LANES), 0) // per_slot
    scale = 1.0 / math.sqrt(head_dim)

    def block_step(j, carry):
        for copy in in_copies(j):
            copy.wait()
        for i in range(BLOCK):
            n = j * BLOCK + i
            b = start + n
            local = lax.rem(pos[b], slots) - base
            owned = (local >= 0) & (local < local_slots)
            safe = jnp.where(owned, local, 0)
            hit = jnp.where(owned, lax.rem(safe, 16 // per_slot), -1)
            span = pl.ds(pl.multiple_of((safe // (16 // per_slot)) * 16, 16), 16)
            for buf, new in ((kbuf, kn_s), (vbuf, vn_s)):
                old = buf[n, span, :].astype(F32)
                fresh = new[pl.ds(pl.multiple_of(b * 16, 16), 16), :]
                buf[n, span, :] = jnp.where(patch_row == hit, fresh, old).astype(BF16)
        scores = []
        for i in range(BLOCK):
            b = start + j * BLOCK + i
            q = q_s[pl.ds(pl.multiple_of(b * qrows, qrows), qrows), :].astype(BF16)
            scores.append(
                lax.dot_general(q, kbuf[j * BLOCK + i], (((1,), (1,)), ((), ())), preferred_element_type=F32)
            )
        probs = []
        for i in range(BLOCK):
            n = j * BLOCK + i
            p = pos[start + n]
            limit = jnp.where(p >= slots - 1, FAR // 2, p) - base
            parts = []
            for t in range(slices):
                own = scores[i][:, t * LANES : (t + 1) * LANES]
                other = pltpu.roll(own, heads, 0)
                other = jnp.where(
                    low_half, pltpu.roll(other, LANES - kvs, 1), pltpu.roll(other, kvs, 1)
                )
                ok = slot_of_col <= limit - t * (LANES // per_slot)
                parts.append(jnp.where(ok, (own + other) * scale, -jnp.inf))
            top = functools.reduce(jnp.maximum, parts)
            top = jnp.max(top, axis=1, keepdims=True)
            floor = jnp.where(top == -jnp.inf, 0.0, top)
            parts = [jnp.exp(part - floor) for part in parts]
            total = jnp.sum(functools.reduce(jnp.add, parts), axis=1, keepdims=True)
            span = pl.ds(pl.multiple_of(n * qrows, qrows), qrows)
            m_s[span, :] = jnp.broadcast_to(top, (qrows, LANES))
            l_s[span, :] = jnp.broadcast_to(total, (qrows, LANES))
            probs.append(jnp.concatenate([part.astype(BF16) for part in parts], axis=1))
        for i in range(BLOCK):
            n = j * BLOCK + i
            span = pl.ds(pl.multiple_of(n * qrows, qrows), qrows)
            o_s[span, :] = jnp.dot(probs[i], vbuf[n], preferred_element_type=F32)
        for copy in out_copies(j):
            copy.start()
        return carry

    lax.fori_loop(0, n_blocks, block_step, 0)

    left = lax.broadcasted_iota(jnp.int32, (half, LANES), 1) < LANES // 2
    for h in range(heads):
        lo, hi = pl.ds(h, half, stride=qrows), pl.ds(heads + h, half, stride=qrows)
        part_ref[h, 0], part_ref[h, 1] = o_s[lo, :], o_s[hi, :]
        part_ref[h, 2] = jnp.where(left, m_s[lo, :], l_s[lo, :])
    for j in range(n_blocks):
        for copy in out_copies(j):
            copy.wait()


def first_half(positions, tokens, gain, w_q, w_k, w_v, rows_k, rows_v):
    rows, width = tokens.shape
    head_dim = 2 * LANES
    heads = w_q.shape[1] // head_dim
    kvs = w_k.shape[1] // head_dim
    qrows = 2 * heads
    vmem = pl.BlockSpec(memory_space=pltpu.VMEM)
    hbm = pl.BlockSpec(memory_space=pltpu.HBM)
    n_blocks = rows // 2 // BLOCK
    tile = lambda n: pltpu.VMEM((rows * n, LANES), F32)
    return pl.pallas_call(
        first_kernel,
        out_shape=(
            pltpu.VMEM((heads, 3, rows // 2, LANES), F32),
            jax.ShapeDtypeStruct(rows_k.shape, BF16),
            jax.ShapeDtypeStruct(rows_v.shape, BF16),
            tile(qrows), tile(qrows), tile(qrows),
            *(pltpu.VMEM((rows * qrows, LANES), jnp.int32) for _ in range(2)),
            tile(16), tile(16),
        ),
        in_specs=[hbm] * 8,
        out_specs=(vmem, hbm, hbm) + (vmem,) * 7,
        scratch_shapes=[
            pltpu.VMEM((heads + 2 * kvs, width, head_dim), BF16),
            pltpu.VMEM((rows // 2, *rows_k.shape[1:]), BF16),
            pltpu.VMEM((rows // 2, *rows_v.shape[1:]), BF16),
            tile(1),
            pltpu.VMEM((rows // 2 * qrows, LANES), F32),
            pltpu.VMEM((rows // 2 * qrows, LANES), F32),
            pltpu.VMEM((rows // 2 * qrows, LANES), F32),
            pltpu.SMEM((rows,), jnp.int32),
            pltpu.VMEM(tokens.shape, BF16),
            pltpu.VMEM(gain.shape, BF16),
            pltpu.SemaphoreType.DMA((heads + 2 * kvs,)),
            pltpu.SemaphoreType.DMA((n_blocks,)),
            pltpu.SemaphoreType.DMA((n_blocks,)),
            pltpu.SemaphoreType.DMA((2,)),
            pltpu.SemaphoreType.DMA((3,)),
        ],
        compiler_params=pltpu.CompilerParams(vmem_limit_bytes=36 << 20),
        name="first",
    )(*(pltpu.with_memory_space_constraint(v, pltpu.HBM) for v in (positions, tokens, gain, w_q, w_k, w_v, rows_k, rows_v)))


def combine(mine, theirs):
    left = lax.broadcasted_iota(jnp.int32, mine[2].shape, mine[2].ndim - 1) < LANES // 2
    axis = mine[2].ndim - 1

    def unpack(stats):
        turned = pltpu.roll(stats, LANES // 2, axis)
        return jnp.where(left, stats, turned), jnp.where(left, turned, stats)

    (m_a, l_a), (m_b, l_b) = unpack(mine[2]), unpack(theirs[2])
    top = jnp.maximum(m_a, m_b)
    f_a = jnp.where(m_a == -jnp.inf, 0.0, jnp.exp(m_a - top))
    f_b = jnp.where(m_b == -jnp.inf, 0.0, jnp.exp(m_b - top))
    return mine[0] * f_a + theirs[0] * f_b, mine[1] * f_a + theirs[1] * f_b, top, l_a * f_a + l_b * f_b


def layer_kernel(
    kv_heads, x_hbm, gm_hbm, wo_hbm, wg_hbm, wu_hbm, wd_hbm, ck_hbm, cv_hbm,
    far_ref, q_s, kx_s, vx_s, lim_s, hid_s,
    out_ref, kbuf, vbuf,
    ring, o_s, m_s, l_s, part, rd, sx, rx,
    po, ro, so, yo, hb, act, pm, rm, sm, ym, ob,
    x_ref, gm_ref,
    small_sem, k_sem, v_sem, o_sem, c_sem, send_sem, recv_sem,
):
    rows, width = x_ref.shape
    head_dim = ring.shape[2]
    heads = far_ref.shape[0]
    kvs = kv_heads
    group = heads // kvs
    per_slot, qrows = 2 * kvs, 2 * heads
    key_rows = ck_hbm.shape[1]
    local_slots = key_rows // per_slot
    slices = key_rows // LANES
    n_blocks = rows // 2 // BLOCK
    mine_h = heads // 2
    half, quarter = rows // 2, rows // 4
    sp, tp = lax.axis_index("sp"), lax.axis_index("tp")
    x, k = sp // 2, lax.rem(sp, 2)
    d_dev, x_dev, y_dev = {"sp": x * 2 + 1 - k}, {"sp": (1 - x) * 2 + k}, {"tp": 1 - tp}
    m_cols = act.shape[1]

    barrier = pltpu.get_barrier_semaphore()
    for dev in (d_dev, x_dev, y_dev):
        pl.semaphore_signal(barrier, inc=1, device_id=dev, device_id_type=MESH)

    counter = [0]

    def remote(src, dst, dev):
        n = counter[0]
        counter[0] += 1
        return pltpu.make_async_remote_copy(
            src_ref=src, dst_ref=dst, send_sem=send_sem.at[n], recv_sem=recv_sem.at[n],
            device_id=dev, device_id_type=MESH,
        )

    def in_copies(j):
        near, here = pl.ds(x * half + j * BLOCK, BLOCK), pl.ds(j * BLOCK, BLOCK)
        return (
            pltpu.make_async_copy(ck_hbm.at[near], kbuf.at[here], k_sem.at[j]),
            pltpu.make_async_copy(cv_hbm.at[near], vbuf.at[here], v_sem.at[j]),
        )

    small = [
        pltpu.make_async_copy(src, dst, small_sem.at[i])
        for i, (src, dst) in enumerate(
            ((x_hbm, x_ref), (gm_hbm, gm_ref))
        )
    ]
    def read(blocks):
        for j in blocks:
            for copy in in_copies(j):
                copy.start()

    read(range(EAGER[0]))

    n_w = 0
    o_rows = mine_h * head_dim
    per_o = width // o_rows
    o_copies = [
        pltpu.make_async_copy(
            wo_hbm.at[pl.ds(k * o_rows, o_rows), pl.ds(c * head_dim, head_dim)],
            ring.at[n_w + c // per_o, pl.ds((c % per_o) * o_rows, o_rows)],
            o_sem.at[c],
        )
        for c in range(width // head_dim)
    ]
    n_gate = m_cols // head_dim
    ring_at = lambda i: (n_w + 2 + i) % SLOTS
    chunks = []
    for c in range(n_gate):
        at = pl.ds(pl.multiple_of(k * m_cols + c * head_dim, LANES), head_dim)
        chunks += [wg_hbm.at[:, at], wu_hbm.at[:, at]]
    for c in range(width // head_dim):
        chunks.append(wd_hbm.at[pl.ds(pl.multiple_of(k * m_cols, LANES), m_cols), pl.ds(c * head_dim, head_dim)])
    chunks = [
        pltpu.make_async_copy(src, ring.at[ring_at(i)], c_sem.at[i]) for i, src in enumerate(chunks)
    ]
    queue = iter(chunks)

    started = [0]

    def fetch(n, limit=len(chunks)):
        n = min(n, limit - started[0])
        started[0] += n
        for copy in itertools.islice(queue, n):
            copy.start()

    row = lax.broadcasted_iota(jnp.int32, (qrows, LANES), 0)
    col = lax.broadcasted_iota(jnp.int32, (qrows, LANES), 1)
    half_of_col = (col // kvs) % 2
    fits = (half_of_col == row // heads) & (col % kvs == (row % heads) // group)
    slot_of_col = jnp.where(fits, col // per_slot, FAR)
    low_half = half_of_col == 0
    scale = 1.0 / math.sqrt(head_dim)

    def block_step(j, carry):
        for copy in in_copies(j):
            copy.wait()
        first = x * half + j * BLOCK
        at_rows = [pl.ds(pl.multiple_of((first + i) * qrows, qrows), qrows) for i in range(BLOCK)]
        scores = []
        for i in range(BLOCK):
            scores.append(
                lax.dot_general(
                    q_s[at_rows[i], :].astype(BF16), kbuf[j * BLOCK + i], (((1,), (1,)), ((), ())),
                    preferred_element_type=F32,
                )
            )
        probs, news = [], []
        for i in range(BLOCK):
            limit, hidden = lim_s[at_rows[i], :], hid_s[at_rows[i], :]
            fresh = q_s[at_rows[i], :] * kx_s[at_rows[i], :]
            fresh = jnp.sum(fresh + pltpu.roll(fresh, heads, 0), axis=1, keepdims=True) * scale
            fresh = jnp.where(hidden[:, :1] >= 0, fresh, -jnp.inf)
            parts = []
            for t in range(slices):
                own = scores[i][:, t * LANES : (t + 1) * LANES]
                other = pltpu.roll(own, heads, 0)
                other = jnp.where(
                    low_half, pltpu.roll(other, LANES - kvs, 1), pltpu.roll(other, kvs, 1)
                )
                shift = t * (LANES // per_slot)
                ok = (slot_of_col <= limit - shift) & (slot_of_col != hidden - shift)
                parts.append(jnp.where(ok, (own + other) * scale, -jnp.inf))
            top = functools.reduce(jnp.maximum, parts)
            top = jnp.maximum(jnp.max(top, axis=1, keepdims=True), fresh)
            floor = jnp.where(top == -jnp.inf, 0.0, top)
            parts = [jnp.exp(part_t - floor) for part_t in parts]
            new = jnp.exp(fresh - floor)
            total = jnp.sum(functools.reduce(jnp.add, parts), axis=1, keepdims=True) + new
            at = pl.ds(pl.multiple_of((j * BLOCK + i) * qrows, qrows), qrows)
            m_s[at, :] = jnp.broadcast_to(top, (qrows, LANES))
            l_s[at, :] = jnp.broadcast_to(total, (qrows, LANES))
            news.append(new)
            probs.append(jnp.concatenate([part_t.astype(BF16) for part_t in parts], axis=1))
        for i in range(BLOCK):
            at = pl.ds(pl.multiple_of((j * BLOCK + i) * qrows, qrows), qrows)
            o_s[at, :] = (
                jnp.dot(probs[i], vbuf[j * BLOCK + i], preferred_element_type=F32) + news[i] * vx_s[at_rows[i], :]
            )
        return carry

    size = rows // GROUPS
    my_heads, their_heads = pl.ds(k * mine_h, mine_h), pl.ds((1 - k) * mine_h, mine_h)
    near = 1
    spans = [pl.ds(0, half)] + [pl.ds(half + g * size, size) for g in range(GROUPS // 2)]
    inner = [pl.ds(g * size, size) for g in range(GROUPS // 2)]
    sources = [far_ref.at[their_heads]] + [part.at[their_heads, :, at] for at in inner]
    swaps_a = [remote(src, rd.at[:, :, at], d_dev) for src, at in zip(sources, spans)]
    cross_a = remote(sx, rx, x_dev)
    left = lambda n: lax.broadcasted_iota(jnp.int32, (mine_h, n, LANES), 2) < LANES // 2
    joined = [None] * len(spans)

    def publish(g):
        at = inner[g - near]
        for h in range(heads):
            lo = pl.ds((g - near) * size * qrows + h, size, stride=qrows)
            hi = pl.ds((g - near) * size * qrows + heads + h, size, stride=qrows)
            part[h, 0, at], part[h, 1, at] = o_s[lo, :], o_s[hi, :]
            part[h, 2, at] = jnp.where(left(size)[0], m_s[lo, :], l_s[lo, :])
        swaps_a[g].start()

    def chip(g):
        swaps_a[g].wait_recv()
        at = spans[g]
        here, local = (far_ref, at) if g < near else (part, inner[g - near])
        o_a, o_b, m, l = combine(
            [here[my_heads, i, local] for i in range(3)], [rd[:, i, at] for i in range(3)]
        )
        value = [o_a, o_b, jnp.where(left(m.shape[1]), m, l)]
        if g < near:
            for i in range(3):
                sx[:, i] = value[i]
            cross_a.start()
        joined[g] = value

    pl.semaphore_wait(barrier, 3)
    for g in range(near):
        swaps_a[g].start()
    read(range(*EAGER))
    for copy in small:
        copy.start()
    step = n_blocks // 2
    lax.fori_loop(0, step, block_step, 0)
    for g in range(near):
        chip(g)
    read(range(EAGER[1], n_blocks))
    publish(near)
    for copy in o_copies:
        copy.start()
    lax.fori_loop(step, n_blocks, block_step, 0)
    publish(near + 1)
    fetch(3)
    for g in range(near, len(spans)):
        chip(g)
    cross_a.wait_recv()
    pieces = []
    for g in range(GROUPS // 2):
        o_a, o_b, _, l = combine(joined[near + g], [rx[:, i, inner[g]] for i in range(3)])
        o_a, o_b = (o_a / l).astype(BF16), (o_b / l).astype(BF16)
        pieces.append(jnp.concatenate([v[h] for h in range(mine_h) for v in (o_a, o_b)], axis=-1))
    attended = jnp.concatenate(pieces, axis=0)
    for copy in small:
        copy.wait()

    own, other = pl.ds(k * quarter, quarter), pl.ds((1 - k) * quarter, quarter)
    my_rows = pl.ds(pl.multiple_of(x * half + k * quarter, quarter), quarter)
    x_peer_rows = pl.ds(pl.multiple_of((1 - x) * half + k * quarter, quarter), quarter)
    columns = lambda a, b: pl.ds(a * head_dim, (b - a) * head_dim)
    cols = [columns(a, b) for a, b in zip(CUTS, CUTS[1:])]
    joint = [columns(0, CUTS[-2]), columns(*CUTS[-2:])]
    last_of = {CHUNKS - 2: 0, CHUNKS - 1: 1}

    def staged(dot, swap, cross, *rest):
        for c in range(CHUNKS + 2):
            if c < CHUNKS:
                dot(c)
            if c >= 2:
                swap(c - 2)
        for c in range(CHUNKS):
            cross(c)
        for c in range(CHUNKS + len(rest) - 1):
            for s, stage in enumerate(rest):
                if 0 <= c - s < CHUNKS:
                    stage(c - s)

    swaps = [remote(po.at[other, c], ro.at[:, c], d_dev) for c in cols]
    crosses = [remote(so.at[:, c], yo.at[:, c], y_dev) for c in cols]
    gathers = [remote(hb.at[own, c], hb.at[own, c], d_dev) for c in joint]

    def o_dot(c):
        for i in range(CUTS[c], CUTS[c + 1]):
            o_copies[i].wait()
            w = ring[n_w + i // per_o, (i % per_o) * o_rows : (i % per_o + 1) * o_rows, :]
            po[:, i * head_dim : (i + 1) * head_dim] = jnp.dot(attended, w, preferred_element_type=F32)
        swaps[c].start()

    def o_swap(c):
        swaps[c].wait_recv()
        so[:, cols[c]] = po[own, cols[c]] + ro[:, cols[c]]
        crosses[c].start()
        if c == CHUNKS - 1:
            fetch(15)

    def o_cross(c):
        crosses[c].wait_recv()
        total = so[:, cols[c]] + yo[:, cols[c]]
        hb[own, cols[c]] = (x_ref[my_rows, cols[c]].astype(F32) + total).astype(BF16).astype(F32)
        if c in last_of:
            gathers[last_of[c]].start()

    def o_gather(c):
        if c in last_of:
            gathers[last_of[c]].wait_recv()

    staged(o_dot, o_swap, o_cross, o_gather)
    fetch(SLOTS, SLOTS)

    normed_m = rms_norm(hb[...], gm_ref[...])
    for c in range(n_gate):
        chunks[2 * c].wait()
        chunks[2 * c + 1].wait()
        gate = jnp.dot(normed_m, ring[ring_at(2 * c)], preferred_element_type=F32)
        up = jnp.dot(normed_m, ring[ring_at(2 * c + 1)], preferred_element_type=F32)
        act[:, c * head_dim : (c + 1) * head_dim] = (jax.nn.silu(gate) * up).astype(BF16)
        fetch(2)

    swaps_m = [remote(pm.at[other, c], rm.at[:, c], d_dev) for c in cols]
    crosses_m = [remote(sm.at[:, c], ym.at[:, c], y_dev) for c in cols]
    to_core = [remote(ob.at[my_rows], ob.at[my_rows], d_dev)]
    to_x = [remote(ob.at[my_rows, c], ob.at[my_rows, c], x_dev) for c in cols]
    onward = [remote(ob.at[x_peer_rows, c], ob.at[x_peer_rows, c], d_dev) for c in joint]

    def m_dot(c):
        for i in range(CUTS[c], CUTS[c + 1]):
            chunks[2 * n_gate + i].wait()
            pm[:, i * head_dim : (i + 1) * head_dim] = jnp.dot(
                act[...], ring[ring_at(2 * n_gate + i)], preferred_element_type=F32
            )
        swaps_m[c].start()

    def m_swap(c):
        swaps_m[c].wait_recv()
        sm[:, cols[c]] = pm[own, cols[c]] + rm[:, cols[c]]
        crosses_m[c].start()

    def m_cross(c):
        crosses_m[c].wait_recv()
        total = sm[:, cols[c]] + ym[:, cols[c]]
        ob[my_rows, cols[c]] = (hb[own, cols[c]] + total).astype(BF16).astype(F32)
        to_x[c].start()
        if c == CHUNKS - 1:
            to_core[0].start()

    def m_gather(c):
        to_x[c].wait_recv()
        if c in last_of:
            onward[last_of[c]].start()

    def m_last(c):
        if c == 0:
            to_core[0].wait_recv()
        if c in last_of:
            at = joint[last_of[c]]
            onward[last_of[c]].wait_recv()
            out_ref[:, at] = ob[:, at].astype(BF16)

    staged(m_dot, m_swap, m_cross, m_gather, m_last)
    for copy in [*swaps_a, cross_a, *swaps, *crosses, *gathers, *swaps_m, *crosses_m, *to_core, *to_x, *onward]:
        copy.wait_send()


def layer(tokens, gain, w_o, w_gate, w_up, w_down, rows_k, rows_v, kvs, carried):
    rows, width = tokens.shape
    head_dim = 2 * LANES
    heads = carried[0].shape[0]
    qrows = 2 * heads
    half, quarter = rows // 2, rows // 4
    cut = w_gate.shape[1] // 2
    n_blocks = half // BLOCK
    vmem = pl.BlockSpec(memory_space=pltpu.VMEM)
    hbm = pl.BlockSpec(memory_space=pltpu.HBM)
    flat = lambda n: pltpu.VMEM((n, width), F32)
    stats = lambda h, n: pltpu.VMEM((h, 3, n, LANES), F32)
    dma = lambda n: pltpu.SemaphoreType.DMA((n,))
    n_remote = GROUPS // 2 + 2 + 5 * CHUNKS + 5
    args = (tokens, gain, w_o, w_gate, w_up, w_down, rows_k, rows_v)
    shape = (half, *rows_k.shape[1:])
    return pl.pallas_call(
        functools.partial(layer_kernel, kvs),
        out_shape=(
            pltpu.VMEM(tokens.shape, BF16),
            pltpu.VMEM(shape, BF16),
            pltpu.VMEM(shape, BF16),
        ),
        in_specs=[hbm] * len(args) + [vmem] * len(carried),
        out_specs=(vmem,) * 3,
        scratch_shapes=[
            pltpu.VMEM((SLOTS, width, head_dim), BF16),
            *(pltpu.VMEM((half * qrows, LANES), F32) for _ in range(3)),
            stats(heads, half), stats(heads // 2, rows), stats(heads // 2, half), stats(heads // 2, half),
            flat(half), flat(quarter), flat(quarter), flat(quarter), flat(half),
            pltpu.VMEM((half, cut), BF16),
            flat(half), flat(quarter), flat(quarter), flat(quarter), flat(rows),
            pltpu.VMEM(tokens.shape, BF16),
            pltpu.VMEM(gain.shape, BF16),
            dma(2), dma(n_blocks), dma(n_blocks), dma(width // head_dim),
            dma(2 * (cut // head_dim) + width // head_dim), dma(n_remote), dma(n_remote),
        ],
        compiler_params=pltpu.CompilerParams(
            vmem_limit_bytes=LAYER_VMEM << 20, collective_id=0, has_side_effects=True
        ),
        name="layer",
    )(*(pltpu.with_memory_space_constraint(v, pltpu.HBM) for v in args), *carried)


def write_kernel(pos_hbm, t_ref, kn_s, vn_s, _bk, _bv, _k, _v, out_hbm, nk_hbm, nv_hbm, kbuf, vbuf, pos, sem, tile_sem, pos_sem, out_sem):
    rows, key_rows, _ = kbuf.shape
    per_slot = 4
    local_slots = key_rows // per_slot
    slots = local_slots * lax.axis_size("sp")
    base = lax.axis_index("sp") * local_slots
    start = lax.axis_index("sp") // 2 * rows
    per_tile = 16 // per_slot
    n_blocks = rows // BLOCK
    tile_row = lax.broadcasted_iota(jnp.int32, (16, LANES), 0) // per_slot

    def copies(j):
        here, near = pl.ds(j * BLOCK, BLOCK), pl.ds(start + j * BLOCK, BLOCK)
        return (
            pltpu.make_async_copy(kbuf.at[here], nk_hbm.at[near], sem.at[0, j]),
            pltpu.make_async_copy(vbuf.at[here], nv_hbm.at[near], sem.at[1, j]),
        )

    def target(b):
        local = lax.rem(pos[b], slots) - base
        owned = (local >= 0) & (local < local_slots)
        safe = jnp.where(owned, local, 0)
        hit = jnp.where(owned, lax.rem(safe, per_tile), -1)
        return hit, pl.ds(pl.multiple_of((safe // per_tile) * 16, 16), 16)

    def tile_copies(n):
        at = target(start + n)[1]
        return (
            pltpu.make_async_copy(kbuf.at[n, at], nk_hbm.at[start + n, at], tile_sem.at[0]),
            pltpu.make_async_copy(vbuf.at[n, at], nv_hbm.at[start + n, at], tile_sem.at[1]),
        )

    def patch(n):
        b = start + n
        hit, at = target(b)
        for buf, new in ((kbuf, kn_s), (vbuf, vn_s)):
            fresh = new[pl.ds(pl.multiple_of(b * 16, 16), 16), :]
            buf[n, at, :] = jnp.where(tile_row == hit, fresh, buf[n, at, :].astype(F32)).astype(BF16)

    pos_copy = pltpu.make_async_copy(pos_hbm, pos, pos_sem)
    pos_copy.start()
    for j in range(EARLY):
        for copy in copies(j):
            copy.start()
    out_copy = pltpu.make_async_copy(t_ref, out_hbm, out_sem)
    out_copy.start()
    pos_copy.wait()
    for j in range(EARLY, n_blocks + 1):
        if j < n_blocks:
            for i in range(BLOCK):
                patch(j * BLOCK + i)
        if j > EARLY:
            for copy in copies(j - 1):
                copy.start()
    for j in range(EARLY):
        for copy in copies(j):
            copy.wait()
        for i in range(BLOCK):
            patch(j * BLOCK + i)
        if j:
            for i in range(BLOCK):
                for copy in tile_copies((j - 1) * BLOCK + i):
                    copy.start()
    for i in range(BLOCK):
        for copy in tile_copies((EARLY - 1) * BLOCK + i):
            copy.start()
    for j in range(EARLY, n_blocks):
        for copy in copies(j):
            copy.wait()
    for n in range(EARLY * BLOCK):
        for copy in tile_copies(n):
            copy.wait()
    out_copy.wait()


def write(positions, layer_out, fresh_k, fresh_v, buf_k, buf_v, new_k, new_v):
    vmem = pl.BlockSpec(memory_space=pltpu.VMEM)
    hbm = pl.BlockSpec(memory_space=pltpu.HBM)
    return pl.pallas_call(
        write_kernel,
        out_shape=(
            *(jax.ShapeDtypeStruct(v.shape, BF16) for v in (layer_out, new_k, new_v)),
            pltpu.VMEM(buf_k.shape, BF16),
            pltpu.VMEM(buf_v.shape, BF16),
        ),
        in_specs=[hbm] + [vmem] * 5 + [hbm] * 2,
        out_specs=(hbm, hbm, hbm, vmem, vmem),
        input_output_aliases={4: 3, 5: 4, 6: 1, 7: 2},
        scratch_shapes=[
            pltpu.SMEM(positions.shape, jnp.int32),
            pltpu.SemaphoreType.DMA((2, buf_k.shape[0] // BLOCK)),
            pltpu.SemaphoreType.DMA((2,)),
            pltpu.SemaphoreType.DMA,
            pltpu.SemaphoreType.DMA,
        ],
        compiler_params=pltpu.CompilerParams(vmem_limit_bytes=LAYER_VMEM << 20),
        name="write",
    )(pltpu.with_memory_space_constraint(positions, pltpu.HBM), layer_out, fresh_k, fresh_v, buf_k, buf_v, new_k, new_v)[:3]


def to_rows(cache):
    b, s, kv, d = cache.shape
    return cache.reshape(b, s, kv, d // LANES, LANES).transpose(0, 1, 3, 2, 4).reshape(b, -1, LANES)


def from_rows(rows, shape):
    b, s, kv, d = shape
    return rows.reshape(b, s, d // LANES, kv, LANES).transpose(0, 1, 3, 2, 4).reshape(shape)


def solution(mesh):
    cache_spec = P("dp", "sp", "tp", None)
    row_spec = P("dp", None)
    col_spec = P(None, "tp")
    in_specs = (row_spec, P("dp"), cache_spec, cache_spec, P(None), col_spec, col_spec, col_spec, P("tp", None), P(None), col_spec, col_spec, P("tp", None))
    out_specs = (row_spec, cache_spec, cache_spec)

    def local_step(tokens, positions, cache_k, cache_v, attn_gain, w_q, w_k, w_v, w_o, mlp_gain, w_gate, w_up, w_down):
        old_k, old_v = to_rows(cache_k), to_rows(cache_v)
        far, rows_k, rows_v, *carried, fresh_k, fresh_v = first_half(
            positions, tokens, attn_gain, w_q, w_k, w_v, old_k, old_v
        )
        out, buf_k, buf_v = layer(
            tokens, mlp_gain, w_o, w_gate, w_up, w_down, old_k, old_v, cache_k.shape[2], (far, *carried)
        )
        layer_out, rows_k, rows_v = write(positions, out, fresh_k, fresh_v, buf_k, buf_v, rows_k, rows_v)
        new_k = from_rows(rows_k, cache_k.shape)
        new_v = from_rows(rows_v, cache_v.shape)
        return layer_out, new_k, new_v

    return jax.shard_map(local_step, mesh=mesh, in_specs=in_specs, out_specs=out_specs, check_vma=False)
```

```python
import functools
import itertools
import math

import jax
import jax.numpy as jnp
from jax import lax
from jax.experimental import pallas as pl
from jax.experimental.pallas import tpu as pltpu
from jax.sharding import PartitionSpec as P

NORM_EPS = 1e-5
ROPE_THETA = 10000.0
LANES = 128
F32 = jnp.float32
BF16 = jnp.bfloat16
FAR = 1 << 28
BLOCK = 4
EARLY = 3
EAGER = (3, 8)
FIRST = 4
SLOTS = 22
LAYER_VMEM = 35
CHUNKS = 5
GROUPS = 4
MESH = pl.DeviceIdType.MESH


def rms_norm(values, gain):
    wide = values.astype(F32)
    inv_rms = lax.rsqrt(jnp.mean(wide * wide, axis=-1, keepdims=True) + NORM_EPS)
    return (wide * inv_rms * gain.astype(F32)).astype(BF16)


def first_kernel(
    pos_hbm, x_hbm, gain_hbm, wq_hbm, wk_hbm, wv_hbm, ck_hbm, cv_hbm,
    part_ref, nk_hbm, nv_hbm, q_s, kx_s, vx_s, lim_s, hid_s, kn_s, vn_s,
    wbuf, kbuf, vbuf, ang_s, o_s, m_s, l_s,
    pos, x_ref, gain_ref, w_sem, k_sem, v_sem, out_sem, x_sem,
):
    rows = x_ref.shape[0]
    head_dim = 2 * LANES
    heads = wq_hbm.shape[1] // head_dim
    kvs = wk_hbm.shape[1] // head_dim
    group = heads // kvs
    per_slot = 2 * kvs
    qrows = 2 * heads
    key_rows = ck_hbm.shape[1]
    local_slots = key_rows // per_slot
    slots = local_slots * lax.axis_size("sp")
    slices = key_rows // LANES
    half = rows // 2
    n_blocks = half // BLOCK
    start = (1 - lax.axis_index("sp") // 2) * half
    base = lax.axis_index("sp") * local_slots

    def w_copy(n):
        src, col = (
            (wk_hbm, n) if n < kvs else (wv_hbm, n - kvs) if n < 2 * kvs else (wq_hbm, n - 2 * kvs)
        )
        return pltpu.make_async_copy(src.at[:, pl.ds(col * head_dim, head_dim)], wbuf.at[n], w_sem.at[n])

    def in_copies(j):
        far, here = pl.ds(start + j * BLOCK, BLOCK), pl.ds(j * BLOCK, BLOCK)
        return (
            pltpu.make_async_copy(ck_hbm.at[far], kbuf.at[here], k_sem.at[j]),
            pltpu.make_async_copy(cv_hbm.at[far], vbuf.at[here], v_sem.at[j]),
        )

    def out_copies(j):
        far, here = pl.ds(start + j * BLOCK, BLOCK), pl.ds(j * BLOCK, BLOCK)
        return (
            pltpu.make_async_copy(kbuf.at[here], nk_hbm.at[far], out_sem.at[0]),
            pltpu.make_async_copy(vbuf.at[here], nv_hbm.at[far], out_sem.at[1]),
        )

    small = [
        pltpu.make_async_copy(src, dst, x_sem.at[i])
        for i, (src, dst) in enumerate(((pos_hbm, pos), (x_hbm, x_ref), (gain_hbm, gain_ref)))
    ]
    for copy in small:
        copy.start()
    n_w = heads + 2 * kvs
    for n in range(n_w):
        w_copy(n).start()

    lane = lax.broadcasted_iota(jnp.int32, (1, LANES), 1).astype(F32)
    freq = jnp.exp2(lane * (-math.log2(ROPE_THETA) / LANES))

    for copy in small[1:]:
        copy.wait()
    for j in range(FIRST):
        for copy in in_copies(j):
            copy.start()
    normed = rms_norm(x_ref[...], gain_ref[...])
    small[0].wait()

    def angle_row(b, carry):
        p = pos[b]
        ang_s[pl.ds(b, 1), :] = freq * p.astype(F32)
        local = lax.rem(p, slots) - base
        owned = (local >= 0) & (local < local_slots)
        span = pl.ds(pl.multiple_of(b * qrows, qrows), qrows)
        lim_s[span, :] = jnp.full((qrows, LANES), jnp.where(p >= slots - 1, FAR // 2, p) - base, jnp.int32)
        hid_s[span, :] = jnp.full((qrows, LANES), jnp.where(owned, local, -FAR), jnp.int32)
        return carry

    lax.fori_loop(0, rows, angle_row, 0, unroll=8)
    angles = ang_s[...]
    cos_t, sin_t = jnp.cos(angles), jnp.sin(angles)
    for n in range(n_w):
        w_copy(n).wait()
        if FIRST + n < n_blocks:
            for copy in in_copies(FIRST + n):
                copy.start()
        lin = jnp.dot(normed, wbuf[n], preferred_element_type=F32)
        first, second = lin[:, :LANES], lin[:, LANES:]
        if not kvs <= n < 2 * kvs:
            first, second = first * cos_t - second * sin_t, second * cos_t + first * sin_t
        first, second = first.astype(BF16).astype(F32), second.astype(BF16).astype(F32)
        if n >= 2 * kvs:
            h = n - 2 * kvs
            q_s[pl.ds(h, rows, stride=qrows), :] = first
            q_s[pl.ds(heads + h, rows, stride=qrows), :] = second
        else:
            dst, tile, kv = (kn_s, kx_s, n) if n < kvs else (vn_s, vx_s, n - kvs)
            for rep in range(16 // per_slot):
                dst[pl.ds(rep * per_slot + kv, rows, stride=16), :] = first
                dst[pl.ds(rep * per_slot + kvs + kv, rows, stride=16), :] = second
            for g in range(group):
                tile[pl.ds(kv * group + g, rows, stride=qrows), :] = first
                tile[pl.ds(heads + kv * group + g, rows, stride=qrows), :] = second

    row = lax.broadcasted_iota(jnp.int32, (qrows, LANES), 0)
    col = lax.broadcasted_iota(jnp.int32, (qrows, LANES), 1)
    half_of_col = (col // kvs) % 2
    fits = (half_of_col == row // heads) & (col % kvs == (row % heads) // group)
    slot_of_col = jnp.where(fits, col // per_slot, FAR)
    low_half = half_of_col == 0
    patch_row = lax.broadcasted_iota(jnp.int32, (16, LANES), 0) // per_slot
    scale = 1.0 / math.sqrt(head_dim)

    def block_step(j, carry):
        for copy in in_copies(j):
            copy.wait()
        for i in range(BLOCK):
            n = j * BLOCK + i
            b = start + n
            local = lax.rem(pos[b], slots) - base
            owned = (local >= 0) & (local < local_slots)
            safe = jnp.where(owned, local, 0)
            hit = jnp.where(owned, lax.rem(safe, 16 // per_slot), -1)
            span = pl.ds(pl.multiple_of((safe // (16 // per_slot)) * 16, 16), 16)
            for buf, new in ((kbuf, kn_s), (vbuf, vn_s)):
                old = buf[n, span, :].astype(F32)
                fresh = new[pl.ds(pl.multiple_of(b * 16, 16), 16), :]
                buf[n, span, :] = jnp.where(patch_row == hit, fresh, old).astype(BF16)
        scores = []
        for i in range(BLOCK):
            b = start + j * BLOCK + i
            q = q_s[pl.ds(pl.multiple_of(b * qrows, qrows), qrows), :].astype(BF16)
            scores.append(
                lax.dot_general(q, kbuf[j * BLOCK + i], (((1,), (1,)), ((), ())), preferred_element_type=F32)
            )
        probs = []
        for i in range(BLOCK):
            n = j * BLOCK + i
            p = pos[start + n]
            limit = jnp.where(p >= slots - 1, FAR // 2, p) - base
            parts = []
            for t in range(slices):
                own = scores[i][:, t * LANES : (t + 1) * LANES]
                other = pltpu.roll(own, heads, 0)
                other = jnp.where(
                    low_half, pltpu.roll(other, LANES - kvs, 1), pltpu.roll(other, kvs, 1)
                )
                ok = slot_of_col <= limit - t * (LANES // per_slot)
                parts.append(jnp.where(ok, (own + other) * scale, -jnp.inf))
            top = functools.reduce(jnp.maximum, parts)
            top = jnp.max(top, axis=1, keepdims=True)
            floor = jnp.where(top == -jnp.inf, 0.0, top)
            parts = [jnp.exp(part - floor) for part in parts]
            total = jnp.sum(functools.reduce(jnp.add, parts), axis=1, keepdims=True)
            span = pl.ds(pl.multiple_of(n * qrows, qrows), qrows)
            m_s[span, :] = jnp.broadcast_to(top, (qrows, LANES))
            l_s[span, :] = jnp.broadcast_to(total, (qrows, LANES))
            probs.append(jnp.concatenate([part.astype(BF16) for part in parts], axis=1))
        for i in range(BLOCK):
            n = j * BLOCK + i
            span = pl.ds(pl.multiple_of(n * qrows, qrows), qrows)
            o_s[span, :] = jnp.dot(probs[i], vbuf[n], preferred_element_type=F32)
        for copy in out_copies(j):
            copy.start()
        return carry

    lax.fori_loop(0, n_blocks, block_step, 0)

    left = lax.broadcasted_iota(jnp.int32, (half, LANES), 1) < LANES // 2
    for h in range(heads):
        lo, hi = pl.ds(h, half, stride=qrows), pl.ds(heads + h, half, stride=qrows)
        part_ref[h, 0], part_ref[h, 1] = o_s[lo, :], o_s[hi, :]
        part_ref[h, 2] = jnp.where(left, m_s[lo, :], l_s[lo, :])
    for j in range(n_blocks):
        for copy in out_copies(j):
            copy.wait()


def first_half(positions, tokens, gain, w_q, w_k, w_v, rows_k, rows_v):
    rows, width = tokens.shape
    head_dim = 2 * LANES
    heads = w_q.shape[1] // head_dim
    kvs = w_k.shape[1] // head_dim
    qrows = 2 * heads
    vmem = pl.BlockSpec(memory_space=pltpu.VMEM)
    hbm = pl.BlockSpec(memory_space=pltpu.HBM)
    n_blocks = rows // 2 // BLOCK
    tile = lambda n: pltpu.VMEM((rows * n, LANES), F32)
    return pl.pallas_call(
        first_kernel,
        out_shape=(
            pltpu.VMEM((heads, 3, rows // 2, LANES), F32),
            jax.ShapeDtypeStruct(rows_k.shape, BF16),
            jax.ShapeDtypeStruct(rows_v.shape, BF16),
            tile(qrows), tile(qrows), tile(qrows),
            *(pltpu.VMEM((rows * qrows, LANES), jnp.int32) for _ in range(2)),
            tile(16), tile(16),
        ),
        in_specs=[hbm] * 8,
        out_specs=(vmem, hbm, hbm) + (vmem,) * 7,
        scratch_shapes=[
            pltpu.VMEM((heads + 2 * kvs, width, head_dim), BF16),
            pltpu.VMEM((rows // 2, *rows_k.shape[1:]), BF16),
            pltpu.VMEM((rows // 2, *rows_v.shape[1:]), BF16),
            tile(1),
            pltpu.VMEM((rows // 2 * qrows, LANES), F32),
            pltpu.VMEM((rows // 2 * qrows, LANES), F32),
            pltpu.VMEM((rows // 2 * qrows, LANES), F32),
            pltpu.SMEM((rows,), jnp.int32),
            pltpu.VMEM(tokens.shape, BF16),
            pltpu.VMEM(gain.shape, BF16),
            pltpu.SemaphoreType.DMA((heads + 2 * kvs,)),
            pltpu.SemaphoreType.DMA((n_blocks,)),
            pltpu.SemaphoreType.DMA((n_blocks,)),
            pltpu.SemaphoreType.DMA((2,)),
            pltpu.SemaphoreType.DMA((3,)),
        ],
        compiler_params=pltpu.CompilerParams(vmem_limit_bytes=36 << 20),
        name="first",
    )(*(pltpu.with_memory_space_constraint(v, pltpu.HBM) for v in (positions, tokens, gain, w_q, w_k, w_v, rows_k, rows_v)))


def combine(mine, theirs):
    left = lax.broadcasted_iota(jnp.int32, mine[2].shape, mine[2].ndim - 1) < LANES // 2
    axis = mine[2].ndim - 1

    def unpack(stats):
        turned = pltpu.roll(stats, LANES // 2, axis)
        return jnp.where(left, stats, turned), jnp.where(left, turned, stats)

    (m_a, l_a), (m_b, l_b) = unpack(mine[2]), unpack(theirs[2])
    top = jnp.maximum(m_a, m_b)
    f_a = jnp.where(m_a == -jnp.inf, 0.0, jnp.exp(m_a - top))
    f_b = jnp.where(m_b == -jnp.inf, 0.0, jnp.exp(m_b - top))
    return mine[0] * f_a + theirs[0] * f_b, mine[1] * f_a + theirs[1] * f_b, top, l_a * f_a + l_b * f_b


def layer_kernel(
    kv_heads, x_hbm, gm_hbm, wo_hbm, wg_hbm, wu_hbm, wd_hbm, ck_hbm, cv_hbm,
    far_ref, q_s, kx_s, vx_s, lim_s, hid_s,
    out_ref, kbuf, vbuf,
    ring, o_s, m_s, l_s, part, rd, sx, rx,
    po, ro, so, yo, hb, act, pm, rm, sm, ym, ob,
    x_ref, gm_ref,
    small_sem, k_sem, v_sem, o_sem, c_sem, send_sem, recv_sem,
):
    rows, width = x_ref.shape
    head_dim = ring.shape[2]
    heads = far_ref.shape[0]
    kvs = kv_heads
    group = heads // kvs
    per_slot, qrows = 2 * kvs, 2 * heads
    key_rows = ck_hbm.shape[1]
    local_slots = key_rows // per_slot
    slices = key_rows // LANES
    n_blocks = rows // 2 // BLOCK
    mine_h = heads // 2
    half, quarter = rows // 2, rows // 4
    sp, tp = lax.axis_index("sp"), lax.axis_index("tp")
    x, k = sp // 2, lax.rem(sp, 2)
    d_dev, x_dev, y_dev = {"sp": x * 2 + 1 - k}, {"sp": (1 - x) * 2 + k}, {"tp": 1 - tp}
    m_cols = act.shape[1]
    span = width // CHUNKS

    barrier = pltpu.get_barrier_semaphore()
    for dev in (d_dev, x_dev, y_dev):
        pl.semaphore_signal(barrier, inc=1, device_id=dev, device_id_type=MESH)

    counter = [0]

    def remote(src, dst, dev):
        n = counter[0]
        counter[0] += 1
        return pltpu.make_async_remote_copy(
            src_ref=src, dst_ref=dst, send_sem=send_sem.at[n], recv_sem=recv_sem.at[n],
            device_id=dev, device_id_type=MESH,
        )

    def in_copies(j):
        near, here = pl.ds(x * half + j * BLOCK, BLOCK), pl.ds(j * BLOCK, BLOCK)
        return (
            pltpu.make_async_copy(ck_hbm.at[near], kbuf.at[here], k_sem.at[j]),
            pltpu.make_async_copy(cv_hbm.at[near], vbuf.at[here], v_sem.at[j]),
        )

    small = [
        pltpu.make_async_copy(src, dst, small_sem.at[i])
        for i, (src, dst) in enumerate(
            ((x_hbm, x_ref), (gm_hbm, gm_ref))
        )
    ]
    def read(blocks):
        for j in blocks:
            for copy in in_copies(j):
                copy.start()

    read(range(EAGER[0]))

    n_w = 0
    o_rows = mine_h * head_dim
    per_o = width // o_rows
    o_copies = [
        pltpu.make_async_copy(
            wo_hbm.at[pl.ds(k * o_rows, o_rows), pl.ds(c * head_dim, head_dim)],
            ring.at[n_w + c // per_o, pl.ds((c % per_o) * o_rows, o_rows)],
            o_sem.at[c],
        )
        for c in range(width // head_dim)
    ]
    n_gate = m_cols // head_dim
    ring_at = lambda i: (n_w + 2 + i) % SLOTS
    chunks = []
    for c in range(n_gate):
        at = pl.ds(pl.multiple_of(k * m_cols + c * head_dim, LANES), head_dim)
        chunks += [wg_hbm.at[:, at], wu_hbm.at[:, at]]
    for c in range(width // head_dim):
        chunks.append(wd_hbm.at[pl.ds(pl.multiple_of(k * m_cols, LANES), m_cols), pl.ds(c * head_dim, head_dim)])
    chunks = [
        pltpu.make_async_copy(src, ring.at[ring_at(i)], c_sem.at[i]) for i, src in enumerate(chunks)
    ]
    queue = iter(chunks)

    started = [0]

    def fetch(n, limit=len(chunks)):
        n = min(n, limit - started[0])
        started[0] += n
        for copy in itertools.islice(queue, n):
            copy.start()

    row = lax.broadcasted_iota(jnp.int32, (qrows, LANES), 0)
    col = lax.broadcasted_iota(jnp.int32, (qrows, LANES), 1)
    half_of_col = (col // kvs) % 2
    fits = (half_of_col == row // heads) & (col % kvs == (row % heads) // group)
    slot_of_col = jnp.where(fits, col // per_slot, FAR)
    low_half = half_of_col == 0
    scale = 1.0 / math.sqrt(head_dim)

    def block_step(j, carry):
        for copy in in_copies(j):
            copy.wait()
        first = x * half + j * BLOCK
        at_rows = [pl.ds(pl.multiple_of((first + i) * qrows, qrows), qrows) for i in range(BLOCK)]
        scores = []
        for i in range(BLOCK):
            scores.append(
                lax.dot_general(
                    q_s[at_rows[i], :].astype(BF16), kbuf[j * BLOCK + i], (((1,), (1,)), ((), ())),
                    preferred_element_type=F32,
                )
            )
        probs, news = [], []
        for i in range(BLOCK):
            limit, hidden = lim_s[at_rows[i], :], hid_s[at_rows[i], :]
            fresh = q_s[at_rows[i], :] * kx_s[at_rows[i], :]
            fresh = jnp.sum(fresh + pltpu.roll(fresh, heads, 0), axis=1, keepdims=True) * scale
            fresh = jnp.where(hidden[:, :1] >= 0, fresh, -jnp.inf)
            parts = []
            for t in range(slices):
                own = scores[i][:, t * LANES : (t + 1) * LANES]
                other = pltpu.roll(own, heads, 0)
                other = jnp.where(
                    low_half, pltpu.roll(other, LANES - kvs, 1), pltpu.roll(other, kvs, 1)
                )
                shift = t * (LANES // per_slot)
                ok = (slot_of_col <= limit - shift) & (slot_of_col != hidden - shift)
                parts.append(jnp.where(ok, (own + other) * scale, -jnp.inf))
            top = functools.reduce(jnp.maximum, parts)
            top = jnp.maximum(jnp.max(top, axis=1, keepdims=True), fresh)
            floor = jnp.where(top == -jnp.inf, 0.0, top)
            parts = [jnp.exp(part_t - floor) for part_t in parts]
            new = jnp.exp(fresh - floor)
            total = jnp.sum(functools.reduce(jnp.add, parts), axis=1, keepdims=True) + new
            at = pl.ds(pl.multiple_of((j * BLOCK + i) * qrows, qrows), qrows)
            m_s[at, :] = jnp.broadcast_to(top, (qrows, LANES))
            l_s[at, :] = jnp.broadcast_to(total, (qrows, LANES))
            news.append(new)
            probs.append(jnp.concatenate([part_t.astype(BF16) for part_t in parts], axis=1))
        for i in range(BLOCK):
            at = pl.ds(pl.multiple_of((j * BLOCK + i) * qrows, qrows), qrows)
            o_s[at, :] = (
                jnp.dot(probs[i], vbuf[j * BLOCK + i], preferred_element_type=F32) + news[i] * vx_s[at_rows[i], :]
            )
        return carry

    size = rows // GROUPS
    my_heads, their_heads = pl.ds(k * mine_h, mine_h), pl.ds((1 - k) * mine_h, mine_h)
    near = 1
    spans = [pl.ds(0, half)] + [pl.ds(half + g * size, size) for g in range(GROUPS // 2)]
    inner = [pl.ds(g * size, size) for g in range(GROUPS // 2)]
    sources = [far_ref.at[their_heads]] + [part.at[their_heads, :, at] for at in inner]
    swaps_a = [remote(src, rd.at[:, :, at], d_dev) for src, at in zip(sources, spans)]
    cross_a = remote(sx, rx, x_dev)
    left = lambda n: lax.broadcasted_iota(jnp.int32, (mine_h, n, LANES), 2) < LANES // 2
    joined = [None] * len(spans)

    def publish(g):
        at = inner[g - near]
        for h in range(heads):
            lo = pl.ds((g - near) * size * qrows + h, size, stride=qrows)
            hi = pl.ds((g - near) * size * qrows + heads + h, size, stride=qrows)
            part[h, 0, at], part[h, 1, at] = o_s[lo, :], o_s[hi, :]
            part[h, 2, at] = jnp.where(left(size)[0], m_s[lo, :], l_s[lo, :])
        swaps_a[g].start()

    def chip(g):
        swaps_a[g].wait_recv()
        at = spans[g]
        here, local = (far_ref, at) if g < near else (part, inner[g - near])
        o_a, o_b, m, l = combine(
            [here[my_heads, i, local] for i in range(3)], [rd[:, i, at] for i in range(3)]
        )
        value = [o_a, o_b, jnp.where(left(m.shape[1]), m, l)]
        if g < near:
            for i in range(3):
                sx[:, i] = value[i]
            cross_a.start()
        joined[g] = value

    pl.semaphore_wait(barrier, 3)
    for g in range(near):
        swaps_a[g].start()
    read(range(*EAGER))
    for copy in small:
        copy.start()
    step = n_blocks // 2
    lax.fori_loop(0, step, block_step, 0)
    for g in range(near):
        chip(g)
    read(range(EAGER[1], n_blocks))
    publish(near)
    for copy in o_copies:
        copy.start()
    lax.fori_loop(step, n_blocks, block_step, 0)
    publish(near + 1)
    fetch(3)
    for g in range(near, len(spans)):
        chip(g)
    cross_a.wait_recv()
    pieces = []
    for g in range(GROUPS // 2):
        o_a, o_b, _, l = combine(joined[near + g], [rx[:, i, inner[g]] for i in range(3)])
        o_a, o_b = (o_a / l).astype(BF16), (o_b / l).astype(BF16)
        pieces.append(jnp.concatenate([v[h] for h in range(mine_h) for v in (o_a, o_b)], axis=-1))
    attended = jnp.concatenate(pieces, axis=0)
    for copy in small:
        copy.wait()

    own, other = pl.ds(k * quarter, quarter), pl.ds((1 - k) * quarter, quarter)
    my_rows = pl.ds(pl.multiple_of(x * half + k * quarter, quarter), quarter)
    x_peer_rows = pl.ds(pl.multiple_of((1 - x) * half + k * quarter, quarter), quarter)
    cols = [pl.ds(c * span, span) for c in range(CHUNKS)]
    per_span = span // head_dim
    cuts = (0, 3, CHUNKS)
    joint = [pl.ds(a * span, (b - a) * span) for a, b in zip(cuts, cuts[1:])]
    last_of = {b - 1: i for i, b in enumerate(cuts[1:])}

    def staged(dot, swap, cross, *rest):
        for c in range(CHUNKS + 2):
            if c < CHUNKS:
                dot(c)
            if c >= 2:
                swap(c - 2)
        for c in range(CHUNKS):
            cross(c)
        for c in range(CHUNKS + len(rest) - 1):
            for s, stage in enumerate(rest):
                if 0 <= c - s < CHUNKS:
                    stage(c - s)

    swaps = [remote(po.at[other, c], ro.at[:, c], d_dev) for c in cols]
    crosses = [remote(so.at[:, c], yo.at[:, c], y_dev) for c in cols]
    gathers = [remote(hb.at[own, c], hb.at[own, c], d_dev) for c in joint]

    def o_dot(c):
        for i in range(c * per_span, (c + 1) * per_span):
            o_copies[i].wait()
            w = ring[n_w + i // per_o, (i % per_o) * o_rows : (i % per_o + 1) * o_rows, :]
            po[:, i * head_dim : (i + 1) * head_dim] = jnp.dot(attended, w, preferred_element_type=F32)
        swaps[c].start()

    def o_swap(c):
        swaps[c].wait_recv()
        so[:, cols[c]] = po[own, cols[c]] + ro[:, cols[c]]
        crosses[c].start()
        if c == CHUNKS - 1:
            fetch(15)

    def o_cross(c):
        crosses[c].wait_recv()
        total = so[:, cols[c]] + yo[:, cols[c]]
        hb[own, cols[c]] = (x_ref[my_rows, cols[c]].astype(F32) + total).astype(BF16).astype(F32)
        if c in last_of:
            gathers[last_of[c]].start()

    def o_gather(c):
        if c in last_of:
            gathers[last_of[c]].wait_recv()

    staged(o_dot, o_swap, o_cross, o_gather)
    fetch(SLOTS, SLOTS)

    normed_m = rms_norm(hb[...], gm_ref[...])
    for c in range(n_gate):
        chunks[2 * c].wait()
        chunks[2 * c + 1].wait()
        gate = jnp.dot(normed_m, ring[ring_at(2 * c)], preferred_element_type=F32)
        up = jnp.dot(normed_m, ring[ring_at(2 * c + 1)], preferred_element_type=F32)
        act[:, c * head_dim : (c + 1) * head_dim] = (jax.nn.silu(gate) * up).astype(BF16)
        fetch(2)

    swaps_m = [remote(pm.at[other, c], rm.at[:, c], d_dev) for c in cols]
    crosses_m = [remote(sm.at[:, c], ym.at[:, c], y_dev) for c in cols]
    to_core = [remote(ob.at[my_rows], ob.at[my_rows], d_dev)]
    to_x = [remote(ob.at[my_rows, c], ob.at[my_rows, c], x_dev) for c in cols]
    onward = [remote(ob.at[x_peer_rows, c], ob.at[x_peer_rows, c], d_dev) for c in joint]

    def m_dot(c):
        for i in range(c * per_span, (c + 1) * per_span):
            chunks[2 * n_gate + i].wait()
            pm[:, i * head_dim : (i + 1) * head_dim] = jnp.dot(
                act[...], ring[ring_at(2 * n_gate + i)], preferred_element_type=F32
            )
        swaps_m[c].start()

    def m_swap(c):
        swaps_m[c].wait_recv()
        sm[:, cols[c]] = pm[own, cols[c]] + rm[:, cols[c]]
        crosses_m[c].start()

    def m_cross(c):
        crosses_m[c].wait_recv()
        total = sm[:, cols[c]] + ym[:, cols[c]]
        ob[my_rows, cols[c]] = (hb[own, cols[c]] + total).astype(BF16).astype(F32)
        to_x[c].start()
        if c == CHUNKS - 1:
            to_core[0].start()

    def m_gather(c):
        to_x[c].wait_recv()
        if c in last_of:
            onward[last_of[c]].start()

    def m_last(c):
        if c == 0:
            to_core[0].wait_recv()
        if c in last_of:
            at = joint[last_of[c]]
            onward[last_of[c]].wait_recv()
            out_ref[:, at] = ob[:, at].astype(BF16)

    staged(m_dot, m_swap, m_cross, m_gather, m_last)
    for copy in [*swaps_a, cross_a, *swaps, *crosses, *gathers, *swaps_m, *crosses_m, *to_core, *to_x, *onward]:
        copy.wait_send()


def layer(tokens, gain, w_o, w_gate, w_up, w_down, rows_k, rows_v, kvs, carried):
    rows, width = tokens.shape
    head_dim = 2 * LANES
    heads = carried[0].shape[0]
    qrows = 2 * heads
    half, quarter = rows // 2, rows // 4
    cut = w_gate.shape[1] // 2
    n_blocks = half // BLOCK
    vmem = pl.BlockSpec(memory_space=pltpu.VMEM)
    hbm = pl.BlockSpec(memory_space=pltpu.HBM)
    flat = lambda n: pltpu.VMEM((n, width), F32)
    stats = lambda h, n: pltpu.VMEM((h, 3, n, LANES), F32)
    dma = lambda n: pltpu.SemaphoreType.DMA((n,))
    n_remote = GROUPS // 2 + 2 + 5 * CHUNKS + 5
    args = (tokens, gain, w_o, w_gate, w_up, w_down, rows_k, rows_v)
    shape = (half, *rows_k.shape[1:])
    return pl.pallas_call(
        functools.partial(layer_kernel, kvs),
        out_shape=(
            pltpu.VMEM(tokens.shape, BF16),
            pltpu.VMEM(shape, BF16),
            pltpu.VMEM(shape, BF16),
        ),
        in_specs=[hbm] * len(args) + [vmem] * len(carried),
        out_specs=(vmem,) * 3,
        scratch_shapes=[
            pltpu.VMEM((SLOTS, width, head_dim), BF16),
            *(pltpu.VMEM((half * qrows, LANES), F32) for _ in range(3)),
            stats(heads, half), stats(heads // 2, rows), stats(heads // 2, half), stats(heads // 2, half),
            flat(half), flat(quarter), flat(quarter), flat(quarter), flat(half),
            pltpu.VMEM((half, cut), BF16),
            flat(half), flat(quarter), flat(quarter), flat(quarter), flat(rows),
            pltpu.VMEM(tokens.shape, BF16),
            pltpu.VMEM(gain.shape, BF16),
            dma(2), dma(n_blocks), dma(n_blocks), dma(width // head_dim),
            dma(2 * (cut // head_dim) + width // head_dim), dma(n_remote), dma(n_remote),
        ],
        compiler_params=pltpu.CompilerParams(
            vmem_limit_bytes=LAYER_VMEM << 20, collective_id=0, has_side_effects=True
        ),
        name="layer",
    )(*(pltpu.with_memory_space_constraint(v, pltpu.HBM) for v in args), *carried)


def write_kernel(pos_hbm, t_ref, kn_s, vn_s, _bk, _bv, _k, _v, out_hbm, nk_hbm, nv_hbm, kbuf, vbuf, pos, sem, tile_sem, pos_sem, out_sem):
    rows, key_rows, _ = kbuf.shape
    per_slot = 4
    local_slots = key_rows // per_slot
    slots = local_slots * lax.axis_size("sp")
    base = lax.axis_index("sp") * local_slots
    start = lax.axis_index("sp") // 2 * rows
    per_tile = 16 // per_slot
    n_blocks = rows // BLOCK
    tile_row = lax.broadcasted_iota(jnp.int32, (16, LANES), 0) // per_slot

    def copies(j):
        here, near = pl.ds(j * BLOCK, BLOCK), pl.ds(start + j * BLOCK, BLOCK)
        return (
            pltpu.make_async_copy(kbuf.at[here], nk_hbm.at[near], sem.at[0, j]),
            pltpu.make_async_copy(vbuf.at[here], nv_hbm.at[near], sem.at[1, j]),
        )

    def target(b):
        local = lax.rem(pos[b], slots) - base
        owned = (local >= 0) & (local < local_slots)
        safe = jnp.where(owned, local, 0)
        hit = jnp.where(owned, lax.rem(safe, per_tile), -1)
        return hit, pl.ds(pl.multiple_of((safe // per_tile) * 16, 16), 16)

    def tile_copies(n):
        at = target(start + n)[1]
        return (
            pltpu.make_async_copy(kbuf.at[n, at], nk_hbm.at[start + n, at], tile_sem.at[0]),
            pltpu.make_async_copy(vbuf.at[n, at], nv_hbm.at[start + n, at], tile_sem.at[1]),
        )

    def patch(n):
        b = start + n
        hit, at = target(b)
        for buf, new in ((kbuf, kn_s), (vbuf, vn_s)):
            fresh = new[pl.ds(pl.multiple_of(b * 16, 16), 16), :]
            buf[n, at, :] = jnp.where(tile_row == hit, fresh, buf[n, at, :].astype(F32)).astype(BF16)

    pos_copy = pltpu.make_async_copy(pos_hbm, pos, pos_sem)
    pos_copy.start()
    for j in range(EARLY):
        for copy in copies(j):
            copy.start()
    out_copy = pltpu.make_async_copy(t_ref, out_hbm, out_sem)
    out_copy.start()
    pos_copy.wait()
    for j in range(EARLY, n_blocks + 1):
        if j < n_blocks:
            for i in range(BLOCK):
                patch(j * BLOCK + i)
        if j > EARLY:
            for copy in copies(j - 1):
                copy.start()
    for j in range(EARLY):
        for copy in copies(j):
            copy.wait()
        for i in range(BLOCK):
            patch(j * BLOCK + i)
        if j:
            for i in range(BLOCK):
                for copy in tile_copies((j - 1) * BLOCK + i):
                    copy.start()
    for i in range(BLOCK):
        for copy in tile_copies((EARLY - 1) * BLOCK + i):
            copy.start()
    for j in range(EARLY, n_blocks):
        for copy in copies(j):
            copy.wait()
    for n in range(EARLY * BLOCK):
        for copy in tile_copies(n):
            copy.wait()
    out_copy.wait()


def write(positions, layer_out, fresh_k, fresh_v, buf_k, buf_v, new_k, new_v):
    vmem = pl.BlockSpec(memory_space=pltpu.VMEM)
    hbm = pl.BlockSpec(memory_space=pltpu.HBM)
    return pl.pallas_call(
        write_kernel,
        out_shape=(
            *(jax.ShapeDtypeStruct(v.shape, BF16) for v in (layer_out, new_k, new_v)),
            pltpu.VMEM(buf_k.shape, BF16),
            pltpu.VMEM(buf_v.shape, BF16),
        ),
        in_specs=[hbm] + [vmem] * 5 + [hbm] * 2,
        out_specs=(hbm, hbm, hbm, vmem, vmem),
        input_output_aliases={4: 3, 5: 4, 6: 1, 7: 2},
        scratch_shapes=[
            pltpu.SMEM(positions.shape, jnp.int32),
            pltpu.SemaphoreType.DMA((2, buf_k.shape[0] // BLOCK)),
            pltpu.SemaphoreType.DMA((2,)),
            pltpu.SemaphoreType.DMA,
            pltpu.SemaphoreType.DMA,
        ],
        compiler_params=pltpu.CompilerParams(vmem_limit_bytes=LAYER_VMEM << 20),
        name="write",
    )(pltpu.with_memory_space_constraint(positions, pltpu.HBM), layer_out, fresh_k, fresh_v, buf_k, buf_v, new_k, new_v)[:3]


def to_rows(cache):
    b, s, kv, d = cache.shape
    return cache.reshape(b, s, kv, d // LANES, LANES).transpose(0, 1, 3, 2, 4).reshape(b, -1, LANES)


def from_rows(rows, shape):
    b, s, kv, d = shape
    return rows.reshape(b, s, d // LANES, kv, LANES).transpose(0, 1, 3, 2, 4).reshape(shape)


def solution(mesh):
    cache_spec = P("dp", "sp", "tp", None)
    row_spec = P("dp", None)
    col_spec = P(None, "tp")
    in_specs = (row_spec, P("dp"), cache_spec, cache_spec, P(None), col_spec, col_spec, col_spec, P("tp", None), P(None), col_spec, col_spec, P("tp", None))
    out_specs = (row_spec, cache_spec, cache_spec)

    def local_step(tokens, positions, cache_k, cache_v, attn_gain, w_q, w_k, w_v, w_o, mlp_gain, w_gate, w_up, w_down):
        old_k, old_v = to_rows(cache_k), to_rows(cache_v)
        far, rows_k, rows_v, *carried, fresh_k, fresh_v = first_half(
            positions, tokens, attn_gain, w_q, w_k, w_v, old_k, old_v
        )
        out, buf_k, buf_v = layer(
            tokens, mlp_gain, w_o, w_gate, w_up, w_down, old_k, old_v, cache_k.shape[2], (far, *carried)
        )
        layer_out, rows_k, rows_v = write(positions, out, fresh_k, fresh_v, buf_k, buf_v, rows_k, rows_v)
        new_k = from_rows(rows_k, cache_k.shape)
        new_v = from_rows(rows_v, cache_v.shape)
        return layer_out, new_k, new_v

    return jax.shard_map(local_step, mesh=mesh, in_specs=in_specs, out_specs=out_specs, check_vma=False)
```

```python
import functools
import itertools
import math

import jax
import jax.numpy as jnp
from jax import lax
from jax.experimental import pallas as pl
from jax.experimental.pallas import tpu as pltpu
from jax.sharding import PartitionSpec as P

NORM_EPS = 1e-5
ROPE_THETA = 10000.0
LANES = 128
F32 = jnp.float32
BF16 = jnp.bfloat16
FAR = 1 << 28
BLOCK = 4
EARLY = 3
EAGER = (3, 8)
FIRST = 4
SLOTS = 22
LAYER_VMEM = 35
CHUNKS = 5
GROUPS = 4
MESH = pl.DeviceIdType.MESH


def rms_norm(values, gain):
    wide = values.astype(F32)
    inv_rms = lax.rsqrt(jnp.mean(wide * wide, axis=-1, keepdims=True) + NORM_EPS)
    return (wide * inv_rms * gain.astype(F32)).astype(BF16)


def first_kernel(
    pos_hbm, x_hbm, gain_hbm, wq_hbm, wk_hbm, wv_hbm, ck_hbm, cv_hbm,
    part_ref, nk_hbm, nv_hbm, q_s, kx_s, vx_s, lim_s, hid_s, kn_s, vn_s,
    wbuf, kbuf, vbuf, ang_s, o_s, m_s, l_s,
    pos, x_ref, gain_ref, w_sem, k_sem, v_sem, out_sem, x_sem,
):
    rows = x_ref.shape[0]
    head_dim = 2 * LANES
    heads = wq_hbm.shape[1] // head_dim
    kvs = wk_hbm.shape[1] // head_dim
    group = heads // kvs
    per_slot = 2 * kvs
    qrows = 2 * heads
    key_rows = ck_hbm.shape[1]
    local_slots = key_rows // per_slot
    slots = local_slots * lax.axis_size("sp")
    slices = key_rows // LANES
    half = rows // 2
    n_blocks = half // BLOCK
    start = (1 - lax.axis_index("sp") // 2) * half
    base = lax.axis_index("sp") * local_slots

    def w_copy(n):
        src, col = (
            (wk_hbm, n) if n < kvs else (wv_hbm, n - kvs) if n < 2 * kvs else (wq_hbm, n - 2 * kvs)
        )
        return pltpu.make_async_copy(src.at[:, pl.ds(col * head_dim, head_dim)], wbuf.at[n], w_sem.at[n])

    def in_copies(j):
        far, here = pl.ds(start + j * BLOCK, BLOCK), pl.ds(j * BLOCK, BLOCK)
        return (
            pltpu.make_async_copy(ck_hbm.at[far], kbuf.at[here], k_sem.at[j]),
            pltpu.make_async_copy(cv_hbm.at[far], vbuf.at[here], v_sem.at[j]),
        )

    def out_copies(j):
        far, here = pl.ds(start + j * BLOCK, BLOCK), pl.ds(j * BLOCK, BLOCK)
        return (
            pltpu.make_async_copy(kbuf.at[here], nk_hbm.at[far], out_sem.at[0]),
            pltpu.make_async_copy(vbuf.at[here], nv_hbm.at[far], out_sem.at[1]),
        )

    small = [
        pltpu.make_async_copy(src, dst, x_sem.at[i])
        for i, (src, dst) in enumerate(((pos_hbm, pos), (x_hbm, x_ref), (gain_hbm, gain_ref)))
    ]
    for copy in small:
        copy.start()
    n_w = heads + 2 * kvs
    for n in range(n_w // 4):
        w_copy(n).start()

    lane = lax.broadcasted_iota(jnp.int32, (1, LANES), 1).astype(F32)
    freq = jnp.exp2(lane * (-math.log2(ROPE_THETA) / LANES))

    for copy in small[1:]:
        copy.wait()
    for n in range(n_w // 4, n_w):
        w_copy(n).start()
    normed = rms_norm(x_ref[...], gain_ref[...])
    small[0].wait()
    for j in range(FIRST):
        for copy in in_copies(j):
            copy.start()

    def angle_row(b, carry):
        p = pos[b]
        ang_s[pl.ds(b, 1), :] = freq * p.astype(F32)
        local = lax.rem(p, slots) - base
        owned = (local >= 0) & (local < local_slots)
        span = pl.ds(pl.multiple_of(b * qrows, qrows), qrows)
        lim_s[span, :] = jnp.full((qrows, LANES), jnp.where(p >= slots - 1, FAR // 2, p) - base, jnp.int32)
        hid_s[span, :] = jnp.full((qrows, LANES), jnp.where(owned, local, -FAR), jnp.int32)
        return carry

    lax.fori_loop(0, rows, angle_row, 0, unroll=8)
    angles = ang_s[...]
    cos_t, sin_t = jnp.cos(angles), jnp.sin(angles)
    for n in range(n_w):
        w_copy(n).wait()
        if FIRST + n < n_blocks:
            for copy in in_copies(FIRST + n):
                copy.start()
        lin = jnp.dot(normed, wbuf[n], preferred_element_type=F32)
        first, second = lin[:, :LANES], lin[:, LANES:]
        if not kvs <= n < 2 * kvs:
            first, second = first * cos_t - second * sin_t, second * cos_t + first * sin_t
        first, second = first.astype(BF16).astype(F32), second.astype(BF16).astype(F32)
        if n >= 2 * kvs:
            h = n - 2 * kvs
            q_s[pl.ds(h, rows, stride=qrows), :] = first
            q_s[pl.ds(heads + h, rows, stride=qrows), :] = second
        else:
            dst, tile, kv = (kn_s, kx_s, n) if n < kvs else (vn_s, vx_s, n - kvs)
            for rep in range(16 // per_slot):
                dst[pl.ds(rep * per_slot + kv, rows, stride=16), :] = first
                dst[pl.ds(rep * per_slot + kvs + kv, rows, stride=16), :] = second
            for g in range(group):
                tile[pl.ds(kv * group + g, rows, stride=qrows), :] = first
                tile[pl.ds(heads + kv * group + g, rows, stride=qrows), :] = second

    row = lax.broadcasted_iota(jnp.int32, (qrows, LANES), 0)
    col = lax.broadcasted_iota(jnp.int32, (qrows, LANES), 1)
    half_of_col = (col // kvs) % 2
    fits = (half_of_col == row // heads) & (col % kvs == (row % heads) // group)
    slot_of_col = jnp.where(fits, col // per_slot, FAR)
    low_half = half_of_col == 0
    patch_row = lax.broadcasted_iota(jnp.int32, (16, LANES), 0) // per_slot
    scale = 1.0 / math.sqrt(head_dim)

    def block_step(j, carry):
        for copy in in_copies(j):
            copy.wait()
        for i in range(BLOCK):
            n = j * BLOCK + i
            b = start + n
            local = lax.rem(pos[b], slots) - base
            owned = (local >= 0) & (local < local_slots)
            safe = jnp.where(owned, local, 0)
            hit = jnp.where(owned, lax.rem(safe, 16 // per_slot), -1)
            span = pl.ds(pl.multiple_of((safe // (16 // per_slot)) * 16, 16), 16)
            for buf, new in ((kbuf, kn_s), (vbuf, vn_s)):
                old = buf[n, span, :].astype(F32)
                fresh = new[pl.ds(pl.multiple_of(b * 16, 16), 16), :]
                buf[n, span, :] = jnp.where(patch_row == hit, fresh, old).astype(BF16)
        scores = []
        for i in range(BLOCK):
            b = start + j * BLOCK + i
            q = q_s[pl.ds(pl.multiple_of(b * qrows, qrows), qrows), :].astype(BF16)
            scores.append(
                lax.dot_general(q, kbuf[j * BLOCK + i], (((1,), (1,)), ((), ())), preferred_element_type=F32)
            )
        probs = []
        for i in range(BLOCK):
            n = j * BLOCK + i
            p = pos[start + n]
            limit = jnp.where(p >= slots - 1, FAR // 2, p) - base
            parts = []
            for t in range(slices):
                own = scores[i][:, t * LANES : (t + 1) * LANES]
                other = pltpu.roll(own, heads, 0)
                other = jnp.where(
                    low_half, pltpu.roll(other, LANES - kvs, 1), pltpu.roll(other, kvs, 1)
                )
                ok = slot_of_col <= limit - t * (LANES // per_slot)
                parts.append(jnp.where(ok, (own + other) * scale, -jnp.inf))
            top = functools.reduce(jnp.maximum, parts)
            top = jnp.max(top, axis=1, keepdims=True)
            floor = jnp.where(top == -jnp.inf, 0.0, top)
            parts = [jnp.exp(part - floor) for part in parts]
            total = jnp.sum(functools.reduce(jnp.add, parts), axis=1, keepdims=True)
            span = pl.ds(pl.multiple_of(n * qrows, qrows), qrows)
            m_s[span, :] = jnp.broadcast_to(top, (qrows, LANES))
            l_s[span, :] = jnp.broadcast_to(total, (qrows, LANES))
            probs.append(jnp.concatenate([part.astype(BF16) for part in parts], axis=1))
        for i in range(BLOCK):
            n = j * BLOCK + i
            span = pl.ds(pl.multiple_of(n * qrows, qrows), qrows)
            o_s[span, :] = jnp.dot(probs[i], vbuf[n], preferred_element_type=F32)
        for copy in out_copies(j):
            copy.start()
        return carry

    lax.fori_loop(0, n_blocks, block_step, 0)

    left = lax.broadcasted_iota(jnp.int32, (half, LANES), 1) < LANES // 2
    for h in range(heads):
        lo, hi = pl.ds(h, half, stride=qrows), pl.ds(heads + h, half, stride=qrows)
        part_ref[h, 0], part_ref[h, 1] = o_s[lo, :], o_s[hi, :]
        part_ref[h, 2] = jnp.where(left, m_s[lo, :], l_s[lo, :])
    for j in range(n_blocks):
        for copy in out_copies(j):
            copy.wait()


def first_half(positions, tokens, gain, w_q, w_k, w_v, rows_k, rows_v):
    rows, width = tokens.shape
    head_dim = 2 * LANES
    heads = w_q.shape[1] // head_dim
    kvs = w_k.shape[1] // head_dim
    qrows = 2 * heads
    vmem = pl.BlockSpec(memory_space=pltpu.VMEM)
    hbm = pl.BlockSpec(memory_space=pltpu.HBM)
    n_blocks = rows // 2 // BLOCK
    tile = lambda n: pltpu.VMEM((rows * n, LANES), F32)
    return pl.pallas_call(
        first_kernel,
        out_shape=(
            pltpu.VMEM((heads, 3, rows // 2, LANES), F32),
            jax.ShapeDtypeStruct(rows_k.shape, BF16),
            jax.ShapeDtypeStruct(rows_v.shape, BF16),
            tile(qrows), tile(qrows), tile(qrows),
            *(pltpu.VMEM((rows * qrows, LANES), jnp.int32) for _ in range(2)),
            tile(16), tile(16),
        ),
        in_specs=[hbm] * 8,
        out_specs=(vmem, hbm, hbm) + (vmem,) * 7,
        scratch_shapes=[
            pltpu.VMEM((heads + 2 * kvs, width, head_dim), BF16),
            pltpu.VMEM((rows // 2, *rows_k.shape[1:]), BF16),
            pltpu.VMEM((rows // 2, *rows_v.shape[1:]), BF16),
            tile(1),
            pltpu.VMEM((rows // 2 * qrows, LANES), F32),
            pltpu.VMEM((rows // 2 * qrows, LANES), F32),
            pltpu.VMEM((rows // 2 * qrows, LANES), F32),
            pltpu.SMEM((rows,), jnp.int32),
            pltpu.VMEM(tokens.shape, BF16),
            pltpu.VMEM(gain.shape, BF16),
            pltpu.SemaphoreType.DMA((heads + 2 * kvs,)),
            pltpu.SemaphoreType.DMA((n_blocks,)),
            pltpu.SemaphoreType.DMA((n_blocks,)),
            pltpu.SemaphoreType.DMA((2,)),
            pltpu.SemaphoreType.DMA((3,)),
        ],
        compiler_params=pltpu.CompilerParams(vmem_limit_bytes=36 << 20),
        name="first",
    )(*(pltpu.with_memory_space_constraint(v, pltpu.HBM) for v in (positions, tokens, gain, w_q, w_k, w_v, rows_k, rows_v)))


def combine(mine, theirs):
    left = lax.broadcasted_iota(jnp.int32, mine[2].shape, mine[2].ndim - 1) < LANES // 2
    axis = mine[2].ndim - 1

    def unpack(stats):
        turned = pltpu.roll(stats, LANES // 2, axis)
        return jnp.where(left, stats, turned), jnp.where(left, turned, stats)

    (m_a, l_a), (m_b, l_b) = unpack(mine[2]), unpack(theirs[2])
    top = jnp.maximum(m_a, m_b)
    f_a = jnp.where(m_a == -jnp.inf, 0.0, jnp.exp(m_a - top))
    f_b = jnp.where(m_b == -jnp.inf, 0.0, jnp.exp(m_b - top))
    return mine[0] * f_a + theirs[0] * f_b, mine[1] * f_a + theirs[1] * f_b, top, l_a * f_a + l_b * f_b


def layer_kernel(
    kv_heads, x_hbm, gm_hbm, wo_hbm, wg_hbm, wu_hbm, wd_hbm, ck_hbm, cv_hbm,
    far_ref, q_s, kx_s, vx_s, lim_s, hid_s,
    out_ref, kbuf, vbuf,
    ring, o_s, m_s, l_s, part, rd, sx, rx,
    po, ro, so, yo, hb, act, pm, rm, sm, ym, ob,
    x_ref, gm_ref,
    small_sem, k_sem, v_sem, o_sem, c_sem, send_sem, recv_sem,
):
    rows, width = x_ref.shape
    head_dim = ring.shape[2]
    heads = far_ref.shape[0]
    kvs = kv_heads
    group = heads // kvs
    per_slot, qrows = 2 * kvs, 2 * heads
    key_rows = ck_hbm.shape[1]
    local_slots = key_rows // per_slot
    slices = key_rows // LANES
    n_blocks = rows // 2 // BLOCK
    mine_h = heads // 2
    half, quarter = rows // 2, rows // 4
    sp, tp = lax.axis_index("sp"), lax.axis_index("tp")
    x, k = sp // 2, lax.rem(sp, 2)
    d_dev, x_dev, y_dev = {"sp": x * 2 + 1 - k}, {"sp": (1 - x) * 2 + k}, {"tp": 1 - tp}
    m_cols = act.shape[1]
    span = width // CHUNKS

    barrier = pltpu.get_barrier_semaphore()
    for dev in (d_dev, x_dev, y_dev):
        pl.semaphore_signal(barrier, inc=1, device_id=dev, device_id_type=MESH)

    counter = [0]

    def remote(src, dst, dev):
        n = counter[0]
        counter[0] += 1
        return pltpu.make_async_remote_copy(
            src_ref=src, dst_ref=dst, send_sem=send_sem.at[n], recv_sem=recv_sem.at[n],
            device_id=dev, device_id_type=MESH,
        )

    def in_copies(j):
        near, here = pl.ds(x * half + j * BLOCK, BLOCK), pl.ds(j * BLOCK, BLOCK)
        return (
            pltpu.make_async_copy(ck_hbm.at[near], kbuf.at[here], k_sem.at[j]),
            pltpu.make_async_copy(cv_hbm.at[near], vbuf.at[here], v_sem.at[j]),
        )

    small = [
        pltpu.make_async_copy(src, dst, small_sem.at[i])
        for i, (src, dst) in enumerate(
            ((x_hbm, x_ref), (gm_hbm, gm_ref))
        )
    ]
    def read(blocks):
        for j in blocks:
            for copy in in_copies(j):
                copy.start()

    read(range(EAGER[0]))

    n_w = 0
    o_rows = mine_h * head_dim
    per_o = width // o_rows
    o_copies = [
        pltpu.make_async_copy(
            wo_hbm.at[pl.ds(k * o_rows, o_rows), pl.ds(c * head_dim, head_dim)],
            ring.at[n_w + c // per_o, pl.ds((c % per_o) * o_rows, o_rows)],
            o_sem.at[c],
        )
        for c in range(width // head_dim)
    ]
    n_gate = m_cols // head_dim
    ring_at = lambda i: (n_w + 2 + i) % SLOTS
    chunks = []
    for c in range(n_gate):
        at = pl.ds(pl.multiple_of(k * m_cols + c * head_dim, LANES), head_dim)
        chunks += [wg_hbm.at[:, at], wu_hbm.at[:, at]]
    for c in range(width // head_dim):
        chunks.append(wd_hbm.at[pl.ds(pl.multiple_of(k * m_cols, LANES), m_cols), pl.ds(c * head_dim, head_dim)])
    chunks = [
        pltpu.make_async_copy(src, ring.at[ring_at(i)], c_sem.at[i]) for i, src in enumerate(chunks)
    ]
    queue = iter(chunks)

    started = [0]

    def fetch(n, limit=len(chunks)):
        n = min(n, limit - started[0])
        started[0] += n
        for copy in itertools.islice(queue, n):
            copy.start()

    row = lax.broadcasted_iota(jnp.int32, (qrows, LANES), 0)
    col = lax.broadcasted_iota(jnp.int32, (qrows, LANES), 1)
    half_of_col = (col // kvs) % 2
    fits = (half_of_col == row // heads) & (col % kvs == (row % heads) // group)
    slot_of_col = jnp.where(fits, col // per_slot, FAR)
    low_half = half_of_col == 0
    scale = 1.0 / math.sqrt(head_dim)

    def block_step(j, carry):
        for copy in in_copies(j):
            copy.wait()
        first = x * half + j * BLOCK
        at_rows = [pl.ds(pl.multiple_of((first + i) * qrows, qrows), qrows) for i in range(BLOCK)]
        scores = []
        for i in range(BLOCK):
            scores.append(
                lax.dot_general(
                    q_s[at_rows[i], :].astype(BF16), kbuf[j * BLOCK + i], (((1,), (1,)), ((), ())),
                    preferred_element_type=F32,
                )
            )
        probs, news = [], []
        for i in range(BLOCK):
            limit, hidden = lim_s[at_rows[i], :], hid_s[at_rows[i], :]
            fresh = q_s[at_rows[i], :] * kx_s[at_rows[i], :]
            fresh = jnp.sum(fresh + pltpu.roll(fresh, heads, 0), axis=1, keepdims=True) * scale
            fresh = jnp.where(hidden[:, :1] >= 0, fresh, -jnp.inf)
            parts = []
            for t in range(slices):
                own = scores[i][:, t * LANES : (t + 1) * LANES]
                other = pltpu.roll(own, heads, 0)
                other = jnp.where(
                    low_half, pltpu.roll(other, LANES - kvs, 1), pltpu.roll(other, kvs, 1)
                )
                shift = t * (LANES // per_slot)
                ok = (slot_of_col <= limit - shift) & (slot_of_col != hidden - shift)
                parts.append(jnp.where(ok, (own + other) * scale, -jnp.inf))
            top = functools.reduce(jnp.maximum, parts)
            top = jnp.maximum(jnp.max(top, axis=1, keepdims=True), fresh)
            floor = jnp.where(top == -jnp.inf, 0.0, top)
            parts = [jnp.exp(part_t - floor) for part_t in parts]
            new = jnp.exp(fresh - floor)
            total = jnp.sum(functools.reduce(jnp.add, parts), axis=1, keepdims=True) + new
            at = pl.ds(pl.multiple_of((j * BLOCK + i) * qrows, qrows), qrows)
            m_s[at, :] = jnp.broadcast_to(top, (qrows, LANES))
            l_s[at, :] = jnp.broadcast_to(total, (qrows, LANES))
            news.append(new)
            probs.append(jnp.concatenate([part_t.astype(BF16) for part_t in parts], axis=1))
        for i in range(BLOCK):
            at = pl.ds(pl.multiple_of((j * BLOCK + i) * qrows, qrows), qrows)
            o_s[at, :] = (
                jnp.dot(probs[i], vbuf[j * BLOCK + i], preferred_element_type=F32) + news[i] * vx_s[at_rows[i], :]
            )
        return carry

    size = rows // GROUPS
    my_heads, their_heads = pl.ds(k * mine_h, mine_h), pl.ds((1 - k) * mine_h, mine_h)
    near = 1
    spans = [pl.ds(0, half)] + [pl.ds(half + g * size, size) for g in range(GROUPS // 2)]
    inner = [pl.ds(g * size, size) for g in range(GROUPS // 2)]
    sources = [far_ref.at[their_heads]] + [part.at[their_heads, :, at] for at in inner]
    swaps_a = [remote(src, rd.at[:, :, at], d_dev) for src, at in zip(sources, spans)]
    cross_a = remote(sx, rx, x_dev)
    left = lambda n: lax.broadcasted_iota(jnp.int32, (mine_h, n, LANES), 2) < LANES // 2
    joined = [None] * len(spans)

    def publish(g):
        at = inner[g - near]
        for h in range(heads):
            lo = pl.ds((g - near) * size * qrows + h, size, stride=qrows)
            hi = pl.ds((g - near) * size * qrows + heads + h, size, stride=qrows)
            part[h, 0, at], part[h, 1, at] = o_s[lo, :], o_s[hi, :]
            part[h, 2, at] = jnp.where(left(size)[0], m_s[lo, :], l_s[lo, :])
        swaps_a[g].start()

    def chip(g):
        swaps_a[g].wait_recv()
        at = spans[g]
        here, local = (far_ref, at) if g < near else (part, inner[g - near])
        o_a, o_b, m, l = combine(
            [here[my_heads, i, local] for i in range(3)], [rd[:, i, at] for i in range(3)]
        )
        value = [o_a, o_b, jnp.where(left(m.shape[1]), m, l)]
        if g < near:
            for i in range(3):
                sx[:, i] = value[i]
            cross_a.start()
        joined[g] = value

    pl.semaphore_wait(barrier, 3)
    for g in range(near):
        swaps_a[g].start()
    read(range(*EAGER))
    for copy in small:
        copy.start()
    step = n_blocks // 2
    lax.fori_loop(0, step, block_step, 0)
    for g in range(near):
        chip(g)
    read(range(EAGER[1], n_blocks))
    publish(near)
    for copy in o_copies:
        copy.start()
    lax.fori_loop(step, n_blocks, block_step, 0)
    publish(near + 1)
    fetch(3)
    for g in range(near, len(spans)):
        chip(g)
    cross_a.wait_recv()
    pieces = []
    for g in range(GROUPS // 2):
        o_a, o_b, _, l = combine(joined[near + g], [rx[:, i, inner[g]] for i in range(3)])
        o_a, o_b = (o_a / l).astype(BF16), (o_b / l).astype(BF16)
        pieces.append(jnp.concatenate([v[h] for h in range(mine_h) for v in (o_a, o_b)], axis=-1))
    attended = jnp.concatenate(pieces, axis=0)
    for copy in small:
        copy.wait()

    own, other = pl.ds(k * quarter, quarter), pl.ds((1 - k) * quarter, quarter)
    my_rows = pl.ds(pl.multiple_of(x * half + k * quarter, quarter), quarter)
    x_peer_rows = pl.ds(pl.multiple_of((1 - x) * half + k * quarter, quarter), quarter)
    cols = [pl.ds(c * span, span) for c in range(CHUNKS)]
    per_span = span // head_dim
    cuts = (0, 3, CHUNKS)
    joint = [pl.ds(a * span, (b - a) * span) for a, b in zip(cuts, cuts[1:])]
    last_of = {b - 1: i for i, b in enumerate(cuts[1:])}

    def staged(dot, swap, cross, *rest):
        for c in range(CHUNKS + 2):
            if c < CHUNKS:
                dot(c)
            if c >= 2:
                swap(c - 2)
        for c in range(CHUNKS):
            cross(c)
        for c in range(CHUNKS + len(rest) - 1):
            for s, stage in enumerate(rest):
                if 0 <= c - s < CHUNKS:
                    stage(c - s)

    swaps = [remote(po.at[other, c], ro.at[:, c], d_dev) for c in cols]
    crosses = [remote(so.at[:, c], yo.at[:, c], y_dev) for c in cols]
    gathers = [remote(hb.at[own, c], hb.at[own, c], d_dev) for c in joint]

    def o_dot(c):
        for i in range(c * per_span, (c + 1) * per_span):
            o_copies[i].wait()
            w = ring[n_w + i // per_o, (i % per_o) * o_rows : (i % per_o + 1) * o_rows, :]
            po[:, i * head_dim : (i + 1) * head_dim] = jnp.dot(attended, w, preferred_element_type=F32)
        swaps[c].start()

    def o_swap(c):
        swaps[c].wait_recv()
        so[:, cols[c]] = po[own, cols[c]] + ro[:, cols[c]]
        crosses[c].start()
        if c == CHUNKS - 1:
            fetch(15)

    def o_cross(c):
        crosses[c].wait_recv()
        total = so[:, cols[c]] + yo[:, cols[c]]
        hb[own, cols[c]] = (x_ref[my_rows, cols[c]].astype(F32) + total).astype(BF16).astype(F32)
        if c in last_of:
            gathers[last_of[c]].start()

    def o_gather(c):
        if c in last_of:
            gathers[last_of[c]].wait_recv()

    staged(o_dot, o_swap, o_cross, o_gather)
    fetch(SLOTS, SLOTS)

    normed_m = rms_norm(hb[...], gm_ref[...])
    for c in range(n_gate):
        chunks[2 * c].wait()
        chunks[2 * c + 1].wait()
        gate = jnp.dot(normed_m, ring[ring_at(2 * c)], preferred_element_type=F32)
        up = jnp.dot(normed_m, ring[ring_at(2 * c + 1)], preferred_element_type=F32)
        act[:, c * head_dim : (c + 1) * head_dim] = (jax.nn.silu(gate) * up).astype(BF16)
        fetch(2)

    swaps_m = [remote(pm.at[other, c], rm.at[:, c], d_dev) for c in cols]
    crosses_m = [remote(sm.at[:, c], ym.at[:, c], y_dev) for c in cols]
    to_core = [remote(ob.at[my_rows], ob.at[my_rows], d_dev)]
    to_x = [remote(ob.at[my_rows, c], ob.at[my_rows, c], x_dev) for c in cols]
    onward = [remote(ob.at[x_peer_rows, c], ob.at[x_peer_rows, c], d_dev) for c in joint]

    def m_dot(c):
        for i in range(c * per_span, (c + 1) * per_span):
            chunks[2 * n_gate + i].wait()
            pm[:, i * head_dim : (i + 1) * head_dim] = jnp.dot(
                act[...], ring[ring_at(2 * n_gate + i)], preferred_element_type=F32
            )
        swaps_m[c].start()

    def m_swap(c):
        swaps_m[c].wait_recv()
        sm[:, cols[c]] = pm[own, cols[c]] + rm[:, cols[c]]
        crosses_m[c].start()

    def m_cross(c):
        crosses_m[c].wait_recv()
        total = sm[:, cols[c]] + ym[:, cols[c]]
        ob[my_rows, cols[c]] = (hb[own, cols[c]] + total).astype(BF16).astype(F32)
        to_x[c].start()
        if c == CHUNKS - 1:
            to_core[0].start()

    def m_gather(c):
        to_x[c].wait_recv()
        if c in last_of:
            onward[last_of[c]].start()

    def m_last(c):
        if c == 0:
            to_core[0].wait_recv()
        if c in last_of:
            at = joint[last_of[c]]
            onward[last_of[c]].wait_recv()
            out_ref[:, at] = ob[:, at].astype(BF16)

    staged(m_dot, m_swap, m_cross, m_gather, m_last)
    for copy in [*swaps_a, cross_a, *swaps, *crosses, *gathers, *swaps_m, *crosses_m, *to_core, *to_x, *onward]:
        copy.wait_send()


def layer(tokens, gain, w_o, w_gate, w_up, w_down, rows_k, rows_v, kvs, carried):
    rows, width = tokens.shape
    head_dim = 2 * LANES
    heads = carried[0].shape[0]
    qrows = 2 * heads
    half, quarter = rows // 2, rows // 4
    cut = w_gate.shape[1] // 2
    n_blocks = half // BLOCK
    vmem = pl.BlockSpec(memory_space=pltpu.VMEM)
    hbm = pl.BlockSpec(memory_space=pltpu.HBM)
    flat = lambda n: pltpu.VMEM((n, width), F32)
    stats = lambda h, n: pltpu.VMEM((h, 3, n, LANES), F32)
    dma = lambda n: pltpu.SemaphoreType.DMA((n,))
    n_remote = GROUPS // 2 + 2 + 5 * CHUNKS + 5
    args = (tokens, gain, w_o, w_gate, w_up, w_down, rows_k, rows_v)
    shape = (half, *rows_k.shape[1:])
    return pl.pallas_call(
        functools.partial(layer_kernel, kvs),
        out_shape=(
            pltpu.VMEM(tokens.shape, BF16),
            pltpu.VMEM(shape, BF16),
            pltpu.VMEM(shape, BF16),
        ),
        in_specs=[hbm] * len(args) + [vmem] * len(carried),
        out_specs=(vmem,) * 3,
        scratch_shapes=[
            pltpu.VMEM((SLOTS, width, head_dim), BF16),
            *(pltpu.VMEM((half * qrows, LANES), F32) for _ in range(3)),
            stats(heads, half), stats(heads // 2, rows), stats(heads // 2, half), stats(heads // 2, half),
            flat(half), flat(quarter), flat(quarter), flat(quarter), flat(half),
            pltpu.VMEM((half, cut), BF16),
            flat(half), flat(quarter), flat(quarter), flat(quarter), flat(rows),
            pltpu.VMEM(tokens.shape, BF16),
            pltpu.VMEM(gain.shape, BF16),
            dma(2), dma(n_blocks), dma(n_blocks), dma(width // head_dim),
            dma(2 * (cut // head_dim) + width // head_dim), dma(n_remote), dma(n_remote),
        ],
        compiler_params=pltpu.CompilerParams(
            vmem_limit_bytes=LAYER_VMEM << 20, collective_id=0, has_side_effects=True
        ),
        name="layer",
    )(*(pltpu.with_memory_space_constraint(v, pltpu.HBM) for v in args), *carried)


def write_kernel(pos_hbm, t_ref, kn_s, vn_s, _bk, _bv, _k, _v, out_hbm, nk_hbm, nv_hbm, kbuf, vbuf, pos, sem, tile_sem, pos_sem, out_sem):
    rows, key_rows, _ = kbuf.shape
    per_slot = 4
    local_slots = key_rows // per_slot
    slots = local_slots * lax.axis_size("sp")
    base = lax.axis_index("sp") * local_slots
    start = lax.axis_index("sp") // 2 * rows
    per_tile = 16 // per_slot
    n_blocks = rows // BLOCK
    tile_row = lax.broadcasted_iota(jnp.int32, (16, LANES), 0) // per_slot

    def copies(j):
        here, near = pl.ds(j * BLOCK, BLOCK), pl.ds(start + j * BLOCK, BLOCK)
        return (
            pltpu.make_async_copy(kbuf.at[here], nk_hbm.at[near], sem.at[0, j]),
            pltpu.make_async_copy(vbuf.at[here], nv_hbm.at[near], sem.at[1, j]),
        )

    def target(b):
        local = lax.rem(pos[b], slots) - base
        owned = (local >= 0) & (local < local_slots)
        safe = jnp.where(owned, local, 0)
        hit = jnp.where(owned, lax.rem(safe, per_tile), -1)
        return hit, pl.ds(pl.multiple_of((safe // per_tile) * 16, 16), 16)

    def tile_copies(n):
        at = target(start + n)[1]
        return (
            pltpu.make_async_copy(kbuf.at[n, at], nk_hbm.at[start + n, at], tile_sem.at[0]),
            pltpu.make_async_copy(vbuf.at[n, at], nv_hbm.at[start + n, at], tile_sem.at[1]),
        )

    def patch(n):
        b = start + n
        hit, at = target(b)
        for buf, new in ((kbuf, kn_s), (vbuf, vn_s)):
            fresh = new[pl.ds(pl.multiple_of(b * 16, 16), 16), :]
            buf[n, at, :] = jnp.where(tile_row == hit, fresh, buf[n, at, :].astype(F32)).astype(BF16)

    pos_copy = pltpu.make_async_copy(pos_hbm, pos, pos_sem)
    pos_copy.start()
    for j in range(EARLY):
        for copy in copies(j):
            copy.start()
    out_copy = pltpu.make_async_copy(t_ref, out_hbm, out_sem)
    out_copy.start()
    pos_copy.wait()
    for j in range(EARLY, n_blocks + 1):
        if j < n_blocks:
            for i in range(BLOCK):
                patch(j * BLOCK + i)
        if j > EARLY:
            for copy in copies(j - 1):
                copy.start()
    for j in range(EARLY):
        for copy in copies(j):
            copy.wait()
        for i in range(BLOCK):
            patch(j * BLOCK + i)
        if j:
            for i in range(BLOCK):
                for copy in tile_copies((j - 1) * BLOCK + i):
                    copy.start()
    for i in range(BLOCK):
        for copy in tile_copies((EARLY - 1) * BLOCK + i):
            copy.start()
    for j in range(EARLY, n_blocks):
        for copy in copies(j):
            copy.wait()
    for n in range(EARLY * BLOCK):
        for copy in tile_copies(n):
            copy.wait()
    out_copy.wait()


def write(positions, layer_out, fresh_k, fresh_v, buf_k, buf_v, new_k, new_v):
    vmem = pl.BlockSpec(memory_space=pltpu.VMEM)
    hbm = pl.BlockSpec(memory_space=pltpu.HBM)
    return pl.pallas_call(
        write_kernel,
        out_shape=(
            *(jax.ShapeDtypeStruct(v.shape, BF16) for v in (layer_out, new_k, new_v)),
            pltpu.VMEM(buf_k.shape, BF16),
            pltpu.VMEM(buf_v.shape, BF16),
        ),
        in_specs=[hbm] + [vmem] * 5 + [hbm] * 2,
        out_specs=(hbm, hbm, hbm, vmem, vmem),
        input_output_aliases={4: 3, 5: 4, 6: 1, 7: 2},
        scratch_shapes=[
            pltpu.SMEM(positions.shape, jnp.int32),
            pltpu.SemaphoreType.DMA((2, buf_k.shape[0] // BLOCK)),
            pltpu.SemaphoreType.DMA((2,)),
            pltpu.SemaphoreType.DMA,
            pltpu.SemaphoreType.DMA,
        ],
        compiler_params=pltpu.CompilerParams(vmem_limit_bytes=LAYER_VMEM << 20),
        name="write",
    )(pltpu.with_memory_space_constraint(positions, pltpu.HBM), layer_out, fresh_k, fresh_v, buf_k, buf_v, new_k, new_v)[:3]


def to_rows(cache):
    b, s, kv, d = cache.shape
    return cache.reshape(b, s, kv, d // LANES, LANES).transpose(0, 1, 3, 2, 4).reshape(b, -1, LANES)


def from_rows(rows, shape):
    b, s, kv, d = shape
    return rows.reshape(b, s, d // LANES, kv, LANES).transpose(0, 1, 3, 2, 4).reshape(shape)


def solution(mesh):
    cache_spec = P("dp", "sp", "tp", None)
    row_spec = P("dp", None)
    col_spec = P(None, "tp")
    in_specs = (row_spec, P("dp"), cache_spec, cache_spec, P(None), col_spec, col_spec, col_spec, P("tp", None), P(None), col_spec, col_spec, P("tp", None))
    out_specs = (row_spec, cache_spec, cache_spec)

    def local_step(tokens, positions, cache_k, cache_v, attn_gain, w_q, w_k, w_v, w_o, mlp_gain, w_gate, w_up, w_down):
        old_k, old_v = to_rows(cache_k), to_rows(cache_v)
        far, rows_k, rows_v, *carried, fresh_k, fresh_v = first_half(
            positions, tokens, attn_gain, w_q, w_k, w_v, old_k, old_v
        )
        out, buf_k, buf_v = layer(
            tokens, mlp_gain, w_o, w_gate, w_up, w_down, old_k, old_v, cache_k.shape[2], (far, *carried)
        )
        layer_out, rows_k, rows_v = write(positions, out, fresh_k, fresh_v, buf_k, buf_v, rows_k, rows_v)
        new_k = from_rows(rows_k, cache_k.shape)
        new_v = from_rows(rows_v, cache_v.shape)
        return layer_out, new_k, new_v

    return jax.shard_map(local_step, mesh=mesh, in_specs=in_specs, out_specs=out_specs, check_vma=False)
```

```python
import functools
import itertools
import math

import jax
import jax.numpy as jnp
from jax import lax
from jax.experimental import pallas as pl
from jax.experimental.pallas import tpu as pltpu
from jax.sharding import PartitionSpec as P

NORM_EPS = 1e-5
ROPE_THETA = 10000.0
LANES = 128
F32 = jnp.float32
BF16 = jnp.bfloat16
FAR = 1 << 28
BLOCK = 4
EARLY = 3
WIDE = 8
EAGER = (2, 4)
FIRST = 4
SLOTS = 22
LAYER_VMEM = 35
CHUNKS = 5
GROUPS = 4
MESH = pl.DeviceIdType.MESH


def rms_norm(values, gain):
    wide = values.astype(F32)
    inv_rms = lax.rsqrt(jnp.mean(wide * wide, axis=-1, keepdims=True) + NORM_EPS)
    return (wide * inv_rms * gain.astype(F32)).astype(BF16)


def first_kernel(
    pos_hbm, x_hbm, gain_hbm, wq_hbm, wk_hbm, wv_hbm, ck_hbm, cv_hbm,
    part_ref, nk_hbm, nv_hbm, q_s, kx_s, vx_s, lim_s, hid_s, kn_s, vn_s,
    wbuf, kbuf, vbuf, ang_s, o_s, m_s, l_s,
    pos, x_ref, gain_ref, w_sem, k_sem, v_sem, out_sem, x_sem,
):
    rows = x_ref.shape[0]
    head_dim = 2 * LANES
    heads = wq_hbm.shape[1] // head_dim
    kvs = wk_hbm.shape[1] // head_dim
    group = heads // kvs
    per_slot = 2 * kvs
    qrows = 2 * heads
    key_rows = ck_hbm.shape[1]
    local_slots = key_rows // per_slot
    slots = local_slots * lax.axis_size("sp")
    slices = key_rows // LANES
    half = rows // 2
    n_blocks = half // BLOCK
    start = (1 - lax.axis_index("sp") // 2) * half
    base = lax.axis_index("sp") * local_slots

    def w_copy(n):
        src, col = (
            (wk_hbm, n) if n < kvs else (wv_hbm, n - kvs) if n < 2 * kvs else (wq_hbm, n - 2 * kvs)
        )
        return pltpu.make_async_copy(src.at[:, pl.ds(col * head_dim, head_dim)], wbuf.at[n], w_sem.at[n])

    def in_copies(j):
        far, here = pl.ds(start + j * BLOCK, BLOCK), pl.ds(j * BLOCK, BLOCK)
        return (
            pltpu.make_async_copy(ck_hbm.at[far], kbuf.at[here], k_sem.at[j]),
            pltpu.make_async_copy(cv_hbm.at[far], vbuf.at[here], v_sem.at[j]),
        )

    def out_copies(j):
        far, here = pl.ds(start + j * BLOCK, BLOCK), pl.ds(j * BLOCK, BLOCK)
        return (
            pltpu.make_async_copy(kbuf.at[here], nk_hbm.at[far], out_sem.at[0]),
            pltpu.make_async_copy(vbuf.at[here], nv_hbm.at[far], out_sem.at[1]),
        )

    small = [
        pltpu.make_async_copy(src, dst, x_sem.at[i])
        for i, (src, dst) in enumerate(((pos_hbm, pos), (x_hbm, x_ref), (gain_hbm, gain_ref)))
    ]
    for copy in small:
        copy.start()
    n_w = heads + 2 * kvs
    for n in range(n_w // 2):
        w_copy(n).start()

    lane = lax.broadcasted_iota(jnp.int32, (1, LANES), 1).astype(F32)
    freq = jnp.exp2(lane * (-math.log2(ROPE_THETA) / LANES))

    for copy in small:
        copy.wait()
    for n in range(n_w // 2, n_w):
        w_copy(n).start()
    for j in range(FIRST):
        for copy in in_copies(j):
            copy.start()

    def angle_row(b, carry):
        p = pos[b]
        ang_s[pl.ds(b, 1), :] = freq * p.astype(F32)
        local = lax.rem(p, slots) - base
        owned = (local >= 0) & (local < local_slots)
        span = pl.ds(pl.multiple_of(b * qrows, qrows), qrows)
        lim_s[span, :] = jnp.full((qrows, LANES), jnp.where(p >= slots - 1, FAR // 2, p) - base, jnp.int32)
        hid_s[span, :] = jnp.full((qrows, LANES), jnp.where(owned, local, -FAR), jnp.int32)
        return carry

    lax.fori_loop(0, rows, angle_row, 0, unroll=8)
    angles = ang_s[...]
    cos_t, sin_t = jnp.cos(angles), jnp.sin(angles)
    normed = rms_norm(x_ref[...], gain_ref[...])

    for n in range(n_w):
        w_copy(n).wait()
        if FIRST + n < n_blocks:
            for copy in in_copies(FIRST + n):
                copy.start()
        lin = jnp.dot(normed, wbuf[n], preferred_element_type=F32)
        first, second = lin[:, :LANES], lin[:, LANES:]
        if not kvs <= n < 2 * kvs:
            first, second = first * cos_t - second * sin_t, second * cos_t + first * sin_t
        first, second = first.astype(BF16).astype(F32), second.astype(BF16).astype(F32)
        if n >= 2 * kvs:
            h = n - 2 * kvs
            q_s[pl.ds(h, rows, stride=qrows), :] = first
            q_s[pl.ds(heads + h, rows, stride=qrows), :] = second
        else:
            dst, tile, kv = (kn_s, kx_s, n) if n < kvs else (vn_s, vx_s, n - kvs)
            for rep in range(16 // per_slot):
                dst[pl.ds(rep * per_slot + kv, rows, stride=16), :] = first
                dst[pl.ds(rep * per_slot + kvs + kv, rows, stride=16), :] = second
            for g in range(group):
                tile[pl.ds(kv * group + g, rows, stride=qrows), :] = first
                tile[pl.ds(heads + kv * group + g, rows, stride=qrows), :] = second

    row = lax.broadcasted_iota(jnp.int32, (qrows, LANES), 0)
    col = lax.broadcasted_iota(jnp.int32, (qrows, LANES), 1)
    half_of_col = (col // kvs) % 2
    fits = (half_of_col == row // heads) & (col % kvs == (row % heads) // group)
    slot_of_col = jnp.where(fits, col // per_slot, FAR)
    low_half = half_of_col == 0
    patch_row = lax.broadcasted_iota(jnp.int32, (16, LANES), 0) // per_slot
    scale = 1.0 / math.sqrt(head_dim)

    def block_step(j, carry):
        for copy in in_copies(j):
            copy.wait()
        for i in range(BLOCK):
            n = j * BLOCK + i
            b = start + n
            local = lax.rem(pos[b], slots) - base
            owned = (local >= 0) & (local < local_slots)
            safe = jnp.where(owned, local, 0)
            hit = jnp.where(owned, lax.rem(safe, 16 // per_slot), -1)
            span = pl.ds(pl.multiple_of((safe // (16 // per_slot)) * 16, 16), 16)
            for buf, new in ((kbuf, kn_s), (vbuf, vn_s)):
                old = buf[n, span, :].astype(F32)
                fresh = new[pl.ds(pl.multiple_of(b * 16, 16), 16), :]
                buf[n, span, :] = jnp.where(patch_row == hit, fresh, old).astype(BF16)
        scores = []
        for i in range(BLOCK):
            b = start + j * BLOCK + i
            q = q_s[pl.ds(pl.multiple_of(b * qrows, qrows), qrows), :].astype(BF16)
            scores.append(
                lax.dot_general(q, kbuf[j * BLOCK + i], (((1,), (1,)), ((), ())), preferred_element_type=F32)
            )
        probs = []
        for i in range(BLOCK):
            n = j * BLOCK + i
            p = pos[start + n]
            limit = jnp.where(p >= slots - 1, FAR // 2, p) - base
            parts = []
            for t in range(slices):
                own = scores[i][:, t * LANES : (t + 1) * LANES]
                other = pltpu.roll(own, heads, 0)
                other = jnp.where(
                    low_half, pltpu.roll(other, LANES - kvs, 1), pltpu.roll(other, kvs, 1)
                )
                ok = slot_of_col <= limit - t * (LANES // per_slot)
                parts.append(jnp.where(ok, (own + other) * scale, -jnp.inf))
            top = functools.reduce(jnp.maximum, parts)
            top = jnp.max(top, axis=1, keepdims=True)
            floor = jnp.where(top == -jnp.inf, 0.0, top)
            parts = [jnp.exp(part - floor) for part in parts]
            total = jnp.sum(functools.reduce(jnp.add, parts), axis=1, keepdims=True)
            span = pl.ds(pl.multiple_of(n * qrows, qrows), qrows)
            m_s[span, :] = jnp.broadcast_to(top, (qrows, LANES))
            l_s[span, :] = jnp.broadcast_to(total, (qrows, LANES))
            probs.append(jnp.concatenate([part.astype(BF16) for part in parts], axis=1))
        for i in range(BLOCK):
            n = j * BLOCK + i
            span = pl.ds(pl.multiple_of(n * qrows, qrows), qrows)
            o_s[span, :] = jnp.dot(probs[i], vbuf[n], preferred_element_type=F32)
        for copy in out_copies(j):
            copy.start()
        return carry

    lax.fori_loop(0, n_blocks, block_step, 0)

    left = lax.broadcasted_iota(jnp.int32, (half, LANES), 1) < LANES // 2
    for h in range(heads):
        lo, hi = pl.ds(h, half, stride=qrows), pl.ds(heads + h, half, stride=qrows)
        part_ref[h, 0], part_ref[h, 1] = o_s[lo, :], o_s[hi, :]
        part_ref[h, 2] = jnp.where(left, m_s[lo, :], l_s[lo, :])
    for j in range(n_blocks):
        for copy in out_copies(j):
            copy.wait()


def first_half(positions, tokens, gain, w_q, w_k, w_v, rows_k, rows_v):
    rows, width = tokens.shape
    head_dim = 2 * LANES
    heads = w_q.shape[1] // head_dim
    kvs = w_k.shape[1] // head_dim
    qrows = 2 * heads
    vmem = pl.BlockSpec(memory_space=pltpu.VMEM)
    hbm = pl.BlockSpec(memory_space=pltpu.HBM)
    n_blocks = rows // 2 // BLOCK
    tile = lambda n: pltpu.VMEM((rows * n, LANES), F32)
    return pl.pallas_call(
        first_kernel,
        out_shape=(
            pltpu.VMEM((heads, 3, rows // 2, LANES), F32),
            jax.ShapeDtypeStruct(rows_k.shape, BF16),
            jax.ShapeDtypeStruct(rows_v.shape, BF16),
            tile(qrows), tile(qrows), tile(qrows),
            *(pltpu.VMEM((rows * qrows, LANES), jnp.int32) for _ in range(2)),
            tile(16), tile(16),
        ),
        in_specs=[hbm] * 8,
        out_specs=(vmem, hbm, hbm) + (vmem,) * 7,
        scratch_shapes=[
            pltpu.VMEM((heads + 2 * kvs, width, head_dim), BF16),
            pltpu.VMEM((rows // 2, *rows_k.shape[1:]), BF16),
            pltpu.VMEM((rows // 2, *rows_v.shape[1:]), BF16),
            tile(1),
            pltpu.VMEM((rows // 2 * qrows, LANES), F32),
            pltpu.VMEM((rows // 2 * qrows, LANES), F32),
            pltpu.VMEM((rows // 2 * qrows, LANES), F32),
            pltpu.SMEM((rows,), jnp.int32),
            pltpu.VMEM(tokens.shape, BF16),
            pltpu.VMEM(gain.shape, BF16),
            pltpu.SemaphoreType.DMA((heads + 2 * kvs,)),
            pltpu.SemaphoreType.DMA((n_blocks,)),
            pltpu.SemaphoreType.DMA((n_blocks,)),
            pltpu.SemaphoreType.DMA((2,)),
            pltpu.SemaphoreType.DMA((3,)),
        ],
        compiler_params=pltpu.CompilerParams(vmem_limit_bytes=36 << 20),
        name="first",
    )(*(pltpu.with_memory_space_constraint(v, pltpu.HBM) for v in (positions, tokens, gain, w_q, w_k, w_v, rows_k, rows_v)))


def combine(mine, theirs):
    left = lax.broadcasted_iota(jnp.int32, mine[2].shape, mine[2].ndim - 1) < LANES // 2
    axis = mine[2].ndim - 1

    def unpack(stats):
        turned = pltpu.roll(stats, LANES // 2, axis)
        return jnp.where(left, stats, turned), jnp.where(left, turned, stats)

    (m_a, l_a), (m_b, l_b) = unpack(mine[2]), unpack(theirs[2])
    top = jnp.maximum(m_a, m_b)
    f_a = jnp.where(m_a == -jnp.inf, 0.0, jnp.exp(m_a - top))
    f_b = jnp.where(m_b == -jnp.inf, 0.0, jnp.exp(m_b - top))
    return mine[0] * f_a + theirs[0] * f_b, mine[1] * f_a + theirs[1] * f_b, top, l_a * f_a + l_b * f_b


def layer_kernel(
    kv_heads, x_hbm, gm_hbm, wo_hbm, wg_hbm, wu_hbm, wd_hbm, ck_hbm, cv_hbm,
    far_ref, q_s, kx_s, vx_s, lim_s, hid_s,
    out_ref, kbuf, vbuf,
    ring, o_s, m_s, l_s, part, rd, sx, rx,
    po, ro, so, yo, hb, act, pm, rm, sm, ym, ob,
    x_ref, gm_ref,
    small_sem, k_sem, v_sem, o_sem, c_sem, send_sem, recv_sem,
):
    rows, width = x_ref.shape
    head_dim = ring.shape[2]
    heads = far_ref.shape[0]
    kvs = kv_heads
    group = heads // kvs
    per_slot, qrows = 2 * kvs, 2 * heads
    key_rows = ck_hbm.shape[1]
    local_slots = key_rows // per_slot
    slices = key_rows // LANES
    n_blocks = rows // 2 // WIDE
    mine_h = heads // 2
    half, quarter = rows // 2, rows // 4
    sp, tp = lax.axis_index("sp"), lax.axis_index("tp")
    x, k = sp // 2, lax.rem(sp, 2)
    d_dev, x_dev, y_dev = {"sp": x * 2 + 1 - k}, {"sp": (1 - x) * 2 + k}, {"tp": 1 - tp}
    m_cols = act.shape[1]
    span = width // CHUNKS

    barrier = pltpu.get_barrier_semaphore()
    for dev in (d_dev, x_dev, y_dev):
        pl.semaphore_signal(barrier, inc=1, device_id=dev, device_id_type=MESH)

    counter = [0]

    def remote(src, dst, dev):
        n = counter[0]
        counter[0] += 1
        return pltpu.make_async_remote_copy(
            src_ref=src, dst_ref=dst, send_sem=send_sem.at[n], recv_sem=recv_sem.at[n],
            device_id=dev, device_id_type=MESH,
        )

    def in_copies(j):
        near, here = pl.ds(x * half + j * WIDE, WIDE), pl.ds(j * WIDE, WIDE)
        return (
            pltpu.make_async_copy(ck_hbm.at[near], kbuf.at[here], k_sem.at[j]),
            pltpu.make_async_copy(cv_hbm.at[near], vbuf.at[here], v_sem.at[j]),
        )

    small = [
        pltpu.make_async_copy(src, dst, small_sem.at[i])
        for i, (src, dst) in enumerate(
            ((x_hbm, x_ref), (gm_hbm, gm_ref))
        )
    ]
    def read(blocks):
        for j in blocks:
            for copy in in_copies(j):
                copy.start()

    read(range(EAGER[0]))

    n_w = 0
    o_rows = mine_h * head_dim
    per_o = width // o_rows
    o_copies = [
        pltpu.make_async_copy(
            wo_hbm.at[pl.ds(k * o_rows, o_rows), pl.ds(c * head_dim, head_dim)],
            ring.at[n_w + c // per_o, pl.ds((c % per_o) * o_rows, o_rows)],
            o_sem.at[c],
        )
        for c in range(width // head_dim)
    ]
    n_gate = m_cols // head_dim
    ring_at = lambda i: (n_w + 2 + i) % SLOTS
    chunks = []
    for c in range(n_gate):
        at = pl.ds(pl.multiple_of(k * m_cols + c * head_dim, LANES), head_dim)
        chunks += [wg_hbm.at[:, at], wu_hbm.at[:, at]]
    for c in range(width // head_dim):
        chunks.append(wd_hbm.at[pl.ds(pl.multiple_of(k * m_cols, LANES), m_cols), pl.ds(c * head_dim, head_dim)])
    chunks = [
        pltpu.make_async_copy(src, ring.at[ring_at(i)], c_sem.at[i]) for i, src in enumerate(chunks)
    ]
    queue = iter(chunks)

    started = [0]

    def fetch(n, limit=len(chunks)):
        n = min(n, limit - started[0])
        started[0] += n
        for copy in itertools.islice(queue, n):
            copy.start()

    row = lax.broadcasted_iota(jnp.int32, (qrows, LANES), 0)
    col = lax.broadcasted_iota(jnp.int32, (qrows, LANES), 1)
    half_of_col = (col // kvs) % 2
    fits = (half_of_col == row // heads) & (col % kvs == (row % heads) // group)
    slot_of_col = jnp.where(fits, col // per_slot, FAR)
    low_half = half_of_col == 0
    scale = 1.0 / math.sqrt(head_dim)

    def block_step(j, carry):
        for copy in in_copies(j):
            copy.wait()
        first = x * half + j * WIDE
        at_rows = [pl.ds(pl.multiple_of((first + i) * qrows, qrows), qrows) for i in range(WIDE)]
        scores = []
        for i in range(WIDE):
            scores.append(
                lax.dot_general(
                    q_s[at_rows[i], :].astype(BF16), kbuf[j * WIDE + i], (((1,), (1,)), ((), ())),
                    preferred_element_type=F32,
                )
            )
        probs, news = [], []
        for i in range(WIDE):
            limit, hidden = lim_s[at_rows[i], :], hid_s[at_rows[i], :]
            fresh = q_s[at_rows[i], :] * kx_s[at_rows[i], :]
            fresh = jnp.sum(fresh + pltpu.roll(fresh, heads, 0), axis=1, keepdims=True) * scale
            fresh = jnp.where(hidden[:, :1] >= 0, fresh, -jnp.inf)
            parts = []
            for t in range(slices):
                own = scores[i][:, t * LANES : (t + 1) * LANES]
                other = pltpu.roll(own, heads, 0)
                other = jnp.where(
                    low_half, pltpu.roll(other, LANES - kvs, 1), pltpu.roll(other, kvs, 1)
                )
                shift = t * (LANES // per_slot)
                ok = (slot_of_col <= limit - shift) & (slot_of_col != hidden - shift)
                parts.append(jnp.where(ok, (own + other) * scale, -jnp.inf))
            top = functools.reduce(jnp.maximum, parts)
            top = jnp.maximum(jnp.max(top, axis=1, keepdims=True), fresh)
            floor = jnp.where(top == -jnp.inf, 0.0, top)
            parts = [jnp.exp(part_t - floor) for part_t in parts]
            new = jnp.exp(fresh - floor)
            total = jnp.sum(functools.reduce(jnp.add, parts), axis=1, keepdims=True) + new
            at = pl.ds(pl.multiple_of((j * WIDE + i) * qrows, qrows), qrows)
            m_s[at, :] = jnp.broadcast_to(top, (qrows, LANES))
            l_s[at, :] = jnp.broadcast_to(total, (qrows, LANES))
            news.append(new)
            probs.append(jnp.concatenate([part_t.astype(BF16) for part_t in parts], axis=1))
        for i in range(WIDE):
            at = pl.ds(pl.multiple_of((j * WIDE + i) * qrows, qrows), qrows)
            o_s[at, :] = (
                jnp.dot(probs[i], vbuf[j * WIDE + i], preferred_element_type=F32) + news[i] * vx_s[at_rows[i], :]
            )
        return carry

    size = rows // GROUPS
    my_heads, their_heads = pl.ds(k * mine_h, mine_h), pl.ds((1 - k) * mine_h, mine_h)
    near = 1
    spans = [pl.ds(0, half)] + [pl.ds(half + g * size, size) for g in range(GROUPS // 2)]
    inner = [pl.ds(g * size, size) for g in range(GROUPS // 2)]
    sources = [far_ref.at[their_heads]] + [part.at[their_heads, :, at] for at in inner]
    swaps_a = [remote(src, rd.at[:, :, at], d_dev) for src, at in zip(sources, spans)]
    cross_a = remote(sx, rx, x_dev)
    left = lambda n: lax.broadcasted_iota(jnp.int32, (mine_h, n, LANES), 2) < LANES // 2
    joined = [None] * len(spans)

    def publish(g):
        at = inner[g - near]
        for h in range(heads):
            lo = pl.ds((g - near) * size * qrows + h, size, stride=qrows)
            hi = pl.ds((g - near) * size * qrows + heads + h, size, stride=qrows)
            part[h, 0, at], part[h, 1, at] = o_s[lo, :], o_s[hi, :]
            part[h, 2, at] = jnp.where(left(size)[0], m_s[lo, :], l_s[lo, :])
        swaps_a[g].start()

    def chip(g):
        swaps_a[g].wait_recv()
        at = spans[g]
        here, local = (far_ref, at) if g < near else (part, inner[g - near])
        o_a, o_b, m, l = combine(
            [here[my_heads, i, local] for i in range(3)], [rd[:, i, at] for i in range(3)]
        )
        value = [o_a, o_b, jnp.where(left(m.shape[1]), m, l)]
        if g < near:
            for i in range(3):
                sx[:, i] = value[i]
            cross_a.start()
        joined[g] = value

    pl.semaphore_wait(barrier, 3)
    for g in range(near):
        swaps_a[g].start()
    read(range(*EAGER))
    for copy in small:
        copy.start()
    step = n_blocks // 2
    lax.fori_loop(0, step, block_step, 0)
    for g in range(near):
        chip(g)
    read(range(EAGER[1], n_blocks))
    publish(near)
    for copy in o_copies:
        copy.start()
    lax.fori_loop(step, n_blocks, block_step, 0)
    publish(near + 1)
    fetch(3)
    for g in range(near, len(spans)):
        chip(g)
    cross_a.wait_recv()
    pieces = []
    for g in range(GROUPS // 2):
        o_a, o_b, _, l = combine(joined[near + g], [rx[:, i, inner[g]] for i in range(3)])
        o_a, o_b = (o_a / l).astype(BF16), (o_b / l).astype(BF16)
        pieces.append(jnp.concatenate([v[h] for h in range(mine_h) for v in (o_a, o_b)], axis=-1))
    attended = jnp.concatenate(pieces, axis=0)
    for copy in small:
        copy.wait()

    own, other = pl.ds(k * quarter, quarter), pl.ds((1 - k) * quarter, quarter)
    my_rows = pl.ds(pl.multiple_of(x * half + k * quarter, quarter), quarter)
    x_peer_rows = pl.ds(pl.multiple_of((1 - x) * half + k * quarter, quarter), quarter)
    cols = [pl.ds(c * span, span) for c in range(CHUNKS)]
    per_span = span // head_dim
    cuts = (0, 3, CHUNKS)
    joint = [pl.ds(a * span, (b - a) * span) for a, b in zip(cuts, cuts[1:])]
    last_of = {b - 1: i for i, b in enumerate(cuts[1:])}

    def staged(dot, swap, cross, *rest):
        for c in range(CHUNKS + 2):
            if c < CHUNKS:
                dot(c)
            if c >= 2:
                swap(c - 2)
        for c in range(CHUNKS):
            cross(c)
        for c in range(CHUNKS + len(rest) - 1):
            for s, stage in enumerate(rest):
                if 0 <= c - s < CHUNKS:
                    stage(c - s)

    swaps = [remote(po.at[other, c], ro.at[:, c], d_dev) for c in cols]
    crosses = [remote(so.at[:, c], yo.at[:, c], y_dev) for c in cols]
    gathers = [remote(hb.at[own, c], hb.at[own, c], d_dev) for c in joint]

    def o_dot(c):
        for i in range(c * per_span, (c + 1) * per_span):
            o_copies[i].wait()
            w = ring[n_w + i // per_o, (i % per_o) * o_rows : (i % per_o + 1) * o_rows, :]
            po[:, i * head_dim : (i + 1) * head_dim] = jnp.dot(attended, w, preferred_element_type=F32)
        swaps[c].start()

    def o_swap(c):
        swaps[c].wait_recv()
        so[:, cols[c]] = po[own, cols[c]] + ro[:, cols[c]]
        crosses[c].start()
        if c == CHUNKS - 1:
            fetch(15)

    def o_cross(c):
        crosses[c].wait_recv()
        total = so[:, cols[c]] + yo[:, cols[c]]
        hb[own, cols[c]] = (x_ref[my_rows, cols[c]].astype(F32) + total).astype(BF16).astype(F32)
        if c in last_of:
            gathers[last_of[c]].start()

    def o_gather(c):
        if c in last_of:
            gathers[last_of[c]].wait_recv()

    staged(o_dot, o_swap, o_cross, o_gather)
    fetch(SLOTS, SLOTS)

    normed_m = rms_norm(hb[...], gm_ref[...])
    for c in range(n_gate):
        chunks[2 * c].wait()
        chunks[2 * c + 1].wait()
        gate = jnp.dot(normed_m, ring[ring_at(2 * c)], preferred_element_type=F32)
        up = jnp.dot(normed_m, ring[ring_at(2 * c + 1)], preferred_element_type=F32)
        act[:, c * head_dim : (c + 1) * head_dim] = (jax.nn.silu(gate) * up).astype(BF16)
        fetch(2)

    swaps_m = [remote(pm.at[other, c], rm.at[:, c], d_dev) for c in cols]
    crosses_m = [remote(sm.at[:, c], ym.at[:, c], y_dev) for c in cols]
    to_core = [remote(ob.at[my_rows], ob.at[my_rows], d_dev)]
    to_x = [remote(ob.at[my_rows, c], ob.at[my_rows, c], x_dev) for c in cols]
    onward = [remote(ob.at[x_peer_rows, c], ob.at[x_peer_rows, c], d_dev) for c in joint]

    def m_dot(c):
        for i in range(c * per_span, (c + 1) * per_span):
            chunks[2 * n_gate + i].wait()
            pm[:, i * head_dim : (i + 1) * head_dim] = jnp.dot(
                act[...], ring[ring_at(2 * n_gate + i)], preferred_element_type=F32
            )
        swaps_m[c].start()

    def m_swap(c):
        swaps_m[c].wait_recv()
        sm[:, cols[c]] = pm[own, cols[c]] + rm[:, cols[c]]
        crosses_m[c].start()

    def m_cross(c):
        crosses_m[c].wait_recv()
        total = sm[:, cols[c]] + ym[:, cols[c]]
        ob[my_rows, cols[c]] = (hb[own, cols[c]] + total).astype(BF16).astype(F32)
        to_x[c].start()
        if c == CHUNKS - 1:
            to_core[0].start()

    def m_gather(c):
        to_x[c].wait_recv()
        if c in last_of:
            onward[last_of[c]].start()

    def m_last(c):
        if c == 0:
            to_core[0].wait_recv()
        if c in last_of:
            at = joint[last_of[c]]
            onward[last_of[c]].wait_recv()
            out_ref[:, at] = ob[:, at].astype(BF16)

    staged(m_dot, m_swap, m_cross, m_gather, m_last)
    for copy in [*swaps_a, cross_a, *swaps, *crosses, *gathers, *swaps_m, *crosses_m, *to_core, *to_x, *onward]:
        copy.wait_send()


def layer(tokens, gain, w_o, w_gate, w_up, w_down, rows_k, rows_v, kvs, carried):
    rows, width = tokens.shape
    head_dim = 2 * LANES
    heads = carried[0].shape[0]
    qrows = 2 * heads
    half, quarter = rows // 2, rows // 4
    cut = w_gate.shape[1] // 2
    n_blocks = half // WIDE
    vmem = pl.BlockSpec(memory_space=pltpu.VMEM)
    hbm = pl.BlockSpec(memory_space=pltpu.HBM)
    flat = lambda n: pltpu.VMEM((n, width), F32)
    stats = lambda h, n: pltpu.VMEM((h, 3, n, LANES), F32)
    dma = lambda n: pltpu.SemaphoreType.DMA((n,))
    n_remote = GROUPS // 2 + 2 + 5 * CHUNKS + 5
    args = (tokens, gain, w_o, w_gate, w_up, w_down, rows_k, rows_v)
    shape = (half, *rows_k.shape[1:])
    return pl.pallas_call(
        functools.partial(layer_kernel, kvs),
        out_shape=(
            pltpu.VMEM(tokens.shape, BF16),
            pltpu.VMEM(shape, BF16),
            pltpu.VMEM(shape, BF16),
        ),
        in_specs=[hbm] * len(args) + [vmem] * len(carried),
        out_specs=(vmem,) * 3,
        scratch_shapes=[
            pltpu.VMEM((SLOTS, width, head_dim), BF16),
            *(pltpu.VMEM((half * qrows, LANES), F32) for _ in range(3)),
            stats(heads, half), stats(heads // 2, rows), stats(heads // 2, half), stats(heads // 2, half),
            flat(half), flat(quarter), flat(quarter), flat(quarter), flat(half),
            pltpu.VMEM((half, cut), BF16),
            flat(half), flat(quarter), flat(quarter), flat(quarter), flat(rows),
            pltpu.VMEM(tokens.shape, BF16),
            pltpu.VMEM(gain.shape, BF16),
            dma(2), dma(n_blocks), dma(n_blocks), dma(width // head_dim),
            dma(2 * (cut // head_dim) + width // head_dim), dma(n_remote), dma(n_remote),
        ],
        compiler_params=pltpu.CompilerParams(
            vmem_limit_bytes=LAYER_VMEM << 20, collective_id=0, has_side_effects=True
        ),
        name="layer",
    )(*(pltpu.with_memory_space_constraint(v, pltpu.HBM) for v in args), *carried)


def write_kernel(pos_hbm, t_ref, kn_s, vn_s, _bk, _bv, _k, _v, out_hbm, nk_hbm, nv_hbm, kbuf, vbuf, pos, sem, tile_sem, pos_sem, out_sem):
    rows, key_rows, _ = kbuf.shape
    per_slot = 4
    local_slots = key_rows // per_slot
    slots = local_slots * lax.axis_size("sp")
    base = lax.axis_index("sp") * local_slots
    start = lax.axis_index("sp") // 2 * rows
    per_tile = 16 // per_slot
    n_blocks = rows // BLOCK
    tile_row = lax.broadcasted_iota(jnp.int32, (16, LANES), 0) // per_slot

    def copies(j):
        here, near = pl.ds(j * BLOCK, BLOCK), pl.ds(start + j * BLOCK, BLOCK)
        return (
            pltpu.make_async_copy(kbuf.at[here], nk_hbm.at[near], sem.at[0, j]),
            pltpu.make_async_copy(vbuf.at[here], nv_hbm.at[near], sem.at[1, j]),
        )

    def target(b):
        local = lax.rem(pos[b], slots) - base
        owned = (local >= 0) & (local < local_slots)
        safe = jnp.where(owned, local, 0)
        hit = jnp.where(owned, lax.rem(safe, per_tile), -1)
        return hit, pl.ds(pl.multiple_of((safe // per_tile) * 16, 16), 16)

    def tile_copies(n):
        at = target(start + n)[1]
        return (
            pltpu.make_async_copy(kbuf.at[n, at], nk_hbm.at[start + n, at], tile_sem.at[0]),
            pltpu.make_async_copy(vbuf.at[n, at], nv_hbm.at[start + n, at], tile_sem.at[1]),
        )

    def patch(n):
        b = start + n
        hit, at = target(b)
        for buf, new in ((kbuf, kn_s), (vbuf, vn_s)):
            fresh = new[pl.ds(pl.multiple_of(b * 16, 16), 16), :]
            buf[n, at, :] = jnp.where(tile_row == hit, fresh, buf[n, at, :].astype(F32)).astype(BF16)

    pos_copy = pltpu.make_async_copy(pos_hbm, pos, pos_sem)
    pos_copy.start()
    for j in range(EARLY):
        for copy in copies(j):
            copy.start()
    out_copy = pltpu.make_async_copy(t_ref, out_hbm, out_sem)
    out_copy.start()
    pos_copy.wait()
    for j in range(EARLY, n_blocks + 1):
        if j < n_blocks:
            for i in range(BLOCK):
                patch(j * BLOCK + i)
        if j > EARLY:
            for copy in copies(j - 1):
                copy.start()
    for j in range(EARLY):
        for copy in copies(j):
            copy.wait()
        for i in range(BLOCK):
            patch(j * BLOCK + i)
        if j:
            for i in range(BLOCK):
                for copy in tile_copies((j - 1) * BLOCK + i):
                    copy.start()
    for i in range(BLOCK):
        for copy in tile_copies((EARLY - 1) * BLOCK + i):
            copy.start()
    for j in range(EARLY, n_blocks):
        for copy in copies(j):
            copy.wait()
    for n in range(EARLY * BLOCK):
        for copy in tile_copies(n):
            copy.wait()
    out_copy.wait()


def write(positions, layer_out, fresh_k, fresh_v, buf_k, buf_v, new_k, new_v):
    vmem = pl.BlockSpec(memory_space=pltpu.VMEM)
    hbm = pl.BlockSpec(memory_space=pltpu.HBM)
    return pl.pallas_call(
        write_kernel,
        out_shape=(
            *(jax.ShapeDtypeStruct(v.shape, BF16) for v in (layer_out, new_k, new_v)),
            pltpu.VMEM(buf_k.shape, BF16),
            pltpu.VMEM(buf_v.shape, BF16),
        ),
        in_specs=[hbm] + [vmem] * 5 + [hbm] * 2,
        out_specs=(hbm, hbm, hbm, vmem, vmem),
        input_output_aliases={4: 3, 5: 4, 6: 1, 7: 2},
        scratch_shapes=[
            pltpu.SMEM(positions.shape, jnp.int32),
            pltpu.SemaphoreType.DMA((2, buf_k.shape[0] // BLOCK)),
            pltpu.SemaphoreType.DMA((2,)),
            pltpu.SemaphoreType.DMA,
            pltpu.SemaphoreType.DMA,
        ],
        compiler_params=pltpu.CompilerParams(vmem_limit_bytes=LAYER_VMEM << 20),
        name="write",
    )(pltpu.with_memory_space_constraint(positions, pltpu.HBM), layer_out, fresh_k, fresh_v, buf_k, buf_v, new_k, new_v)[:3]


def to_rows(cache):
    b, s, kv, d = cache.shape
    return cache.reshape(b, s, kv, d // LANES, LANES).transpose(0, 1, 3, 2, 4).reshape(b, -1, LANES)


def from_rows(rows, shape):
    b, s, kv, d = shape
    return rows.reshape(b, s, d // LANES, kv, LANES).transpose(0, 1, 3, 2, 4).reshape(shape)


def solution(mesh):
    cache_spec = P("dp", "sp", "tp", None)
    row_spec = P("dp", None)
    col_spec = P(None, "tp")
    in_specs = (row_spec, P("dp"), cache_spec, cache_spec, P(None), col_spec, col_spec, col_spec, P("tp", None), P(None), col_spec, col_spec, P("tp", None))
    out_specs = (row_spec, cache_spec, cache_spec)

    def local_step(tokens, positions, cache_k, cache_v, attn_gain, w_q, w_k, w_v, w_o, mlp_gain, w_gate, w_up, w_down):
        old_k, old_v = to_rows(cache_k), to_rows(cache_v)
        far, rows_k, rows_v, *carried, fresh_k, fresh_v = first_half(
            positions, tokens, attn_gain, w_q, w_k, w_v, old_k, old_v
        )
        out, buf_k, buf_v = layer(
            tokens, mlp_gain, w_o, w_gate, w_up, w_down, old_k, old_v, cache_k.shape[2], (far, *carried)
        )
        layer_out, rows_k, rows_v = write(positions, out, fresh_k, fresh_v, buf_k, buf_v, rows_k, rows_v)
        new_k = from_rows(rows_k, cache_k.shape)
        new_v = from_rows(rows_v, cache_v.shape)
        return layer_out, new_k, new_v

    return jax.shard_map(local_step, mesh=mesh, in_specs=in_specs, out_specs=out_specs, check_vma=False)
```
